256 devices in a mesh: groups: 2 (over y), lon: 128 (over z, x, core).
Axes of the slice: x: 4, y: 2, z: 16, core: 2. Of those that a mesh axis runs over, the one named last changes fastest.
The devices are a block of a 4x16x16 slice.
Arguments:
- fields: bfloat16 [4, 24, 1536, 192], P('groups', None, 'lon'), parts along dimension 0, may hold values from -6 to 6
- norm_gain: float32 [192], replicated, may hold values from 0.25 to 1.75
- qkv_weight: bfloat16 [192, 576], replicated, may hold values from -2.5 to 2.5
- proj_weight: bfloat16 [192, 192], replicated, may hold values from -0.4375 to 0.4375
- bias_table: float32 [4, 6, 3312], replicated, may hold values from -4 to 4
- bias_index: int32 [144, 144], replicated, may hold values from 0 to 3311
- region_ids: int32 [2, 24], replicated, may hold values from 0 to 2
- mlp_gain: float32 [192], replicated, may hold values from 0.25 to 1.75
- up_weight: bfloat16 [192, 768], replicated, may hold values from -0.4375 to 0.4375
- down_weight: bfloat16 [768, 192], replicated, may hold values from -0.21875 to 0.21875
- merge_gain: float32 [768], replicated, may hold values from 0.25 to 1.75
- merge_weight: bfloat16 [768, 384], replicated, may hold values from -0.21875 to 0.21875
- cotangent: bfloat16 [4, 12, 768, 384], P('groups', None, 'lon'), parts along dimension 0, may hold values from -12 to 12
Outputs:
- merged: bfloat16 [4, 12, 768, 384], P('groups', None, 'lon'), parts along dimension 0
- field_grad: bfloat16 [4, 24, 1536, 192], P('groups', None, 'lon'), parts along dimension 0
- qkv_grad: float32 [384, 576], P('groups'), parts along dimension 0
- proj_grad: float32 [384, 192], P('groups'), parts along dimension 0
- up_grad: float32 [384, 768], P('groups'), parts along dimension 0
- down_grad: float32 [1536, 192], P('groups'), parts along dimension 0
- merge_grad: float32 [1536, 384], P('groups'), parts along dimension 0
- table_grad: float32 [8, 6, 3312], P('groups'), parts along dimension 0
The draws below stay inside these ranges and needn't reach their ends.
There are 2 independent parts, one for each index of `groups`. The reference program is written for one: setup_inputs(seed, part) draws one part's arguments, and reference() takes and returns one part's arrays. A program takes and returns all parts, laid end to end along the dimension named above; an argument that names none is the same for every part. Nothing has to cross between parts.
All inputs are finite; a program needn't handle non-finite values.
Results may differ from the reference program's by a relative error of at most 0.019.
The reference program's roundings to bfloat16 on the way count: a program that leaves them out, or rounds other values in their place, can miss the bound.
Values may be sent and summed in bfloat16 or wider, within the bound.
No kernel may reach another device: no remote copies, remote signals or barrier semaphores. Data moves between devices by JAX's collectives and lax.ppermute only.
A program may use at most 192 MiB of HBM per device.

```python
import jax
import jax.numpy as jnp
from jax import lax

C = 192
MLP = 768
HEADS = 6
HEAD = 32
WZ = 2
WLAT = 6
WLON = 12
HALF = 6
WIN = 144
BPOS = 3312
Z = 2
LAT = 24
NLON = 1536
TYPES = 4


def draw_qkv_weight(key, part):
    entries = jnp.clip(jax.random.normal(key, (C, 3 * C), jnp.float32), -6.0, 6.0) * C ** (-0.5)
    entries = jnp.clip(entries, -2.5, 2.5)
    return entries.astype(jnp.bfloat16)


def draw_cotangent(key, part):
    dims_full = (Z, LAT // 2, NLON // 2, 2 * C)
    position = jnp.arange(NLON // 2).astype(jnp.float32) / (NLON // 2)
    rising = jnp.exp(jnp.log(3.0) * position)[None, None, :, None]
    noise_part = jnp.clip(jax.random.normal(key, dims_full, jnp.float32), -4.0, 4.0)
    return (noise_part * rising).astype(jnp.bfloat16)


def set_ends(array, stream_key, least, top_value):
    longest = array.shape.index(max(array.shape))
    spots = []
    for shift in (0, 1):
        where = [jax.random.randint(jax.random.fold_in(stream_key, axis), (), 0, length) for axis, length in enumerate(array.shape)]
        where[longest] = (where[longest] + shift) % array.shape[longest]
        spots.append(tuple(where))
    return array.at[spots[0]].set(least).at[spots[1]].set(top_value)


def steps_of(rng, shape, shards, least, top_value):
    gain = 1.0
    for dim, blocks in shards:
        draws = jax.random.uniform(jax.random.fold_in(jax.random.fold_in(rng, 6), dim), (blocks,), jnp.float32, least / len(shards), top_value / len(shards))
        gain = gain * jnp.repeat(jnp.exp(draws), shape[dim] // blocks).reshape((-1,) + (1,) * (len(shape) - 1 - dim))
    return gain


def bell_draw(rng, shape, scale, most, cuts=(), dtype=jnp.bfloat16):
    drawn = jax.random.normal(rng, shape, jnp.float32) * scale
    if len(cuts) > 0:
        drawn = steps_of(rng, shape, cuts, -0.22, 0.18) * drawn
    return jnp.clip(drawn, min=-most, max=most).astype(dtype)


def setup_inputs(seed: int = 0, part: int = 0) -> dict:
    streams_of = jax.random.split(jax.random.key(seed), 14)
    part_splits = jax.random.split(jax.random.fold_in(streams_of[13], part), 14)
    fields = bell_draw(part_splits[0], (Z, LAT, NLON, C), 1.0, 6.0, ((2, 128),))
    norm_gain = jnp.clip(1.0 + 0.15 * jax.random.normal(streams_of[1], (C,), jnp.float32), 0.25, 1.75)
    qkv_weight = draw_qkv_weight(jax.random.fold_in(streams_of[13], 71), part)
    proj_weight = bell_draw(streams_of[3], (C, C), C ** -0.5, 0.4375)
    bias_table = bell_draw(streams_of[4], (TYPES, HEADS, BPOS), 1.0, 4.0, (), jnp.float32)
    bias_index = set_ends(jax.random.randint(streams_of[5], (WIN, WIN), 0, BPOS), jax.random.fold_in(streams_of[5], 1), 0, BPOS - 1).astype(jnp.int32)
    region_ids = set_ends(jax.random.randint(streams_of[6], (Z, LAT), 0, 3), jax.random.fold_in(streams_of[6], 1), 0, 2).astype(jnp.int32)
    mlp_gain = jnp.clip(1.0 + 0.15 * jax.random.normal(streams_of[7], (C,), jnp.float32), 0.25, 1.75)
    up_weight = bell_draw(streams_of[8], (C, MLP), C ** -0.5, 0.4375)
    down_weight = bell_draw(streams_of[9], (MLP, C), MLP ** -0.5, 0.21875)
    merge_gain = jnp.clip(1.0 + 0.15 * jax.random.normal(streams_of[10], (4 * C,), jnp.float32), 0.25, 1.75)
    merge_weight = bell_draw(streams_of[11], (4 * C, 2 * C), (4 * C) ** -0.5, 0.21875)
    cotangent = draw_cotangent(jax.random.fold_in(jax.random.fold_in(streams_of[13], part), 71), part)
    return {"fields": fields, "norm_gain": norm_gain, "qkv_weight": qkv_weight, "proj_weight": proj_weight, "bias_table": bias_table, "bias_index": bias_index, "region_ids": region_ids, "mlp_gain": mlp_gain, "up_weight": up_weight, "down_weight": down_weight, "merge_gain": merge_gain, "merge_weight": merge_weight, "cotangent": cotangent}


def layer_norm(values, norm_gain):
    average = lax.optimization_barrier(jnp.mean(values, axis=-1, keepdims=True))
    centred = values - average
    variance = lax.optimization_barrier(jnp.mean(centred * centred, axis=-1, keepdims=True))
    return centred * lax.rsqrt(variance + 1e-05) * norm_gain

def to_windows(grid_in):
    levels, latitudes, longitudes, features = grid_in.shape
    blocks = grid_in.reshape(levels // WZ, WZ, latitudes // WLAT, WLAT, longitudes // WLON, WLON, features)
    blocks = blocks.transpose(0, 2, 4, 1, 3, 5, 6)
    return blocks.reshape(levels // WZ * (latitudes // WLAT), longitudes // WLON, WIN, features)

def from_windows(windows, levels, latitudes):
    number = windows.shape[1]
    features = windows.shape[3]
    blocks = windows.reshape(levels // WZ, latitudes // WLAT, number, WZ, WLAT, WLON, features)
    blocks = blocks.transpose(0, 3, 1, 4, 2, 5, 6)
    return blocks.reshape(levels, latitudes, number * WLON, features)

def region_mask(region_ids):
    labels = region_ids.reshape(Z // WZ, WZ, LAT // WLAT, WLAT).transpose(0, 2, 1, 3)
    labels = jnp.repeat(labels.reshape(TYPES, WZ * WLAT), WLON, axis=1)
    return labels[:, :, None] == labels[:, None, :]

def regroup(grid_in):
    levels, latitudes, longitudes, features = grid_in.shape
    blocks = grid_in.reshape(levels, latitudes // 2, 2, longitudes // 2, 2, features)
    return blocks.transpose(0, 1, 3, 2, 4, 5).reshape(levels, latitudes // 2, longitudes // 2, 4 * features)

def attend_one(tokens_win, qkv_weight, proj_weight, bias_rows, same_region, probe_qkv, probe_proj):
    triple = (jnp.dot(tokens_win, qkv_weight, preferred_element_type=jnp.float32) + probe_qkv).astype(jnp.bfloat16)
    shaped = triple.reshape(tokens_win.shape[:2] + (3, HEADS, HEAD)).astype(jnp.float32)
    scores = jnp.einsum('wqhd,wkhd->whqk', shaped[:, :, 0], shaped[:, :, 1]) * HEAD ** (-0.5) + bias_rows
    scores = jnp.where(same_region, scores, -1e+30)
    row_max = lax.optimization_barrier(jnp.max(scores, axis=-1, keepdims=True))
    weights = jnp.exp(scores - row_max)
    probability = (weights / lax.optimization_barrier(jnp.sum(weights, axis=-1, keepdims=True))).astype(jnp.bfloat16)
    mixed_heads = jnp.einsum('whqk,wkhd->wqhd', probability.astype(jnp.float32), shaped[:, :, 2])
    mixed_heads = mixed_heads.astype(jnp.bfloat16).reshape(tokens_win.shape)
    result = jnp.dot(mixed_heads, proj_weight, preferred_element_type=jnp.float32) + probe_proj
    return (result.astype(jnp.bfloat16), mixed_heads)

def weight_term(inputs, grads):
    rows_in = inputs.reshape(-1, inputs.shape[-1])
    rows_out = grads.reshape(-1, grads.shape[-1]).astype(jnp.bfloat16)
    return jnp.dot(rows_in.T, rows_out, preferred_element_type=jnp.float32)

def table_sums(grad_bias, bias_index):
    flat = grad_bias.reshape(TYPES * HEADS, WIN * WIN).T
    summed = jax.ops.segment_sum(flat, bias_index.reshape(-1), num_segments=BPOS)
    return summed.T.reshape(TYPES, HEADS, BPOS)

def reference(fields, norm_gain, qkv_weight, proj_weight, bias_table, bias_index, region_ids, mlp_gain, up_weight, down_weight, merge_gain, merge_weight, cotangent):
    same_region = region_mask(region_ids)
    bias_rows = jnp.take(bias_table, bias_index, axis=2)

    def forward(fields_in, bias_in, probes):
        probe_qkv, probe_proj, probe_up, probe_down, probe_merge = probes
        field_f32 = fields_in.astype(jnp.float32)
        normed = layer_norm(field_f32, norm_gain).astype(jnp.bfloat16)
        rolled = jnp.roll(normed, -HALF, axis=2)
        tokens_win = to_windows(rolled)

        def per_type(parts):
            return attend_one(parts[0], qkv_weight, proj_weight, parts[1][None], parts[2], parts[3], parts[4])
        result, mixed_heads = lax.map(jax.checkpoint(per_type), (tokens_win, bias_in, same_region, probe_qkv, probe_proj))
        branch = jnp.roll(from_windows(result, Z, LAT), HALF, axis=2)
        after_attn = lax.optimization_barrier((field_f32 + branch.astype(jnp.float32)).astype(jnp.bfloat16))
        after_f32 = after_attn.astype(jnp.float32)
        normed_mlp = layer_norm(after_f32, mlp_gain).astype(jnp.bfloat16)
        hidden = jax.nn.gelu(jnp.dot(normed_mlp, up_weight, preferred_element_type=jnp.float32) + probe_up, approximate=False).astype(jnp.bfloat16)
        after_mlp = (after_f32 + jnp.dot(hidden, down_weight, preferred_element_type=jnp.float32) + probe_down).astype(jnp.bfloat16)
        normed_merge = layer_norm(regroup(after_mlp).astype(jnp.float32), merge_gain).astype(jnp.bfloat16)
        merged = (jnp.dot(normed_merge, merge_weight, preferred_element_type=jnp.float32) + probe_merge).astype(jnp.bfloat16)
        return (merged, (tokens_win, mixed_heads, normed_mlp, hidden, normed_merge))
    windows_lon = NLON // WLON
    probes = (jnp.zeros((TYPES, windows_lon, WIN, 3 * C), jnp.float32), jnp.zeros((TYPES, windows_lon, WIN, C), jnp.float32), jnp.zeros((Z, LAT, NLON, MLP), jnp.float32), jnp.zeros((Z, LAT, NLON, C), jnp.float32), jnp.zeros((Z, LAT // 2, NLON // 2, 2 * C), jnp.float32))
    merged, backward, stored = jax.vjp(forward, fields, bias_rows, probes, has_aux=True)
    field_grad, grad_bias, grad_probes = backward(cotangent)
    tokens_win, mixed_heads, normed_mlp, hidden, normed_merge = stored
    grad_qkv, grad_proj, grad_up, grad_down, grad_merge = grad_probes
    factor = float(Z * LAT * NLON) ** (-0.5)
    qkv_grad = weight_term(tokens_win, grad_qkv) * factor
    proj_grad = weight_term(mixed_heads, grad_proj) * factor
    up_grad = weight_term(normed_mlp, grad_up) * factor
    down_grad = weight_term(hidden, grad_down) * factor
    merge_grad = weight_term(normed_merge, grad_merge) * factor
    table_grad = table_sums(grad_bias, bias_index) * factor
    return (merged, field_grad, qkv_grad, proj_grad, up_grad, down_grad, merge_grad, table_grad)
```

```python
import jax
import jax.numpy as jnp
from jax import lax
from jax.sharding import PartitionSpec as P

C = 192
MLP = 768
HEADS = 6
HEAD = 32
WZ = 2
WLAT = 6
WLON = 12
HALF = 6
WIN = 144
BPOS = 3312
Z = 2
LAT = 24
TYPES = 4


def passed_along(value, axis, steps):
    count = lax.axis_size(axis)
    pairs = [(source, (source + steps) % count) for source in range(count)]
    return lax.ppermute(value, axis, pairs)


def shortened(array):
    return jax.tree.map(lambda a: a.astype(jnp.bfloat16) if a.dtype == jnp.float32 else a, array)


def layer_norm(values, norm_gain):
    average = jnp.mean(values, axis=-1, keepdims=True)
    centred = values - average
    variance = jnp.mean(centred * centred, axis=-1, keepdims=True)
    return centred * lax.rsqrt(variance + 1e-05) * norm_gain


def to_windows(grid_in):
    levels, latitudes, longitudes, features = grid_in.shape
    blocks = grid_in.reshape(
        levels // WZ, WZ, latitudes // WLAT, WLAT, longitudes // WLON, WLON, features
    )
    blocks = blocks.transpose(0, 2, 4, 1, 3, 5, 6)
    return blocks.reshape(levels // WZ * (latitudes // WLAT), longitudes // WLON, WIN, features)


def from_windows(windows, levels, latitudes):
    number = windows.shape[1]
    features = windows.shape[3]
    blocks = windows.reshape(levels // WZ, latitudes // WLAT, number, WZ, WLAT, WLON, features)
    blocks = blocks.transpose(0, 3, 1, 4, 2, 5, 6)
    return blocks.reshape(levels, latitudes, number * WLON, features)


def region_mask(region_ids):
    labels = region_ids.reshape(Z // WZ, WZ, LAT // WLAT, WLAT).transpose(0, 2, 1, 3)
    labels = jnp.repeat(labels.reshape(TYPES, WZ * WLAT), WLON, axis=1)
    return labels[:, :, None] == labels[:, None, :]


def regroup(grid_in):
    levels, latitudes, longitudes, features = grid_in.shape
    blocks = grid_in.reshape(levels, latitudes // 2, 2, longitudes // 2, 2, features)
    return blocks.transpose(0, 1, 3, 2, 4, 5).reshape(
        levels, latitudes // 2, longitudes // 2, 4 * features
    )


def attend_one(tokens_win, qkv_weight, proj_weight, bias_rows, same_region, probe_qkv, probe_proj):
    triple = (
        jnp.dot(tokens_win, qkv_weight, preferred_element_type=jnp.float32) + probe_qkv
    ).astype(jnp.bfloat16)
    shaped = triple.reshape(tokens_win.shape[:2] + (3, HEADS, HEAD)).astype(jnp.float32)
    scores = (
        jnp.einsum("wqhd,wkhd->whqk", shaped[:, :, 0], shaped[:, :, 1]) * HEAD ** (-0.5) + bias_rows
    )
    scores = jnp.where(same_region, scores, -1e30)
    row_max = jnp.max(scores, axis=-1, keepdims=True)
    weights = jnp.exp(scores - row_max)
    probability = (weights / jnp.sum(weights, axis=-1, keepdims=True)).astype(jnp.bfloat16)
    mixed_heads = jnp.einsum("whqk,wkhd->wqhd", probability.astype(jnp.float32), shaped[:, :, 2])
    mixed_heads = mixed_heads.astype(jnp.bfloat16).reshape(tokens_win.shape)
    result = jnp.dot(mixed_heads, proj_weight, preferred_element_type=jnp.float32) + probe_proj
    return (result.astype(jnp.bfloat16), mixed_heads)


def weight_term(inputs, grads):
    rows_in = inputs.reshape(-1, inputs.shape[-1])
    rows_out = grads.reshape(-1, grads.shape[-1]).astype(jnp.bfloat16)
    return jnp.dot(rows_in.T, rows_out, preferred_element_type=jnp.float32)


def table_sums(grad_bias, bias_index):
    flat = grad_bias.reshape(TYPES * HEADS, WIN * WIN).T
    summed = jax.ops.segment_sum(flat, bias_index.reshape(-1), num_segments=BPOS)
    return summed.T.reshape(TYPES, HEADS, BPOS)


LANES = 128
CORES = 2
ACROSS = 4


def groups_of(count, inner, size):
    return [
        [block * inner * size + offset + member * inner for member in range(size)]
        for block in range(count // (inner * size))
        for offset in range(inner)
    ]


def summed_over(parts, axis):
    count = lax.axis_size(axis)
    place = lax.axis_index(axis)
    along = count // (CORES * ACROSS)
    core = place % CORES
    rows, lanes = parts.shape[1:]
    pairs = [(i, i ^ 1) for i in range(count)]
    half = parts.reshape(CORES, -1, lanes)
    mine = lax.dynamic_index_in_dim(half, core, 0, keepdims=False)
    other = lax.ppermute(lax.dynamic_index_in_dim(half, 1 - core, 0, keepdims=False), axis, pairs)
    held = (mine.astype(jnp.float32) + other.astype(jnp.float32)).astype(jnp.bfloat16)

    def exchanged(value, inner, size):
        return lax.all_to_all(
            value, axis, 0, 0, axis_index_groups=groups_of(count, inner, size)
        )

    def reduced(value, inner, size):
        got = exchanged(value.reshape(size, -1, lanes), inner, size)
        return jnp.sum(got.astype(jnp.float32), axis=0).astype(jnp.bfloat16)

    def gathered(value, inner, size):
        return exchanged(
            jnp.broadcast_to(value[None], (size, *value.shape)), inner, size
        ).reshape(-1, lanes)

    held = reduced(held, CORES, ACROSS)
    held = reduced(held, CORES * ACROSS, along)
    held = gathered(held, CORES * ACROSS, along)
    held = gathered(held, CORES, ACROSS)
    other = lax.ppermute(held, axis, pairs)
    return jnp.where(
        core == 0, jnp.concatenate([held, other]), jnp.concatenate([other, held])
    )


def local(
    fields,
    norm_gain,
    qkv_weight,
    proj_weight,
    bias_table,
    bias_index,
    region_ids,
    mlp_gain,
    up_weight,
    down_weight,
    merge_gain,
    merge_weight,
    cotangent,
):
    local_len = fields.shape[2]
    count = lax.axis_size("lon")
    same_region = region_mask(region_ids)
    bias_rows = jnp.take(bias_table, bias_index, axis=2)
    attend_types = jax.vmap(attend_one, in_axes=(0, None, None, 0, 0, 0, 0))
    east = passed_along(fields[:, :, :HALF], "lon", -1)
    east_cotangent = passed_along(cotangent[:, :, : HALF // 2], "lon", -1)
    fields_win = jnp.concatenate([fields[:, :, HALF:], east], axis=2)
    cotangent_win = jnp.concatenate([cotangent[:, :, HALF // 2 :], east_cotangent], axis=2)
    windows_lon = local_len // WLON

    def forward(field_in, bias_in, probes):
        probe_qkv, probe_proj, probe_up, probe_down, probe_merge = probes
        normed = layer_norm(field_in, norm_gain).astype(jnp.bfloat16)
        tokens_win = to_windows(normed)
        result, mixed_heads = attend_types(
            tokens_win, qkv_weight, proj_weight, bias_in, same_region, probe_qkv, probe_proj
        )
        branch = from_windows(result, Z, LAT)
        after_attn = lax.optimization_barrier(
            (field_in + branch.astype(jnp.float32)).astype(jnp.bfloat16)
        )
        after_f32 = after_attn.astype(jnp.float32)
        normed_mlp = layer_norm(after_f32, mlp_gain).astype(jnp.bfloat16)
        hidden = jax.nn.gelu(
            jnp.dot(normed_mlp, up_weight, preferred_element_type=jnp.float32) + probe_up,
            approximate=False,
        ).astype(jnp.bfloat16)
        after_mlp = (
            after_f32
            + jnp.dot(hidden, down_weight, preferred_element_type=jnp.float32)
            + probe_down
        ).astype(jnp.bfloat16)
        normed_merge = layer_norm(regroup(after_mlp).astype(jnp.float32), merge_gain).astype(
            jnp.bfloat16
        )
        merged_out = (
            jnp.dot(normed_merge, merge_weight, preferred_element_type=jnp.float32) + probe_merge
        ).astype(jnp.bfloat16)
        return (merged_out, (tokens_win, mixed_heads, normed_mlp, hidden, normed_merge))

    merged_win, backward, stored = jax.vjp(
        forward,
        fields_win.astype(jnp.float32),
        bias_rows[:, None],
        (
            jnp.zeros((TYPES, windows_lon, WIN, 3 * C), jnp.float32),
            jnp.zeros((TYPES, windows_lon, WIN, C), jnp.float32),
            jnp.zeros((Z, LAT, local_len, MLP), jnp.float32),
            jnp.zeros((Z, LAT, local_len, C), jnp.float32),
            jnp.zeros((Z, LAT // 2, local_len // 2, 2 * C), jnp.float32),
        ),
        has_aux=True,
    )
    grad_field_win, grad_bias, grad_probes = backward(cotangent_win)
    grad_qkv, grad_proj, grad_up, grad_down, grad_merge = grad_probes
    tokens_win, mixed_heads, normed_mlp, hidden, normed_merge = stored
    grad_field_win = grad_field_win.astype(jnp.bfloat16)
    first = passed_along(merged_win[:, :, (local_len - HALF) // 2 :], "lon", 1)
    merged = jnp.concatenate([first, merged_win[:, :, : (local_len - HALF) // 2]], axis=2)
    first_grad = passed_along(grad_field_win[:, :, local_len - HALF :], "lon", 1)
    field_grad = jnp.concatenate([first_grad, grad_field_win[:, :, : local_len - HALF]], axis=2)
    terms = (
        weight_term(tokens_win, grad_qkv),
        weight_term(mixed_heads, grad_proj),
        weight_term(normed_mlp, grad_up),
        weight_term(hidden, grad_down),
        weight_term(normed_merge, grad_merge),
        table_sums(grad_bias[:, 0], bias_index),
    )
    flat = jnp.concatenate([t.astype(jnp.bfloat16).reshape(-1) for t in terms])
    rows = -(-flat.size // (count * LANES * 8)) * 8
    flat = jnp.pad(flat, (0, count * rows * LANES - flat.size)).reshape(count, rows, LANES)
    total = summed_over(flat, "lon").reshape(-1).astype(jnp.float32)
    factor = float(Z * LAT * local_len * count) ** (-0.5)
    outs, start = [], 0
    for t in terms:
        outs.append(total[start : start + t.size].reshape(t.shape) * factor)
        start += t.size
    return (merged, field_grad, *outs)


def solution(mesh):
    return jax.shard_map(
        local,
        mesh=mesh,
        in_specs=(
            P("groups", None, "lon", None),
            P(),
            P(),
            P(),
            P(),
            P(),
            P(),
            P(),
            P(),
            P(),
            P(),
            P(),
            P("groups", None, "lon", None),
        ),
        out_specs=(
            P("groups", None, "lon", None),
            P("groups", None, "lon", None),
            P("groups", None),
            P("groups", None),
            P("groups", None),
            P("groups", None),
            P("groups", None),
            P("groups", None, None),
        ),
        check_vma=False,
    )
```

```python
import jax
import jax.numpy as jnp
from jax import lax
from jax.experimental import pallas as pl
from jax.experimental.pallas import tpu as pltpu
from jax.sharding import PartitionSpec as P

C = 192
MLP = 768
HEADS = 6
HEAD = 32
HALF = 6
WIN = 144
BPOS = 3312
LAT = 24
TYPES = 4
TOK = TYPES * WIN
LEVELS = 2
LANES = 128
MAIN = 128
REST = WIN - MAIN
TH = TYPES * HEADS
LOW = 256
HIGH = -(-BPOS // LOW)
MTOK = 160
EPS = 1e-5
MASKED = -1e30
F32 = jnp.float32
BF = jnp.bfloat16
CORES = 2
ACROSS = 4

TROWS = 320
O_UP = 0
O_MERGE = O_UP + 6 * C
O_DOWN = O_MERGE + 3 * MLP
O_QKV = O_DOWN + 6 * C
O_QKV_TAIL = O_QKV + 4 * C
O_PROJ = O_QKV_TAIL + C // 2
O_PROJ_TAIL = O_PROJ + C
O_TABLE = O_PROJ_TAIL + C // 2
O_END = O_TABLE + 2 * TROWS


def dot(a, b):
    return jnp.dot(a, b, preferred_element_type=F32)


def dot_nt(a, b):
    return lax.dot_general(a, b, (((1,), (1,)), ((), ())), preferred_element_type=F32)


def dot_tn(a, b):
    return lax.dot_general(a, b, (((0,), (0,)), ((), ())), preferred_element_type=F32)


def div(n, d):
    return (n * -(-(1 << 16) // d)) >> 16


def onehot(rows, cols, of_row=None, of_col=None):
    if of_row is not None:
        target = of_row(lax.broadcasted_iota(jnp.int32, (rows, 1), 0))
        place = lax.broadcasted_iota(jnp.int32, (rows, cols), 1)
    else:
        target = of_col(lax.broadcasted_iota(jnp.int32, (1, cols), 1))
        place = lax.broadcasted_iota(jnp.int32, (rows, cols), 0)
    return jnp.where(place == target, 1.0, 0.0).astype(BF)


def cell_of_token(n):
    kind = div(n, 72)
    rest = n - 72 * kind
    lat = div(rest, 12)
    return (rest - 12 * lat) * LAT + kind * 6 + lat


def token_of_group(n):
    quarter = div(n, 40)
    rest = n - 40 * quarter
    level = div(rest, 18)
    part = rest - 18 * level
    lat = div(part, 6)
    token = level * 72 + (2 * lat + (quarter >> 1)) * 12 + 2 * (part - 6 * lat) + (quarter & 1)
    return jnp.where(rest < 36, token, -1)


def group_of_token(n):
    level = div(n, 72)
    rest = n - 72 * level
    lat = div(rest, 12)
    lon = rest - 12 * lat
    return ((lat & 1) * 2 + (lon & 1)) * 40 + level * 18 + (lat >> 1) * 6 + (lon >> 1)


def cell_of_merged(n):
    kind = div(n, 40)
    rest = n - 40 * kind
    level = div(rest, 18)
    part = rest - 18 * level
    lat = div(part, 6)
    lon = part - 6 * lat
    half = jnp.where(lon < 3, 0, 1)
    row = half * 72 + (3 * kind + lat) * 6 + (lon - 3 * half) * 2 + level
    return jnp.where(rest < 36, row, -1)


def normalised(values):
    centred = values - jnp.mean(values, axis=-1, keepdims=True)
    scale = lax.rsqrt(jnp.mean(centred * centred, axis=-1, keepdims=True) + EPS)
    return centred * scale, scale


def norm_grad(grad, unit, scale, gain):
    scaled = grad * gain
    return scale * (
        scaled
        - jnp.mean(scaled, axis=-1, keepdims=True)
        - unit * jnp.mean(scaled * unit, axis=-1, keepdims=True)
    )


def rounded(values):
    return values.astype(BF).astype(F32)


def low_onehot(low):
    return jnp.where(
        lax.broadcasted_iota(jnp.int32, (LOW, low.shape[1]), 0) == low, 1.0, 0.0
    ).astype(BF)


def bias_kernel(table_ref, index_ref, region_ref, main_ref, tail_ref, part_ref, last_ref, turned_ref):
    for high in range(HIGH):
        width = min(LOW, BPOS - high * LOW)
        piece = table_ref[:, high * LOW : high * LOW + width]
        if width < LOW:
            piece = jnp.concatenate([piece, jnp.zeros((TH, LOW - width), F32)], axis=1)
        leading = rounded(piece)
        part_ref[high * TH : (high + 1) * TH, :LOW] = leading
        part_ref[high * TH : (high + 1) * TH, LOW:] = piece - leading
    turned_ref[...] = jnp.transpose(index_ref[:, MAIN:])
    parts = part_ref[...].astype(BF)

    def looked_up(index):
        low = low_onehot(index & (LOW - 1))
        high_row = index >> 8
        found = dot(parts, jnp.concatenate([low, low], axis=0))
        chosen = found[0:TH]
        for high in range(1, HIGH):
            chosen = jnp.where(high_row == high, found[high * TH : (high + 1) * TH], chosen)
        return chosen

    def row_block(block, carry):
        base = pl.multiple_of(block * 8, 8)
        rows = index_ref[pl.ds(base, 8), :MAIN]
        for part in range(2):
            index = jnp.concatenate([rows[4 * part + n : 4 * part + n + 1] for n in range(4)], axis=1)
            got = looked_up(index)
            for n in range(4):
                main_ref[pl.ds(base + 4 * part + n, TH, stride=WIN), :] = got[:, n * MAIN : (n + 1) * MAIN]
        return carry

    lax.fori_loop(0, WIN // 8, row_block, 0)
    blank = jnp.zeros((1, LOW - WIN), jnp.int32)
    for key in range(0, REST, 2):
        index = jnp.concatenate(
            [turned_ref[key : key + 1, :], blank, turned_ref[key + 1 : key + 2, :], blank], axis=1
        )
        got = looked_up(index)
        for n in range(2):
            last_ref[pl.ds(key + n, TH, stride=REST), :] = got[:, 256 * n : 256 * n + 128]
            last_ref[pl.ds(TH * REST + key + n, TH, stride=REST), :] = got[:, 256 * n + 128 : 256 * n + 256]
    for kind in range(TYPES):
        across = jnp.zeros((1, WIN), jnp.int32)
        down = jnp.zeros((WIN, 1), jnp.int32)
        column = lax.broadcasted_iota(jnp.int32, (1, WIN), 1)
        row = lax.broadcasted_iota(jnp.int32, (WIN, 1), 0)
        for group in range(12):
            label = region_ref[group // 6, 6 * kind + group % 6]
            across = jnp.where((column >= 12 * group) & (column < 12 * group + 12), label, across)
            down = jnp.where((row >= 12 * group) & (row < 12 * group + 12), label, down)
        same = down == across
        for head in range(HEADS):
            th = head * TYPES + kind
            rows = slice(th * WIN, (th + 1) * WIN)
            main_ref[rows, :] = jnp.where(same[:, :MAIN], main_ref[rows, :], MASKED)
            tail = jnp.concatenate(
                [
                    jnp.transpose(last_ref[th * REST : (th + 1) * REST, :]),
                    jnp.transpose(last_ref[(TH + th) * REST : (TH + th + 1) * REST, :REST]),
                ],
                axis=0,
            )
            tail_ref[rows, :REST] = jnp.where(same[:, MAIN:], tail, MASKED)


def bias_rows(table, index, regions):
    whole = pl.BlockSpec(memory_space=pltpu.VMEM)
    return pl.pallas_call(
        bias_kernel,
        out_shape=[jax.ShapeDtypeStruct((TH * WIN, LANES), F32)] * 2,
        in_specs=[whole, whole, pl.BlockSpec(memory_space=pltpu.SMEM)],
        out_specs=[whole, whole],
        scratch_shapes=[
            pltpu.VMEM((HIGH * TH, 2 * LOW), F32),
            pltpu.VMEM((2 * TH * REST, LANES), F32),
            pltpu.VMEM((REST, WIN), jnp.int32),
        ],
        compiler_params=pltpu.CompilerParams(vmem_limit_bytes=16 * 1024 * 1024),
        cost_estimate=pl.CostEstimate(flops=14_000_000_000, bytes_accessed=4_000_000, transcendentals=0),
        name="bias_rows",
    )(table, index, regions)


def block_kernel(
    core_ref, own_ref, east_ref, own_cotangent_ref, east_cotangent_ref,
    norm_gain_ref, qkv_ref, proj_ref, mlp_gain_ref, up_ref, down_ref, merge_gain_ref, merge_ref,
    bias_ref, bias_tail_ref, index_ref,
    keep_ref, send_ref, merged_keep_ref, merged_send_ref, field_keep_ref, field_send_ref,
    x_ref, unit_ref, scale_ref, tokens_ref, q_ref, k_ref, v_ref, p_ref, mixed_ref,
    unit_mlp_ref, scale_mlp_ref, normed_mlp_ref, hidden_ref, slope_ref, after_mlp_ref,
    group_ref, normed_merge_ref, grad_after_ref, grad_up_ref, grad_attn_ref, grad_mixed_ref,
    ds_ref, ds_tail_ref, ds_corner_ref, dq_ref, dk_ref, dv_ref, grads_ref, turned_ref,
):
    to_tokens = onehot(288, 288, of_row=cell_of_token)
    for level in range(LEVELS):
        cells = jnp.concatenate(
            [
                own_ref[level].astype(F32).reshape(144, C),
                east_ref[level].astype(F32).reshape(144, C),
            ],
            axis=0,
        ).astype(BF)
        ordered = dot(to_tokens, cells)
        for kind in range(TYPES):
            x_ref[WIN * kind + 72 * level : WIN * kind + 72 * level + 72, :] = ordered[72 * kind : 72 * kind + 72]
    unit, scale = normalised(x_ref[...])
    unit_ref[...] = unit
    scale_ref[...] = scale
    tokens = (unit * norm_gain_ref[...]).astype(BF)
    tokens_ref[...] = tokens
    q_ref[...] = dot(tokens, qkv_ref[:, 0:C]).astype(BF)
    k_ref[...] = dot(tokens, qkv_ref[:, C : 2 * C]).astype(BF)
    v_ref[...] = dot(tokens, qkv_ref[:, 2 * C :]).astype(BF)
    lane = lax.broadcasted_iota(jnp.int32, (1, C), 1)
    of_head = [
        jnp.where((lane >= HEAD * h) & (lane < HEAD * (h + 1)), 1.0, 0.0).astype(BF) for h in range(HEADS)
    ]
    temper = HEAD ** (-0.5)

    def attend(kind, carry):
        rows = pl.ds(pl.multiple_of(kind * WIN, 16), WIN)
        q, k, v = q_ref[rows, :], k_ref[rows, :], v_ref[rows, :]
        mixed = jnp.zeros((WIN, C), F32)
        for h in range(HEADS):
            th = h * TYPES + kind
            scores_at = pl.ds(pl.multiple_of(th * WIN, 16), WIN)
            bias = jnp.concatenate([bias_ref[scores_at, :], bias_tail_ref[scores_at, :REST]], axis=1)
            scores = dot_nt(q * of_head[h], k) * temper + bias
            weights = jnp.exp(scores - jnp.max(scores, axis=-1, keepdims=True))
            p = (weights * (1.0 / jnp.sum(weights, axis=-1, keepdims=True))).astype(BF)
            p_ref[th] = p
            mixed = mixed + dot(p, v * of_head[h])
        mixed_ref[rows, :] = mixed.astype(BF)
        return carry

    lax.fori_loop(0, TYPES, attend, 0)
    after_attn = rounded(x_ref[...] + rounded(dot(mixed_ref[...], proj_ref[...])))
    x_ref[...] = after_attn
    unit, scale = normalised(after_attn)
    unit_mlp_ref[...] = unit
    scale_mlp_ref[...] = scale
    normed_mlp = (unit * mlp_gain_ref[...]).astype(BF)
    normed_mlp_ref[...] = normed_mlp
    for part in range(3):
        cols = slice(256 * part, 256 * part + 256)
        u = dot(normed_mlp, up_ref[:, cols])
        below = 0.5 * (1.0 + lax.erf(u * 0.5**0.5))
        hidden_ref[:, cols] = (u * below).astype(BF)
        slope_ref[:, cols] = below + u * (jnp.exp(u * u * (-0.5)) * 0.3989422804014327)
    after_mlp_ref[...] = (x_ref[...] + dot_nt(hidden_ref[...], down_ref[...])).astype(BF)

    to_groups = onehot(160, WIN, of_row=token_of_group)
    for kind in range(TYPES):
        grouped = dot(to_groups, after_mlp_ref[WIN * kind : WIN * kind + WIN, :])
        for quarter in range(4):
            group_ref[quarter, 40 * kind : 40 * kind + 40, :] = grouped[40 * quarter : 40 * quarter + 40]
    quarters = [group_ref[n] for n in range(4)]
    mean = sum(jnp.sum(v, axis=-1, keepdims=True) for v in quarters) * (1.0 / MLP)
    centred = [v - mean for v in quarters]
    variance = sum(jnp.sum(v * v, axis=-1, keepdims=True) for v in centred) * (1.0 / MLP)
    scale_merge = lax.rsqrt(variance + EPS)
    merged = jnp.zeros((MTOK, 2 * C), F32)
    for n in range(4):
        unit = centred[n] * scale_merge
        group_ref[n] = unit
        normed_merge = (unit * merge_gain_ref[n : n + 1, :]).astype(BF)
        normed_merge_ref[n] = normed_merge
        merged = merged + dot(normed_merge, merge_ref[C * n : C * (n + 1), :])
    merged_cells = dot(onehot(144, MTOK, of_col=cell_of_merged), merged.astype(BF)).astype(BF)
    merged_keep_ref[...] = merged_cells[:72]
    merged_send_ref[...] = merged_cells[72:]
    cotangent = jnp.concatenate(
        [own_cotangent_ref[...].astype(F32), east_cotangent_ref[...].astype(F32)], axis=0
    ).astype(BF)
    grad_merged = dot(onehot(MTOK, 144, of_row=cell_of_merged), cotangent).astype(BF)

    scaled, total, along = [], 0.0, 0.0
    for n in range(4):
        grad = dot_tn(normed_merge_ref[n], grad_merged).astype(BF)
        for b in range(3):
            start = O_MERGE + MLP * b + C * n
            grads_ref[start : start + C, :] = grad[:, 128 * b : 128 * b + 128]
        value = rounded(dot_nt(grad_merged, merge_ref[C * n : C * (n + 1), :])) * merge_gain_ref[n : n + 1, :]
        total = total + jnp.sum(value, axis=-1, keepdims=True)
        along = along + jnp.sum(value * group_ref[n], axis=-1, keepdims=True)
        scaled.append(value)
    total = total * (1.0 / MLP)
    along = along * (1.0 / MLP)
    for n in range(4):
        group_ref[n] = scale_merge * (scaled[n] - total - group_ref[n] * along)
    from_groups = onehot(WIN, 160, of_row=group_of_token)
    for kind in range(TYPES):
        grouped = jnp.concatenate([group_ref[n, 40 * kind : 40 * kind + 40, :] for n in range(4)], axis=0)
        grad_after_ref[WIN * kind : WIN * kind + WIN, :] = dot(from_groups, grouped.astype(BF)).astype(BF)

    grad_after = grad_after_ref[...]
    for part in range(3):
        cols = slice(256 * part, 256 * part + 256)
        grad_up_ref[:, cols] = (rounded(dot(grad_after, down_ref[:, cols])) * slope_ref[:, cols]).astype(BF)
    grad_down = dot_tn(grad_after, hidden_ref[...]).astype(BF)
    grad_up = dot_tn(normed_mlp_ref[...], grad_up_ref[...]).astype(BF)
    for b in range(6):
        grads_ref[O_DOWN + C * b : O_DOWN + C * (b + 1), :] = grad_down[:, 128 * b : 128 * b + 128]
        grads_ref[O_UP + C * b : O_UP + C * (b + 1), :] = grad_up[:, 128 * b : 128 * b + 128]
    grad_normed = rounded(dot_nt(grad_up_ref[...], up_ref[...]))
    grad_attn = (
        grad_after.astype(F32)
        + norm_grad(grad_normed, unit_mlp_ref[...], scale_mlp_ref[...], mlp_gain_ref[...])
    ).astype(BF)
    grad_attn_ref[...] = grad_attn

    grad_proj = dot_tn(mixed_ref[...], grad_attn).astype(BF)
    grads_ref[O_PROJ : O_PROJ + C, :] = grad_proj[:, :128]
    grads_ref[O_PROJ_TAIL : O_PROJ_TAIL + C // 2, :] = jnp.concatenate(
        [grad_proj[: C // 2, 128:], grad_proj[C // 2 :, 128:]], axis=1
    )
    grad_mixed_ref[...] = dot_nt(grad_attn, proj_ref[...]).astype(BF)
    ds_corner_ref[...] = jnp.zeros(ds_corner_ref.shape, F32)

    def attend_back(kind, carry):
        rows = pl.ds(pl.multiple_of(kind * WIN, 16), WIN)
        q, k, v, grad = q_ref[rows, :], k_ref[rows, :], v_ref[rows, :], grad_mixed_ref[rows, :]
        dq = jnp.zeros((WIN, C), F32)
        dk = jnp.zeros((WIN, C), F32)
        dv = jnp.zeros((WIN, C), F32)
        for h in range(HEADS):
            th = h * TYPES + kind
            grad_head = grad * of_head[h]
            p = p_ref[th]
            wide = p.astype(F32)
            dp = rounded(dot_nt(grad_head, v))
            ds = wide * (dp - jnp.sum(wide * dp, axis=-1, keepdims=True))
            ds_ref[pl.ds(pl.multiple_of(th * WIN, 16), WIN), :] = ds[:, :MAIN]
            turned = jnp.transpose(
                jnp.concatenate([ds[:, MAIN:], jnp.zeros((WIN, LANES - REST), F32)], axis=1)
            )
            at = pl.ds(pl.multiple_of(th * REST, 16), REST)
            ds_tail_ref[at, :] = turned[:REST, :MAIN]
            ds_corner_ref[at, :REST] = turned[:REST, MAIN:]
            grad_scores = (ds * temper).astype(BF)
            dv = dv + dot_tn(p, grad_head)
            dk = dk + dot_tn(grad_scores, q * of_head[h])
            dq = dq + dot(grad_scores, k * of_head[h])
        dq_ref[rows, :] = dq.astype(BF)
        dk_ref[rows, :] = dk.astype(BF)
        dv_ref[rows, :] = dv.astype(BF)
        return carry

    lax.fori_loop(0, TYPES, attend_back, 0)
    grad_triple = jnp.concatenate([dq_ref[...], dk_ref[...], dv_ref[...]], axis=1)
    grad_qkv = dot_tn(tokens_ref[...], grad_triple).astype(BF)
    for b in range(4):
        grads_ref[O_QKV + C * b : O_QKV + C * (b + 1), :] = grad_qkv[:, 128 * b : 128 * b + 128]
    grads_ref[O_QKV_TAIL : O_QKV_TAIL + C // 2, :] = jnp.concatenate(
        [grad_qkv[: C // 2, 512:], grad_qkv[C // 2 :, 512:]], axis=1
    )
    grad_normed = rounded(dot_nt(grad_triple, qkv_ref[...]))
    x_ref[...] = grad_attn_ref[...].astype(F32) + norm_grad(
        grad_normed, unit_ref[...], scale_ref[...], norm_gain_ref[...]
    )
    to_cells = onehot(288, 288, of_col=cell_of_token)
    for level in range(LEVELS):
        ordered = jnp.concatenate(
            [x_ref[WIN * kind + 72 * level : WIN * kind + 72 * level + 72, :] for kind in range(TYPES)], axis=0
        )
        cells = dot(to_cells, ordered.astype(BF))
        field_keep_ref[level] = cells[:144].reshape(HALF, LAT, C).astype(BF)
        field_send_ref[level] = cells[144:].reshape(HALF, LAT, C).astype(BF)

    turned_ref[...] = jnp.transpose(index_ref[:, MAIN:])

    def table_terms(index, slab):
        high_row = index >> 8
        spread = [jnp.where(high_row == n, slab, 0.0) for n in range(HIGH)]
        spread.append(jnp.zeros((TROWS - HIGH * TH, index.shape[1]), F32))
        return dot_nt(jnp.concatenate(spread, axis=0).astype(BF), low_onehot(index & (LOW - 1)))

    def row_block(block, carry):
        base = pl.multiple_of(block * 8, 8)
        rows = index_ref[pl.ds(base, 8), :MAIN]
        index = jnp.concatenate([rows[n : n + 1] for n in range(8)], axis=1)
        slab = jnp.concatenate([ds_ref[pl.ds(base + n, TH, stride=WIN), :] for n in range(8)], axis=1)
        return carry + table_terms(index, slab)

    table = lax.fori_loop(0, WIN // 8, row_block, jnp.zeros((TROWS, LOW), F32))
    blank = jnp.zeros((1, LOW - WIN), jnp.int32)
    for key in range(0, REST, 4):
        index, slab = [], []
        for n in range(key, key + 4):
            index += [turned_ref[n : n + 1, :], blank]
            slab += [ds_tail_ref[pl.ds(n, TH, stride=REST), :], ds_corner_ref[pl.ds(n, TH, stride=REST), :]]
        table = table + table_terms(jnp.concatenate(index, axis=1), jnp.concatenate(slab, axis=1))
    table = table.astype(BF)
    grads_ref[O_TABLE : O_TABLE + TROWS, :] = table[:, :LANES]
    grads_ref[O_TABLE + TROWS : O_END, :] = table[:, LANES:]
    half = keep_ref.shape[0]
    grads_ref[O_END:, :] = jnp.zeros((2 * half - O_END, LANES), BF)
    core = core_ref[0]
    keep_ref[...] = grads_ref[pl.ds(pl.multiple_of(core * half, 16), half), :]
    send_ref[...] = grads_ref[pl.ds(pl.multiple_of((1 - core) * half, 16), half), :]


def block(half_rows, *args):
    shape = jax.ShapeDtypeStruct
    whole = pl.BlockSpec(memory_space=pltpu.VMEM)
    scratch = [
        ((TOK, C), F32), ((TOK, C), F32), ((TOK, 1), F32), ((TOK, C), BF), ((TOK, C), BF), ((TOK, C), BF),
        ((TOK, C), BF), ((TH, WIN, WIN), BF), ((TOK, C), BF),
        ((TOK, C), F32), ((TOK, 1), F32), ((TOK, C), BF), ((TOK, MLP), BF), ((TOK, MLP), F32), ((TOK, C), BF),
        ((4, MTOK, C), F32), ((4, MTOK, C), BF), ((TOK, C), BF), ((TOK, MLP), BF), ((TOK, C), BF), ((TOK, C), BF),
        ((TH * WIN, LANES), F32), ((TH * REST, LANES), F32), ((TH * REST, LANES), F32),
        ((TOK, C), BF), ((TOK, C), BF), ((TOK, C), BF), ((2 * half_rows, LANES), BF), ((REST, WIN), jnp.int32),
    ]
    return pl.pallas_call(
        block_kernel,
        out_shape=[
            shape((half_rows, LANES), BF),
            shape((half_rows, LANES), BF),
            shape((72, 2 * C), BF),
            shape((72, 2 * C), BF),
            shape((LEVELS, HALF, LAT, C), BF),
            shape((LEVELS, HALF, LAT, C), BF),
        ],
        in_specs=[pl.BlockSpec(memory_space=pltpu.SMEM)] + [whole] * (len(args) - 1),
        out_specs=[whole] * 6,
        scratch_shapes=[pltpu.VMEM(*item) for item in scratch],
        compiler_params=pltpu.CompilerParams(vmem_limit_bytes=40 * 1024 * 1024),
        cost_estimate=pl.CostEstimate(flops=24_000_000_000, bytes_accessed=12_000_000, transcendentals=2_000_000),
        name="block",
    )(*args)


def finish_kernel(factor, core_ref, held_ref, other_ref, qkv_ref, proj_ref, up_ref, down_ref, merge_ref, table_ref, grads_ref):
    core = core_ref[0]
    half = held_ref.shape[0]
    grads_ref[pl.ds(pl.multiple_of(core * half, 16), half), :] = held_ref[...]
    grads_ref[pl.ds(pl.multiple_of((1 - core) * half, 16), half), :] = other_ref[...]

    def part(start, rows):
        return grads_ref[start : start + rows, :].astype(F32) * factor

    for b in range(6):
        up_ref[:, 128 * b : 128 * b + 128] = part(O_UP + C * b, C)
        down_ref[:, 128 * b : 128 * b + 128] = part(O_DOWN + C * b, C)
    for b in range(3):
        merge_ref[:, 128 * b : 128 * b + 128] = part(O_MERGE + MLP * b, MLP)
    for b in range(4):
        qkv_ref[:, 128 * b : 128 * b + 128] = part(O_QKV + C * b, C)
    tail = part(O_QKV_TAIL, C // 2)
    qkv_ref[: C // 2, 512:] = tail[:, :64]
    qkv_ref[C // 2 :, 512:] = tail[:, 64:]
    proj_ref[:, :128] = part(O_PROJ, C)
    tail = part(O_PROJ_TAIL, C // 2)
    proj_ref[: C // 2, 128:] = tail[:, :64]
    proj_ref[C // 2 :, 128:] = tail[:, 64:]
    for side in range(2):
        table = part(O_TABLE + TROWS * side, TROWS)
        for high in range(HIGH):
            start = high * LOW + side * LANES
            width = min(LANES, BPOS - start)
            for head in range(HEADS):
                row = high * TH + head * TYPES
                table_ref[head, :, start : start + width] = table[row : row + TYPES, :width]


def finish(core, held, other, factor):
    shape = jax.ShapeDtypeStruct
    whole = pl.BlockSpec(memory_space=pltpu.VMEM)
    return pl.pallas_call(
        lambda *refs: finish_kernel(factor, *refs),
        out_shape=[
            shape((C, 3 * C), F32),
            shape((C, C), F32),
            shape((C, MLP), F32),
            shape((C, MLP), F32),
            shape((MLP, 2 * C), F32),
            shape((HEADS, TYPES, BPOS), F32),
        ],
        in_specs=[pl.BlockSpec(memory_space=pltpu.SMEM), whole, whole],
        out_specs=[whole] * 6,
        scratch_shapes=[pltpu.VMEM((2 * held.shape[0], LANES), BF)],
        compiler_params=pltpu.CompilerParams(vmem_limit_bytes=16 * 1024 * 1024),
        name="finish",
    )(core, held, other)


def passed_along(value, axis, steps):
    count = lax.axis_size(axis)
    return lax.ppermute(value, axis, [(source, (source + steps) % count) for source in range(count)])


def groups_of(count, apart, size):
    return [
        [start * apart * size + offset + member * apart for member in range(size)]
        for start in range(count // (apart * size))
        for offset in range(apart)
    ]


def summed_over(keep, send, axis):
    count = lax.axis_size(axis)
    along = count // (CORES * ACROSS)
    pairs = [(i, i ^ 1) for i in range(count)]
    held = (keep.astype(F32) + lax.ppermute(send, axis, pairs).astype(F32)).astype(BF)

    def exchanged(value, apart, size):
        return lax.all_to_all(value, axis, 0, 0, axis_index_groups=groups_of(count, apart, size))

    def reduced(value, apart, size):
        got = exchanged(value.reshape(size, -1, LANES), apart, size)
        return jnp.sum(got.astype(F32), axis=0).astype(BF)

    def gathered(value, apart, size):
        return exchanged(jnp.broadcast_to(value[None], (size, *value.shape)), apart, size).reshape(-1, LANES)

    held = reduced(held, CORES, ACROSS)
    held = reduced(held, CORES * ACROSS, along)
    held = gathered(held, CORES * ACROSS, along)
    held = gathered(held, CORES, ACROSS)
    return held, lax.ppermute(held, axis, pairs)


def local(
    fields,
    norm_gain,
    qkv_weight,
    proj_weight,
    bias_table,
    bias_index,
    region_ids,
    mlp_gain,
    up_weight,
    down_weight,
    merge_gain,
    merge_weight,
    cotangent,
):
    count = lax.axis_size("lon")
    core = (lax.axis_index("lon") % CORES).astype(jnp.int32).reshape(1)
    by_lon = fields.transpose(0, 2, 1, 3)
    by_lat = cotangent.transpose(1, 2, 0, 3)
    east = passed_along(by_lon[:, :HALF], "lon", -1)
    east_cotangent = passed_along(by_lat[:, : HALF // 2], "lon", -1)
    bias, bias_tail = bias_rows(bias_table.transpose(1, 0, 2).reshape(TH, BPOS), bias_index, region_ids)
    half_rows = -(-O_END // (count * 8)) * 8 * count // CORES
    keep, send, merged_keep, merged_send, field_keep, field_send = block(
        half_rows,
        core,
        by_lon[:, HALF:],
        east,
        by_lat[:, HALF // 2 :].reshape(72, 2 * C),
        east_cotangent.reshape(72, 2 * C),
        norm_gain.reshape(1, C),
        qkv_weight,
        proj_weight,
        mlp_gain.reshape(1, C),
        up_weight,
        down_weight.T,
        merge_gain.reshape(4, C),
        merge_weight,
        bias,
        bias_tail,
        bias_index,
    )
    held, other = summed_over(keep, send, "lon")
    half = (12, HALF // 2, LEVELS, 2 * C)
    merged_west = passed_along(merged_send, "lon", 1)
    field_west = passed_along(field_send, "lon", 1)
    merged = jnp.concatenate([merged_west.reshape(half), merged_keep.reshape(half)], axis=1)
    field_grad = jnp.concatenate([field_west, field_keep], axis=1)
    factor = float(LEVELS * LAT * fields.shape[2] * count) ** (-0.5)
    qkv_grad, proj_grad, up_grad, down_grad, merge_grad, table_grad = finish(core, held, other, factor)
    return (
        merged.transpose(2, 0, 1, 3),
        field_grad.transpose(0, 2, 1, 3),
        qkv_grad,
        proj_grad,
        up_grad,
        down_grad.T,
        merge_grad,
        table_grad.transpose(1, 0, 2),
    )


def solution(mesh):
    whole = P("groups", None, "lon", None)
    return jax.shard_map(
        local,
        mesh=mesh,
        in_specs=(whole, *[P()] * 11, whole),
        out_specs=(whole, whole, *[P("groups", None)] * 5, P("groups", None, None)),
        check_vma=False,
    )
```

```python
import jax
import jax.numpy as jnp
from jax import lax
from jax.experimental import pallas as pl
from jax.experimental.pallas import tpu as pltpu
from jax.sharding import PartitionSpec as P

C = 192
MLP = 768
HEADS = 6
HEAD = 32
HALF = 6
WIN = 144
BPOS = 3312
LAT = 24
TYPES = 4
TOK = TYPES * WIN
LEVELS = 2
LANES = 128
MAIN = 128
REST = WIN - MAIN
TH = TYPES * HEADS
LOW = 256
HIGH = -(-BPOS // LOW)
MTOK = 160
EPS = 1e-5
MASKED = -1e30
F32 = jnp.float32
BF = jnp.bfloat16
CORES = 2
ACROSS = 4

TROWS = 320
O_UP = 0
O_MERGE = O_UP + 6 * C
O_DOWN = O_MERGE + 3 * MLP
O_QKV = O_DOWN + 6 * C
O_QKV_TAIL = O_QKV + 4 * C
O_PROJ = O_QKV_TAIL + C // 2
O_PROJ_TAIL = O_PROJ + C
O_TABLE = O_PROJ_TAIL + C // 2
O_END = O_TABLE + 2 * TROWS


def dot(a, b):
    return jnp.dot(a, b, preferred_element_type=F32)


def dot_nt(a, b):
    return lax.dot_general(a, b, (((1,), (1,)), ((), ())), preferred_element_type=F32)


def dot_tn(a, b):
    return lax.dot_general(a, b, (((0,), (0,)), ((), ())), preferred_element_type=F32)


def div(n, d):
    return (n * -(-(1 << 16) // d)) >> 16


def onehot(rows, cols, of_row=None, of_col=None):
    if of_row is not None:
        target = of_row(lax.broadcasted_iota(jnp.int32, (rows, 1), 0))
        place = lax.broadcasted_iota(jnp.int32, (rows, cols), 1)
    else:
        target = of_col(lax.broadcasted_iota(jnp.int32, (1, cols), 1))
        place = lax.broadcasted_iota(jnp.int32, (rows, cols), 0)
    return jnp.where(place == target, 1.0, 0.0).astype(BF)


def cell_of_token(n):
    kind = div(n, 72)
    rest = n - 72 * kind
    lat = div(rest, 12)
    return (rest - 12 * lat) * LAT + kind * 6 + lat


def token_of_group(n):
    quarter = div(n, 40)
    rest = n - 40 * quarter
    level = div(rest, 18)
    part = rest - 18 * level
    lat = div(part, 6)
    token = level * 72 + (2 * lat + (quarter >> 1)) * 12 + 2 * (part - 6 * lat) + (quarter & 1)
    return jnp.where(rest < 36, token, -1)


def group_of_token(n):
    level = div(n, 72)
    rest = n - 72 * level
    lat = div(rest, 12)
    lon = rest - 12 * lat
    return ((lat & 1) * 2 + (lon & 1)) * 40 + level * 18 + (lat >> 1) * 6 + (lon >> 1)


def cell_of_merged(n):
    kind = div(n, 40)
    rest = n - 40 * kind
    level = div(rest, 18)
    part = rest - 18 * level
    lat = div(part, 6)
    lon = part - 6 * lat
    half = jnp.where(lon < 3, 0, 1)
    row = half * 72 + (3 * kind + lat) * 6 + (lon - 3 * half) * 2 + level
    return jnp.where(rest < 36, row, -1)


def normalised(values):
    centred = values - jnp.mean(values, axis=-1, keepdims=True)
    scale = lax.rsqrt(jnp.mean(centred * centred, axis=-1, keepdims=True) + EPS)
    return centred * scale, scale


def norm_grad(grad, unit, scale, gain):
    scaled = grad * gain
    return scale * (
        scaled
        - jnp.mean(scaled, axis=-1, keepdims=True)
        - unit * jnp.mean(scaled * unit, axis=-1, keepdims=True)
    )


def rounded(values):
    return values.astype(BF).astype(F32)


def low_onehot(low):
    place = lax.broadcasted_iota(jnp.int32, (LOW, 1), 0).astype(F32).astype(BF)
    hit = jnp.broadcast_to(place, (LOW, low.shape[1])) == low.astype(F32).astype(BF)
    return jnp.where(hit, jnp.array(1, BF), jnp.array(0, BF))


def bias_kernel(table_ref, index_ref, region_ref, main_ref, tail_ref, part_ref, last_ref, turned_ref, mask_ref):
    for high in range(HIGH):
        width = min(LOW, BPOS - high * LOW)
        for head in range(HEADS):
            piece = table_ref[head, :, high * LOW : high * LOW + width]
            if width < LOW:
                piece = jnp.concatenate([piece, jnp.zeros((TYPES, LOW - width), F32)], axis=1)
            leading = rounded(piece)
            row = high * TH + head * TYPES
            part_ref[row : row + TYPES, :LOW] = leading
            part_ref[row : row + TYPES, LOW:] = piece - leading
    turned_ref[...] = jnp.transpose(index_ref[:, MAIN:])
    parts = part_ref[...].astype(BF)

    kind_of = lax.broadcasted_iota(jnp.int32, (TH, 1), 0) & (TYPES - 1)
    column = lax.broadcasted_iota(jnp.int32, (1, LANES), 1)
    labels = []
    for group in range(12):
        label = jnp.zeros((TH, 1), jnp.int32)
        for kind in range(TYPES):
            label = jnp.where(kind_of == kind, region_ref[group // 6, 6 * kind + group % 6], label)
        labels.append(label)
    keys = jnp.zeros((TH, LANES), jnp.int32)
    for group in range(11):
        keys = jnp.where((column >= 12 * group) & (column < 12 * group + 12), labels[group], keys)
    for group in range(12):
        mask_ref[TH * group : TH * (group + 1), :] = jnp.where(keys == labels[group], 0.0, MASKED)

    def looked_up(index):
        low = low_onehot(index & (LOW - 1))
        high_row = index >> 8
        found = dot(parts, jnp.concatenate([low, low], axis=0))
        chosen = found[0:TH]
        for high in range(1, HIGH):
            chosen = jnp.where(high_row == high, found[high * TH : (high + 1) * TH], chosen)
        return chosen

    def row_block(block, carry):
        base = pl.multiple_of(block * 8, 8)
        rows = index_ref[pl.ds(base, 8), :MAIN]
        for part in range(2):
            index = jnp.concatenate([rows[4 * part + n : 4 * part + n + 1] for n in range(4)], axis=1)
            got = looked_up(index)
            for n in range(4):
                row = base + 4 * part + n
                mask = mask_ref[pl.ds(pl.multiple_of(div(row, 12) * TH, 8), TH), :]
                main_ref[pl.ds(row, TH, stride=WIN), :] = got[:, n * MAIN : (n + 1) * MAIN] + mask
        return carry

    lax.fori_loop(0, WIN // 8, row_block, 0, unroll=6)
    for start in range(0, REST, 4):
        got = looked_up(jnp.concatenate([turned_ref[start + n : start + n + 1, :MAIN] for n in range(4)], axis=1))
        for n in range(4):
            group = (MAIN + start + n) // 12
            mask = mask_ref[TH * group : TH * (group + 1), :]
            last_ref[pl.ds(start + n, TH, stride=REST), :] = got[:, n * MAIN : (n + 1) * MAIN] + mask
    got = looked_up(jnp.concatenate([turned_ref[n : n + 1, MAIN:] for n in range(REST)], axis=1))
    apart = jnp.where(labels[10] == labels[11], 0.0, MASKED)
    split = 132 - MAIN
    for n in range(REST):
        half = got[:, LANES * (n // 8) : LANES * (n // 8 + 1)]
        half = half if n % 8 == 0 else pltpu.roll(half, LANES - REST * (n % 8), 1)
        other = (column < split) if n >= split else (column >= split)
        last_ref[pl.ds(TH * REST + n, TH, stride=REST), :] = half + jnp.where(other, apart, 0.0)
    for th in range(TH):
        rows = slice(th * WIN, th * WIN + MAIN)
        tail_ref[rows, :REST] = jnp.transpose(last_ref[th * REST : (th + 1) * REST, :])
        rows = slice(th * WIN + MAIN, (th + 1) * WIN)
        tail_ref[rows, :REST] = jnp.transpose(last_ref[(TH + th) * REST : (TH + th + 1) * REST, :])[:REST]


def bias_rows(table, index, regions):
    whole = pl.BlockSpec(memory_space=pltpu.VMEM)
    return pl.pallas_call(
        bias_kernel,
        out_shape=[jax.ShapeDtypeStruct((TH * WIN, LANES), F32)] * 2,
        in_specs=[whole, whole, pl.BlockSpec(memory_space=pltpu.SMEM)],
        out_specs=[whole, whole],
        scratch_shapes=[
            pltpu.VMEM((HIGH * TH, 2 * LOW), F32),
            pltpu.VMEM((2 * TH * REST, LANES), F32),
            pltpu.VMEM((REST, WIN), jnp.int32),
            pltpu.VMEM((12 * TH, LANES), F32),
        ],
        compiler_params=pltpu.CompilerParams(vmem_limit_bytes=16 * 1024 * 1024),
        cost_estimate=pl.CostEstimate(flops=14_000_000_000, bytes_accessed=4_000_000, transcendentals=0),
        name="bias_rows",
    )(table, index, regions)


def block_kernel(
    core_ref, own_ref, east_ref, own_cotangent_ref, east_cotangent_ref,
    norm_gain_ref, qkv_ref, proj_ref, mlp_gain_ref, up_ref, down_ref, merge_gain_ref, merge_ref,
    bias_ref, bias_tail_ref, index_ref,
    keep_ref, send_ref, merged_keep_ref, merged_send_ref, field_keep_ref, field_send_ref,
    x_ref, unit_ref, scale_ref, tokens_ref, q_ref, k_ref, v_ref, p_ref, mixed_ref,
    unit_mlp_ref, scale_mlp_ref, normed_mlp_ref, hidden_ref, slope_ref, after_mlp_ref,
    group_ref, normed_merge_ref, grad_after_ref, grad_up_ref, grad_attn_ref, grad_mixed_ref,
    ds_ref, ds_tail_ref, ds_corner_ref, triple_ref, grads_ref, turned_ref, cells_ref,
):
    to_tokens = onehot(288, 288, of_row=cell_of_token)
    for level in range(LEVELS):
        cells = jnp.concatenate(
            [
                own_ref[level, HALF:].astype(F32).reshape(144, C),
                east_ref[level].astype(F32).reshape(144, C),
            ],
            axis=0,
        ).astype(BF)
        ordered = dot(to_tokens, cells)
        for kind in range(TYPES):
            x_ref[WIN * kind + 72 * level : WIN * kind + 72 * level + 72, :] = ordered[72 * kind : 72 * kind + 72]
    unit, scale = normalised(x_ref[...])
    unit_ref[...] = unit
    scale_ref[...] = scale
    tokens = (unit * norm_gain_ref[...]).astype(BF)
    tokens_ref[...] = tokens
    q_ref[...] = dot(tokens, qkv_ref[:, 0:C]).astype(BF)
    k_ref[...] = dot(tokens, qkv_ref[:, C : 2 * C]).astype(BF)
    v_ref[...] = dot(tokens, qkv_ref[:, 2 * C :]).astype(BF)
    lane = lax.broadcasted_iota(jnp.int32, (1, C), 1)
    of_head = [
        jnp.where((lane >= HEAD * h) & (lane < HEAD * (h + 1)), 1.0, 0.0).astype(BF) for h in range(HEADS)
    ]
    temper = HEAD ** (-0.5)

    def attend(kind, carry):
        rows = pl.ds(pl.multiple_of(kind * WIN, 16), WIN)
        q, k, v = q_ref[rows, :], k_ref[rows, :], v_ref[rows, :]
        mixed = jnp.zeros((WIN, C), F32)
        products = dot_nt(jnp.concatenate([q * of_head[h] for h in range(HEADS)], axis=0), k)
        for h in range(HEADS):
            th = h * TYPES + kind
            scores_at = pl.ds(pl.multiple_of(th * WIN, 16), WIN)
            bias = jnp.concatenate([bias_ref[scores_at, :], bias_tail_ref[scores_at, :REST]], axis=1)
            scores = products[WIN * h : WIN * (h + 1)] * temper + bias
            weights = jnp.exp(scores - jnp.max(scores, axis=-1, keepdims=True))
            p = weights * (1.0 / jnp.sum(weights, axis=-1, keepdims=True))
            p_ref[th] = p
            mixed = mixed + dot(p.astype(BF), v * of_head[h])
        mixed_ref[rows, :] = mixed.astype(BF)
        return carry

    lax.fori_loop(0, TYPES, attend, 0)
    after_attn = rounded(x_ref[...] + rounded(dot(mixed_ref[...], proj_ref[...])))
    x_ref[...] = after_attn
    unit, scale = normalised(after_attn)
    unit_mlp_ref[...] = unit
    scale_mlp_ref[...] = scale
    normed_mlp = (unit * mlp_gain_ref[...]).astype(BF)
    normed_mlp_ref[...] = normed_mlp
    for part in range(3):
        cols = slice(256 * part, 256 * part + 256)
        u = dot(normed_mlp, up_ref[:, cols])
        below = 0.5 * (1.0 + lax.erf(u * 0.5**0.5))
        hidden_ref[:, cols] = (u * below).astype(BF)
        slope_ref[:, cols] = below + u * (jnp.exp(u * u * (-0.5)) * 0.3989422804014327)
    after_mlp_ref[...] = (x_ref[...] + dot_nt(hidden_ref[...], down_ref[...])).astype(BF)

    to_groups = onehot(160, WIN, of_row=token_of_group)
    for kind in range(TYPES):
        grouped = dot(to_groups, after_mlp_ref[WIN * kind : WIN * kind + WIN, :])
        for quarter in range(4):
            group_ref[quarter, 40 * kind : 40 * kind + 40, :] = grouped[40 * quarter : 40 * quarter + 40]
    quarters = [group_ref[n] for n in range(4)]
    mean = sum(jnp.sum(v, axis=-1, keepdims=True) for v in quarters) * (1.0 / MLP)
    centred = [v - mean for v in quarters]
    variance = sum(jnp.sum(v * v, axis=-1, keepdims=True) for v in centred) * (1.0 / MLP)
    scale_merge = lax.rsqrt(variance + EPS)
    merged = jnp.zeros((MTOK, 2 * C), F32)
    for n in range(4):
        unit = centred[n] * scale_merge
        group_ref[n] = unit
        normed_merge = (unit * merge_gain_ref[:, C * n : C * (n + 1)]).astype(BF)
        normed_merge_ref[n] = normed_merge
        merged = merged + dot(normed_merge, merge_ref[C * n : C * (n + 1), :])
    merged_cells = dot(onehot(144, MTOK, of_col=cell_of_merged), merged.astype(BF))
    for lat in range(12):
        for lon in range(HALF // 2):
            row = (lat * 3 + lon) * 2
            merged_keep_ref[lat, lon] = merged_cells[row : row + 2].astype(BF)
            merged_send_ref[lat, lon] = merged_cells[72 + row : 74 + row].astype(BF)
    for lat in range(12):
        for lon in range(HALF // 2):
            row = (lat * 3 + lon) * 2
            cells_ref[row : row + 2, :] = own_cotangent_ref[lat, 3 + lon].astype(F32)
            cells_ref[72 + row : 74 + row, :] = east_cotangent_ref[lat, lon].astype(F32)
    grad_merged = dot(onehot(MTOK, 144, of_row=cell_of_merged), cells_ref[...].astype(BF)).astype(BF)

    scaled, total, along = [], 0.0, 0.0
    for n in range(4):
        grad = dot_tn(normed_merge_ref[n], grad_merged).astype(BF)
        for b in range(3):
            start = O_MERGE + MLP * b + C * n
            grads_ref[start : start + C, :] = grad[:, 128 * b : 128 * b + 128]
        value = rounded(dot_nt(grad_merged, merge_ref[C * n : C * (n + 1), :])) * merge_gain_ref[:, C * n : C * (n + 1)]
        total = total + jnp.sum(value, axis=-1, keepdims=True)
        along = along + jnp.sum(value * group_ref[n], axis=-1, keepdims=True)
        scaled.append(value)
    total = total * (1.0 / MLP)
    along = along * (1.0 / MLP)
    for n in range(4):
        group_ref[n] = scale_merge * (scaled[n] - total - group_ref[n] * along)
    from_groups = onehot(WIN, 160, of_row=group_of_token)
    for kind in range(TYPES):
        grouped = jnp.concatenate([group_ref[n, 40 * kind : 40 * kind + 40, :] for n in range(4)], axis=0)
        grad_after_ref[WIN * kind : WIN * kind + WIN, :] = dot(from_groups, grouped.astype(BF)).astype(BF)

    grad_after = grad_after_ref[...]
    for part in range(3):
        cols = slice(256 * part, 256 * part + 256)
        grad_up_ref[:, cols] = (rounded(dot(grad_after, down_ref[:, cols])) * slope_ref[:, cols]).astype(BF)
    grad_down = dot_tn(grad_after, hidden_ref[...]).astype(BF)
    grad_up = dot_tn(normed_mlp_ref[...], grad_up_ref[...]).astype(BF)
    for b in range(6):
        grads_ref[O_DOWN + C * b : O_DOWN + C * (b + 1), :] = grad_down[:, 128 * b : 128 * b + 128]
        grads_ref[O_UP + C * b : O_UP + C * (b + 1), :] = grad_up[:, 128 * b : 128 * b + 128]
    grad_normed = rounded(dot_nt(grad_up_ref[...], up_ref[...]))
    grad_attn = (
        grad_after.astype(F32)
        + norm_grad(grad_normed, unit_mlp_ref[...], scale_mlp_ref[...], mlp_gain_ref[...])
    ).astype(BF)
    grad_attn_ref[...] = grad_attn

    grad_proj = dot_tn(mixed_ref[...], grad_attn).astype(BF)
    grads_ref[O_PROJ : O_PROJ + C, :] = grad_proj[:, :128]
    grads_ref[O_PROJ_TAIL : O_PROJ_TAIL + C // 2, :] = jnp.concatenate(
        [grad_proj[: C // 2, 128:], grad_proj[C // 2 :, 128:]], axis=1
    )
    grad_mixed_ref[...] = dot_nt(grad_attn, proj_ref[...]).astype(BF)
    ds_corner_ref[...] = jnp.zeros(ds_corner_ref.shape, F32)

    last_keys = onehot(REST, WIN, of_row=lambda n: n + MAIN)

    def attend_back(kind, carry):
        rows = pl.ds(pl.multiple_of(kind * WIN, 16), WIN)
        v, grad = v_ref[rows, :], grad_mixed_ref[rows, :]
        q_turned, k_turned, grad_turned = (jnp.transpose(a) for a in (q_ref[rows, :], k_ref[rows, :], grad))
        products = dot_nt(jnp.concatenate([grad * of_head[h] for h in range(HEADS)], axis=0), v)
        dq, dk, dv = [], [], []
        for h in range(HEADS):
            th = h * TYPES + kind
            lanes = slice(HEAD * h, HEAD * (h + 1))
            p = p_ref[th]
            weighted = p * products[WIN * h : WIN * (h + 1)]
            ds = weighted - p * jnp.sum(weighted, axis=-1, keepdims=True)
            ds_ref[pl.ds(pl.multiple_of(th * WIN, 16), WIN), :] = ds[:, :MAIN]
            ds = ds.astype(BF)
            turned = dot_nt(jnp.concatenate([k_turned[lanes], last_keys], axis=0), ds)
            at = pl.ds(pl.multiple_of(th * REST, 16), REST)
            ds_tail_ref[at, :] = turned[HEAD:, :MAIN]
            ds_corner_ref[at, :REST] = turned[HEAD:, MAIN:]
            dq.append(turned[:HEAD])
            dk.append(dot(q_turned[lanes], ds))
            dv.append(dot(grad_turned[lanes], p.astype(BF)))
        triple = jnp.concatenate([a * temper for a in dq + dk] + dv, axis=0).astype(BF)
        triple_ref[rows, :] = jnp.transpose(triple)
        return carry

    lax.fori_loop(0, TYPES, attend_back, 0)
    grad_triple = triple_ref[...]
    grad_qkv = dot_tn(tokens_ref[...], grad_triple).astype(BF)
    for b in range(4):
        grads_ref[O_QKV + C * b : O_QKV + C * (b + 1), :] = grad_qkv[:, 128 * b : 128 * b + 128]
    grads_ref[O_QKV_TAIL : O_QKV_TAIL + C // 2, :] = jnp.concatenate(
        [grad_qkv[: C // 2, 512:], grad_qkv[C // 2 :, 512:]], axis=1
    )
    grad_normed = rounded(dot_nt(grad_triple, qkv_ref[...]))
    x_ref[...] = grad_attn_ref[...].astype(F32) + norm_grad(
        grad_normed, unit_ref[...], scale_ref[...], norm_gain_ref[...]
    )
    to_cells = onehot(288, 288, of_col=cell_of_token)
    for level in range(LEVELS):
        ordered = jnp.concatenate(
            [x_ref[WIN * kind + 72 * level : WIN * kind + 72 * level + 72, :] for kind in range(TYPES)], axis=0
        )
        cells = dot(to_cells, ordered.astype(BF))
        field_keep_ref[level] = cells[:144].reshape(HALF, LAT, C).astype(BF)
        field_send_ref[level] = cells[144:].reshape(HALF, LAT, C).astype(BF)

    turned_ref[...] = jnp.transpose(index_ref[:, MAIN:])

    def table_terms(index, slab):
        high_row = index >> 8
        spread = [jnp.where(high_row == n, slab, 0.0) for n in range(HIGH)]
        spread.append(jnp.zeros((TROWS - HIGH * TH, index.shape[1]), F32))
        return dot_nt(jnp.concatenate(spread, axis=0).astype(BF), low_onehot(index & (LOW - 1)))

    def row_block(block, carry):
        base = pl.multiple_of(block * 8, 8)
        rows = index_ref[pl.ds(base, 8), :MAIN]
        index = jnp.concatenate([rows[n : n + 1] for n in range(8)], axis=1)
        slab = jnp.concatenate([ds_ref[pl.ds(base + n, TH, stride=WIN), :] for n in range(8)], axis=1)
        return carry + table_terms(index, slab)

    table = lax.fori_loop(0, WIN // 8, row_block, jnp.zeros((TROWS, LOW), F32), unroll=6)
    blank = jnp.zeros((1, LOW - WIN), jnp.int32)
    for key in range(0, REST, 4):
        index, slab = [], []
        for n in range(key, key + 4):
            index += [turned_ref[n : n + 1, :], blank]
            slab += [ds_tail_ref[pl.ds(n, TH, stride=REST), :], ds_corner_ref[pl.ds(n, TH, stride=REST), :]]
        table = table + table_terms(jnp.concatenate(index, axis=1), jnp.concatenate(slab, axis=1))
    table = table.astype(BF)
    grads_ref[O_TABLE : O_TABLE + TROWS, :] = table[:, :LANES]
    grads_ref[O_TABLE + TROWS : O_END, :] = table[:, LANES:]
    half = keep_ref.shape[0]
    grads_ref[O_END:, :] = jnp.zeros((2 * half - O_END, LANES), BF)
    core = core_ref[0]
    keep_ref[...] = grads_ref[pl.ds(pl.multiple_of(core * half, 16), half), :]
    send_ref[...] = grads_ref[pl.ds(pl.multiple_of((1 - core) * half, 16), half), :]


def block(half_rows, *args):
    shape = jax.ShapeDtypeStruct
    whole = pl.BlockSpec(memory_space=pltpu.VMEM)
    scratch = [
        ((TOK, C), F32), ((TOK, C), F32), ((TOK, 1), F32), ((TOK, C), BF), ((TOK, C), BF), ((TOK, C), BF),
        ((TOK, C), BF), ((TH, WIN, WIN), F32), ((TOK, C), BF),
        ((TOK, C), F32), ((TOK, 1), F32), ((TOK, C), BF), ((TOK, MLP), BF), ((TOK, MLP), F32), ((TOK, C), BF),
        ((4, MTOK, C), F32), ((4, MTOK, C), BF), ((TOK, C), BF), ((TOK, MLP), BF), ((TOK, C), BF), ((TOK, C), BF),
        ((TH * WIN, LANES), F32), ((TH * REST, LANES), F32), ((TH * REST, LANES), F32),
        ((TOK, 3 * C), BF), ((2 * half_rows, LANES), BF), ((REST, WIN), jnp.int32),
        ((144, 2 * C), F32),
    ]
    return pl.pallas_call(
        block_kernel,
        out_shape=[
            shape((half_rows, LANES), BF),
            shape((half_rows, LANES), BF),
            shape((12, HALF // 2, LEVELS, 2 * C), BF),
            shape((12, HALF // 2, LEVELS, 2 * C), BF),
            shape((LEVELS, HALF, LAT, C), BF),
            shape((LEVELS, HALF, LAT, C), BF),
        ],
        in_specs=[pl.BlockSpec(memory_space=pltpu.SMEM)] + [whole] * (len(args) - 1),
        out_specs=[whole] * 6,
        scratch_shapes=[pltpu.VMEM(*item) for item in scratch],
        compiler_params=pltpu.CompilerParams(vmem_limit_bytes=24 * 1024 * 1024),
        cost_estimate=pl.CostEstimate(flops=24_000_000_000, bytes_accessed=12_000_000, transcendentals=2_000_000),
        name="block",
    )(*args)


def finish_kernel(factor, core_ref, held_ref, other_ref, qkv_ref, proj_ref, up_ref, down_ref, merge_ref, table_ref, grads_ref):
    core = core_ref[0]
    half = held_ref.shape[0]
    grads_ref[pl.ds(pl.multiple_of(core * half, 16), half), :] = held_ref[...]
    grads_ref[pl.ds(pl.multiple_of((1 - core) * half, 16), half), :] = other_ref[...]

    def part(start, rows):
        return grads_ref[start : start + rows, :].astype(F32) * factor

    for b in range(6):
        up_ref[:, 128 * b : 128 * b + 128] = part(O_UP + C * b, C)
        down_ref[:, 128 * b : 128 * b + 128] = part(O_DOWN + C * b, C)
    for b in range(3):
        merge_ref[:, 128 * b : 128 * b + 128] = part(O_MERGE + MLP * b, MLP)
    for b in range(4):
        qkv_ref[:, 128 * b : 128 * b + 128] = part(O_QKV + C * b, C)
    tail = part(O_QKV_TAIL, C // 2)
    qkv_ref[: C // 2, 512:] = tail[:, :64]
    qkv_ref[C // 2 :, 512:] = tail[:, 64:]
    proj_ref[:, :128] = part(O_PROJ, C)
    tail = part(O_PROJ_TAIL, C // 2)
    proj_ref[: C // 2, 128:] = tail[:, :64]
    proj_ref[C // 2 :, 128:] = tail[:, 64:]
    for side in range(2):
        table = part(O_TABLE + TROWS * side, TROWS)
        for high in range(HIGH):
            start = high * LOW + side * LANES
            width = min(LANES, BPOS - start)
            for head in range(HEADS):
                row = high * TH + head * TYPES
                table_ref[head, :, start : start + width] = table[row : row + TYPES, :width]


def finish(core, held, other, factor):
    shape = jax.ShapeDtypeStruct
    whole = pl.BlockSpec(memory_space=pltpu.VMEM)
    return pl.pallas_call(
        lambda *refs: finish_kernel(factor, *refs),
        out_shape=[
            shape((C, 3 * C), F32),
            shape((C, C), F32),
            shape((C, MLP), F32),
            shape((C, MLP), F32),
            shape((MLP, 2 * C), F32),
            shape((HEADS, TYPES, BPOS), F32),
        ],
        in_specs=[pl.BlockSpec(memory_space=pltpu.SMEM), whole, whole],
        out_specs=[whole] * 6,
        scratch_shapes=[pltpu.VMEM((2 * held.shape[0], LANES), BF)],
        compiler_params=pltpu.CompilerParams(vmem_limit_bytes=16 * 1024 * 1024),
        name="finish",
    )(core, held, other)


def passed_along(value, axis, steps):
    count = lax.axis_size(axis)
    return lax.ppermute(value, axis, [(source, (source + steps) % count) for source in range(count)])


def groups_of(count, apart, size):
    return [
        [start * apart * size + offset + member * apart for member in range(size)]
        for start in range(count // (apart * size))
        for offset in range(apart)
    ]


def summed_over(keep, send, axis, others):
    count = lax.axis_size(axis)
    along = count // (CORES * ACROSS)
    pairs = [(i, i ^ 1) for i in range(count)]
    held = (keep.astype(F32) + lax.ppermute(send, axis, pairs).astype(F32)).astype(BF)

    def exchanged(value, apart, size):
        return lax.all_to_all(value, axis, 0, 0, axis_index_groups=groups_of(count, apart, size))

    def reduced(value, apart, size):
        got = exchanged(value.reshape(size, -1, LANES), apart, size)
        return jnp.sum(got.astype(F32), axis=0).astype(BF)

    def gathered(value, apart, size):
        return exchanged(jnp.broadcast_to(value[None], (size, *value.shape)), apart, size).reshape(-1, LANES)

    held = reduced(held, CORES, ACROSS)
    held, *others = lax.optimization_barrier((held, *others))
    held = reduced(held, CORES * ACROSS, along)
    held = gathered(held, CORES * ACROSS, along)
    held = gathered(held, CORES, ACROSS)
    return held, lax.ppermute(held, axis, pairs), others


def local(
    fields,
    norm_gain,
    qkv_weight,
    proj_weight,
    bias_table,
    bias_index,
    region_ids,
    mlp_gain,
    up_weight,
    down_weight,
    merge_gain,
    merge_weight,
    cotangent,
):
    count = lax.axis_size("lon")
    core = (lax.axis_index("lon") % CORES).astype(jnp.int32).reshape(1)
    by_lon = fields.transpose(0, 2, 1, 3)
    by_lat = cotangent.transpose(1, 2, 0, 3)
    east = passed_along(by_lon[:, :HALF], "lon", -1)
    east_cotangent = passed_along(by_lat[:, : HALF // 2], "lon", -1)
    table, core, merge_gain = lax.optimization_barrier(
        (bias_table.transpose(1, 0, 2), core, merge_gain.reshape(1, 4 * C))
    )
    bias, bias_tail = bias_rows(table, bias_index, region_ids)
    half_rows = -(-O_END // (count * 8)) * 8 * count // CORES
    keep, send, merged_keep, merged_send, field_keep, field_send = block(
        half_rows,
        core,
        by_lon,
        east,
        by_lat,
        east_cotangent,
        norm_gain.reshape(1, C),
        qkv_weight,
        proj_weight,
        mlp_gain.reshape(1, C),
        up_weight,
        down_weight.T,
        merge_gain,
        merge_weight,
        bias,
        bias_tail,
        bias_index,
    )
    merged_west = passed_along(merged_send, "lon", 1)
    field_west = passed_along(field_send, "lon", 1)
    held, other, (merged_west, field_west) = summed_over(keep, send, "lon", (merged_west, field_west))
    merged = jnp.concatenate([merged_west, merged_keep], axis=1)
    field_grad = jnp.concatenate([field_west, field_keep], axis=1)
    factor = float(LEVELS * LAT * fields.shape[2] * count) ** (-0.5)
    qkv_grad, proj_grad, up_grad, down_grad, merge_grad, table_grad = finish(core, held, other, factor)
    return (
        merged.transpose(2, 0, 1, 3),
        field_grad.transpose(0, 2, 1, 3),
        qkv_grad,
        proj_grad,
        up_grad,
        down_grad.T,
        merge_grad,
        table_grad.transpose(1, 0, 2),
    )


def solution(mesh):
    whole = P("groups", None, "lon", None)
    return jax.shard_map(
        local,
        mesh=mesh,
        in_specs=(whole, *[P()] * 11, whole),
        out_specs=(whole, whole, *[P("groups", None)] * 5, P("groups", None, None)),
        check_vma=False,
    )
```

```python
import jax
import jax.numpy as jnp
from jax import lax
from jax.experimental import pallas as pl
from jax.experimental.pallas import tpu as pltpu
from jax.sharding import PartitionSpec as P

C = 192
MLP = 768
HEADS = 6
HEAD = 32
HALF = 6
WIN = 144
BPOS = 3312
LAT = 24
TYPES = 4
TOK = TYPES * WIN
LEVELS = 2
LANES = 128
MAIN = 128
REST = WIN - MAIN
TH = TYPES * HEADS
LOW = 256
HIGH = -(-BPOS // LOW)
MTOK = 160
EPS = 1e-5
MASKED = -1e30
F32 = jnp.float32
BF = jnp.bfloat16
CORES = 2
ACROSS = 4

TROWS = 320
O_UP = 0
O_MERGE = O_UP + 6 * C
O_DOWN = O_MERGE + 3 * MLP
O_QKV = O_DOWN + 6 * C
O_QKV_TAIL = O_QKV + 4 * C
O_PROJ = O_QKV_TAIL + C // 2
O_PROJ_TAIL = O_PROJ + C
O_TABLE = O_PROJ_TAIL + C // 2
O_END = O_TABLE + 2 * TROWS


def dot(a, b):
    return jnp.dot(a, b, preferred_element_type=F32)


def dot_nt(a, b):
    return lax.dot_general(a, b, (((1,), (1,)), ((), ())), preferred_element_type=F32)


def dot_tn(a, b):
    return lax.dot_general(a, b, (((0,), (0,)), ((), ())), preferred_element_type=F32)


def div(n, d):
    return (n * -(-(1 << 16) // d)) >> 16


def onehot(rows, cols, of_row=None, of_col=None):
    if of_row is not None:
        target = of_row(lax.broadcasted_iota(jnp.int32, (rows, 1), 0))
        place = lax.broadcasted_iota(jnp.int32, (rows, cols), 1)
    else:
        target = of_col(lax.broadcasted_iota(jnp.int32, (1, cols), 1))
        place = lax.broadcasted_iota(jnp.int32, (rows, cols), 0)
    return jnp.where(place == target, 1.0, 0.0).astype(BF)


def cell_of_token(n):
    kind = div(n, 72)
    rest = n - 72 * kind
    lat = div(rest, 12)
    return (rest - 12 * lat) * LAT + kind * 6 + lat


def token_of_group(n):
    quarter = div(n, 40)
    rest = n - 40 * quarter
    level = div(rest, 18)
    part = rest - 18 * level
    lat = div(part, 6)
    token = level * 72 + (2 * lat + (quarter >> 1)) * 12 + 2 * (part - 6 * lat) + (quarter & 1)
    return jnp.where(rest < 36, token, -1)


def group_of_token(n):
    level = div(n, 72)
    rest = n - 72 * level
    lat = div(rest, 12)
    lon = rest - 12 * lat
    return ((lat & 1) * 2 + (lon & 1)) * 40 + level * 18 + (lat >> 1) * 6 + (lon >> 1)


def cell_of_merged(n):
    kind = div(n, 40)
    rest = n - 40 * kind
    level = div(rest, 18)
    part = rest - 18 * level
    lat = div(part, 6)
    lon = part - 6 * lat
    half = jnp.where(lon < 3, 0, 1)
    row = half * 72 + (3 * kind + lat) * 6 + (lon - 3 * half) * 2 + level
    return jnp.where(rest < 36, row, -1)


def normalised(values):
    centred = values - jnp.mean(values, axis=-1, keepdims=True)
    scale = lax.rsqrt(jnp.mean(centred * centred, axis=-1, keepdims=True) + EPS)
    return centred * scale, scale


def norm_grad(grad, unit, scale, gain):
    scaled = grad * gain
    return scale * (
        scaled
        - jnp.mean(scaled, axis=-1, keepdims=True)
        - unit * jnp.mean(scaled * unit, axis=-1, keepdims=True)
    )


def rounded(values):
    return values.astype(BF).astype(F32)


def low_onehot(low):
    place = lax.broadcasted_iota(jnp.int32, (LOW, 1), 0).astype(F32).astype(BF)
    hit = jnp.broadcast_to(place, (LOW, low.shape[1])) == low.astype(F32).astype(BF)
    return jnp.where(hit, jnp.array(1, BF), jnp.array(0, BF))


def bias_kernel(table_ref, index_ref, regions_ref, main_ref, tail_ref, part_ref, last_ref, turned_ref, mask_ref, region_ref, sem):
    copy = pltpu.make_async_copy(regions_ref, region_ref, sem)
    copy.start()
    for high in range(HIGH):
        width = min(LOW, BPOS - high * LOW)
        for head in range(HEADS):
            piece = table_ref[head, :, high * LOW : high * LOW + width]
            if width < LOW:
                piece = jnp.concatenate([piece, jnp.zeros((TYPES, LOW - width), F32)], axis=1)
            leading = rounded(piece)
            row = high * TH + head * TYPES
            part_ref[row : row + TYPES, :LOW] = leading
            part_ref[row : row + TYPES, LOW:] = piece - leading
    turned_ref[...] = jnp.transpose(index_ref[:, MAIN:])
    parts = part_ref[...].astype(BF)

    def looked_up(index):
        low = low_onehot(index & (LOW - 1))
        high_row = index >> 8
        found = dot(parts, jnp.concatenate([low, low], axis=0))
        chosen = found[0:TH]
        for high in range(1, HIGH):
            chosen = jnp.where(high_row == high, found[high * TH : (high + 1) * TH], chosen)
        return chosen

    for start in range(0, REST, 4):
        got = looked_up(jnp.concatenate([turned_ref[start + n : start + n + 1, :MAIN] for n in range(4)], axis=1))
        for n in range(4):
            last_ref[pl.ds(start + n, TH, stride=REST), :] = got[:, n * MAIN : (n + 1) * MAIN]
    got = looked_up(jnp.concatenate([turned_ref[n : n + 1, MAIN:] for n in range(REST)], axis=1))
    for n in range(REST):
        half = got[:, LANES * (n // 8) : LANES * (n // 8 + 1)]
        half = half if n % 8 == 0 else pltpu.roll(half, LANES - REST * (n % 8), 1)
        last_ref[pl.ds(TH * REST + n, TH, stride=REST), :] = half
    copy.wait()
    kind_of = lax.broadcasted_iota(jnp.int32, (TH, 1), 0) & (TYPES - 1)
    column = lax.broadcasted_iota(jnp.int32, (1, LANES), 1)
    labels = []
    for group in range(12):
        label = jnp.zeros((TH, 1), jnp.int32)
        for kind in range(TYPES):
            label = jnp.where(kind_of == kind, region_ref[group // 6, 6 * kind + group % 6], label)
        labels.append(label)
    keys = jnp.zeros((TH, LANES), jnp.int32)
    for group in range(11):
        keys = jnp.where((column >= 12 * group) & (column < 12 * group + 12), labels[group], keys)
    for group in range(12):
        mask_ref[TH * group : TH * (group + 1), :] = jnp.where(keys == labels[group], 0.0, MASKED)

    def row_block(block, carry):
        base = pl.multiple_of(block * 8, 8)
        rows = index_ref[pl.ds(base, 8), :MAIN]
        for part in range(2):
            index = jnp.concatenate([rows[4 * part + n : 4 * part + n + 1] for n in range(4)], axis=1)
            got = looked_up(index)
            for n in range(4):
                row = base + 4 * part + n
                mask = mask_ref[pl.ds(pl.multiple_of(div(row, 12) * TH, 8), TH), :]
                main_ref[pl.ds(row, TH, stride=WIN), :] = got[:, n * MAIN : (n + 1) * MAIN] + mask
        return carry

    lax.fori_loop(0, WIN // 8, row_block, 0, unroll=6)
    apart = jnp.where(labels[10] == labels[11], 0.0, MASKED)
    split = 132 - MAIN
    for n in range(REST):
        group = (MAIN + n) // 12
        rows = pl.ds(n, TH, stride=REST)
        last_ref[rows, :] = last_ref[rows, :] + mask_ref[TH * group : TH * (group + 1), :]
        rows = pl.ds(TH * REST + n, TH, stride=REST)
        other = (column < split) if n >= split else (column >= split)
        last_ref[rows, :] = last_ref[rows, :] + jnp.where(other, apart, 0.0)
    for th in range(TH):
        rows = slice(th * WIN, th * WIN + MAIN)
        tail_ref[rows, :REST] = jnp.transpose(last_ref[th * REST : (th + 1) * REST, :])
        rows = slice(th * WIN + MAIN, (th + 1) * WIN)
        tail_ref[rows, :REST] = jnp.transpose(last_ref[(TH + th) * REST : (TH + th + 1) * REST, :])[:REST]


def stage_kernel(fields_ref, cotangent_ref, table_ref, index_ref, gain_ref, field_ref, half_ref, table_out, index_out, gain_out, sems):
    copies = [
        pltpu.make_async_copy(source, target, sems.at[n])
        for n, (source, target) in enumerate(
            [
                (fields_ref.at[:, :HALF], field_ref),
                (cotangent_ref.at[:, : HALF // 2], half_ref),
                (table_ref, table_out),
                (index_ref, index_out),
                (gain_ref, gain_out.at[0]),
            ]
        )
    ]
    for copy in copies:
        copy.start()
    for copy in copies:
        copy.wait()


def stage(fields, cotangent, table, index, gain):
    shape = jax.ShapeDtypeStruct
    whole = pl.BlockSpec(memory_space=pltpu.VMEM)
    return pl.pallas_call(
        stage_kernel,
        out_shape=[
            shape((LEVELS, HALF, LAT, C), BF),
            shape((12, HALF // 2, LEVELS, 2 * C), BF),
            shape(table.shape, F32),
            shape(index.shape, jnp.int32),
            shape((1, 4 * C), F32),
        ],
        in_specs=[pl.BlockSpec(memory_space=pltpu.HBM)] * 5,
        out_specs=[whole] * 5,
        scratch_shapes=[pltpu.SemaphoreType.DMA((5,))],
        compiler_params=pltpu.CompilerParams(vmem_limit_bytes=4 * 1024 * 1024),
        name="stage",
    )(*(pltpu.with_memory_space_constraint(a, pltpu.HBM) for a in (fields, cotangent, table, index, gain)))


def bias_rows(table, index, regions):
    whole = pl.BlockSpec(memory_space=pltpu.VMEM)
    return pl.pallas_call(
        bias_kernel,
        out_shape=[jax.ShapeDtypeStruct((TH * WIN, LANES), F32)] * 2,
        in_specs=[whole, whole, pl.BlockSpec(memory_space=pltpu.HBM)],
        out_specs=[whole, whole],
        scratch_shapes=[
            pltpu.VMEM((HIGH * TH, 2 * LOW), F32),
            pltpu.VMEM((2 * TH * REST, LANES), F32),
            pltpu.VMEM((REST, WIN), jnp.int32),
            pltpu.VMEM((12 * TH, LANES), F32),
            pltpu.SMEM((LEVELS, LAT), jnp.int32),
            pltpu.SemaphoreType.DMA,
        ],
        compiler_params=pltpu.CompilerParams(vmem_limit_bytes=16 * 1024 * 1024),
        cost_estimate=pl.CostEstimate(flops=14_000_000_000, bytes_accessed=4_000_000, transcendentals=0),
        name="bias_rows",
    )(table, index, pltpu.with_memory_space_constraint(regions, pltpu.HBM))


def block_kernel(
    core_ref, own_ref, east_ref, own_cotangent_ref, east_cotangent_ref,
    norm_gain_ref, qkv_ref, proj_ref, mlp_gain_ref, up_ref, down_ref, merge_gain_ref, merge_ref,
    bias_ref, bias_tail_ref, index_ref,
    keep_ref, send_ref, merged_keep_ref, merged_send_ref, field_keep_ref, field_send_ref,
    x_ref, unit_ref, scale_ref, tokens_ref, q_ref, k_ref, v_ref, p_ref, mixed_ref,
    unit_mlp_ref, scale_mlp_ref, normed_mlp_ref, hidden_ref, slope_ref, after_mlp_ref,
    group_ref, normed_merge_ref, grad_after_ref, grad_up_ref, grad_attn_ref, grad_mixed_ref,
    ds_ref, ds_tail_ref, ds_corner_ref, triple_ref, grads_ref, turned_ref, cells_ref,
):
    to_tokens = onehot(288, 288, of_row=cell_of_token)
    for level in range(LEVELS):
        cells = jnp.concatenate(
            [
                own_ref[level, HALF:].astype(F32).reshape(144, C),
                east_ref[level].astype(F32).reshape(144, C),
            ],
            axis=0,
        ).astype(BF)
        ordered = dot(to_tokens, cells)
        for kind in range(TYPES):
            x_ref[WIN * kind + 72 * level : WIN * kind + 72 * level + 72, :] = ordered[72 * kind : 72 * kind + 72]
    unit, scale = normalised(x_ref[...])
    unit_ref[...] = unit
    scale_ref[...] = scale
    tokens = (unit * norm_gain_ref[...]).astype(BF)
    tokens_ref[...] = tokens
    q_ref[...] = dot(tokens, qkv_ref[:, 0:C]).astype(BF)
    k_ref[...] = dot(tokens, qkv_ref[:, C : 2 * C]).astype(BF)
    v_ref[...] = dot(tokens, qkv_ref[:, 2 * C :]).astype(BF)
    lane = lax.broadcasted_iota(jnp.int32, (1, C), 1)
    of_head = [
        jnp.where((lane >= HEAD * h) & (lane < HEAD * (h + 1)), 1.0, 0.0).astype(BF) for h in range(HEADS)
    ]
    temper = HEAD ** (-0.5)

    def attend(kind, carry):
        rows = pl.ds(pl.multiple_of(kind * WIN, 16), WIN)
        q, k, v = q_ref[rows, :], k_ref[rows, :], v_ref[rows, :]
        mixed = jnp.zeros((WIN, C), F32)
        products = dot_nt(jnp.concatenate([q * of_head[h] for h in range(HEADS)], axis=0), k)
        for h in range(HEADS):
            th = h * TYPES + kind
            scores_at = pl.ds(pl.multiple_of(th * WIN, 16), WIN)
            bias = jnp.concatenate([bias_ref[scores_at, :], bias_tail_ref[scores_at, :REST]], axis=1)
            scores = products[WIN * h : WIN * (h + 1)] * temper + bias
            weights = jnp.exp(scores - jnp.max(scores, axis=-1, keepdims=True))
            p = weights * (1.0 / jnp.sum(weights, axis=-1, keepdims=True))
            p_ref[th] = p
            mixed = mixed + dot(p.astype(BF), v * of_head[h])
        mixed_ref[rows, :] = mixed.astype(BF)
        return carry

    lax.fori_loop(0, TYPES, attend, 0)
    after_attn = rounded(x_ref[...] + rounded(dot(mixed_ref[...], proj_ref[...])))
    x_ref[...] = after_attn
    unit, scale = normalised(after_attn)
    unit_mlp_ref[...] = unit
    scale_mlp_ref[...] = scale
    normed_mlp = (unit * mlp_gain_ref[...]).astype(BF)
    normed_mlp_ref[...] = normed_mlp
    for part in range(3):
        cols = slice(256 * part, 256 * part + 256)
        u = dot(normed_mlp, up_ref[:, cols])
        below = 0.5 * (1.0 + lax.erf(u * 0.5**0.5))
        hidden_ref[:, cols] = (u * below).astype(BF)
        slope_ref[:, cols] = below + u * (jnp.exp(u * u * (-0.5)) * 0.3989422804014327)
    after_mlp_ref[...] = (x_ref[...] + dot_nt(hidden_ref[...], down_ref[...])).astype(BF)

    to_groups = onehot(160, WIN, of_row=token_of_group)
    for kind in range(TYPES):
        grouped = dot(to_groups, after_mlp_ref[WIN * kind : WIN * kind + WIN, :])
        for quarter in range(4):
            group_ref[quarter, 40 * kind : 40 * kind + 40, :] = grouped[40 * quarter : 40 * quarter + 40]
    quarters = [group_ref[n] for n in range(4)]
    mean = sum(jnp.sum(v, axis=-1, keepdims=True) for v in quarters) * (1.0 / MLP)
    centred = [v - mean for v in quarters]
    variance = sum(jnp.sum(v * v, axis=-1, keepdims=True) for v in centred) * (1.0 / MLP)
    scale_merge = lax.rsqrt(variance + EPS)
    merged = jnp.zeros((MTOK, 2 * C), F32)
    for n in range(4):
        unit = centred[n] * scale_merge
        group_ref[n] = unit
        normed_merge = (unit * merge_gain_ref[:, C * n : C * (n + 1)]).astype(BF)
        normed_merge_ref[n] = normed_merge
        merged = merged + dot(normed_merge, merge_ref[C * n : C * (n + 1), :])
    merged_cells = dot(onehot(144, MTOK, of_col=cell_of_merged), merged.astype(BF))
    for lat in range(12):
        for lon in range(HALF // 2):
            row = (lat * 3 + lon) * 2
            merged_keep_ref[lat, lon] = merged_cells[row : row + 2].astype(BF)
            merged_send_ref[lat, lon] = merged_cells[72 + row : 74 + row].astype(BF)
    for lat in range(12):
        for lon in range(HALF // 2):
            row = (lat * 3 + lon) * 2
            cells_ref[row : row + 2, :] = own_cotangent_ref[lat, 3 + lon].astype(F32)
            cells_ref[72 + row : 74 + row, :] = east_cotangent_ref[lat, lon].astype(F32)
    grad_merged = dot(onehot(MTOK, 144, of_row=cell_of_merged), cells_ref[...].astype(BF)).astype(BF)

    scaled, total, along = [], 0.0, 0.0
    for n in range(4):
        grad = dot_tn(normed_merge_ref[n], grad_merged).astype(BF)
        for b in range(3):
            start = O_MERGE + MLP * b + C * n
            grads_ref[start : start + C, :] = grad[:, 128 * b : 128 * b + 128]
        value = rounded(dot_nt(grad_merged, merge_ref[C * n : C * (n + 1), :])) * merge_gain_ref[:, C * n : C * (n + 1)]
        total = total + jnp.sum(value, axis=-1, keepdims=True)
        along = along + jnp.sum(value * group_ref[n], axis=-1, keepdims=True)
        scaled.append(value)
    total = total * (1.0 / MLP)
    along = along * (1.0 / MLP)
    for n in range(4):
        group_ref[n] = scale_merge * (scaled[n] - total - group_ref[n] * along)
    from_groups = onehot(WIN, 160, of_row=group_of_token)
    for kind in range(TYPES):
        grouped = jnp.concatenate([group_ref[n, 40 * kind : 40 * kind + 40, :] for n in range(4)], axis=0)
        grad_after_ref[WIN * kind : WIN * kind + WIN, :] = dot(from_groups, grouped.astype(BF)).astype(BF)

    grad_after = grad_after_ref[...]
    for part in range(3):
        cols = slice(256 * part, 256 * part + 256)
        grad_up_ref[:, cols] = (rounded(dot(grad_after, down_ref[:, cols])) * slope_ref[:, cols]).astype(BF)
    grad_down = dot_tn(grad_after, hidden_ref[...]).astype(BF)
    grad_up = dot_tn(normed_mlp_ref[...], grad_up_ref[...]).astype(BF)
    for b in range(6):
        grads_ref[O_DOWN + C * b : O_DOWN + C * (b + 1), :] = grad_down[:, 128 * b : 128 * b + 128]
        grads_ref[O_UP + C * b : O_UP + C * (b + 1), :] = grad_up[:, 128 * b : 128 * b + 128]
    grad_normed = rounded(dot_nt(grad_up_ref[...], up_ref[...]))
    grad_attn = (
        grad_after.astype(F32)
        + norm_grad(grad_normed, unit_mlp_ref[...], scale_mlp_ref[...], mlp_gain_ref[...])
    ).astype(BF)
    grad_attn_ref[...] = grad_attn

    grad_proj = dot_tn(mixed_ref[...], grad_attn).astype(BF)
    grads_ref[O_PROJ : O_PROJ + C, :] = grad_proj[:, :128]
    grads_ref[O_PROJ_TAIL : O_PROJ_TAIL + C // 2, :] = jnp.concatenate(
        [grad_proj[: C // 2, 128:], grad_proj[C // 2 :, 128:]], axis=1
    )
    grad_mixed_ref[...] = dot_nt(grad_attn, proj_ref[...]).astype(BF)
    ds_corner_ref[...] = jnp.zeros(ds_corner_ref.shape, F32)

    last_keys = onehot(REST, WIN, of_row=lambda n: n + MAIN)

    def attend_back(kind, carry):
        rows = pl.ds(pl.multiple_of(kind * WIN, 16), WIN)
        v, grad = v_ref[rows, :], grad_mixed_ref[rows, :]
        q_turned, k_turned, grad_turned = (jnp.transpose(a) for a in (q_ref[rows, :], k_ref[rows, :], grad))
        products = dot_nt(jnp.concatenate([grad * of_head[h] for h in range(HEADS)], axis=0), v)
        dq, dk, dv = [], [], []
        for h in range(HEADS):
            th = h * TYPES + kind
            lanes = slice(HEAD * h, HEAD * (h + 1))
            p = p_ref[th]
            weighted = p * products[WIN * h : WIN * (h + 1)]
            ds = weighted - p * jnp.sum(weighted, axis=-1, keepdims=True)
            ds_ref[pl.ds(pl.multiple_of(th * WIN, 16), WIN), :] = ds[:, :MAIN]
            ds = ds.astype(BF)
            turned = dot_nt(jnp.concatenate([k_turned[lanes], last_keys], axis=0), ds)
            at = pl.ds(pl.multiple_of(th * REST, 16), REST)
            ds_tail_ref[at, :] = turned[HEAD:, :MAIN]
            ds_corner_ref[at, :REST] = turned[HEAD:, MAIN:]
            dq.append(turned[:HEAD])
            dk.append(dot(q_turned[lanes], ds))
            dv.append(dot(grad_turned[lanes], p.astype(BF)))
        triple = jnp.concatenate([a * temper for a in dq + dk] + dv, axis=0).astype(BF)
        triple_ref[rows, :] = jnp.transpose(triple)
        return carry

    lax.fori_loop(0, TYPES, attend_back, 0)
    grad_triple = triple_ref[...]
    grad_qkv = dot_tn(tokens_ref[...], grad_triple).astype(BF)
    for b in range(4):
        grads_ref[O_QKV + C * b : O_QKV + C * (b + 1), :] = grad_qkv[:, 128 * b : 128 * b + 128]
    grads_ref[O_QKV_TAIL : O_QKV_TAIL + C // 2, :] = jnp.concatenate(
        [grad_qkv[: C // 2, 512:], grad_qkv[C // 2 :, 512:]], axis=1
    )
    grad_normed = rounded(dot_nt(grad_triple, qkv_ref[...]))
    x_ref[...] = grad_attn_ref[...].astype(F32) + norm_grad(
        grad_normed, unit_ref[...], scale_ref[...], norm_gain_ref[...]
    )
    to_cells = onehot(288, 288, of_col=cell_of_token)
    for level in range(LEVELS):
        ordered = jnp.concatenate(
            [x_ref[WIN * kind + 72 * level : WIN * kind + 72 * level + 72, :] for kind in range(TYPES)], axis=0
        )
        cells = dot(to_cells, ordered.astype(BF))
        field_keep_ref[level] = cells[:144].reshape(HALF, LAT, C).astype(BF)
        field_send_ref[level] = cells[144:].reshape(HALF, LAT, C).astype(BF)

    turned_ref[...] = jnp.transpose(index_ref[:, MAIN:])

    def table_terms(index, slab):
        high_row = index >> 8
        spread = [jnp.where(high_row == n, slab, 0.0) for n in range(HIGH)]
        spread.append(jnp.zeros((TROWS - HIGH * TH, index.shape[1]), F32))
        return dot_nt(jnp.concatenate(spread, axis=0).astype(BF), low_onehot(index & (LOW - 1)))

    def row_block(block, carry):
        base = pl.multiple_of(block * 8, 8)
        rows = index_ref[pl.ds(base, 8), :MAIN]
        index = jnp.concatenate([rows[n : n + 1] for n in range(8)], axis=1)
        slab = jnp.concatenate([ds_ref[pl.ds(base + n, TH, stride=WIN), :] for n in range(8)], axis=1)
        return carry + table_terms(index, slab)

    table = lax.fori_loop(0, WIN // 8, row_block, jnp.zeros((TROWS, LOW), F32), unroll=6)
    blank = jnp.zeros((1, LOW - WIN), jnp.int32)
    for key in range(0, REST, 4):
        index, slab = [], []
        for n in range(key, key + 4):
            index += [turned_ref[n : n + 1, :], blank]
            slab += [ds_tail_ref[pl.ds(n, TH, stride=REST), :], ds_corner_ref[pl.ds(n, TH, stride=REST), :]]
        table = table + table_terms(jnp.concatenate(index, axis=1), jnp.concatenate(slab, axis=1))
    table = table.astype(BF)
    grads_ref[O_TABLE : O_TABLE + TROWS, :] = table[:, :LANES]
    grads_ref[O_TABLE + TROWS : O_END, :] = table[:, LANES:]
    half = keep_ref.shape[0]
    if 2 * half > O_END:
        grads_ref[O_END:, :] = jnp.zeros((2 * half - O_END, LANES), BF)
    core = core_ref[0]
    keep_ref[...] = grads_ref[pl.ds(pl.multiple_of(core * half, 16), half), :]
    send_ref[...] = grads_ref[pl.ds(pl.multiple_of((1 - core) * half, 16), half), :]


def block(half_rows, *args):
    shape = jax.ShapeDtypeStruct
    whole = pl.BlockSpec(memory_space=pltpu.VMEM)
    scratch = [
        ((TOK, C), F32), ((TOK, C), F32), ((TOK, 1), F32), ((TOK, C), BF), ((TOK, C), BF), ((TOK, C), BF),
        ((TOK, C), BF), ((TH, WIN, WIN), F32), ((TOK, C), BF),
        ((TOK, C), F32), ((TOK, 1), F32), ((TOK, C), BF), ((TOK, MLP), BF), ((TOK, MLP), F32), ((TOK, C), BF),
        ((4, MTOK, C), F32), ((4, MTOK, C), BF), ((TOK, C), BF), ((TOK, MLP), BF), ((TOK, C), BF), ((TOK, C), BF),
        ((TH * WIN, LANES), F32), ((TH * REST, LANES), F32), ((TH * REST, LANES), F32),
        ((TOK, 3 * C), BF), ((2 * half_rows, LANES), BF), ((REST, WIN), jnp.int32),
        ((144, 2 * C), F32),
    ]
    return pl.pallas_call(
        block_kernel,
        out_shape=[
            shape((half_rows, LANES), BF),
            shape((half_rows, LANES), BF),
            shape((12, HALF // 2, LEVELS, 2 * C), BF),
            shape((12, HALF // 2, LEVELS, 2 * C), BF),
            shape((LEVELS, HALF, LAT, C), BF),
            shape((LEVELS, HALF, LAT, C), BF),
        ],
        in_specs=[pl.BlockSpec(memory_space=pltpu.SMEM)] + [whole] * (len(args) - 1),
        out_specs=[whole] * 6,
        scratch_shapes=[pltpu.VMEM(*item) for item in scratch],
        compiler_params=pltpu.CompilerParams(vmem_limit_bytes=24 * 1024 * 1024),
        cost_estimate=pl.CostEstimate(flops=24_000_000_000, bytes_accessed=12_000_000, transcendentals=2_000_000),
        name="block",
    )(*args)


def finish_kernel(
    factor, core_ref, held_ref, other_ref, merged_west_ref, merged_keep_ref, field_west_ref, field_keep_ref,
    merged_ref, field_ref, qkv_ref, proj_ref, up_ref, down_ref, merge_ref, table_ref, grads_ref,
):
    core = core_ref[0]
    half = held_ref.shape[0]
    grads_ref[pl.ds(pl.multiple_of(core * half, 16), half), :] = held_ref[...]
    grads_ref[pl.ds(pl.multiple_of((1 - core) * half, 16), half), :] = other_ref[...]

    merged_ref[:, : HALF // 2] = merged_west_ref[...]
    merged_ref[:, HALF // 2 :] = merged_keep_ref[...]
    field_ref[:, :HALF] = field_west_ref[...]
    field_ref[:, HALF:] = field_keep_ref[...]

    def part(start, rows):
        return grads_ref[start : start + rows, :].astype(F32) * factor

    for b in range(6):
        up_ref[:, 128 * b : 128 * b + 128] = part(O_UP + C * b, C)
        down_ref[:, 128 * b : 128 * b + 128] = part(O_DOWN + C * b, C)
    for b in range(3):
        merge_ref[:, 128 * b : 128 * b + 128] = part(O_MERGE + MLP * b, MLP)
    for b in range(4):
        qkv_ref[:, 128 * b : 128 * b + 128] = part(O_QKV + C * b, C)
    tail = part(O_QKV_TAIL, C // 2)
    qkv_ref[: C // 2, 512:] = tail[:, :64]
    qkv_ref[C // 2 :, 512:] = tail[:, 64:]
    proj_ref[:, :128] = part(O_PROJ, C)
    tail = part(O_PROJ_TAIL, C // 2)
    proj_ref[: C // 2, 128:] = tail[:, :64]
    proj_ref[C // 2 :, 128:] = tail[:, 64:]
    for side in range(2):
        table = part(O_TABLE + TROWS * side, TROWS)
        for high in range(HIGH):
            start = high * LOW + side * LANES
            width = min(LANES, BPOS - start)
            for head in range(HEADS):
                row = high * TH + head * TYPES
                table_ref[head, :, start : start + width] = table[row : row + TYPES, :width]


def finish(core, held, other, cells, factor):
    shape = jax.ShapeDtypeStruct
    whole = pl.BlockSpec(memory_space=pltpu.VMEM)
    return pl.pallas_call(
        lambda *refs: finish_kernel(factor, *refs),
        out_shape=[
            shape((12, HALF, LEVELS, 2 * C), BF),
            shape((LEVELS, 2 * HALF, LAT, C), BF),
            shape((C, 3 * C), F32),
            shape((C, C), F32),
            shape((C, MLP), F32),
            shape((C, MLP), F32),
            shape((MLP, 2 * C), F32),
            shape((HEADS, TYPES, BPOS), F32),
        ],
        in_specs=[pl.BlockSpec(memory_space=pltpu.SMEM)] + [whole] * 6,
        out_specs=[whole] * 8,
        scratch_shapes=[pltpu.VMEM((2 * held.shape[0], LANES), BF)],
        compiler_params=pltpu.CompilerParams(vmem_limit_bytes=16 * 1024 * 1024),
        name="finish",
    )(core, held, other, *cells)


def passed_along(value, axis, steps):
    count = lax.axis_size(axis)
    return lax.ppermute(value, axis, [(source, (source + steps) % count) for source in range(count)])


def groups_of(count, apart, size):
    return [
        [start * apart * size + offset + member * apart for member in range(size)]
        for start in range(count // (apart * size))
        for offset in range(apart)
    ]


def summed_over(keep, send, axis):
    count = lax.axis_size(axis)
    along = count // (CORES * ACROSS)
    pairs = [(i, i ^ 1) for i in range(count)]
    arrived = lax.ppermute(send, axis, pairs)
    held = (keep.astype(F32) + arrived.astype(F32)).astype(BF)

    def exchanged(value, apart, size):
        return lax.all_to_all(value, axis, 0, 0, axis_index_groups=groups_of(count, apart, size))

    def reduced(value, apart, size):
        got = exchanged(value.reshape(size, -1, *value.shape[1:]), apart, size)
        return jnp.sum(got.astype(F32), axis=0).astype(BF)

    def gathered(value, apart, size):
        return exchanged(jnp.broadcast_to(value[None], (size, *value.shape)), apart, size).reshape(-1, *value.shape[1:])

    held = reduced(held, CORES, ACROSS)
    held = reduced(held.reshape(-1, 2, LANES), CORES * ACROSS, along)
    held = gathered(held, CORES * ACROSS, along).reshape(-1, LANES)
    held = gathered(held, CORES, ACROSS)
    return held, lax.ppermute(held, axis, pairs)


def local(
    fields,
    norm_gain,
    qkv_weight,
    proj_weight,
    bias_table,
    bias_index,
    region_ids,
    mlp_gain,
    up_weight,
    down_weight,
    merge_gain,
    merge_weight,
    cotangent,
):
    count = lax.axis_size("lon")
    core = (lax.axis_index("lon") % CORES).astype(jnp.int32).reshape(1)
    by_lon = fields.transpose(0, 2, 1, 3)
    by_lat = cotangent.transpose(1, 2, 0, 3)
    field_head, cotangent_head, table, index, merge_gain = stage(
        by_lon, by_lat, bias_table.transpose(1, 0, 2), bias_index, merge_gain
    )
    east = passed_along(field_head, "lon", -1)
    east_cotangent = passed_along(cotangent_head, "lon", -1)
    table, core = lax.optimization_barrier((table, core))
    bias, bias_tail = bias_rows(table, index, region_ids)
    half_rows = -(-O_END // (count * 2)) * 2 * count // CORES
    keep, send, merged_keep, merged_send, field_keep, field_send = block(
        half_rows,
        core,
        by_lon,
        east,
        by_lat,
        east_cotangent,
        norm_gain.reshape(1, C),
        qkv_weight,
        proj_weight,
        mlp_gain.reshape(1, C),
        up_weight,
        down_weight.T,
        merge_gain,
        merge_weight,
        bias,
        bias_tail,
        index,
    )
    merged_west = passed_along(merged_send, "lon", 1)
    field_west = passed_along(field_send, "lon", 1)
    held, other = summed_over(keep, send, "lon")
    factor = float(LEVELS * LAT * fields.shape[2] * count) ** (-0.5)
    merged, field_grad, qkv_grad, proj_grad, up_grad, down_grad, merge_grad, table_grad = finish(
        core, held, other, (merged_west, merged_keep, field_west, field_keep), factor
    )
    return (
        merged.transpose(2, 0, 1, 3),
        field_grad.transpose(0, 2, 1, 3),
        qkv_grad,
        proj_grad,
        up_grad,
        down_grad.T,
        merge_grad,
        table_grad.transpose(1, 0, 2),
    )


def solution(mesh):
    whole = P("groups", None, "lon", None)

    return jax.shard_map(
        local,
        mesh=mesh,
        in_specs=(whole, *[P()] * 11, whole),
        out_specs=(whole, whole, *[P("groups", None)] * 5, P("groups", None, None)),
        check_vma=False,
    )
```

```python
import jax
import jax.numpy as jnp
from jax import lax
from jax.experimental import pallas as pl
from jax.experimental.pallas import tpu as pltpu
from jax.sharding import PartitionSpec as P

C = 192
MLP = 768
HEADS = 6
HEAD = 32
HALF = 6
WIN = 144
BPOS = 3312
LAT = 24
TYPES = 4
TOK = TYPES * WIN
LEVELS = 2
LANES = 128
MAIN = 128
REST = WIN - MAIN
TH = TYPES * HEADS
LOW = 256
HIGH = -(-BPOS // LOW)
MTOK = 160
EPS = 1e-5
MASKED = -1e30
F32 = jnp.float32
BF = jnp.bfloat16
CORES = 2
ACROSS = 4

TROWS = 320
O_UP = 0
O_MERGE = O_UP + 6 * C
O_DOWN = O_MERGE + 3 * MLP
O_QKV = O_DOWN + 6 * C
O_QKV_TAIL = O_QKV + 4 * C
O_PROJ = O_QKV_TAIL + C // 2
O_PROJ_TAIL = O_PROJ + C
O_TABLE = O_PROJ_TAIL + C // 2
O_END = O_TABLE + 2 * TROWS


def dot(a, b):
    return jnp.dot(a, b, preferred_element_type=F32)


def dot_nt(a, b):
    return lax.dot_general(a, b, (((1,), (1,)), ((), ())), preferred_element_type=F32)


def dot_tn(a, b):
    return lax.dot_general(a, b, (((0,), (0,)), ((), ())), preferred_element_type=F32)


def div(n, d):
    return (n * -(-(1 << 16) // d)) >> 16


def onehot(rows, cols, of_row=None, of_col=None):
    if of_row is not None:
        target = of_row(lax.broadcasted_iota(jnp.int32, (rows, 1), 0))
        place = lax.broadcasted_iota(jnp.int32, (rows, cols), 1)
    else:
        target = of_col(lax.broadcasted_iota(jnp.int32, (1, cols), 1))
        place = lax.broadcasted_iota(jnp.int32, (rows, cols), 0)
    return jnp.where(place == target, 1.0, 0.0).astype(BF)


def cell_of_token(n):
    kind = div(n, 72)
    rest = n - 72 * kind
    lat = div(rest, 12)
    return (rest - 12 * lat) * LAT + kind * 6 + lat


def token_of_group(n):
    quarter = div(n, 40)
    rest = n - 40 * quarter
    level = div(rest, 18)
    part = rest - 18 * level
    lat = div(part, 6)
    token = level * 72 + (2 * lat + (quarter >> 1)) * 12 + 2 * (part - 6 * lat) + (quarter & 1)
    return jnp.where(rest < 36, token, -1)


def group_of_token(n):
    level = div(n, 72)
    rest = n - 72 * level
    lat = div(rest, 12)
    lon = rest - 12 * lat
    return ((lat & 1) * 2 + (lon & 1)) * 40 + level * 18 + (lat >> 1) * 6 + (lon >> 1)


def cell_of_merged(n):
    kind = div(n, 40)
    rest = n - 40 * kind
    level = div(rest, 18)
    part = rest - 18 * level
    lat = div(part, 6)
    lon = part - 6 * lat
    half = jnp.where(lon < 3, 0, 1)
    row = half * 72 + (3 * kind + lat) * 6 + (lon - 3 * half) * 2 + level
    return jnp.where(rest < 36, row, -1)


def normalised(values):
    centred = values - jnp.mean(values, axis=-1, keepdims=True)
    scale = lax.rsqrt(jnp.mean(centred * centred, axis=-1, keepdims=True) + EPS)
    return centred * scale, scale


def norm_grad(grad, unit, scale, gain):
    scaled = grad * gain
    return scale * (
        scaled
        - jnp.mean(scaled, axis=-1, keepdims=True)
        - unit * jnp.mean(scaled * unit, axis=-1, keepdims=True)
    )


def rounded(values):
    return values.astype(BF).astype(F32)


def low_onehot(low):
    place = lax.broadcasted_iota(jnp.int32, (LOW, 1), 0).astype(F32).astype(BF)
    hit = jnp.broadcast_to(place, (LOW, low.shape[1])) == low.astype(F32).astype(BF)
    return jnp.where(hit, jnp.array(1, BF), jnp.array(0, BF))


def bias_kernel(table_ref, index_ref, regions_ref, main_ref, tail_ref, part_ref, last_ref, turned_ref, mask_ref, region_ref, sem):
    copy = pltpu.make_async_copy(regions_ref, region_ref, sem)
    copy.start()
    for high in range(HIGH):
        width = min(LOW, BPOS - high * LOW)
        for head in range(HEADS):
            piece = table_ref[head, :, high * LOW : high * LOW + width]
            if width < LOW:
                piece = jnp.concatenate([piece, jnp.zeros((TYPES, LOW - width), F32)], axis=1)
            row = high * TH + head * TYPES
            part_ref[row : row + TYPES, :] = piece
    turned_ref[...] = jnp.transpose(index_ref[:, MAIN:])
    parts = part_ref[...].astype(BF)

    def looked_up(index):
        low = low_onehot(index & (LOW - 1))
        high_row = index >> 8
        found = dot(parts, low)
        chosen = found[0:TH]
        for high in range(1, HIGH):
            chosen = jnp.where(high_row == high, found[high * TH : (high + 1) * TH], chosen)
        return chosen

    for start in range(0, REST, 4):
        got = looked_up(jnp.concatenate([turned_ref[start + n : start + n + 1, :MAIN] for n in range(4)], axis=1))
        for n in range(4):
            last_ref[pl.ds(start + n, TH, stride=REST), :] = got[:, n * MAIN : (n + 1) * MAIN]
    got = looked_up(jnp.concatenate([turned_ref[n : n + 1, MAIN:] for n in range(REST)], axis=1))
    for n in range(REST):
        half = got[:, LANES * (n // 8) : LANES * (n // 8 + 1)]
        half = half if n % 8 == 0 else pltpu.roll(half, LANES - REST * (n % 8), 1)
        last_ref[pl.ds(TH * REST + n, TH, stride=REST), :] = half
    copy.wait()
    kind_of = lax.broadcasted_iota(jnp.int32, (TH, 1), 0) & (TYPES - 1)
    column = lax.broadcasted_iota(jnp.int32, (1, LANES), 1)
    labels = []
    for group in range(12):
        label = jnp.zeros((TH, 1), jnp.int32)
        for kind in range(TYPES):
            label = jnp.where(kind_of == kind, region_ref[group // 6, 6 * kind + group % 6], label)
        labels.append(label)
    keys = jnp.zeros((TH, LANES), jnp.int32)
    for group in range(11):
        keys = jnp.where((column >= 12 * group) & (column < 12 * group + 12), labels[group], keys)
    for group in range(12):
        mask_ref[TH * group : TH * (group + 1), :] = jnp.where(keys == labels[group], 0.0, MASKED)

    def row_block(block, carry):
        base = pl.multiple_of(block * 8, 8)
        rows = index_ref[pl.ds(base, 8), :MAIN]
        for part in range(2):
            index = jnp.concatenate([rows[4 * part + n : 4 * part + n + 1] for n in range(4)], axis=1)
            got = looked_up(index)
            for n in range(4):
                row = base + 4 * part + n
                mask = mask_ref[pl.ds(pl.multiple_of(div(row, 12) * TH, 8), TH), :]
                main_ref[pl.ds(row, TH, stride=WIN), :] = got[:, n * MAIN : (n + 1) * MAIN] + mask
        return carry

    lax.fori_loop(0, WIN // 8, row_block, 0, unroll=True)
    apart = jnp.where(labels[10] == labels[11], 0.0, MASKED)
    split = 132 - MAIN
    for n in range(REST):
        group = (MAIN + n) // 12
        rows = pl.ds(n, TH, stride=REST)
        last_ref[rows, :] = last_ref[rows, :] + mask_ref[TH * group : TH * (group + 1), :]
        rows = pl.ds(TH * REST + n, TH, stride=REST)
        other = (column < split) if n >= split else (column >= split)
        last_ref[rows, :] = last_ref[rows, :] + jnp.where(other, apart, 0.0)
    for th in range(TH):
        rows = slice(th * WIN, th * WIN + MAIN)
        tail_ref[rows, :REST] = jnp.transpose(last_ref[th * REST : (th + 1) * REST, :])
        rows = slice(th * WIN + MAIN, (th + 1) * WIN)
        tail_ref[rows, :REST] = jnp.transpose(last_ref[(TH + th) * REST : (TH + th + 1) * REST, :])[:REST]


def stage_kernel(fields_ref, cotangent_ref, table_ref, index_ref, gain_ref, field_ref, half_ref, table_out, index_out, gain_out, sems):
    copies = [
        pltpu.make_async_copy(source, target, sems.at[n])
        for n, (source, target) in enumerate(
            [
                (fields_ref.at[:, HALF:], field_ref),
                (cotangent_ref.at[:, HALF // 2 :], half_ref),
                (table_ref, table_out),
                (index_ref, index_out),
                (gain_ref, gain_out.at[0]),
            ]
        )
    ]
    for copy in copies:
        copy.start()
    for copy in copies:
        copy.wait()


def stage(fields, cotangent, table, index, gain):
    shape = jax.ShapeDtypeStruct
    whole = pl.BlockSpec(memory_space=pltpu.VMEM)
    return pl.pallas_call(
        stage_kernel,
        out_shape=[
            shape((LEVELS, HALF, LAT, C), BF),
            shape((12, HALF // 2, LEVELS, 2 * C), BF),
            shape(table.shape, F32),
            shape(index.shape, jnp.int32),
            shape((1, 4 * C), F32),
        ],
        in_specs=[pl.BlockSpec(memory_space=pltpu.HBM)] * 5,
        out_specs=[whole] * 5,
        scratch_shapes=[pltpu.SemaphoreType.DMA((5,))],
        compiler_params=pltpu.CompilerParams(vmem_limit_bytes=4 * 1024 * 1024),
        name="stage",
    )(*(pltpu.with_memory_space_constraint(a, pltpu.HBM) for a in (fields, cotangent, table, index, gain)))


def bias_rows(table, index, regions):
    whole = pl.BlockSpec(memory_space=pltpu.VMEM)
    return pl.pallas_call(
        bias_kernel,
        out_shape=[jax.ShapeDtypeStruct((TH * WIN, LANES), F32)] * 2,
        in_specs=[whole, whole, pl.BlockSpec(memory_space=pltpu.HBM)],
        out_specs=[whole, whole],
        scratch_shapes=[
            pltpu.VMEM((HIGH * TH, LOW), F32),
            pltpu.VMEM((2 * TH * REST, LANES), F32),
            pltpu.VMEM((REST, WIN), jnp.int32),
            pltpu.VMEM((12 * TH, LANES), F32),
            pltpu.SMEM((LEVELS, LAT), jnp.int32),
            pltpu.SemaphoreType.DMA,
        ],
        compiler_params=pltpu.CompilerParams(vmem_limit_bytes=16 * 1024 * 1024),
        cost_estimate=pl.CostEstimate(flops=14_000_000_000, bytes_accessed=4_000_000, transcendentals=0),
        name="bias_rows",
    )(table, index, pltpu.with_memory_space_constraint(regions, pltpu.HBM))


def block_kernel(
    core_ref, own_ref, west_ref, own_cotangent_ref, west_cotangent_ref,
    norm_gain_ref, qkv_ref, proj_ref, mlp_gain_ref, up_ref, down_ref, merge_gain_ref, merge_ref,
    bias_ref, bias_tail_ref, index_ref,
    keep_ref, send_ref, merged_ref, triple_ref, grad_attn_ref, unit_ref, scale_ref,
    x_ref, tokens_ref, q_ref, k_ref, v_ref, p_ref, mixed_ref,
    unit_mlp_ref, scale_mlp_ref, normed_mlp_ref, hidden_ref, slope_ref, after_mlp_ref,
    group_ref, normed_merge_ref, grad_after_ref, grad_up_ref, grad_mixed_ref,
    ds_ref, ds_tail_ref, ds_corner_ref, grads_ref, turned_ref, cells_ref,
):
    to_tokens = onehot(288, 288, of_row=cell_of_token)
    for level in range(LEVELS):
        cells = jnp.concatenate(
            [
                west_ref[level].astype(F32).reshape(144, C),
                own_ref[level, :HALF].astype(F32).reshape(144, C),
            ],
            axis=0,
        ).astype(BF)
        ordered = dot(to_tokens, cells)
        for kind in range(TYPES):
            x_ref[WIN * kind + 72 * level : WIN * kind + 72 * level + 72, :] = ordered[72 * kind : 72 * kind + 72]
    unit, scale = normalised(x_ref[...])
    unit_ref[...] = unit
    scale_ref[...] = scale
    tokens = (unit * norm_gain_ref[...]).astype(BF)
    tokens_ref[...] = tokens
    q_ref[...] = dot(tokens, qkv_ref[:, 0:C]).astype(BF)
    k_ref[...] = dot(tokens, qkv_ref[:, C : 2 * C]).astype(BF)
    v_ref[...] = dot(tokens, qkv_ref[:, 2 * C :]).astype(BF)
    lane = lax.broadcasted_iota(jnp.int32, (1, C), 1)
    of_head = [
        jnp.where((lane >= HEAD * h) & (lane < HEAD * (h + 1)), 1.0, 0.0).astype(BF) for h in range(HEADS)
    ]
    temper = HEAD ** (-0.5)

    def attend(kind, carry):
        rows = pl.ds(pl.multiple_of(kind * WIN, 16), WIN)
        q, k, v = q_ref[rows, :], k_ref[rows, :], v_ref[rows, :]
        mixed = jnp.zeros((WIN, C), F32)
        products = dot_nt(jnp.concatenate([q * of_head[h] for h in range(HEADS)], axis=0), k)
        for h in range(HEADS):
            th = h * TYPES + kind
            scores_at = pl.ds(pl.multiple_of(th * WIN, 16), WIN)
            bias = jnp.concatenate([bias_ref[scores_at, :], bias_tail_ref[scores_at, :REST]], axis=1)
            scores = products[WIN * h : WIN * (h + 1)] * temper + bias
            weights = jnp.exp(scores - jnp.max(scores, axis=-1, keepdims=True))
            p = weights * (1.0 / jnp.sum(weights, axis=-1, keepdims=True))
            p_ref[th] = p
            mixed = mixed + dot(p.astype(BF), v * of_head[h])
        mixed_ref[rows, :] = mixed.astype(BF)
        return carry

    lax.fori_loop(0, TYPES, attend, 0, unroll=True)
    after_attn = rounded(x_ref[...] + rounded(dot(mixed_ref[...], proj_ref[...])))
    x_ref[...] = after_attn
    unit, scale = normalised(after_attn)
    unit_mlp_ref[...] = unit
    scale_mlp_ref[...] = scale
    normed_mlp = (unit * mlp_gain_ref[...]).astype(BF)
    normed_mlp_ref[...] = normed_mlp
    for part in range(3):
        cols = slice(256 * part, 256 * part + 256)
        u = dot(normed_mlp, up_ref[:, cols])
        below = 0.5 * (1.0 + lax.erf(u * 0.5**0.5))
        hidden_ref[:, cols] = (u * below).astype(BF)
        slope_ref[:, cols] = below + u * (jnp.exp(u * u * (-0.5)) * 0.3989422804014327)
    after_mlp_ref[...] = (x_ref[...] + dot_nt(hidden_ref[...], down_ref[...])).astype(BF)

    to_groups = onehot(160, WIN, of_row=token_of_group)
    for kind in range(TYPES):
        grouped = dot(to_groups, after_mlp_ref[WIN * kind : WIN * kind + WIN, :])
        for quarter in range(4):
            group_ref[quarter, 40 * kind : 40 * kind + 40, :] = grouped[40 * quarter : 40 * quarter + 40]
    quarters = [group_ref[n] for n in range(4)]
    mean = sum(jnp.sum(v, axis=-1, keepdims=True) for v in quarters) * (1.0 / MLP)
    centred = [v - mean for v in quarters]
    variance = sum(jnp.sum(v * v, axis=-1, keepdims=True) for v in centred) * (1.0 / MLP)
    scale_merge = lax.rsqrt(variance + EPS)
    merged = jnp.zeros((MTOK, 2 * C), F32)
    for n in range(4):
        unit = centred[n] * scale_merge
        group_ref[n] = unit
        normed_merge = (unit * merge_gain_ref[:, C * n : C * (n + 1)]).astype(BF)
        normed_merge_ref[n] = normed_merge
        merged = merged + dot(normed_merge, merge_ref[C * n : C * (n + 1), :])
    merged_ref[...] = merged.astype(BF)
    for lat in range(12):
        for lon in range(HALF // 2):
            row = (lat * 3 + lon) * 2
            cells_ref[row : row + 2, :] = west_cotangent_ref[lat, lon].astype(F32)
            cells_ref[72 + row : 74 + row, :] = own_cotangent_ref[lat, lon].astype(F32)
    grad_merged = dot(onehot(MTOK, 144, of_row=cell_of_merged), cells_ref[...].astype(BF)).astype(BF)

    scaled, total, along = [], 0.0, 0.0
    for n in range(4):
        grad = dot_tn(normed_merge_ref[n], grad_merged).astype(BF)
        for b in range(3):
            start = O_MERGE + MLP * b + C * n
            grads_ref[start : start + C, :] = grad[:, 128 * b : 128 * b + 128]
        value = rounded(dot_nt(grad_merged, merge_ref[C * n : C * (n + 1), :])) * merge_gain_ref[:, C * n : C * (n + 1)]
        total = total + jnp.sum(value, axis=-1, keepdims=True)
        along = along + jnp.sum(value * group_ref[n], axis=-1, keepdims=True)
        scaled.append(value)
    total = total * (1.0 / MLP)
    along = along * (1.0 / MLP)
    for n in range(4):
        group_ref[n] = scale_merge * (scaled[n] - total - group_ref[n] * along)
    from_groups = onehot(WIN, 160, of_row=group_of_token)
    for kind in range(TYPES):
        grouped = jnp.concatenate([group_ref[n, 40 * kind : 40 * kind + 40, :] for n in range(4)], axis=0)
        grad_after_ref[WIN * kind : WIN * kind + WIN, :] = dot(from_groups, grouped.astype(BF)).astype(BF)

    grad_after = grad_after_ref[...]
    for part in range(3):
        cols = slice(256 * part, 256 * part + 256)
        grad_up_ref[:, cols] = (rounded(dot(grad_after, down_ref[:, cols])) * slope_ref[:, cols]).astype(BF)
    grad_down = dot_tn(grad_after, hidden_ref[...]).astype(BF)
    grad_up = dot_tn(normed_mlp_ref[...], grad_up_ref[...]).astype(BF)
    for b in range(6):
        grads_ref[O_DOWN + C * b : O_DOWN + C * (b + 1), :] = grad_down[:, 128 * b : 128 * b + 128]
        grads_ref[O_UP + C * b : O_UP + C * (b + 1), :] = grad_up[:, 128 * b : 128 * b + 128]
    grad_normed = rounded(dot_nt(grad_up_ref[...], up_ref[...]))
    grad_attn = (
        grad_after.astype(F32)
        + norm_grad(grad_normed, unit_mlp_ref[...], scale_mlp_ref[...], mlp_gain_ref[...])
    ).astype(BF)
    grad_attn_ref[...] = grad_attn

    grad_proj = dot_tn(mixed_ref[...], grad_attn).astype(BF)
    grads_ref[O_PROJ : O_PROJ + C, :] = grad_proj[:, :128]
    grads_ref[O_PROJ_TAIL : O_PROJ_TAIL + C // 2, :] = jnp.concatenate(
        [grad_proj[: C // 2, 128:], grad_proj[C // 2 :, 128:]], axis=1
    )
    grad_mixed_ref[...] = dot_nt(grad_attn, proj_ref[...]).astype(BF)
    ds_corner_ref[...] = jnp.zeros(ds_corner_ref.shape, F32)

    last_keys = onehot(REST, WIN, of_row=lambda n: n + MAIN)

    def attend_back(kind, carry):
        rows = pl.ds(pl.multiple_of(kind * WIN, 16), WIN)
        v, grad = v_ref[rows, :], grad_mixed_ref[rows, :]
        q_turned, k_turned, grad_turned = (jnp.transpose(a) for a in (q_ref[rows, :], k_ref[rows, :], grad))
        products = dot_nt(jnp.concatenate([grad * of_head[h] for h in range(HEADS)], axis=0), v)
        dq, dk, dv = [], [], []
        for h in range(HEADS):
            th = h * TYPES + kind
            lanes = slice(HEAD * h, HEAD * (h + 1))
            p = p_ref[th]
            weighted = p * products[WIN * h : WIN * (h + 1)]
            ds = weighted - p * jnp.sum(weighted, axis=-1, keepdims=True)
            ds_ref[pl.ds(pl.multiple_of(th * WIN, 16), WIN), :] = ds[:, :MAIN]
            ds = ds.astype(BF)
            turned = dot_nt(jnp.concatenate([k_turned[lanes], last_keys], axis=0), ds)
            at = pl.ds(pl.multiple_of(th * REST, 16), REST)
            ds_tail_ref[at, :] = turned[HEAD:, :MAIN]
            ds_corner_ref[at, :REST] = turned[HEAD:, MAIN:]
            dq.append(turned[:HEAD])
            dk.append(dot(q_turned[lanes], ds))
            dv.append(dot(grad_turned[lanes], p.astype(BF)))
        triple = jnp.concatenate([a * temper for a in dq + dk] + dv, axis=0).astype(BF)
        triple_ref[rows, :] = jnp.transpose(triple)
        return carry

    lax.fori_loop(0, TYPES, attend_back, 0, unroll=True)
    grad_triple = triple_ref[...]
    grad_qkv = dot_tn(tokens_ref[...], grad_triple).astype(BF)
    for b in range(4):
        grads_ref[O_QKV + C * b : O_QKV + C * (b + 1), :] = grad_qkv[:, 128 * b : 128 * b + 128]
    grads_ref[O_QKV_TAIL : O_QKV_TAIL + C // 2, :] = jnp.concatenate(
        [grad_qkv[: C // 2, 512:], grad_qkv[C // 2 :, 512:]], axis=1
    )
    turned_ref[...] = jnp.transpose(index_ref[:, MAIN:])

    def table_terms(index, slab):
        high_row = index >> 8
        spread = [jnp.where(high_row == n, slab, 0.0) for n in range(HIGH)]
        spread.append(jnp.zeros((TROWS - HIGH * TH, index.shape[1]), F32))
        return dot_nt(jnp.concatenate(spread, axis=0).astype(BF), low_onehot(index & (LOW - 1)))

    def row_block(block, carry):
        base = pl.multiple_of(block * 8, 8)
        rows = index_ref[pl.ds(base, 8), :MAIN]
        index = jnp.concatenate([rows[n : n + 1] for n in range(8)], axis=1)
        slab = jnp.concatenate([ds_ref[pl.ds(base + n, TH, stride=WIN), :] for n in range(8)], axis=1)
        return carry + table_terms(index, slab)

    table = lax.fori_loop(0, WIN // 8, row_block, jnp.zeros((TROWS, LOW), F32), unroll=9)
    blank = jnp.zeros((1, LOW - WIN), jnp.int32)
    for key in range(0, REST, 4):
        index, slab = [], []
        for n in range(key, key + 4):
            index += [turned_ref[n : n + 1, :], blank]
            slab += [ds_tail_ref[pl.ds(n, TH, stride=REST), :], ds_corner_ref[pl.ds(n, TH, stride=REST), :]]
        table = table + table_terms(jnp.concatenate(index, axis=1), jnp.concatenate(slab, axis=1))
    table = table.astype(BF)
    grads_ref[O_TABLE : O_TABLE + TROWS, :] = table[:, :LANES]
    grads_ref[O_TABLE + TROWS : O_END, :] = table[:, LANES:]
    half = keep_ref.shape[0]
    if 2 * half > O_END:
        grads_ref[O_END:, :] = jnp.zeros((2 * half - O_END, LANES), BF)
    core = core_ref[0]
    keep_ref[...] = grads_ref[pl.ds(pl.multiple_of(core * half, 16), half), :]
    send_ref[...] = grads_ref[pl.ds(pl.multiple_of((1 - core) * half, 16), half), :]


def block(half_rows, *args):
    shape = jax.ShapeDtypeStruct
    whole = pl.BlockSpec(memory_space=pltpu.VMEM)
    scratch = [
        ((TOK, C), F32), ((TOK, C), BF), ((TOK, C), BF), ((TOK, C), BF),
        ((TOK, C), BF), ((TH, WIN, WIN), F32), ((TOK, C), BF),
        ((TOK, C), F32), ((TOK, 1), F32), ((TOK, C), BF), ((TOK, MLP), BF), ((TOK, MLP), F32), ((TOK, C), BF),
        ((4, MTOK, C), F32), ((4, MTOK, C), BF), ((TOK, C), BF), ((TOK, MLP), BF), ((TOK, C), BF),
        ((TH * WIN, LANES), F32), ((TH * REST, LANES), F32), ((TH * REST, LANES), F32),
        ((2 * half_rows, LANES), BF), ((REST, WIN), jnp.int32),
        ((144, 2 * C), F32),
    ]
    return pl.pallas_call(
        block_kernel,
        out_shape=[
            shape((half_rows, LANES), BF),
            shape((half_rows, LANES), BF),
            shape((MTOK, 2 * C), BF),
            shape((TOK, 3 * C), BF),
            shape((TOK, C), BF),
            shape((TOK, C), F32),
            shape((TOK, 1), F32),
        ],
        in_specs=[pl.BlockSpec(memory_space=pltpu.SMEM)] + [whole] * (len(args) - 1),
        out_specs=[whole] * 7,
        scratch_shapes=[pltpu.VMEM(*item) for item in scratch],
        compiler_params=pltpu.CompilerParams(vmem_limit_bytes=24 * 1024 * 1024),
        cost_estimate=pl.CostEstimate(flops=24_000_000_000, bytes_accessed=12_000_000, transcendentals=2_000_000),
        name="block",
    )(*args)


def cells_kernel(
    merged_ref, triple_ref, grad_attn_ref, unit_ref, scale_ref, qkv_ref, gain_ref,
    merged_keep_ref, field_keep_ref, home_ref, x_ref,
):
    grad_normed = rounded(dot_nt(triple_ref[...], qkv_ref[...]))
    x_ref[...] = grad_attn_ref[...].astype(F32) + norm_grad(
        grad_normed, unit_ref[...], scale_ref[...], gain_ref[...]
    )
    to_cells = onehot(288, 288, of_col=cell_of_token)
    for level in range(LEVELS):
        ordered = jnp.concatenate(
            [x_ref[WIN * kind + 72 * level : WIN * kind + 72 * level + 72, :] for kind in range(TYPES)], axis=0
        )
        cells = dot(to_cells, ordered.astype(BF))
        home_ref[HALF * level : HALF * (level + 1)] = cells[:144].reshape(HALF, LAT, C).astype(BF)
        field_keep_ref[level] = cells[144:].reshape(HALF, LAT, C).astype(BF)
    merged_cells = dot(onehot(144, MTOK, of_col=cell_of_merged), merged_ref[...])
    for lat in range(12):
        for lon in range(HALF // 2):
            row = 72 + (lat * 3 + lon) * 2
            merged_keep_ref[lat, lon] = merged_cells[row : row + 2].astype(BF)
    for side in range(2):
        home_ref[12 + 3 * side : 15 + 3 * side] = (
            merged_cells[:72, C * side : C * (side + 1)].reshape(3, LAT, C).astype(BF)
        )


def to_grid(*args):
    shape = jax.ShapeDtypeStruct
    whole = pl.BlockSpec(memory_space=pltpu.VMEM)
    return pl.pallas_call(
        cells_kernel,
        out_shape=[
            shape((12, HALF // 2, LEVELS, 2 * C), BF),
            shape((LEVELS, HALF, LAT, C), BF),
            shape((LEVELS * HALF + 6, LAT, C), BF),
        ],
        in_specs=[whole] * 7,
        out_specs=[whole] * 3,
        scratch_shapes=[pltpu.VMEM((TOK, C), F32)],
        compiler_params=pltpu.CompilerParams(vmem_limit_bytes=12 * 1024 * 1024),
        cost_estimate=pl.CostEstimate(flops=1_500_000_000, bytes_accessed=3_000_000, transcendentals=0),
        name="to_grid",
    )(*args)


def finish_kernel(
    factor, core_ref, held_ref, other_ref, east_ref, merged_keep_ref, field_keep_ref,
    merged_ref, field_ref, qkv_ref, proj_ref, up_ref, down_ref, merge_ref, table_ref, grads_ref,
):
    core = core_ref[0]
    half = held_ref.shape[0]
    grads_ref[pl.ds(pl.multiple_of(core * half, 16), half), :] = held_ref[...]
    grads_ref[pl.ds(pl.multiple_of((1 - core) * half, 16), half), :] = other_ref[...]

    for level in range(LEVELS):
        field_ref[level, HALF:] = east_ref[HALF * level : HALF * (level + 1)]
    field_ref[:, :HALF] = field_keep_ref[...]
    sides = [east_ref[12 + 3 * side : 15 + 3 * side].astype(F32).reshape(72, C) for side in range(2)]
    cells = jnp.concatenate(sides, axis=1)
    for lat in range(12):
        for lon in range(HALF // 2):
            row = (lat * 3 + lon) * 2
            merged_ref[lat, HALF // 2 + lon] = cells[row : row + 2].astype(BF)
    merged_ref[:, : HALF // 2] = merged_keep_ref[...]

    def part(start, rows):
        return grads_ref[start : start + rows, :].astype(F32) * factor

    for b in range(6):
        up_ref[:, 128 * b : 128 * b + 128] = part(O_UP + C * b, C)
        down_ref[:, 128 * b : 128 * b + 128] = part(O_DOWN + C * b, C)
    for b in range(3):
        merge_ref[:, 128 * b : 128 * b + 128] = part(O_MERGE + MLP * b, MLP)
    for b in range(4):
        qkv_ref[:, 128 * b : 128 * b + 128] = part(O_QKV + C * b, C)
    tail = part(O_QKV_TAIL, C // 2)
    qkv_ref[: C // 2, 512:] = tail[:, :64]
    qkv_ref[C // 2 :, 512:] = tail[:, 64:]
    proj_ref[:, :128] = part(O_PROJ, C)
    tail = part(O_PROJ_TAIL, C // 2)
    proj_ref[: C // 2, 128:] = tail[:, :64]
    proj_ref[C // 2 :, 128:] = tail[:, 64:]
    for side in range(2):
        table = part(O_TABLE + TROWS * side, TROWS)
        for high in range(HIGH):
            start = high * LOW + side * LANES
            width = min(LANES, BPOS - start)
            for head in range(HEADS):
                row = high * TH + head * TYPES
                table_ref[head, :, start : start + width] = table[row : row + TYPES, :width]


def finish(core, held, other, cells, factor):
    shape = jax.ShapeDtypeStruct
    whole = pl.BlockSpec(memory_space=pltpu.VMEM)
    return pl.pallas_call(
        lambda *refs: finish_kernel(factor, *refs),
        out_shape=[
            shape((12, HALF, LEVELS, 2 * C), BF),
            shape((LEVELS, 2 * HALF, LAT, C), BF),
            shape((C, 3 * C), F32),
            shape((C, C), F32),
            shape((C, MLP), F32),
            shape((C, MLP), F32),
            shape((MLP, 2 * C), F32),
            shape((HEADS, TYPES, BPOS), F32),
        ],
        in_specs=[pl.BlockSpec(memory_space=pltpu.SMEM)] + [whole] * 5,
        out_specs=[whole] * 8,
        scratch_shapes=[pltpu.VMEM((2 * held.shape[0], LANES), BF)],
        compiler_params=pltpu.CompilerParams(vmem_limit_bytes=16 * 1024 * 1024),
        name="finish",
    )(core, held, other, *cells)


def passed_along(value, axis, steps):
    count = lax.axis_size(axis)
    return lax.ppermute(value, axis, [(source, (source + steps) % count) for source in range(count)])


def groups_of(count, apart, size):
    return [
        [start * apart * size + offset + member * apart for member in range(size)]
        for start in range(count // (apart * size))
        for offset in range(apart)
    ]


def summed_over(keep, send, axis):
    count = lax.axis_size(axis)
    along = count // (CORES * ACROSS)
    pairs = [(i, i ^ 1) for i in range(count)]
    arrived = lax.ppermute(send, axis, pairs)
    held = (keep.astype(F32) + arrived.astype(F32)).astype(BF)

    def exchanged(value, apart, size):
        return lax.all_to_all(value, axis, 0, 0, axis_index_groups=groups_of(count, apart, size))

    def reduced(value, apart, size):
        got = exchanged(value.reshape(size, -1, *value.shape[1:]), apart, size)
        return jnp.sum(got.astype(F32), axis=0).astype(BF)

    def gathered(value, apart, size):
        return exchanged(jnp.broadcast_to(value[None], (size, *value.shape)), apart, size).reshape(-1, *value.shape[1:])

    held = reduced(held, CORES, ACROSS)
    held = reduced(held.reshape(-1, 2, LANES), CORES * ACROSS, along)
    held = gathered(held, CORES * ACROSS, along).reshape(-1, LANES)
    held = gathered(held, CORES, ACROSS)
    return held, lax.ppermute(held, axis, pairs)


def local(
    fields,
    norm_gain,
    qkv_weight,
    proj_weight,
    bias_table,
    bias_index,
    region_ids,
    mlp_gain,
    up_weight,
    down_weight,
    merge_gain,
    merge_weight,
    cotangent,
):
    count = lax.axis_size("lon")
    core = (lax.axis_index("lon") % CORES).astype(jnp.int32).reshape(1)
    by_lon = fields.transpose(0, 2, 1, 3)
    by_lat = cotangent.transpose(1, 2, 0, 3)
    field_last, cotangent_last, table, index, merge_gain = stage(
        by_lon, by_lat, bias_table.transpose(1, 0, 2), bias_index, merge_gain
    )
    west = passed_along(field_last, "lon", 1)
    west_cotangent = passed_along(cotangent_last, "lon", 1)
    table, core = lax.optimization_barrier((table, core))
    bias, bias_tail = bias_rows(table, index, region_ids)
    half_rows = -(-O_END // (count * 2)) * 2 * count // CORES
    keep, send, *results = block(
        half_rows,
        core,
        by_lon,
        west,
        by_lat,
        west_cotangent,
        norm_gain.reshape(1, C),
        qkv_weight,
        proj_weight,
        mlp_gain.reshape(1, C),
        up_weight,
        down_weight.T,
        merge_gain,
        merge_weight,
        bias,
        bias_tail,
        index,
    )
    merged_keep, field_keep, home = to_grid(*results, qkv_weight, norm_gain.reshape(1, C))
    east = passed_along(home, "lon", -1)
    held, other = summed_over(keep, send, "lon")
    factor = float(LEVELS * LAT * fields.shape[2] * count) ** (-0.5)
    merged, field_grad, qkv_grad, proj_grad, up_grad, down_grad, merge_grad, table_grad = finish(
        core, held, other, (east, merged_keep, field_keep), factor
    )
    return (
        merged.transpose(2, 0, 1, 3),
        field_grad.transpose(0, 2, 1, 3),
        qkv_grad,
        proj_grad,
        up_grad,
        down_grad.T,
        merge_grad,
        table_grad.transpose(1, 0, 2),
    )


def solution(mesh):
    whole = P("groups", None, "lon", None)

    return jax.shard_map(
        local,
        mesh=mesh,
        in_specs=(whole, *[P()] * 11, whole),
        out_specs=(whole, whole, *[P("groups", None)] * 5, P("groups", None, None)),
        check_vma=False,
    )
```

```python
import jax
import jax.numpy as jnp
from jax import lax
from jax.experimental import pallas as pl
from jax.experimental.pallas import tpu as pltpu
from jax.sharding import PartitionSpec as P

C = 192
MLP = 768
HEADS = 6
HEAD = 32
HALF = 6
WIN = 144
BPOS = 3312
LAT = 24
TYPES = 4
TOK = TYPES * WIN
LEVELS = 2
LANES = 128
MAIN = 128
REST = WIN - MAIN
TH = TYPES * HEADS
LOW = 256
HIGH = -(-BPOS // LOW)
MTOK = 160
EPS = 1e-5
MASKED = -1e30
F32 = jnp.float32
BF = jnp.bfloat16
CORES = 2
ACROSS = 4

TROWS = 320
TLAST = (HIGH - 1) * TH
LAST = (HIGH - 1) * LOW + LANES
O_UP = 0
O_DOWN = O_UP + 6 * C
O_QKV = O_DOWN + 6 * C
O_QKV_TAIL = O_QKV + 4 * C
O_LAST = O_QKV_TAIL + C // 2
O_MERGE = O_LAST + TROWS - TLAST
O_PROJ = O_MERGE + 3 * MLP
O_PROJ_TAIL = O_PROJ + C
O_TABLE = O_PROJ_TAIL + C // 2
O_END = O_TABLE + TROWS + TLAST


def dot(a, b):
    return jnp.dot(a, b, preferred_element_type=F32)


def dot_nt(a, b):
    return lax.dot_general(a, b, (((1,), (1,)), ((), ())), preferred_element_type=F32)


def dot_tn(a, b):
    return lax.dot_general(a, b, (((0,), (0,)), ((), ())), preferred_element_type=F32)


def div(n, d):
    return (n * -(-(1 << 16) // d)) >> 16


def onehot(rows, cols, of_row=None, of_col=None):
    if of_row is not None:
        target = of_row(lax.broadcasted_iota(jnp.int32, (rows, 1), 0))
        place = lax.broadcasted_iota(jnp.int32, (rows, cols), 1)
    else:
        target = of_col(lax.broadcasted_iota(jnp.int32, (1, cols), 1))
        place = lax.broadcasted_iota(jnp.int32, (rows, cols), 0)
    return jnp.where(place == target, 1.0, 0.0).astype(BF)


def cell_of_token(n):
    kind = div(n, 72)
    rest = n - 72 * kind
    lat = div(rest, 12)
    return (rest - 12 * lat) * LAT + kind * 6 + lat


def token_of_group(n):
    quarter = div(n, 40)
    rest = n - 40 * quarter
    level = div(rest, 18)
    part = rest - 18 * level
    lat = div(part, 6)
    token = level * 72 + (2 * lat + (quarter >> 1)) * 12 + 2 * (part - 6 * lat) + (quarter & 1)
    return jnp.where(rest < 36, token, -1)


def group_of_token(n):
    level = div(n, 72)
    rest = n - 72 * level
    lat = div(rest, 12)
    lon = rest - 12 * lat
    return ((lat & 1) * 2 + (lon & 1)) * 40 + level * 18 + (lat >> 1) * 6 + (lon >> 1)


def cell_of_merged(n):
    kind = div(n, 40)
    rest = n - 40 * kind
    level = div(rest, 18)
    part = rest - 18 * level
    lat = div(part, 6)
    lon = part - 6 * lat
    half = jnp.where(lon < 3, 0, 1)
    row = half * 72 + (3 * kind + lat) * 6 + (lon - 3 * half) * 2 + level
    return jnp.where(rest < 36, row, -1)


def normalised(values):
    centred = values - jnp.mean(values, axis=-1, keepdims=True)
    scale = lax.rsqrt(jnp.mean(centred * centred, axis=-1, keepdims=True) + EPS)
    return centred * scale, scale


def norm_grad(grad, unit, scale, gain):
    scaled = grad * gain
    return scale * (
        scaled
        - jnp.mean(scaled, axis=-1, keepdims=True)
        - unit * jnp.mean(scaled * unit, axis=-1, keepdims=True)
    )


def rounded(values):
    return values.astype(BF).astype(F32)


def low_onehot(low):
    place = lax.broadcasted_iota(jnp.int32, (LOW, 1), 0).astype(F32).astype(BF)
    hit = jnp.broadcast_to(place, (LOW, low.shape[1])) == low.astype(F32).astype(BF)
    return jnp.where(hit, jnp.array(1, BF), jnp.array(0, BF))


def bias_kernel(table_ref, index_ref, regions_ref, main_ref, tail_ref, part_ref, last_ref, turned_ref, mask_ref, region_ref, sem):
    copy = pltpu.make_async_copy(regions_ref, region_ref, sem)
    copy.start()
    for high in range(HIGH):
        width = min(LOW, BPOS - high * LOW)
        for head in range(HEADS):
            piece = table_ref[head, :, high * LOW : high * LOW + width]
            if width < LOW:
                piece = jnp.concatenate([piece, jnp.zeros((TYPES, LOW - width), F32)], axis=1)
            row = high * TH + head * TYPES
            part_ref[row : row + TYPES, :] = piece
    turned_ref[...] = jnp.transpose(index_ref[:, MAIN:])
    parts = part_ref[...].astype(BF)

    def looked_up(index):
        low = low_onehot(index & (LOW - 1))
        high_row = index >> 8
        found = dot(parts, low)
        chosen = found[0:TH]
        for high in range(1, HIGH):
            chosen = jnp.where(high_row == high, found[high * TH : (high + 1) * TH], chosen)
        return chosen

    for start in range(0, REST, 4):
        got = looked_up(jnp.concatenate([turned_ref[start + n : start + n + 1, :MAIN] for n in range(4)], axis=1))
        for n in range(4):
            last_ref[pl.ds(start + n, TH, stride=REST), :] = got[:, n * MAIN : (n + 1) * MAIN]
    got = looked_up(jnp.concatenate([turned_ref[n : n + 1, MAIN:] for n in range(REST)], axis=1))
    for n in range(REST):
        half = got[:, LANES * (n // 8) : LANES * (n // 8 + 1)]
        half = half if n % 8 == 0 else pltpu.roll(half, LANES - REST * (n % 8), 1)
        last_ref[pl.ds(TH * REST + n, TH, stride=REST), :] = half
    copy.wait()
    kind_of = lax.broadcasted_iota(jnp.int32, (TH, 1), 0) & (TYPES - 1)
    column = lax.broadcasted_iota(jnp.int32, (1, LANES), 1)
    labels = []
    for group in range(12):
        label = jnp.zeros((TH, 1), jnp.int32)
        for kind in range(TYPES):
            label = jnp.where(kind_of == kind, region_ref[group // 6, 6 * kind + group % 6], label)
        labels.append(label)
    keys = jnp.zeros((TH, LANES), jnp.int32)
    for group in range(11):
        keys = jnp.where((column >= 12 * group) & (column < 12 * group + 12), labels[group], keys)
    for group in range(12):
        mask_ref[TH * group : TH * (group + 1), :] = jnp.where(keys == labels[group], 0.0, MASKED)

    def row_block(block, carry):
        base = pl.multiple_of(block * 8, 8)
        rows = index_ref[pl.ds(base, 8), :MAIN]
        for part in range(2):
            index = jnp.concatenate([rows[4 * part + n : 4 * part + n + 1] for n in range(4)], axis=1)
            got = looked_up(index)
            for n in range(4):
                row = base + 4 * part + n
                mask = mask_ref[pl.ds(pl.multiple_of(div(row, 12) * TH, 8), TH), :]
                main_ref[pl.ds(row, TH, stride=WIN), :] = got[:, n * MAIN : (n + 1) * MAIN] + mask
        return carry

    lax.fori_loop(0, WIN // 8, row_block, 0, unroll=True)
    apart = jnp.where(labels[10] == labels[11], 0.0, MASKED)
    split = 132 - MAIN
    for n in range(REST):
        group = (MAIN + n) // 12
        rows = pl.ds(n, TH, stride=REST)
        last_ref[rows, :] = last_ref[rows, :] + mask_ref[TH * group : TH * (group + 1), :]
        rows = pl.ds(TH * REST + n, TH, stride=REST)
        other = (column < split) if n >= split else (column >= split)
        last_ref[rows, :] = last_ref[rows, :] + jnp.where(other, apart, 0.0)
    for th in range(TH):
        rows = slice(th * WIN, th * WIN + MAIN)
        tail_ref[rows, :REST] = jnp.transpose(last_ref[th * REST : (th + 1) * REST, :])
        rows = slice(th * WIN + MAIN, (th + 1) * WIN)
        tail_ref[rows, :REST] = jnp.transpose(last_ref[(TH + th) * REST : (TH + th + 1) * REST, :])[:REST]


def stage_kernel(fields_ref, cotangent_ref, table_ref, index_ref, gain_ref, field_ref, half_ref, table_out, index_out, gain_out, sems):
    copies = [
        pltpu.make_async_copy(source, target, sems.at[n])
        for n, (source, target) in enumerate(
            [
                (fields_ref.at[:, HALF:], field_ref),
                (cotangent_ref.at[:, HALF // 2 :], half_ref),
                (table_ref, table_out),
                (index_ref, index_out),
                (gain_ref, gain_out.at[0]),
            ]
        )
    ]
    for copy in copies:
        copy.start()
    for copy in copies:
        copy.wait()


def stage(fields, cotangent, table, index, gain):
    shape = jax.ShapeDtypeStruct
    whole = pl.BlockSpec(memory_space=pltpu.VMEM)
    return pl.pallas_call(
        stage_kernel,
        out_shape=[
            shape((LEVELS, HALF, LAT, C), BF),
            shape((12, HALF // 2, LEVELS, 2 * C), BF),
            shape(table.shape, F32),
            shape(index.shape, jnp.int32),
            shape((1, 4 * C), F32),
        ],
        in_specs=[pl.BlockSpec(memory_space=pltpu.HBM)] * 5,
        out_specs=[whole] * 5,
        scratch_shapes=[pltpu.SemaphoreType.DMA((5,))],
        compiler_params=pltpu.CompilerParams(vmem_limit_bytes=4 * 1024 * 1024),
        name="stage",
    )(*(pltpu.with_memory_space_constraint(a, pltpu.HBM) for a in (fields, cotangent, table, index, gain)))


def bias_rows(table, index, regions):
    whole = pl.BlockSpec(memory_space=pltpu.VMEM)
    return pl.pallas_call(
        bias_kernel,
        out_shape=[jax.ShapeDtypeStruct((TH * WIN, LANES), F32)] * 2,
        in_specs=[whole, whole, pl.BlockSpec(memory_space=pltpu.HBM)],
        out_specs=[whole, whole],
        scratch_shapes=[
            pltpu.VMEM((HIGH * TH, LOW), F32),
            pltpu.VMEM((2 * TH * REST, LANES), F32),
            pltpu.VMEM((REST, WIN), jnp.int32),
            pltpu.VMEM((12 * TH, LANES), F32),
            pltpu.SMEM((LEVELS, LAT), jnp.int32),
            pltpu.SemaphoreType.DMA,
        ],
        compiler_params=pltpu.CompilerParams(vmem_limit_bytes=16 * 1024 * 1024),
        cost_estimate=pl.CostEstimate(flops=14_000_000_000, bytes_accessed=4_000_000, transcendentals=0),
        name="bias_rows",
    )(table, index, pltpu.with_memory_space_constraint(regions, pltpu.HBM))


def block_kernel(
    core_ref, own_ref, west_ref, own_cotangent_ref, west_cotangent_ref,
    norm_gain_ref, qkv_ref, proj_ref, mlp_gain_ref, up_ref, down_ref, merge_gain_ref, merge_ref,
    bias_ref, bias_tail_ref, index_ref,
    keep_ref, send_ref, normed_merge_ref, triple_ref, grad_attn_ref, unit_ref, scale_ref,
    x_ref, tokens_ref, q_ref, k_ref, v_ref, p_ref, mixed_ref,
    unit_mlp_ref, scale_mlp_ref, normed_mlp_ref, hidden_ref, slope_ref, after_mlp_ref,
    group_ref, grad_after_ref, grad_up_ref, grad_mixed_ref,
    ds_ref, ds_tail_ref, ds_corner_ref, grads_ref, turned_ref, cells_ref, grad_merged_ref, scaled_ref,
):
    to_tokens = onehot(288, 288, of_row=cell_of_token)
    for level in range(LEVELS):
        cells = jnp.concatenate(
            [
                west_ref[level].astype(F32).reshape(144, C),
                own_ref[level, :HALF].astype(F32).reshape(144, C),
            ],
            axis=0,
        ).astype(BF)
        ordered = dot(to_tokens, cells)
        for kind in range(TYPES):
            x_ref[WIN * kind + 72 * level : WIN * kind + 72 * level + 72, :] = ordered[72 * kind : 72 * kind + 72]
    unit, scale = normalised(x_ref[...])
    unit_ref[...] = unit
    scale_ref[...] = scale
    tokens = (unit * norm_gain_ref[...]).astype(BF)
    tokens_ref[...] = tokens
    q_ref[...] = dot(tokens, qkv_ref[:, 0:C]).astype(BF)
    k_ref[...] = dot(tokens, qkv_ref[:, C : 2 * C]).astype(BF)
    v_ref[...] = dot(tokens, qkv_ref[:, 2 * C :]).astype(BF)
    for lat in range(12):
        for lon in range(HALF // 2):
            row = (lat * 3 + lon) * 2
            cells_ref[row : row + 2, :] = west_cotangent_ref[lat, lon].astype(F32)
            cells_ref[72 + row : 74 + row, :] = own_cotangent_ref[lat, lon].astype(F32)
    grad_merged_ref[...] = dot(onehot(MTOK, 144, of_row=cell_of_merged), cells_ref[...].astype(BF)).astype(BF)
    for n in range(4):
        value = rounded(dot_nt(grad_merged_ref[...], merge_ref[C * n : C * (n + 1), :]))
        scaled_ref[n] = value * merge_gain_ref[:, C * n : C * (n + 1)]
    lane = lax.broadcasted_iota(jnp.int32, (1, C), 1)
    of_head = [
        jnp.where((lane >= HEAD * h) & (lane < HEAD * (h + 1)), 1.0, 0.0).astype(BF) for h in range(HEADS)
    ]
    temper = HEAD ** (-0.5)

    def attend(kind, carry):
        rows = pl.ds(pl.multiple_of(kind * WIN, 16), WIN)
        q, k, v = q_ref[rows, :], k_ref[rows, :], v_ref[rows, :]
        mixed = jnp.zeros((WIN, C), F32)
        products = dot_nt(jnp.concatenate([q * of_head[h] for h in range(HEADS)], axis=0), k)
        for h in range(HEADS):
            th = h * TYPES + kind
            scores_at = pl.ds(pl.multiple_of(th * WIN, 16), WIN)
            bias = jnp.concatenate([bias_ref[scores_at, :], bias_tail_ref[scores_at, :REST]], axis=1)
            scores = products[WIN * h : WIN * (h + 1)] * temper + bias
            weights = jnp.exp(scores - jnp.max(scores, axis=-1, keepdims=True))
            p = weights * (1.0 / jnp.sum(weights, axis=-1, keepdims=True))
            p_ref[th] = p
            mixed = mixed + dot(p.astype(BF), v * of_head[h])
        mixed_ref[rows, :] = mixed.astype(BF)
        return carry

    lax.fori_loop(0, TYPES, attend, 0, unroll=True)
    after_attn = rounded(x_ref[...] + rounded(dot(mixed_ref[...], proj_ref[...])))
    x_ref[...] = after_attn
    unit, scale = normalised(after_attn)
    unit_mlp_ref[...] = unit
    scale_mlp_ref[...] = scale
    normed_mlp = (unit * mlp_gain_ref[...]).astype(BF)
    normed_mlp_ref[...] = normed_mlp
    for part in range(3):
        cols = slice(256 * part, 256 * part + 256)
        u = dot(normed_mlp, up_ref[:, cols])
        below = 0.5 * (1.0 + lax.erf(u * 0.5**0.5))
        hidden_ref[:, cols] = (u * below).astype(BF)
        slope_ref[:, cols] = below + u * (jnp.exp(u * u * (-0.5)) * 0.3989422804014327)
    after_mlp_ref[...] = (x_ref[...] + dot_nt(hidden_ref[...], down_ref[...])).astype(BF)

    to_groups = onehot(160, WIN, of_row=token_of_group)
    for kind in range(TYPES):
        grouped = dot(to_groups, after_mlp_ref[WIN * kind : WIN * kind + WIN, :])
        for quarter in range(4):
            group_ref[quarter, 40 * kind : 40 * kind + 40, :] = grouped[40 * quarter : 40 * quarter + 40]
    quarters = [group_ref[n] for n in range(4)]
    mean = sum(jnp.sum(v, axis=-1, keepdims=True) for v in quarters) * (1.0 / MLP)
    centred = [v - mean for v in quarters]
    variance = sum(jnp.sum(v * v, axis=-1, keepdims=True) for v in centred) * (1.0 / MLP)
    scale_merge = lax.rsqrt(variance + EPS)
    for n in range(4):
        unit = centred[n] * scale_merge
        group_ref[n] = unit
        normed_merge = (unit * merge_gain_ref[:, C * n : C * (n + 1)]).astype(BF)
        normed_merge_ref[n] = normed_merge
    scaled, total, along = [], 0.0, 0.0
    for n in range(4):
        value = scaled_ref[n]
        total = total + jnp.sum(value, axis=-1, keepdims=True)
        along = along + jnp.sum(value * group_ref[n], axis=-1, keepdims=True)
        scaled.append(value)
    total = total * (1.0 / MLP)
    along = along * (1.0 / MLP)
    for n in range(4):
        group_ref[n] = scale_merge * (scaled[n] - total - group_ref[n] * along)
    from_groups = onehot(WIN, 160, of_row=group_of_token)
    for kind in range(TYPES):
        grouped = jnp.concatenate([group_ref[n, 40 * kind : 40 * kind + 40, :] for n in range(4)], axis=0)
        grad_after_ref[WIN * kind : WIN * kind + WIN, :] = dot(from_groups, grouped.astype(BF)).astype(BF)

    grad_after = grad_after_ref[...]
    for part in range(3):
        cols = slice(256 * part, 256 * part + 256)
        grad_up_ref[:, cols] = (rounded(dot(grad_after, down_ref[:, cols])) * slope_ref[:, cols]).astype(BF)
    grad_normed = rounded(dot_nt(grad_up_ref[...], up_ref[...]))
    grad_attn = (
        grad_after.astype(F32)
        + norm_grad(grad_normed, unit_mlp_ref[...], scale_mlp_ref[...], mlp_gain_ref[...])
    ).astype(BF)
    grad_attn_ref[...] = grad_attn

    grad_mixed_ref[...] = dot_nt(grad_attn, proj_ref[...]).astype(BF)

    def down_terms():
        grad = dot_tn(grad_after_ref[...], hidden_ref[...]).astype(BF)
        for b in range(6):
            grads_ref[O_DOWN + C * b : O_DOWN + C * (b + 1), :] = grad[:, 128 * b : 128 * b + 128]

    def up_terms():
        grad = dot_tn(normed_mlp_ref[...], grad_up_ref[...]).astype(BF)
        for b in range(6):
            grads_ref[O_UP + C * b : O_UP + C * (b + 1), :] = grad[:, 128 * b : 128 * b + 128]

    def merge_terms():
        for n in range(4):
            grad = dot_tn(normed_merge_ref[n], grad_merged_ref[...]).astype(BF)
            for b in range(3):
                start = O_MERGE + MLP * b + C * n
                grads_ref[start : start + C, :] = grad[:, 128 * b : 128 * b + 128]

    def proj_terms():
        grad_proj = dot_tn(mixed_ref[...], grad_attn_ref[...]).astype(BF)
        grads_ref[O_PROJ : O_PROJ + C, :] = grad_proj[:, :128]
        grads_ref[O_PROJ_TAIL : O_PROJ_TAIL + C // 2, :] = jnp.concatenate(
            [grad_proj[: C // 2, 128:], grad_proj[C // 2 :, 128:]], axis=1
        )

    last_keys = onehot(REST, WIN, of_row=lambda n: n + MAIN)

    def attend_back(kind, carry):
        rows = pl.ds(kind * WIN, WIN)
        v, grad = v_ref[rows, :], grad_mixed_ref[rows, :]
        q_turned, k_turned, grad_turned = (jnp.transpose(a) for a in (q_ref[rows, :], k_ref[rows, :], grad))
        products = dot_nt(jnp.concatenate([grad * of_head[h] for h in range(HEADS)], axis=0), v)
        dq, dk, dv = [], [], []
        for h in range(HEADS):
            th = h * TYPES + kind
            lanes = slice(HEAD * h, HEAD * (h + 1))
            p = p_ref[th]
            weighted = p * products[WIN * h : WIN * (h + 1)]
            ds = weighted - p * jnp.sum(weighted, axis=-1, keepdims=True)
            ds_ref[pl.ds(th * WIN, WIN), :] = ds[:, :MAIN]
            ds = ds.astype(BF)
            turned = dot_nt(jnp.concatenate([k_turned[lanes], last_keys], axis=0), ds)
            at = pl.ds(th * REST, REST)
            ds_tail_ref[at, :] = turned[HEAD:, :MAIN]
            ds_corner_ref[at, :REST] = turned[HEAD:, MAIN:]
            dq.append(turned[:HEAD])
            dk.append(dot(q_turned[lanes], ds))
            dv.append(dot(grad_turned[lanes], p.astype(BF)))
        triple = jnp.concatenate([a * temper for a in dq + dk] + dv, axis=0).astype(BF)
        triple_ref[rows, :] = jnp.transpose(triple)
        return carry

    for kind, terms in enumerate((down_terms, up_terms, merge_terms, proj_terms)):
        attend_back(kind, 0)
        terms()
    grad_triple = triple_ref[...]
    grad_qkv = dot_tn(tokens_ref[...], grad_triple).astype(BF)
    for b in range(4):
        grads_ref[O_QKV + C * b : O_QKV + C * (b + 1), :] = grad_qkv[:, 128 * b : 128 * b + 128]
    grads_ref[O_QKV_TAIL : O_QKV_TAIL + C // 2, :] = jnp.concatenate(
        [grad_qkv[: C // 2, 512:], grad_qkv[C // 2 :, 512:]], axis=1
    )
    turned_ref[...] = jnp.transpose(index_ref[:, MAIN:])

    def table_terms(index, slab):
        high_row = index >> 8
        spread = [jnp.where(high_row == n, slab, 0.0) for n in range(HIGH)]
        spread.append(jnp.zeros((TROWS - HIGH * TH, index.shape[1]), F32))
        return dot_nt(jnp.concatenate(spread, axis=0).astype(BF), low_onehot(index & (LOW - 1)))

    def row_block(block, carry):
        base = pl.multiple_of(block * 8, 8)
        rows = index_ref[pl.ds(base, 8), :MAIN]
        index = jnp.concatenate([rows[n : n + 1] for n in range(8)], axis=1)
        slab = jnp.concatenate([ds_ref[pl.ds(base + n, TH, stride=WIN), :] for n in range(8)], axis=1)
        return carry + table_terms(index, slab)

    table = lax.fori_loop(0, WIN // 8, row_block, jnp.zeros((TROWS, LOW), F32), unroll=9)
    index = jnp.concatenate([turned_ref[n : n + 1, :MAIN] for n in range(REST)], axis=1)
    slab = jnp.concatenate([ds_tail_ref[pl.ds(n, TH, stride=REST), :] for n in range(REST)], axis=1)
    table = table + table_terms(index, slab)
    index = jnp.concatenate([turned_ref[n : n + 1, MAIN:] for n in range(REST)], axis=1)
    slab = jnp.concatenate([ds_corner_ref[pl.ds(n, TH, stride=REST), :][:, :REST] for n in range(REST)], axis=1)
    table = table + table_terms(index, slab)
    table = table.astype(BF)
    grads_ref[O_TABLE : O_TABLE + TROWS, :] = table[:, :LANES]
    grads_ref[O_TABLE + TROWS : O_END, :] = table[:TLAST, LANES:]
    grads_ref[O_LAST : O_LAST + TROWS - TLAST, :] = table[TLAST:, LANES:]
    half = keep_ref.shape[0]
    if 2 * half > O_END:
        grads_ref[O_END:, :] = jnp.zeros((2 * half - O_END, LANES), BF)
    core = core_ref[0]
    keep_ref[...] = grads_ref[pl.ds(pl.multiple_of(core * half, 16), half), :]
    send_ref[...] = grads_ref[pl.ds(pl.multiple_of((1 - core) * half, 16), half), :]


def block(half_rows, *args):
    shape = jax.ShapeDtypeStruct
    whole = pl.BlockSpec(memory_space=pltpu.VMEM)
    scratch = [
        ((TOK, C), F32), ((TOK, C), BF), ((TOK, C), BF), ((TOK, C), BF),
        ((TOK, C), BF), ((TH, WIN, WIN), F32), ((TOK, C), BF),
        ((TOK, C), F32), ((TOK, 1), F32), ((TOK, C), BF), ((TOK, MLP), BF), ((TOK, MLP), F32), ((TOK, C), BF),
        ((4, MTOK, C), F32), ((TOK, C), BF), ((TOK, MLP), BF), ((TOK, C), BF),
        ((TH * WIN, LANES), F32), ((TH * REST, LANES), F32), ((TH * REST, LANES), F32),
        ((2 * half_rows, LANES), BF), ((REST, WIN), jnp.int32),
        ((144, 2 * C), F32), ((MTOK, 2 * C), BF), ((4, MTOK, C), F32),
    ]
    return pl.pallas_call(
        block_kernel,
        out_shape=[
            shape((half_rows, LANES), BF),
            shape((half_rows, LANES), BF),
            shape((4, MTOK, C), BF),
            shape((TOK, 3 * C), BF),
            shape((TOK, C), BF),
            shape((TOK, C), F32),
            shape((TOK, 1), F32),
        ],
        in_specs=[pl.BlockSpec(memory_space=pltpu.SMEM)] + [whole] * (len(args) - 1),
        out_specs=[whole] * 7,
        scratch_shapes=[pltpu.VMEM(*item) for item in scratch],
        compiler_params=pltpu.CompilerParams(vmem_limit_bytes=24 * 1024 * 1024),
        cost_estimate=pl.CostEstimate(flops=24_000_000_000, bytes_accessed=12_000_000, transcendentals=2_000_000),
        name="block",
    )(*args)


def cells_kernel(
    normed_merge_ref, triple_ref, grad_attn_ref, unit_ref, scale_ref, qkv_ref, gain_ref, merge_ref,
    merged_keep_ref, field_keep_ref, home_ref, x_ref,
):
    grad_normed = rounded(dot_nt(triple_ref[...], qkv_ref[...]))
    x_ref[...] = grad_attn_ref[...].astype(F32) + norm_grad(
        grad_normed, unit_ref[...], scale_ref[...], gain_ref[...]
    )
    to_cells = onehot(288, 288, of_col=cell_of_token)
    leaving = []
    for level in range(LEVELS):
        ordered = jnp.concatenate(
            [x_ref[WIN * kind + 72 * level : WIN * kind + 72 * level + 72, :] for kind in range(TYPES)], axis=0
        )
        cells = dot(to_cells, ordered.astype(BF))
        leaving.append(cells[:144])
        field_keep_ref[level] = cells[144:].reshape(HALF, LAT, C).astype(BF)
    home_ref[:HALF] = jnp.concatenate(leaving, axis=1).reshape(HALF, LAT, 2 * C).astype(BF)
    merged = sum(dot(normed_merge_ref[n], merge_ref[C * n : C * (n + 1), :]) for n in range(4))
    merged_cells = dot(onehot(144, MTOK, of_col=cell_of_merged), merged.astype(BF))
    for lat in range(12):
        for lon in range(HALF // 2):
            row = 72 + (lat * 3 + lon) * 2
            merged_keep_ref[lat, lon] = merged_cells[row : row + 2].astype(BF)
    home_ref[HALF:] = merged_cells[:72].reshape(3, LAT, 2 * C).astype(BF)


def to_grid(*args):
    shape = jax.ShapeDtypeStruct
    whole = pl.BlockSpec(memory_space=pltpu.VMEM)
    return pl.pallas_call(
        cells_kernel,
        out_shape=[
            shape((12, HALF // 2, LEVELS, 2 * C), BF),
            shape((LEVELS, HALF, LAT, C), BF),
            shape((HALF + 3, LAT, 2 * C), BF),
        ],
        in_specs=[whole] * 8,
        out_specs=[whole] * 3,
        scratch_shapes=[pltpu.VMEM((TOK, C), F32)],
        compiler_params=pltpu.CompilerParams(vmem_limit_bytes=12 * 1024 * 1024),
        cost_estimate=pl.CostEstimate(flops=1_500_000_000, bytes_accessed=3_000_000, transcendentals=0),
        name="to_grid",
    )(*args)


def first_half(part, refs, staged, sems):
    _, _, up_ref, down_ref, qkv_ref, _, _, table_ref = refs
    up, down, qkv, _, _, table = staged
    copies = []

    def leaves(source, target):
        copies.append(pltpu.make_async_copy(source, target, sems.at[len(copies)]))
        copies[-1].start()

    for b in range(6):
        up[:, 128 * b : 128 * b + 128] = part(O_UP + C * b, C)
    leaves(up, up_ref)
    for b in range(6):
        down[:, 128 * b : 128 * b + 128] = part(O_DOWN + C * b, C)
    leaves(down, down_ref)
    for b in range(4):
        qkv[:, 128 * b : 128 * b + 128] = part(O_QKV + C * b, C)
    tail = part(O_QKV_TAIL, C // 2)
    qkv[: C // 2, 512:] = tail[:, :64]
    qkv[C // 2 :, 512:] = tail[:, 64:]
    leaves(qkv, qkv_ref)
    last = part(O_LAST, TROWS - TLAST)
    width = BPOS - LAST
    for head in range(HEADS):
        table[head, :, LAST:] = last[head * TYPES : (head + 1) * TYPES, :width]
    leaves(table.at[:, :, LAST:], table_ref.at[:, :, LAST:])
    for copy in copies:
        copy.wait()


def second_half(part, refs, staged, sems):
    _, _, _, _, _, merge_ref, proj_ref, table_ref = refs
    _, _, _, merge, proj, table = staged
    copies = []

    def leaves(source, target):
        copies.append(pltpu.make_async_copy(source, target, sems.at[len(copies)]))
        copies[-1].start()

    for b in range(3):
        merge[:, 128 * b : 128 * b + 128] = part(O_MERGE + MLP * b, MLP)
    leaves(merge, merge_ref)
    proj[:, :128] = part(O_PROJ, C)
    tail = part(O_PROJ_TAIL, C // 2)
    proj[: C // 2, 128:] = tail[:, :64]
    proj[C // 2 :, 128:] = tail[:, 64:]
    leaves(proj, proj_ref)
    for side in range(2):
        terms = part(O_TABLE + TROWS * side, TLAST if side else TROWS)
        for high in range(HIGH - side):
            start = high * LOW + side * LANES
            for head in range(HEADS):
                row = high * TH + head * TYPES
                table[head, :, start : start + LANES] = terms[row : row + TYPES]
    leaves(table.at[:, :, :LAST], table_ref.at[:, :, :LAST])
    for copy in copies:
        copy.wait()


def half_kernel(factor, own, core_ref, sums_ref, *refs):
    if own:
        outs, scratch = (None, None, *refs[:6]), refs[6:]
    else:
        partner_ref, forwarded_ref, merged_keep_ref, field_keep_ref = refs[:4]
        outs, scratch = refs[10:18], refs[18:]
    staged, sems = scratch[:6], scratch[6]
    core = core_ref[0]
    half = core if own else 1 - core
    copies = []
    if not own:
        merged, field = scratch[7:9]
        east = jnp.where(core == 0, partner_ref[...].astype(F32), forwarded_ref[...].astype(F32))
        for level in range(LEVELS):
            field[level, HALF:] = east[:HALF, :, C * level : C * (level + 1)].astype(BF)
        field[:, :HALF] = field_keep_ref[...]
        copies.append(pltpu.make_async_copy(field, outs[1], sems.at[4]))
        copies[-1].start()
        cells = east[HALF:].reshape(72, 2 * C)
        for lat in range(12):
            for lon in range(HALF // 2):
                row = (lat * 3 + lon) * 2
                merged[lat, HALF // 2 + lon] = cells[row : row + 2].astype(BF)
        merged[:, : HALF // 2] = merged_keep_ref[...]
        copies.append(pltpu.make_async_copy(merged, outs[0], sems.at[5]))
        copies[-1].start()

    def part_of(base):
        return lambda start, rows: sums_ref[start - base : start - base + rows, :].astype(F32) * factor

    @pl.when(half == 0)
    def _():
        first_half(part_of(0), outs, staged, sems)

    @pl.when(half == 1)
    def _():
        second_half(part_of(O_MERGE), outs, staged, sems)

    for copy in copies:
        copy.wait()


def finish(core, held, other, cells, factor):
    shape = jax.ShapeDtypeStruct
    whole = pl.BlockSpec(memory_space=pltpu.VMEM)
    scalar = pl.BlockSpec(memory_space=pltpu.SMEM)
    place = pl.BlockSpec(memory_space=pl.ANY)
    sums = [
        shape((C, MLP), F32),
        shape((C, MLP), F32),
        shape((C, 3 * C), F32),
        shape((MLP, 2 * C), F32),
        shape((C, C), F32),
        shape((HEADS, TYPES, BPOS), F32),
    ]
    scratch = [pltpu.VMEM(item.shape, F32) for item in sums] + [pltpu.SemaphoreType.DMA((6,))]
    grid = [shape((12, HALF, LEVELS, 2 * C), BF), shape((LEVELS, 2 * HALF, LAT, C), BF)]
    params = pltpu.CompilerParams(vmem_limit_bytes=16 * 1024 * 1024)
    begun = pl.pallas_call(
        lambda *refs: half_kernel(factor, True, *refs),
        out_shape=sums,
        in_specs=[scalar, whole],
        out_specs=[place] * 6,
        scratch_shapes=scratch,
        compiler_params=params,
        cost_estimate=pl.CostEstimate(flops=400_000, bytes_accessed=2_500_000, transcendentals=0),
        name="finish_own",
    )(core, held)
    return pl.pallas_call(
        lambda *refs: half_kernel(factor, False, *refs),
        out_shape=[*grid, *sums],
        in_specs=[scalar] + [whole] * 5 + [place] * 6,
        out_specs=[place] * 8,
        scratch_shapes=scratch + [pltpu.VMEM(item.shape, BF) for item in grid],
        input_output_aliases={6 + n: 2 + n for n in range(6)},
        compiler_params=params,
        name="finish_other",
    )(core, other, *cells, *begun)


def passed_along(value, axis, steps):
    count = lax.axis_size(axis)
    return lax.ppermute(value, axis, [(source, (source + steps) % count) for source in range(count)])


def groups_of(count, apart, size):
    return [
        [start * apart * size + offset + member * apart for member in range(size)]
        for start in range(count // (apart * size))
        for offset in range(apart)
    ]


def summed_over(keep, send, axis, partner, forward):
    count = lax.axis_size(axis)
    along = count // (CORES * ACROSS)
    pairs = [(i, i ^ 1) for i in range(count)]
    arrived = lax.ppermute(send, axis, pairs)
    held = (keep.astype(F32) + arrived.astype(F32)).astype(BF)

    def exchanged(value, apart, size):
        return lax.all_to_all(value, axis, 0, 0, axis_index_groups=groups_of(count, apart, size))

    def reduced(value, apart, size):
        got = exchanged(value.reshape(size, -1, *value.shape[1:]), apart, size)
        return jnp.sum(got.astype(F32), axis=0).astype(BF)

    def gathered(value, apart, size):
        return exchanged(jnp.broadcast_to(value[None], (size, *value.shape)), apart, size).reshape(-1, *value.shape[1:])

    held = reduced(held, CORES, ACROSS)
    held, partner = lax.optimization_barrier((held, partner))
    held = reduced(held.reshape(-1, 2, LANES), CORES * ACROSS, along)
    held = gathered(held, CORES * ACROSS, along).reshape(-1, LANES)
    held = gathered(held, CORES, ACROSS)
    held, forwarded = forward(held, partner)
    return held, lax.ppermute(held, axis, pairs), partner, forwarded


def local(
    fields,
    norm_gain,
    qkv_weight,
    proj_weight,
    bias_table,
    bias_index,
    region_ids,
    mlp_gain,
    up_weight,
    down_weight,
    merge_gain,
    merge_weight,
    cotangent,
):
    count = lax.axis_size("lon")
    core = (lax.axis_index("lon") % CORES).astype(jnp.int32).reshape(1)
    by_lon = fields.transpose(0, 2, 1, 3)
    by_lat = cotangent.transpose(1, 2, 0, 3)
    field_last, cotangent_last, table, index, merge_gain = stage(
        by_lon, by_lat, bias_table.transpose(1, 0, 2), bias_index, merge_gain
    )
    west = passed_along(field_last, "lon", 1)
    west_cotangent = passed_along(cotangent_last, "lon", 1)
    table, core = lax.optimization_barrier((table, core))
    bias, bias_tail = bias_rows(table, index, region_ids)
    half_rows = -(-O_END // (count * 2)) * 2 * count // CORES
    keep, send, *results = block(
        half_rows,
        core,
        by_lon,
        west,
        by_lat,
        west_cotangent,
        norm_gain.reshape(1, C),
        qkv_weight,
        proj_weight,
        mlp_gain.reshape(1, C),
        up_weight,
        down_weight.T,
        merge_gain,
        merge_weight,
        bias,
        bias_tail,
        index,
    )
    merged_keep, field_keep, home = to_grid(*results, qkv_weight, norm_gain.reshape(1, C), merge_weight)
    partner = lax.ppermute(home, "lon", [(i, i ^ 1) for i in range(count)])

    def forward(held, leaving):
        held, leaving = lax.optimization_barrier((held, leaving))
        return held, lax.ppermute(leaving, "lon", [(i, (i - CORES) % count) for i in range(1, count, CORES)])

    held, other, partner, forwarded = summed_over(keep, send, "lon", partner, forward)
    factor = float(LEVELS * LAT * fields.shape[2] * count) ** (-0.5)
    merged, field_grad, up_grad, down_grad, qkv_grad, merge_grad, proj_grad, table_grad = finish(
        core, held, other, (partner, forwarded, merged_keep, field_keep), factor
    )
    return (
        merged.transpose(2, 0, 1, 3),
        field_grad.transpose(0, 2, 1, 3),
        qkv_grad,
        proj_grad,
        up_grad,
        down_grad.T,
        merge_grad,
        table_grad.transpose(1, 0, 2),
    )


def solution(mesh):
    whole = P("groups", None, "lon", None)

    return jax.shard_map(
        local,
        mesh=mesh,
        in_specs=(whole, *[P()] * 11, whole),
        out_specs=(whole, whole, *[P("groups", None)] * 5, P("groups", None, None)),
        check_vma=False,
    )
```

```python
import jax
import jax.numpy as jnp
from jax import lax
from jax.experimental import pallas as pl
from jax.experimental.pallas import tpu as pltpu
from jax.sharding import PartitionSpec as P

C = 192
MLP = 768
HEADS = 6
HEAD = 32
HALF = 6
WIN = 144
BPOS = 3312
LAT = 24
TYPES = 4
TOK = TYPES * WIN
LEVELS = 2
LANES = 128
MAIN = 128
REST = WIN - MAIN
TH = TYPES * HEADS
LOW = 256
HIGH = -(-BPOS // LOW)
MTOK = 160
EPS = 1e-5
MASKED = -1e30
F32 = jnp.float32
BF = jnp.bfloat16
CORES = 2
ACROSS = 4

TROWS = 320
MSPLIT = 512
O_UP = 0
O_QKV = O_UP + 6 * C
O_QKV_TAIL = O_QKV + 4 * C
O_PROJ = O_QKV_TAIL + C // 2
O_PROJ_TAIL = O_PROJ + C
O_TABLE = O_PROJ_TAIL + C // 2
O_MERGE_LAST = O_TABLE + 2 * TROWS
O_MERGE = O_MERGE_LAST + MLP - MSPLIT
O_DOWN = O_MERGE + 2 * MLP + MSPLIT
O_END = O_DOWN + 6 * C

DS_TAIL = TH * WIN
DS_CORNER = DS_TAIL + TH * REST
DS_END = DS_CORNER + TH * REST


def dot(a, b):
    return jnp.dot(a, b, preferred_element_type=F32)


def dot_nt(a, b):
    return lax.dot_general(a, b, (((1,), (1,)), ((), ())), preferred_element_type=F32)


def dot_tn(a, b):
    return lax.dot_general(a, b, (((0,), (0,)), ((), ())), preferred_element_type=F32)


def div(n, d):
    return (n * -(-(1 << 16) // d)) >> 16


def onehot(rows, cols, of_row=None, of_col=None):
    if of_row is not None:
        target = of_row(lax.broadcasted_iota(jnp.int32, (rows, 1), 0))
        place = lax.broadcasted_iota(jnp.int32, (rows, cols), 1)
    else:
        target = of_col(lax.broadcasted_iota(jnp.int32, (1, cols), 1))
        place = lax.broadcasted_iota(jnp.int32, (rows, cols), 0)
    return jnp.where(place == target, 1.0, 0.0).astype(BF)


def cell_of_token(n):
    kind = div(n, 72)
    rest = n - 72 * kind
    lat = div(rest, 12)
    return (rest - 12 * lat) * LAT + kind * 6 + lat


def token_of_group(n):
    quarter = div(n, 40)
    rest = n - 40 * quarter
    level = div(rest, 18)
    part = rest - 18 * level
    lat = div(part, 6)
    token = level * 72 + (2 * lat + (quarter >> 1)) * 12 + 2 * (part - 6 * lat) + (quarter & 1)
    return jnp.where(rest < 36, token, -1)


def group_of_token(n):
    level = div(n, 72)
    rest = n - 72 * level
    lat = div(rest, 12)
    lon = rest - 12 * lat
    return ((lat & 1) * 2 + (lon & 1)) * 40 + level * 18 + (lat >> 1) * 6 + (lon >> 1)


def cell_of_merged(n):
    kind = div(n, 40)
    rest = n - 40 * kind
    level = div(rest, 18)
    part = rest - 18 * level
    lat = div(part, 6)
    lon = part - 6 * lat
    half = jnp.where(lon < 3, 0, 1)
    row = half * 72 + (3 * kind + lat) * 6 + (lon - 3 * half) * 2 + level
    return jnp.where(rest < 36, row, -1)


def normalised(values):
    centred = values - jnp.mean(values, axis=-1, keepdims=True)
    scale = lax.rsqrt(jnp.mean(centred * centred, axis=-1, keepdims=True) + EPS)
    return centred * scale, scale


def norm_grad(grad, unit, scale, gain):
    scaled = grad * gain
    return scale * (
        scaled
        - jnp.mean(scaled, axis=-1, keepdims=True)
        - unit * jnp.mean(scaled * unit, axis=-1, keepdims=True)
    )


def rounded(values):
    return values.astype(BF).astype(F32)


def low_onehot(low):
    place = lax.broadcasted_iota(jnp.int32, (LOW, 1), 0).astype(F32).astype(BF)
    hit = jnp.broadcast_to(place, (LOW, low.shape[1])) == low.astype(F32).astype(BF)
    return jnp.where(hit, jnp.array(1, BF), jnp.array(0, BF))


def bias_kernel(table_ref, index_ref, regions_ref, main_ref, tail_ref, part_ref, last_ref, turned_ref, mask_ref, region_ref, sem):
    copy = pltpu.make_async_copy(regions_ref, region_ref, sem)
    copy.start()
    for high in range(HIGH):
        width = min(LOW, BPOS - high * LOW)
        for head in range(HEADS):
            piece = table_ref[head, :, high * LOW : high * LOW + width]
            if width < LOW:
                piece = jnp.concatenate([piece, jnp.zeros((TYPES, LOW - width), F32)], axis=1)
            row = high * TH + head * TYPES
            part_ref[row : row + TYPES, :] = piece
    turned_ref[...] = jnp.transpose(index_ref[:, MAIN:])
    parts = part_ref[...].astype(BF)

    def looked_up(index):
        low = low_onehot(index & (LOW - 1))
        high_row = index >> 8
        found = dot(parts, low)
        chosen = found[0:TH]
        for high in range(1, HIGH):
            chosen = jnp.where(high_row == high, found[high * TH : (high + 1) * TH], chosen)
        return chosen

    for start in range(0, REST, 4):
        got = looked_up(jnp.concatenate([turned_ref[start + n : start + n + 1, :MAIN] for n in range(4)], axis=1))
        for n in range(4):
            last_ref[pl.ds(start + n, TH, stride=REST), :] = got[:, n * MAIN : (n + 1) * MAIN]
    got = looked_up(jnp.concatenate([turned_ref[n : n + 1, MAIN:] for n in range(REST)], axis=1))
    for n in range(REST):
        half = got[:, LANES * (n // 8) : LANES * (n // 8 + 1)]
        half = half if n % 8 == 0 else pltpu.roll(half, LANES - REST * (n % 8), 1)
        last_ref[pl.ds(TH * REST + n, TH, stride=REST), :] = half
    copy.wait()
    kind_of = lax.broadcasted_iota(jnp.int32, (TH, 1), 0) & (TYPES - 1)
    column = lax.broadcasted_iota(jnp.int32, (1, LANES), 1)
    labels = []
    for group in range(12):
        label = jnp.zeros((TH, 1), jnp.int32)
        for kind in range(TYPES):
            label = jnp.where(kind_of == kind, region_ref[group // 6, 6 * kind + group % 6], label)
        labels.append(label)
    keys = jnp.zeros((TH, LANES), jnp.int32)
    for group in range(11):
        keys = jnp.where((column >= 12 * group) & (column < 12 * group + 12), labels[group], keys)
    for group in range(12):
        mask_ref[TH * group : TH * (group + 1), :] = jnp.where(keys == labels[group], 0.0, MASKED)

    def row_block(block, carry):
        base = pl.multiple_of(block * 8, 8)
        rows = index_ref[pl.ds(base, 8), :MAIN]
        for part in range(2):
            index = jnp.concatenate([rows[4 * part + n : 4 * part + n + 1] for n in range(4)], axis=1)
            got = looked_up(index)
            for n in range(4):
                row = base + 4 * part + n
                mask = mask_ref[pl.ds(pl.multiple_of(div(row, 12) * TH, 8), TH), :]
                main_ref[pl.ds(row, TH, stride=WIN), :] = got[:, n * MAIN : (n + 1) * MAIN] + mask
        return carry

    lax.fori_loop(0, WIN // 8, row_block, 0, unroll=True)
    apart = jnp.where(labels[10] == labels[11], 0.0, MASKED)
    split = 132 - MAIN
    for n in range(REST):
        group = (MAIN + n) // 12
        rows = pl.ds(n, TH, stride=REST)
        last_ref[rows, :] = last_ref[rows, :] + mask_ref[TH * group : TH * (group + 1), :]
        rows = pl.ds(TH * REST + n, TH, stride=REST)
        other = (column < split) if n >= split else (column >= split)
        last_ref[rows, :] = last_ref[rows, :] + jnp.where(other, apart, 0.0)
    for th in range(TH):
        rows = slice(th * WIN, th * WIN + MAIN)
        tail_ref[rows, :REST] = jnp.transpose(last_ref[th * REST : (th + 1) * REST, :])
        rows = slice(th * WIN + MAIN, (th + 1) * WIN)
        tail_ref[rows, :REST] = jnp.transpose(last_ref[(TH + th) * REST : (TH + th + 1) * REST, :])[:REST]


def stage_kernel(fields_ref, cotangent_ref, table_ref, index_ref, gain_ref, field_ref, half_ref, table_out, index_out, gain_out, sems):
    copies = [
        pltpu.make_async_copy(source, target, sems.at[n])
        for n, (source, target) in enumerate(
            [
                (fields_ref.at[:, HALF:], field_ref),
                (cotangent_ref.at[:, HALF // 2 :], half_ref),
                (table_ref, table_out),
                (index_ref, index_out),
                (gain_ref, gain_out.at[0]),
            ]
        )
    ]
    for copy in copies:
        copy.start()
    for copy in copies:
        copy.wait()


def stage(fields, cotangent, table, index, gain):
    shape = jax.ShapeDtypeStruct
    whole = pl.BlockSpec(memory_space=pltpu.VMEM)
    return pl.pallas_call(
        stage_kernel,
        out_shape=[
            shape((LEVELS, HALF, LAT, C), BF),
            shape((12, HALF // 2, LEVELS, 2 * C), BF),
            shape(table.shape, F32),
            shape(index.shape, jnp.int32),
            shape((1, 4 * C), F32),
        ],
        in_specs=[pl.BlockSpec(memory_space=pltpu.HBM)] * 5,
        out_specs=[whole] * 5,
        scratch_shapes=[pltpu.SemaphoreType.DMA((5,))],
        compiler_params=pltpu.CompilerParams(vmem_limit_bytes=4 * 1024 * 1024),
        name="stage",
    )(*(pltpu.with_memory_space_constraint(a, pltpu.HBM) for a in (fields, cotangent, table, index, gain)))


def bias_rows(table, index, regions):
    whole = pl.BlockSpec(memory_space=pltpu.VMEM)
    return pl.pallas_call(
        bias_kernel,
        out_shape=[jax.ShapeDtypeStruct((TH * WIN, LANES), F32)] * 2,
        in_specs=[whole, whole, pl.BlockSpec(memory_space=pltpu.HBM)],
        out_specs=[whole, whole],
        scratch_shapes=[
            pltpu.VMEM((HIGH * TH, LOW), F32),
            pltpu.VMEM((2 * TH * REST, LANES), F32),
            pltpu.VMEM((REST, WIN), jnp.int32),
            pltpu.VMEM((12 * TH, LANES), F32),
            pltpu.SMEM((LEVELS, LAT), jnp.int32),
            pltpu.SemaphoreType.DMA,
        ],
        compiler_params=pltpu.CompilerParams(vmem_limit_bytes=16 * 1024 * 1024),
        cost_estimate=pl.CostEstimate(flops=14_000_000_000, bytes_accessed=4_000_000, transcendentals=0),
        name="bias_rows",
    )(table, index, pltpu.with_memory_space_constraint(regions, pltpu.HBM))


def block_kernel(
    own_ref, west_ref, own_cotangent_ref, west_cotangent_ref,
    norm_gain_ref, qkv_ref, proj_ref, mlp_gain_ref, up_ref, down_ref, merge_gain_ref, merge_ref,
    bias_ref, bias_tail_ref,
    grads_ref, tokens_ref, ds_ref, normed_merge_ref, triple_ref, grad_attn_ref, unit_ref, scale_ref,
    x_ref, q_ref, k_ref, v_ref, p_ref, mixed_ref,
    unit_mlp_ref, scale_mlp_ref, normed_mlp_ref, hidden_ref, slope_ref, after_mlp_ref,
    group_ref, grad_after_ref, grad_up_ref, grad_mixed_ref,
    cells_ref, grad_merged_ref, scaled_ref,
):
    to_tokens = onehot(288, 288, of_row=cell_of_token)
    for level in range(LEVELS):
        cells = jnp.concatenate(
            [
                west_ref[level].astype(F32).reshape(144, C),
                own_ref[level, :HALF].astype(F32).reshape(144, C),
            ],
            axis=0,
        ).astype(BF)
        ordered = dot(to_tokens, cells)
        for kind in range(TYPES):
            x_ref[WIN * kind + 72 * level : WIN * kind + 72 * level + 72, :] = ordered[72 * kind : 72 * kind + 72]
    unit, scale = normalised(x_ref[...])
    unit_ref[...] = unit
    scale_ref[...] = scale
    tokens = (unit * norm_gain_ref[...]).astype(BF)
    tokens_ref[...] = tokens
    q_ref[...] = dot(tokens, qkv_ref[:, 0:C]).astype(BF)
    k_ref[...] = dot(tokens, qkv_ref[:, C : 2 * C]).astype(BF)
    v_ref[...] = dot(tokens, qkv_ref[:, 2 * C :]).astype(BF)
    for lat in range(12):
        for lon in range(HALF // 2):
            row = (lat * 3 + lon) * 2
            cells_ref[row : row + 2, :] = west_cotangent_ref[lat, lon].astype(F32)
            cells_ref[72 + row : 74 + row, :] = own_cotangent_ref[lat, lon].astype(F32)
    grad_merged_ref[...] = dot(onehot(MTOK, 144, of_row=cell_of_merged), cells_ref[...].astype(BF)).astype(BF)
    for n in range(4):
        value = rounded(dot_nt(grad_merged_ref[...], merge_ref[C * n : C * (n + 1), :]))
        scaled_ref[n] = value * merge_gain_ref[:, C * n : C * (n + 1)]
    lane = lax.broadcasted_iota(jnp.int32, (1, C), 1)
    of_head = [
        jnp.where((lane >= HEAD * h) & (lane < HEAD * (h + 1)), 1.0, 0.0).astype(BF) for h in range(HEADS)
    ]
    temper = HEAD ** (-0.5)

    def attend(kind, carry):
        rows = pl.ds(pl.multiple_of(kind * WIN, 16), WIN)
        q, k, v = q_ref[rows, :], k_ref[rows, :], v_ref[rows, :]
        mixed = jnp.zeros((WIN, C), F32)
        products = dot_nt(jnp.concatenate([q * of_head[h] for h in range(HEADS)], axis=0), k)
        for h in range(HEADS):
            th = h * TYPES + kind
            scores_at = pl.ds(pl.multiple_of(th * WIN, 16), WIN)
            bias = jnp.concatenate([bias_ref[scores_at, :], bias_tail_ref[scores_at, :REST]], axis=1)
            scores = products[WIN * h : WIN * (h + 1)] * temper + bias
            weights = jnp.exp(scores - jnp.max(scores, axis=-1, keepdims=True))
            p = weights * (1.0 / jnp.sum(weights, axis=-1, keepdims=True))
            p_ref[th] = p
            mixed = mixed + dot(p.astype(BF), v * of_head[h])
        mixed_ref[rows, :] = mixed.astype(BF)
        return carry

    lax.fori_loop(0, TYPES, attend, 0, unroll=True)
    after_attn = rounded(x_ref[...] + rounded(dot(mixed_ref[...], proj_ref[...])))
    x_ref[...] = after_attn
    unit, scale = normalised(after_attn)
    unit_mlp_ref[...] = unit
    scale_mlp_ref[...] = scale
    normed_mlp = (unit * mlp_gain_ref[...]).astype(BF)
    normed_mlp_ref[...] = normed_mlp
    for part in range(3):
        cols = slice(256 * part, 256 * part + 256)
        u = dot(normed_mlp, up_ref[:, cols])
        below = 0.5 * (1.0 + lax.erf(u * 0.5**0.5))
        hidden_ref[:, cols] = (u * below).astype(BF)
        slope_ref[:, cols] = below + u * (jnp.exp(u * u * (-0.5)) * 0.3989422804014327)
    after_mlp_ref[...] = (x_ref[...] + dot_nt(hidden_ref[...], down_ref[...])).astype(BF)

    to_groups = onehot(160, WIN, of_row=token_of_group)
    for kind in range(TYPES):
        grouped = dot(to_groups, after_mlp_ref[WIN * kind : WIN * kind + WIN, :])
        for quarter in range(4):
            group_ref[quarter, 40 * kind : 40 * kind + 40, :] = grouped[40 * quarter : 40 * quarter + 40]
    quarters = [group_ref[n] for n in range(4)]
    mean = sum(jnp.sum(v, axis=-1, keepdims=True) for v in quarters) * (1.0 / MLP)
    centred = [v - mean for v in quarters]
    variance = sum(jnp.sum(v * v, axis=-1, keepdims=True) for v in centred) * (1.0 / MLP)
    scale_merge = lax.rsqrt(variance + EPS)
    for n in range(4):
        unit = centred[n] * scale_merge
        group_ref[n] = unit
        normed_merge = (unit * merge_gain_ref[:, C * n : C * (n + 1)]).astype(BF)
        normed_merge_ref[n] = normed_merge
    scaled, total, along = [], 0.0, 0.0
    for n in range(4):
        value = scaled_ref[n]
        total = total + jnp.sum(value, axis=-1, keepdims=True)
        along = along + jnp.sum(value * group_ref[n], axis=-1, keepdims=True)
        scaled.append(value)
    total = total * (1.0 / MLP)
    along = along * (1.0 / MLP)
    for n in range(4):
        group_ref[n] = scale_merge * (scaled[n] - total - group_ref[n] * along)
    from_groups = onehot(WIN, 160, of_row=group_of_token)
    for kind in range(TYPES):
        grouped = jnp.concatenate([group_ref[n, 40 * kind : 40 * kind + 40, :] for n in range(4)], axis=0)
        grad_after_ref[WIN * kind : WIN * kind + WIN, :] = dot(from_groups, grouped.astype(BF)).astype(BF)

    grad_after = grad_after_ref[...]
    for part in range(3):
        cols = slice(256 * part, 256 * part + 256)
        grad_up_ref[:, cols] = (rounded(dot(grad_after, down_ref[:, cols])) * slope_ref[:, cols]).astype(BF)
    grad_normed = rounded(dot_nt(grad_up_ref[...], up_ref[...]))
    grad_attn = (
        grad_after.astype(F32)
        + norm_grad(grad_normed, unit_mlp_ref[...], scale_mlp_ref[...], mlp_gain_ref[...])
    ).astype(BF)
    grad_attn_ref[...] = grad_attn

    grad_mixed_ref[...] = dot_nt(grad_attn, proj_ref[...]).astype(BF)

    def down_terms():
        grad = dot_tn(grad_after_ref[...], hidden_ref[...]).astype(BF)
        for b in range(6):
            grads_ref[O_DOWN + C * b : O_DOWN + C * (b + 1), :] = grad[:, 128 * b : 128 * b + 128]

    def up_terms():
        grad = dot_tn(normed_mlp_ref[...], grad_up_ref[...]).astype(BF)
        for b in range(6):
            grads_ref[O_UP + C * b : O_UP + C * (b + 1), :] = grad[:, 128 * b : 128 * b + 128]

    def merge_terms():
        for n in range(4):
            grad = dot_tn(normed_merge_ref[n], grad_merged_ref[...]).astype(BF)
            for b in range(2):
                start = O_MERGE + MLP * b + C * n
                grads_ref[start : start + C, :] = grad[:, 128 * b : 128 * b + 128]
            kept = max(0, min(C, MSPLIT - C * n))
            if kept:
                start = O_MERGE + 2 * MLP + C * n
                grads_ref[start : start + kept, :] = grad[:kept, 256:]
            if kept < C:
                start = O_MERGE_LAST + C * n + kept - MSPLIT
                grads_ref[start : start + C - kept, :] = grad[kept:, 256:]

    def proj_terms():
        grad_proj = dot_tn(mixed_ref[...], grad_attn_ref[...]).astype(BF)
        grads_ref[O_PROJ : O_PROJ + C, :] = grad_proj[:, :128]
        grads_ref[O_PROJ_TAIL : O_PROJ_TAIL + C // 2, :] = jnp.concatenate(
            [grad_proj[: C // 2, 128:], grad_proj[C // 2 :, 128:]], axis=1
        )

    last_keys = onehot(REST, WIN, of_row=lambda n: n + MAIN)
    ds_ref[DS_CORNER:, :] = jnp.zeros((TH * REST, LANES), BF)
    grads_ref[O_QKV:O_PROJ, :] = jnp.zeros((O_PROJ - O_QKV, LANES), BF)
    grads_ref[O_TABLE:O_MERGE_LAST, :] = jnp.zeros((O_MERGE_LAST - O_TABLE, LANES), BF)

    def attend_back(kind, carry):
        rows = pl.ds(kind * WIN, WIN)
        v, grad = v_ref[rows, :], grad_mixed_ref[rows, :]
        q_turned, k_turned, grad_turned = (jnp.transpose(a) for a in (q_ref[rows, :], k_ref[rows, :], grad))
        products = dot_nt(jnp.concatenate([grad * of_head[h] for h in range(HEADS)], axis=0), v)
        dq, dk, dv = [], [], []
        for h in range(HEADS):
            th = h * TYPES + kind
            lanes = slice(HEAD * h, HEAD * (h + 1))
            p = p_ref[th]
            weighted = p * products[WIN * h : WIN * (h + 1)]
            ds = weighted - p * jnp.sum(weighted, axis=-1, keepdims=True)
            ds = ds.astype(BF)
            ds_ref[pl.ds(th * WIN, WIN), :] = ds[:, :MAIN]
            turned = dot_nt(jnp.concatenate([k_turned[lanes], last_keys], axis=0), ds)
            tail = turned[HEAD:].astype(BF)
            ds_ref[pl.ds(DS_TAIL + th * REST, REST), :] = tail[:, :MAIN]
            ds_ref[pl.ds(DS_CORNER + th * REST, REST), :REST] = tail[:, MAIN:]
            dq.append(turned[:HEAD])
            dk.append(dot(q_turned[lanes], ds))
            dv.append(dot(grad_turned[lanes], p.astype(BF)))
        triple = jnp.concatenate([a * temper for a in dq + dk] + dv, axis=0).astype(BF)
        triple_ref[rows, :] = jnp.transpose(triple)
        return carry

    for kind, terms in enumerate((down_terms, up_terms, merge_terms, proj_terms)):
        attend_back(kind, 0)
        terms()


def block(half_rows, *args):
    shape = jax.ShapeDtypeStruct
    whole = pl.BlockSpec(memory_space=pltpu.VMEM)
    scratch = [
        ((TOK, C), F32), ((TOK, C), BF), ((TOK, C), BF),
        ((TOK, C), BF), ((TH, WIN, WIN), F32), ((TOK, C), BF),
        ((TOK, C), F32), ((TOK, 1), F32), ((TOK, C), BF), ((TOK, MLP), BF), ((TOK, MLP), F32), ((TOK, C), BF),
        ((4, MTOK, C), F32), ((TOK, C), BF), ((TOK, MLP), BF), ((TOK, C), BF),
        ((144, 2 * C), F32), ((MTOK, 2 * C), BF), ((4, MTOK, C), F32),
    ]
    return pl.pallas_call(
        block_kernel,
        out_shape=[
            shape((2 * half_rows, LANES), BF),
            shape((TOK, C), BF),
            shape((DS_END, LANES), BF),
            shape((4, MTOK, C), BF),
            shape((TOK, 3 * C), BF),
            shape((TOK, C), BF),
            shape((TOK, C), F32),
            shape((TOK, 1), F32),
        ],
        in_specs=[whole] * len(args),
        out_specs=[whole] * 8,
        scratch_shapes=[pltpu.VMEM(*item) for item in scratch],
        compiler_params=pltpu.CompilerParams(vmem_limit_bytes=24 * 1024 * 1024),
        cost_estimate=pl.CostEstimate(flops=24_000_000_000, bytes_accessed=12_000_000, transcendentals=2_000_000),
        name="block",
    )(*args)


def pack_kernel(core_ref, grads_ref, tokens_ref, triple_ref, keep_ref, send_ref):
    half = keep_ref.shape[0]
    core = core_ref[0]
    grad_qkv = dot_tn(tokens_ref[...], triple_ref[...]).astype(BF)
    tail = jnp.concatenate([grad_qkv[: C // 2, 512:], grad_qkv[C // 2 :, 512:]], axis=1)
    keep_ref[...] = grads_ref[pl.ds(pl.multiple_of(core * half, 16), half), :]
    send_ref[...] = grads_ref[pl.ds(pl.multiple_of((1 - core) * half, 16), half), :]
    for owner, target_ref in ((0, keep_ref), (1, send_ref)):

        @pl.when(core == owner)
        def _():
            for b in range(4):
                target_ref[O_QKV + C * b : O_QKV + C * (b + 1), :] = grad_qkv[:, 128 * b : 128 * b + 128]
            target_ref[O_QKV_TAIL : O_QKV_TAIL + C // 2, :] = tail


def pack(core, grads, tokens, triple):
    half = jax.ShapeDtypeStruct((grads.shape[0] // 2, LANES), BF)
    whole = pl.BlockSpec(memory_space=pltpu.VMEM)
    return pl.pallas_call(
        pack_kernel,
        out_shape=[half, half],
        in_specs=[pl.BlockSpec(memory_space=pltpu.SMEM)] + [whole] * 3,
        out_specs=[whole] * 2,
        compiler_params=pltpu.CompilerParams(vmem_limit_bytes=12 * 1024 * 1024),
        cost_estimate=pl.CostEstimate(flops=600_000_000, bytes_accessed=4_000_000, transcendentals=0),
        name="pack",
    )(core, grads, tokens, triple)


def table_kernel(core_ref, own_ref, partner_ref, index_ref, table_ref, ds_ref, turned_ref):
    def table_terms(index, slab):
        high_row = index >> 8
        spread = [jnp.where(high_row == n, slab, 0.0) for n in range(HIGH)]
        spread.append(jnp.zeros((TROWS - HIGH * TH, index.shape[1]), F32))
        return dot_nt(jnp.concatenate(spread, axis=0).astype(BF), low_onehot(index & (LOW - 1)))

    def row_block(block, carry):
        base = pl.multiple_of(block * 8, 8)
        rows = index_ref[pl.ds(base, 8), :MAIN]
        index = jnp.concatenate([rows[n : n + 1] for n in range(8)], axis=1)
        slab = jnp.concatenate([ds_ref[pl.ds(base + n, TH, stride=WIN), :] for n in range(8)], axis=1)
        return carry + table_terms(index, slab)

    @pl.when(core_ref[0] == 0)
    def _():
        ds_ref[...] = own_ref[...].astype(F32) + partner_ref[...].astype(F32)
        turned_ref[...] = jnp.transpose(index_ref[:, MAIN:])
        table = lax.fori_loop(0, WIN // 8, row_block, jnp.zeros((TROWS, LOW), F32), unroll=9)
        index = jnp.concatenate([turned_ref[n : n + 1, :MAIN] for n in range(REST)], axis=1)
        slab = jnp.concatenate([ds_ref[pl.ds(DS_TAIL + n, TH, stride=REST), :] for n in range(REST)], axis=1)
        table = table + table_terms(index, slab)
        index = jnp.concatenate([turned_ref[n : n + 1, MAIN:] for n in range(REST)], axis=1)
        slab = jnp.concatenate(
            [ds_ref[pl.ds(DS_CORNER + n, TH, stride=REST), :][:, :REST] for n in range(REST)], axis=1
        )
        table = (table + table_terms(index, slab)).astype(BF)
        table_ref[:TROWS, :] = table[:, :LANES]
        table_ref[TROWS:, :] = table[:, LANES:]

    @pl.when(core_ref[0] == 1)
    def _():
        table_ref[...] = jnp.zeros(table_ref.shape, BF)


def table_sum(core, own, partner, index):
    whole = pl.BlockSpec(memory_space=pltpu.VMEM)
    return pl.pallas_call(
        table_kernel,
        out_shape=jax.ShapeDtypeStruct((2 * TROWS, LANES), BF),
        in_specs=[pl.BlockSpec(memory_space=pltpu.SMEM)] + [whole] * 3,
        out_specs=whole,
        scratch_shapes=[pltpu.VMEM((DS_END, LANES), F32), pltpu.VMEM((REST, WIN), jnp.int32)],
        compiler_params=pltpu.CompilerParams(vmem_limit_bytes=12 * 1024 * 1024),
        cost_estimate=pl.CostEstimate(flops=4_000_000_000, bytes_accessed=3_000_000, transcendentals=0),
        name="table_sum",
    )(core, own, partner, index)


def join_kernel(core_ref, keep_ref, arrived_ref, table_ref, held_ref):
    held_ref[...] = (keep_ref[...].astype(F32) + arrived_ref[...].astype(F32)).astype(BF)

    @pl.when(core_ref[0] == 0)
    def _():
        held_ref[O_TABLE : O_TABLE + 2 * TROWS, :] = table_ref[...]


def join(core, keep, arrived, table):
    whole = pl.BlockSpec(memory_space=pltpu.VMEM)
    return pl.pallas_call(
        join_kernel,
        out_shape=jax.ShapeDtypeStruct(keep.shape, BF),
        in_specs=[pl.BlockSpec(memory_space=pltpu.SMEM)] + [whole] * 3,
        out_specs=whole,
        compiler_params=pltpu.CompilerParams(vmem_limit_bytes=8 * 1024 * 1024),
        cost_estimate=pl.CostEstimate(flops=400_000, bytes_accessed=2_500_000, transcendentals=0),
        name="join",
    )(core, keep, arrived, table)


def cells_kernel(
    normed_merge_ref, triple_ref, grad_attn_ref, unit_ref, scale_ref, qkv_ref, gain_ref, merge_ref,
    merged_keep_ref, field_keep_ref, home_ref, x_ref,
):
    grad_normed = rounded(dot_nt(triple_ref[...], qkv_ref[...]))
    x_ref[...] = grad_attn_ref[...].astype(F32) + norm_grad(
        grad_normed, unit_ref[...], scale_ref[...], gain_ref[...]
    )
    to_cells = onehot(288, 288, of_col=cell_of_token)
    leaving = []
    for level in range(LEVELS):
        ordered = jnp.concatenate(
            [x_ref[WIN * kind + 72 * level : WIN * kind + 72 * level + 72, :] for kind in range(TYPES)], axis=0
        )
        cells = dot(to_cells, ordered.astype(BF))
        leaving.append(cells[:144])
        field_keep_ref[level] = cells[144:].reshape(HALF, LAT, C).astype(BF)
    home_ref[:HALF] = jnp.concatenate(leaving, axis=1).reshape(HALF, LAT, 2 * C).astype(BF)
    merged = sum(dot(normed_merge_ref[n], merge_ref[C * n : C * (n + 1), :]) for n in range(4))
    merged_cells = dot(onehot(144, MTOK, of_col=cell_of_merged), merged.astype(BF))
    for lat in range(12):
        for lon in range(HALF // 2):
            row = 72 + (lat * 3 + lon) * 2
            merged_keep_ref[lat, lon] = merged_cells[row : row + 2].astype(BF)
    home_ref[HALF:] = merged_cells[:72].reshape(3, LAT, 2 * C).astype(BF)


def to_grid(*args):
    shape = jax.ShapeDtypeStruct
    whole = pl.BlockSpec(memory_space=pltpu.VMEM)
    return pl.pallas_call(
        cells_kernel,
        out_shape=[
            shape((12, HALF // 2, LEVELS, 2 * C), BF),
            shape((LEVELS, HALF, LAT, C), BF),
            shape((HALF + 3, LAT, 2 * C), BF),
        ],
        in_specs=[whole] * 8,
        out_specs=[whole] * 3,
        scratch_shapes=[pltpu.VMEM((TOK, C), F32)],
        compiler_params=pltpu.CompilerParams(vmem_limit_bytes=12 * 1024 * 1024),
        cost_estimate=pl.CostEstimate(flops=1_500_000_000, bytes_accessed=3_000_000, transcendentals=0),
        name="to_grid",
    )(*args)


def first_half(part, refs, staged, leaves):
    _, _, up_ref, _, qkv_ref, merge_ref, proj_ref, table_ref = refs
    up, _, qkv, merge, proj, table = staged
    for b in range(6):
        up[:, 128 * b : 128 * b + 128] = part(O_UP + C * b, C)
    leaves(up, up_ref)
    for b in range(4):
        qkv[:, 128 * b : 128 * b + 128] = part(O_QKV + C * b, C)
    tail = part(O_QKV_TAIL, C // 2)
    qkv[: C // 2, 512:] = tail[:, :64]
    qkv[C // 2 :, 512:] = tail[:, 64:]
    leaves(qkv, qkv_ref)
    for side in range(2):
        terms = part(O_TABLE + TROWS * side, TROWS)
        for high in range(HIGH):
            start = high * LOW + side * LANES
            width = min(LANES, BPOS - start)
            for head in range(HEADS):
                row = high * TH + head * TYPES
                table[head, :, start : start + width] = terms[row : row + TYPES, :width]
    leaves(table, table_ref)
    proj[:, :128] = part(O_PROJ, C)
    tail = part(O_PROJ_TAIL, C // 2)
    proj[: C // 2, 128:] = tail[:, :64]
    proj[C // 2 :, 128:] = tail[:, 64:]
    leaves(proj, proj_ref)
    merge[MSPLIT:, 256:] = part(O_MERGE_LAST, MLP - MSPLIT)
    leaves(merge.at[MSPLIT:, 256:], merge_ref.at[MSPLIT:, 256:])


def second_half(part, refs, staged, leaves):
    _, _, _, down_ref, _, merge_ref, _, _ = refs
    _, down, _, merge, _, _ = staged
    for b in range(2):
        merge[:, 128 * b : 128 * b + 128] = part(O_MERGE + MLP * b, MLP)
    leaves(merge.at[:, :256], merge_ref.at[:, :256])
    for b in range(6):
        down[:, 128 * b : 128 * b + 128] = part(O_DOWN + C * b, C)
    leaves(down, down_ref)
    merge[:MSPLIT, 256:] = part(O_MERGE + 2 * MLP, MSPLIT)
    leaves(merge.at[:MSPLIT, 256:], merge_ref.at[:MSPLIT, 256:])


def half_kernel(factor, own, core_ref, sums_ref, *refs):
    if own:
        outs, scratch = (None, None, *refs[:6]), refs[6:]
    else:
        partner_ref, forwarded_ref, merged_keep_ref, field_keep_ref = refs[:4]
        outs, scratch = refs[10:18], refs[18:]
    staged, sems = scratch[:6], scratch[6]
    core = core_ref[0]
    half = core if own else 1 - core
    copies = []
    if not own:
        merged, field = scratch[7:9]
        east = jnp.where(core == 0, partner_ref[...].astype(F32), forwarded_ref[...].astype(F32))
        for level in range(LEVELS):
            field[level, HALF:] = east[:HALF, :, C * level : C * (level + 1)].astype(BF)
        field[:, :HALF] = field_keep_ref[...]
        copies.append(pltpu.make_async_copy(field, outs[1], sems.at[5]))
        copies[-1].start()
        cells = east[HALF:].reshape(72, 2 * C)
        for lat in range(12):
            for lon in range(HALF // 2):
                row = (lat * 3 + lon) * 2
                merged[lat, HALF // 2 + lon] = cells[row : row + 2].astype(BF)
        merged[:, : HALF // 2] = merged_keep_ref[...]
        copies.append(pltpu.make_async_copy(merged, outs[0], sems.at[6]))
        copies[-1].start()

    def part_of(base):
        return lambda start, rows: sums_ref[start - base : start - base + rows, :].astype(F32) * factor

    for which, fill, base in ((0, first_half, 0), (1, second_half, O_MERGE)):

        @pl.when(half == which)
        def _():
            begun = []

            def leaves(source, target):
                begun.append(pltpu.make_async_copy(source, target, sems.at[len(begun)]))
                begun[-1].start()

            fill(part_of(base), outs, staged, leaves)
            for copy in begun:
                copy.wait()

    for copy in copies:
        copy.wait()


def finish(core, held, other, cells, factor):
    shape = jax.ShapeDtypeStruct
    whole = pl.BlockSpec(memory_space=pltpu.VMEM)
    scalar = pl.BlockSpec(memory_space=pltpu.SMEM)
    place = pl.BlockSpec(memory_space=pl.ANY)
    sums = [
        shape((C, MLP), F32),
        shape((C, MLP), F32),
        shape((C, 3 * C), F32),
        shape((MLP, 2 * C), F32),
        shape((C, C), F32),
        shape((HEADS, TYPES, BPOS), F32),
    ]
    scratch = [pltpu.VMEM(item.shape, F32) for item in sums] + [pltpu.SemaphoreType.DMA((7,))]
    grid = [shape((12, HALF, LEVELS, 2 * C), BF), shape((LEVELS, 2 * HALF, LAT, C), BF)]
    params = pltpu.CompilerParams(vmem_limit_bytes=16 * 1024 * 1024)
    begun = pl.pallas_call(
        lambda *refs: half_kernel(factor, True, *refs),
        out_shape=sums,
        in_specs=[scalar, whole],
        out_specs=[place] * 6,
        scratch_shapes=scratch,
        compiler_params=params,
        cost_estimate=pl.CostEstimate(flops=400_000, bytes_accessed=2_500_000, transcendentals=0),
        name="finish_own",
    )(core, held)
    return pl.pallas_call(
        lambda *refs: half_kernel(factor, False, *refs),
        out_shape=[*grid, *sums],
        in_specs=[scalar] + [whole] * 5 + [place] * 6,
        out_specs=[place] * 8,
        scratch_shapes=scratch + [pltpu.VMEM(item.shape, BF) for item in grid],
        input_output_aliases={6 + n: 2 + n for n in range(6)},
        compiler_params=params,
        name="finish_other",
    )(core, other, *cells, *begun)


def passed_along(value, axis, steps):
    count = lax.axis_size(axis)
    return lax.ppermute(value, axis, [(source, (source + steps) % count) for source in range(count)])


def groups_of(count, apart, size):
    return [
        [start * apart * size + offset + member * apart for member in range(size)]
        for start in range(count // (apart * size))
        for offset in range(apart)
    ]


def summed_over(keep, send, axis, joined, partner, forward):
    count = lax.axis_size(axis)
    along = count // (CORES * ACROSS)
    pairs = [(i, i ^ 1) for i in range(count)]
    arrived = lax.ppermute(send, axis, pairs)
    held = joined(keep, arrived)

    def exchanged(value, apart, size):
        return lax.all_to_all(value, axis, 0, 0, axis_index_groups=groups_of(count, apart, size))

    def reduced(value, apart, size):
        got = exchanged(value.reshape(size, -1, *value.shape[1:]), apart, size)
        return jnp.sum(got.astype(F32), axis=0).astype(BF)

    def gathered(value, apart, size):
        return exchanged(jnp.broadcast_to(value[None], (size, *value.shape)), apart, size).reshape(-1, *value.shape[1:])

    held = reduced(held, CORES, ACROSS)
    held, partner = lax.optimization_barrier((held, partner))
    held = reduced(held.reshape(-1, 2, LANES), CORES * ACROSS, along)
    held = gathered(held, CORES * ACROSS, along).reshape(-1, LANES)
    held = gathered(held, CORES, ACROSS)
    held, forwarded = forward(held, partner)
    return held, lax.ppermute(held, axis, pairs), partner, forwarded


def local(
    fields,
    norm_gain,
    qkv_weight,
    proj_weight,
    bias_table,
    bias_index,
    region_ids,
    mlp_gain,
    up_weight,
    down_weight,
    merge_gain,
    merge_weight,
    cotangent,
):
    count = lax.axis_size("lon")
    core = (lax.axis_index("lon") % CORES).astype(jnp.int32).reshape(1)
    by_lon = fields.transpose(0, 2, 1, 3)
    by_lat = cotangent.transpose(1, 2, 0, 3)
    field_last, cotangent_last, table, index, merge_gain = stage(
        by_lon, by_lat, bias_table.transpose(1, 0, 2), bias_index, merge_gain
    )
    west = passed_along(field_last, "lon", 1)
    west_cotangent = passed_along(cotangent_last, "lon", 1)
    table, core = lax.optimization_barrier((table, core))
    bias, bias_tail = bias_rows(table, index, region_ids)
    half_rows = -(-O_END // (count * 2)) * 2 * count // CORES
    grads, tokens, scores, *results = block(
        half_rows,
        by_lon,
        west,
        by_lat,
        west_cotangent,
        norm_gain.reshape(1, C),
        qkv_weight,
        proj_weight,
        mlp_gain.reshape(1, C),
        up_weight,
        down_weight.T,
        merge_gain,
        merge_weight,
        bias,
        bias_tail,
    )
    pairs = [(i, i ^ 1) for i in range(count)]
    partner_scores = lax.ppermute(scores, "lon", pairs)
    keep, send = pack(core, grads, tokens, results[1])
    merged_keep, field_keep, home = to_grid(*results, qkv_weight, norm_gain.reshape(1, C), merge_weight)
    partner = lax.ppermute(home, "lon", pairs)

    def forward(held, leaving):
        held, leaving = lax.optimization_barrier((held, leaving))
        return held, lax.ppermute(leaving, "lon", [(i, (i - CORES) % count) for i in range(1, count, CORES)])

    table = table_sum(core, scores, partner_scores, index)
    held, other, partner, forwarded = summed_over(
        keep, send, "lon", lambda kept, arrived: join(core, kept, arrived, table), partner, forward
    )
    factor = float(LEVELS * LAT * fields.shape[2] * count) ** (-0.5)
    merged, field_grad, up_grad, down_grad, qkv_grad, merge_grad, proj_grad, table_grad = finish(
        core, held, other, (partner, forwarded, merged_keep, field_keep), factor
    )
    return (
        merged.transpose(2, 0, 1, 3),
        field_grad.transpose(0, 2, 1, 3),
        qkv_grad,
        proj_grad,
        up_grad,
        down_grad.T,
        merge_grad,
        table_grad.transpose(1, 0, 2),
    )


def solution(mesh):
    whole = P("groups", None, "lon", None)

    return jax.shard_map(
        local,
        mesh=mesh,
        in_specs=(whole, *[P()] * 11, whole),
        out_specs=(whole, whole, *[P("groups", None)] * 5, P("groups", None, None)),
        check_vma=False,
    )
```

```python
import jax
import jax.numpy as jnp
from jax import lax
from jax.experimental import pallas as pl
from jax.experimental.pallas import tpu as pltpu
from jax.sharding import PartitionSpec as P

C = 192
MLP = 768
HEADS = 6
HEAD = 32
HALF = 6
WIN = 144
BPOS = 3312
LAT = 24
TYPES = 4
TOK = TYPES * WIN
LEVELS = 2
LANES = 128
MAIN = 128
REST = WIN - MAIN
TH = TYPES * HEADS
LOW = 256
HIGH = -(-BPOS // LOW)
MTOK = 160
EPS = 1e-5
MASKED = -1e30
F32 = jnp.float32
BF = jnp.bfloat16
CORES = 2
ACROSS = 4

TROWS = 320
MSPLIT = 512
O_UP = 0
O_QKV = O_UP + 6 * C
O_QKV_TAIL = O_QKV + 4 * C
O_PROJ = O_QKV_TAIL + C // 2
O_PROJ_TAIL = O_PROJ + C
O_TABLE = O_PROJ_TAIL + C // 2
O_MERGE_LAST = O_TABLE + 2 * TROWS
O_MERGE = O_MERGE_LAST + MLP - MSPLIT
O_DOWN = O_MERGE + 2 * MLP + MSPLIT
O_END = O_DOWN + 6 * C

DS_TAIL = TH * WIN
DS_CORNER = DS_TAIL + TH * REST
DS_END = DS_CORNER + TH * REST


def dot(a, b):
    return jnp.dot(a, b, preferred_element_type=F32)


def dot_nt(a, b):
    return lax.dot_general(a, b, (((1,), (1,)), ((), ())), preferred_element_type=F32)


def dot_tn(a, b):
    return lax.dot_general(a, b, (((0,), (0,)), ((), ())), preferred_element_type=F32)


def div(n, d):
    return (n * -(-(1 << 16) // d)) >> 16


def onehot(rows, cols, of_row=None, of_col=None):
    if of_row is not None:
        target = of_row(lax.broadcasted_iota(jnp.int32, (rows, 1), 0))
        place = lax.broadcasted_iota(jnp.int32, (rows, cols), 1)
    else:
        target = of_col(lax.broadcasted_iota(jnp.int32, (1, cols), 1))
        place = lax.broadcasted_iota(jnp.int32, (rows, cols), 0)
    return jnp.where(place == target, 1.0, 0.0).astype(BF)


def cell_of_token(n):
    kind = div(n, 72)
    rest = n - 72 * kind
    lat = div(rest, 12)
    return (rest - 12 * lat) * LAT + kind * 6 + lat


def token_of_group(n):
    quarter = div(n, 40)
    rest = n - 40 * quarter
    level = div(rest, 18)
    part = rest - 18 * level
    lat = div(part, 6)
    token = level * 72 + (2 * lat + (quarter >> 1)) * 12 + 2 * (part - 6 * lat) + (quarter & 1)
    return jnp.where(rest < 36, token, -1)


def group_of_token(n):
    level = div(n, 72)
    rest = n - 72 * level
    lat = div(rest, 12)
    lon = rest - 12 * lat
    return ((lat & 1) * 2 + (lon & 1)) * 40 + level * 18 + (lat >> 1) * 6 + (lon >> 1)


def cell_of_merged(n):
    kind = div(n, 40)
    rest = n - 40 * kind
    level = div(rest, 18)
    part = rest - 18 * level
    lat = div(part, 6)
    lon = part - 6 * lat
    half = jnp.where(lon < 3, 0, 1)
    row = half * 72 + (3 * kind + lat) * 6 + (lon - 3 * half) * 2 + level
    return jnp.where(rest < 36, row, -1)


def normalised(values):
    centred = values - jnp.mean(values, axis=-1, keepdims=True)
    scale = lax.rsqrt(jnp.mean(centred * centred, axis=-1, keepdims=True) + EPS)
    return centred * scale, scale


def norm_grad(grad, unit, scale, gain):
    scaled = grad * gain
    return scale * (
        scaled
        - jnp.mean(scaled, axis=-1, keepdims=True)
        - unit * jnp.mean(scaled * unit, axis=-1, keepdims=True)
    )


def rounded(values):
    return values.astype(BF).astype(F32)


def low_onehot(low):
    place = lax.broadcasted_iota(jnp.int32, (LOW, 1), 0).astype(F32).astype(BF)
    hit = jnp.broadcast_to(place, (LOW, low.shape[1])) == low.astype(F32).astype(BF)
    return jnp.where(hit, jnp.array(1, BF), jnp.array(0, BF))


def bias_kernel(table_ref, index_ref, regions_ref, main_ref, tail_ref, part_ref, last_ref, turned_ref, mask_ref, region_ref, sem):
    copy = pltpu.make_async_copy(regions_ref, region_ref, sem)
    copy.start()
    for high in range(HIGH):
        width = min(LOW, BPOS - high * LOW)
        for head in range(HEADS):
            piece = table_ref[head, :, high * LOW : high * LOW + width]
            if width < LOW:
                piece = jnp.concatenate([piece, jnp.zeros((TYPES, LOW - width), F32)], axis=1)
            row = high * TH + head * TYPES
            part_ref[row : row + TYPES, :] = piece
    turned_ref[...] = jnp.transpose(index_ref[:, MAIN:])
    parts = part_ref[...].astype(BF)

    def looked_up(index):
        low = low_onehot(index & (LOW - 1))
        high_row = index >> 8
        found = dot(parts, low)
        chosen = found[0:TH]
        for high in range(1, HIGH):
            chosen = jnp.where(high_row == high, found[high * TH : (high + 1) * TH], chosen)
        return chosen

    for start in range(0, REST, 4):
        got = looked_up(jnp.concatenate([turned_ref[start + n : start + n + 1, :MAIN] for n in range(4)], axis=1))
        for n in range(4):
            last_ref[pl.ds(start + n, TH, stride=REST), :] = got[:, n * MAIN : (n + 1) * MAIN]
    got = looked_up(jnp.concatenate([turned_ref[n : n + 1, MAIN:] for n in range(REST)], axis=1))
    for n in range(REST):
        half = got[:, LANES * (n // 8) : LANES * (n // 8 + 1)]
        half = half if n % 8 == 0 else pltpu.roll(half, LANES - REST * (n % 8), 1)
        last_ref[pl.ds(TH * REST + n, TH, stride=REST), :] = half
    copy.wait()
    kind_of = lax.broadcasted_iota(jnp.int32, (TH, 1), 0) & (TYPES - 1)
    column = lax.broadcasted_iota(jnp.int32, (1, LANES), 1)
    labels = []
    for group in range(12):
        label = jnp.zeros((TH, 1), jnp.int32)
        for kind in range(TYPES):
            label = jnp.where(kind_of == kind, region_ref[group // 6, 6 * kind + group % 6], label)
        labels.append(label)
    keys = jnp.zeros((TH, LANES), jnp.int32)
    for group in range(11):
        keys = jnp.where((column >= 12 * group) & (column < 12 * group + 12), labels[group], keys)
    for group in range(12):
        mask_ref[TH * group : TH * (group + 1), :] = jnp.where(keys == labels[group], 0.0, MASKED)

    def row_block(block, carry):
        base = pl.multiple_of(block * 8, 8)
        rows = index_ref[pl.ds(base, 8), :MAIN]
        for part in range(2):
            index = jnp.concatenate([rows[4 * part + n : 4 * part + n + 1] for n in range(4)], axis=1)
            got = looked_up(index)
            for n in range(4):
                row = base + 4 * part + n
                mask = mask_ref[pl.ds(pl.multiple_of(div(row, 12) * TH, 8), TH), :]
                main_ref[pl.ds(row, TH, stride=WIN), :] = got[:, n * MAIN : (n + 1) * MAIN] + mask
        return carry

    lax.fori_loop(0, WIN // 8, row_block, 0, unroll=True)
    apart = jnp.where(labels[10] == labels[11], 0.0, MASKED)
    split = 132 - MAIN
    for n in range(REST):
        group = (MAIN + n) // 12
        rows = pl.ds(n, TH, stride=REST)
        last_ref[rows, :] = last_ref[rows, :] + mask_ref[TH * group : TH * (group + 1), :]
        rows = pl.ds(TH * REST + n, TH, stride=REST)
        other = (column < split) if n >= split else (column >= split)
        last_ref[rows, :] = last_ref[rows, :] + jnp.where(other, apart, 0.0)
    for th in range(TH):
        rows = slice(th * WIN, th * WIN + MAIN)
        tail_ref[rows, :REST] = jnp.transpose(last_ref[th * REST : (th + 1) * REST, :])
        rows = slice(th * WIN + MAIN, (th + 1) * WIN)
        tail_ref[rows, :REST] = jnp.transpose(last_ref[(TH + th) * REST : (TH + th + 1) * REST, :])[:REST]


def stage_kernel(fields_ref, cotangent_ref, table_ref, index_ref, gain_ref, field_ref, half_ref, table_out, index_out, gain_out, sems):
    copies = [
        pltpu.make_async_copy(source, target, sems.at[n])
        for n, (source, target) in enumerate(
            [
                (fields_ref.at[:, HALF:], field_ref),
                (cotangent_ref.at[:, HALF // 2 :], half_ref),
                (table_ref, table_out),
                (index_ref, index_out),
                (gain_ref, gain_out.at[0]),
            ]
        )
    ]
    for copy in copies:
        copy.start()
    for copy in copies:
        copy.wait()


def stage(fields, cotangent, table, index, gain):
    shape = jax.ShapeDtypeStruct
    whole = pl.BlockSpec(memory_space=pltpu.VMEM)
    return pl.pallas_call(
        stage_kernel,
        out_shape=[
            shape((LEVELS, HALF, LAT, C), BF),
            shape((12, HALF // 2, LEVELS, 2 * C), BF),
            shape(table.shape, F32),
            shape(index.shape, jnp.int32),
            shape((1, 4 * C), F32),
        ],
        in_specs=[pl.BlockSpec(memory_space=pltpu.HBM)] * 5,
        out_specs=[whole] * 5,
        scratch_shapes=[pltpu.SemaphoreType.DMA((5,))],
        compiler_params=pltpu.CompilerParams(vmem_limit_bytes=4 * 1024 * 1024),
        name="stage",
    )(*(pltpu.with_memory_space_constraint(a, pltpu.HBM) for a in (fields, cotangent, table, index, gain)))


def bias_rows(table, index, regions):
    whole = pl.BlockSpec(memory_space=pltpu.VMEM)
    return pl.pallas_call(
        bias_kernel,
        out_shape=[jax.ShapeDtypeStruct((TH * WIN, LANES), F32)] * 2,
        in_specs=[whole, whole, pl.BlockSpec(memory_space=pltpu.HBM)],
        out_specs=[whole, whole],
        scratch_shapes=[
            pltpu.VMEM((HIGH * TH, LOW), F32),
            pltpu.VMEM((2 * TH * REST, LANES), F32),
            pltpu.VMEM((REST, WIN), jnp.int32),
            pltpu.VMEM((12 * TH, LANES), F32),
            pltpu.SMEM((LEVELS, LAT), jnp.int32),
            pltpu.SemaphoreType.DMA,
        ],
        compiler_params=pltpu.CompilerParams(vmem_limit_bytes=16 * 1024 * 1024),
        cost_estimate=pl.CostEstimate(flops=14_000_000_000, bytes_accessed=4_000_000, transcendentals=0),
        name="bias_rows",
    )(table, index, pltpu.with_memory_space_constraint(regions, pltpu.HBM))


def block_kernel(
    own_ref, west_ref, own_cotangent_ref, west_cotangent_ref,
    norm_gain_ref, qkv_ref, proj_ref, mlp_gain_ref, up_ref, down_ref, merge_gain_ref, merge_ref,
    bias_ref, bias_tail_ref,
    grads_ref, tokens_ref, ds_ref, normed_merge_ref, triple_ref, grad_attn_ref, unit_ref, scale_ref,
    x_ref, q_ref, k_ref, v_ref, p_ref, mixed_ref,
    unit_mlp_ref, scale_mlp_ref, normed_mlp_ref, hidden_ref, slope_ref, after_mlp_ref,
    group_ref, grad_after_ref, grad_up_ref, grad_mixed_ref,
    cells_ref, grad_merged_ref, scaled_ref,
):
    to_tokens = onehot(288, 288, of_row=cell_of_token)
    for level in range(LEVELS):
        cells = jnp.concatenate(
            [
                west_ref[level].astype(F32).reshape(144, C),
                own_ref[level, :HALF].astype(F32).reshape(144, C),
            ],
            axis=0,
        ).astype(BF)
        ordered = dot(to_tokens, cells)
        for kind in range(TYPES):
            x_ref[WIN * kind + 72 * level : WIN * kind + 72 * level + 72, :] = ordered[72 * kind : 72 * kind + 72]
    unit, scale = normalised(x_ref[...])
    unit_ref[...] = unit
    scale_ref[...] = scale
    tokens = (unit * norm_gain_ref[...]).astype(BF)
    tokens_ref[...] = tokens
    q_ref[...] = dot(tokens, qkv_ref[:, 0:C]).astype(BF)
    k_ref[...] = dot(tokens, qkv_ref[:, C : 2 * C]).astype(BF)
    v_ref[...] = dot(tokens, qkv_ref[:, 2 * C :]).astype(BF)
    for lat in range(12):
        for lon in range(HALF // 2):
            row = (lat * 3 + lon) * 2
            cells_ref[row : row + 2, :] = west_cotangent_ref[lat, lon].astype(F32)
            cells_ref[72 + row : 74 + row, :] = own_cotangent_ref[lat, lon].astype(F32)
    grad_merged_ref[...] = dot(onehot(MTOK, 144, of_row=cell_of_merged), cells_ref[...].astype(BF)).astype(BF)
    for n in range(4):
        value = rounded(dot_nt(grad_merged_ref[...], merge_ref[C * n : C * (n + 1), :]))
        scaled_ref[n] = value * merge_gain_ref[:, C * n : C * (n + 1)]
    lane = lax.broadcasted_iota(jnp.int32, (1, C), 1)
    of_head = [
        jnp.where((lane >= HEAD * h) & (lane < HEAD * (h + 1)), 1.0, 0.0).astype(BF) for h in range(HEADS)
    ]
    temper = HEAD ** (-0.5)

    def attend(kind, carry):
        rows = pl.ds(pl.multiple_of(kind * WIN, 16), WIN)
        q, k, v = q_ref[rows, :], k_ref[rows, :], v_ref[rows, :]
        mixed = jnp.zeros((WIN, C), F32)
        products = dot_nt(jnp.concatenate([q * of_head[h] for h in range(HEADS)], axis=0), k)
        for h in range(HEADS):
            th = h * TYPES + kind
            scores_at = pl.ds(pl.multiple_of(th * WIN, 16), WIN)
            bias = jnp.concatenate([bias_ref[scores_at, :], bias_tail_ref[scores_at, :REST]], axis=1)
            scores = products[WIN * h : WIN * (h + 1)] * temper + bias
            weights = jnp.exp(scores - jnp.max(scores, axis=-1, keepdims=True))
            p = weights * (1.0 / jnp.sum(weights, axis=-1, keepdims=True))
            p_ref[th] = p
            mixed = mixed + dot(p.astype(BF), v * of_head[h])
        mixed_ref[rows, :] = mixed.astype(BF)
        return carry

    lax.fori_loop(0, TYPES, attend, 0, unroll=True)
    after_attn = rounded(x_ref[...] + rounded(dot(mixed_ref[...], proj_ref[...])))
    x_ref[...] = after_attn
    unit, scale = normalised(after_attn)
    unit_mlp_ref[...] = unit
    scale_mlp_ref[...] = scale
    normed_mlp = (unit * mlp_gain_ref[...]).astype(BF)
    normed_mlp_ref[...] = normed_mlp
    for part in range(3):
        cols = slice(256 * part, 256 * part + 256)
        u = dot(normed_mlp, up_ref[:, cols])
        below = 0.5 * (1.0 + lax.erf(u * 0.5**0.5))
        hidden_ref[:, cols] = (u * below).astype(BF)
        slope_ref[:, cols] = below + u * (jnp.exp(u * u * (-0.5)) * 0.3989422804014327)
    after_mlp_ref[...] = (x_ref[...] + dot_nt(hidden_ref[...], down_ref[...])).astype(BF)

    to_groups = onehot(160, WIN, of_row=token_of_group)
    for kind in range(TYPES):
        grouped = dot(to_groups, after_mlp_ref[WIN * kind : WIN * kind + WIN, :])
        for quarter in range(4):
            group_ref[quarter, 40 * kind : 40 * kind + 40, :] = grouped[40 * quarter : 40 * quarter + 40]
    quarters = [group_ref[n] for n in range(4)]
    mean = sum(jnp.sum(v, axis=-1, keepdims=True) for v in quarters) * (1.0 / MLP)
    centred = [v - mean for v in quarters]
    variance = sum(jnp.sum(v * v, axis=-1, keepdims=True) for v in centred) * (1.0 / MLP)
    scale_merge = lax.rsqrt(variance + EPS)
    for n in range(4):
        unit = centred[n] * scale_merge
        group_ref[n] = unit
        normed_merge = (unit * merge_gain_ref[:, C * n : C * (n + 1)]).astype(BF)
        normed_merge_ref[n] = normed_merge
    scaled, total, along = [], 0.0, 0.0
    for n in range(4):
        value = scaled_ref[n]
        total = total + jnp.sum(value, axis=-1, keepdims=True)
        along = along + jnp.sum(value * group_ref[n], axis=-1, keepdims=True)
        scaled.append(value)
    total = total * (1.0 / MLP)
    along = along * (1.0 / MLP)
    for n in range(4):
        group_ref[n] = scale_merge * (scaled[n] - total - group_ref[n] * along)
    from_groups = onehot(WIN, 160, of_row=group_of_token)
    for kind in range(TYPES):
        grouped = jnp.concatenate([group_ref[n, 40 * kind : 40 * kind + 40, :] for n in range(4)], axis=0)
        grad_after_ref[WIN * kind : WIN * kind + WIN, :] = dot(from_groups, grouped.astype(BF)).astype(BF)

    grad_after = grad_after_ref[...]
    for part in range(3):
        cols = slice(256 * part, 256 * part + 256)
        grad_up_ref[:, cols] = (rounded(dot(grad_after, down_ref[:, cols])) * slope_ref[:, cols]).astype(BF)
    grad_normed = rounded(dot_nt(grad_up_ref[...], up_ref[...]))
    grad_attn = (
        grad_after.astype(F32)
        + norm_grad(grad_normed, unit_mlp_ref[...], scale_mlp_ref[...], mlp_gain_ref[...])
    ).astype(BF)
    grad_attn_ref[...] = grad_attn

    grad_mixed_ref[...] = dot_nt(grad_attn, proj_ref[...]).astype(BF)

    def down_terms():
        grad = dot_tn(grad_after_ref[...], hidden_ref[...]).astype(BF)
        for b in range(6):
            grads_ref[O_DOWN + C * b : O_DOWN + C * (b + 1), :] = grad[:, 128 * b : 128 * b + 128]

    def up_terms():
        grad = dot_tn(normed_mlp_ref[...], grad_up_ref[...]).astype(BF)
        for b in range(6):
            grads_ref[O_UP + C * b : O_UP + C * (b + 1), :] = grad[:, 128 * b : 128 * b + 128]

    def merge_terms():
        for n in range(4):
            grad = dot_tn(normed_merge_ref[n], grad_merged_ref[...]).astype(BF)
            for b in range(2):
                start = O_MERGE + MLP * b + C * n
                grads_ref[start : start + C, :] = grad[:, 128 * b : 128 * b + 128]
            kept = max(0, min(C, MSPLIT - C * n))
            if kept:
                start = O_MERGE + 2 * MLP + C * n
                grads_ref[start : start + kept, :] = grad[:kept, 256:]
            if kept < C:
                start = O_MERGE_LAST + C * n + kept - MSPLIT
                grads_ref[start : start + C - kept, :] = grad[kept:, 256:]

    def proj_terms():
        grad_proj = dot_tn(mixed_ref[...], grad_attn_ref[...]).astype(BF)
        grads_ref[O_PROJ : O_PROJ + C, :] = grad_proj[:, :128]
        grads_ref[O_PROJ_TAIL : O_PROJ_TAIL + C // 2, :] = jnp.concatenate(
            [grad_proj[: C // 2, 128:], grad_proj[C // 2 :, 128:]], axis=1
        )

    last_keys = onehot(REST, WIN, of_row=lambda n: n + MAIN)
    ds_ref[DS_CORNER:, :] = jnp.zeros((TH * REST, LANES), BF)
    grads_ref[O_QKV:O_PROJ, :] = jnp.zeros((O_PROJ - O_QKV, LANES), BF)
    grads_ref[O_TABLE:O_MERGE_LAST, :] = jnp.zeros((O_MERGE_LAST - O_TABLE, LANES), BF)

    def attend_back(kind, carry):
        rows = pl.ds(kind * WIN, WIN)
        v, grad = v_ref[rows, :], grad_mixed_ref[rows, :]
        q_turned, k_turned, grad_turned = (jnp.transpose(a) for a in (q_ref[rows, :], k_ref[rows, :], grad))
        products = dot_nt(jnp.concatenate([grad * of_head[h] for h in range(HEADS)], axis=0), v)
        dq, dk, dv = [], [], []
        for h in range(HEADS):
            th = h * TYPES + kind
            lanes = slice(HEAD * h, HEAD * (h + 1))
            p = p_ref[th]
            weighted = p * products[WIN * h : WIN * (h + 1)]
            ds = weighted - p * jnp.sum(weighted, axis=-1, keepdims=True)
            ds = ds.astype(BF)
            ds_ref[pl.ds(th * WIN, WIN), :] = ds[:, :MAIN]
            turned = dot_nt(jnp.concatenate([k_turned[lanes], last_keys], axis=0), ds)
            tail = turned[HEAD:].astype(BF)
            ds_ref[pl.ds(DS_TAIL + th * REST, REST), :] = tail[:, :MAIN]
            ds_ref[pl.ds(DS_CORNER + th * REST, REST), :REST] = tail[:, MAIN:]
            dq.append(turned[:HEAD])
            dk.append(dot(q_turned[lanes], ds))
            dv.append(dot(grad_turned[lanes], p.astype(BF)))
        triple = jnp.concatenate([a * temper for a in dq + dk] + dv, axis=0).astype(BF)
        triple_ref[rows, :] = jnp.transpose(triple)
        return carry

    for kind, terms in enumerate((down_terms, up_terms, merge_terms, proj_terms)):
        attend_back(kind, 0)
        terms()


def block(half_rows, *args):
    shape = jax.ShapeDtypeStruct
    whole = pl.BlockSpec(memory_space=pltpu.VMEM)
    scratch = [
        ((TOK, C), F32), ((TOK, C), BF), ((TOK, C), BF),
        ((TOK, C), BF), ((TH, WIN, WIN), F32), ((TOK, C), BF),
        ((TOK, C), F32), ((TOK, 1), F32), ((TOK, C), BF), ((TOK, MLP), BF), ((TOK, MLP), F32), ((TOK, C), BF),
        ((4, MTOK, C), F32), ((TOK, C), BF), ((TOK, MLP), BF), ((TOK, C), BF),
        ((144, 2 * C), F32), ((MTOK, 2 * C), BF), ((4, MTOK, C), F32),
    ]
    return pl.pallas_call(
        block_kernel,
        out_shape=[
            shape((2 * half_rows, LANES), BF),
            shape((TOK, C), BF),
            shape((DS_END, LANES), BF),
            shape((4, MTOK, C), BF),
            shape((TOK, 3 * C), BF),
            shape((TOK, C), BF),
            shape((TOK, C), F32),
            shape((TOK, 1), F32),
        ],
        in_specs=[whole] * len(args),
        out_specs=[whole] * 8,
        scratch_shapes=[pltpu.VMEM(*item) for item in scratch],
        compiler_params=pltpu.CompilerParams(vmem_limit_bytes=24 * 1024 * 1024),
        cost_estimate=pl.CostEstimate(flops=24_000_000_000, bytes_accessed=12_000_000, transcendentals=2_000_000),
        name="block",
    )(*args)


def pack_kernel(core_ref, grads_ref, tokens_ref, triple_ref, keep_ref, send_ref):
    half = keep_ref.shape[0]
    core = core_ref[0]
    grad_qkv = dot_tn(tokens_ref[...], triple_ref[...]).astype(BF)
    tail = jnp.concatenate([grad_qkv[: C // 2, 512:], grad_qkv[C // 2 :, 512:]], axis=1)
    keep_ref[...] = grads_ref[pl.ds(pl.multiple_of(core * half, 16), half), :]
    send_ref[...] = grads_ref[pl.ds(pl.multiple_of((1 - core) * half, 16), half), :]
    for owner, target_ref in ((0, keep_ref), (1, send_ref)):

        @pl.when(core == owner)
        def _():
            for b in range(4):
                target_ref[O_QKV + C * b : O_QKV + C * (b + 1), :] = grad_qkv[:, 128 * b : 128 * b + 128]
            target_ref[O_QKV_TAIL : O_QKV_TAIL + C // 2, :] = tail


def pack(core, grads, tokens, triple):
    half = jax.ShapeDtypeStruct((grads.shape[0] // 2, LANES), BF)
    whole = pl.BlockSpec(memory_space=pltpu.VMEM)
    return pl.pallas_call(
        pack_kernel,
        out_shape=[half, half],
        in_specs=[pl.BlockSpec(memory_space=pltpu.SMEM)] + [whole] * 3,
        out_specs=[whole] * 2,
        compiler_params=pltpu.CompilerParams(vmem_limit_bytes=12 * 1024 * 1024),
        cost_estimate=pl.CostEstimate(flops=600_000_000, bytes_accessed=4_000_000, transcendentals=0),
        name="pack",
    )(core, grads, tokens, triple)


def table_kernel(core_ref, own_ref, partner_ref, index_ref, table_ref, ds_ref, turned_ref):
    def table_terms(index, slab):
        high_row = index >> 8
        spread = [jnp.where(high_row == n, slab, 0.0) for n in range(HIGH)]
        spread.append(jnp.zeros((TROWS - HIGH * TH, index.shape[1]), F32))
        return dot_nt(jnp.concatenate(spread, axis=0).astype(BF), low_onehot(index & (LOW - 1)))

    def row_block(block, carry):
        base = pl.multiple_of(block * 8, 8)
        rows = index_ref[pl.ds(base, 8), :MAIN]
        index = jnp.concatenate([rows[n : n + 1] for n in range(8)], axis=1)
        slab = jnp.concatenate([ds_ref[pl.ds(base + n, TH, stride=WIN), :] for n in range(8)], axis=1)
        return carry + table_terms(index, slab)

    @pl.when(core_ref[0] == 0)
    def _():
        ds_ref[...] = own_ref[...].astype(F32) + partner_ref[...].astype(F32)
        turned_ref[...] = jnp.transpose(index_ref[:, MAIN:])
        table = lax.fori_loop(0, WIN // 8, row_block, jnp.zeros((TROWS, LOW), F32), unroll=9)
        index = jnp.concatenate([turned_ref[n : n + 1, :MAIN] for n in range(REST)], axis=1)
        slab = jnp.concatenate([ds_ref[pl.ds(DS_TAIL + n, TH, stride=REST), :] for n in range(REST)], axis=1)
        table = table + table_terms(index, slab)
        index = jnp.concatenate([turned_ref[n : n + 1, MAIN:] for n in range(REST)], axis=1)
        slab = jnp.concatenate(
            [ds_ref[pl.ds(DS_CORNER + n, TH, stride=REST), :][:, :REST] for n in range(REST)], axis=1
        )
        table = (table + table_terms(index, slab)).astype(BF)
        table_ref[:TROWS, :] = table[:, :LANES]
        table_ref[TROWS:, :] = table[:, LANES:]

    @pl.when(core_ref[0] == 1)
    def _():
        table_ref[...] = jnp.zeros(table_ref.shape, BF)


def table_sum(core, own, partner, index):
    whole = pl.BlockSpec(memory_space=pltpu.VMEM)
    return pl.pallas_call(
        table_kernel,
        out_shape=jax.ShapeDtypeStruct((2 * TROWS, LANES), BF),
        in_specs=[pl.BlockSpec(memory_space=pltpu.SMEM)] + [whole] * 3,
        out_specs=whole,
        scratch_shapes=[pltpu.VMEM((DS_END, LANES), F32), pltpu.VMEM((REST, WIN), jnp.int32)],
        compiler_params=pltpu.CompilerParams(vmem_limit_bytes=12 * 1024 * 1024),
        cost_estimate=pl.CostEstimate(flops=4_000_000_000, bytes_accessed=3_000_000, transcendentals=0),
        name="table_sum",
    )(core, own, partner, index)


def join_kernel(core_ref, keep_ref, arrived_ref, table_ref, held_ref):
    held_ref[...] = (keep_ref[...].astype(F32) + arrived_ref[...].astype(F32)).astype(BF)

    @pl.when(core_ref[0] == 0)
    def _():
        held_ref[O_TABLE : O_TABLE + 2 * TROWS, :] = table_ref[...]


def join(core, keep, arrived, table):
    whole = pl.BlockSpec(memory_space=pltpu.VMEM)
    return pl.pallas_call(
        join_kernel,
        out_shape=jax.ShapeDtypeStruct(keep.shape, BF),
        in_specs=[pl.BlockSpec(memory_space=pltpu.SMEM)] + [whole] * 3,
        out_specs=whole,
        compiler_params=pltpu.CompilerParams(vmem_limit_bytes=8 * 1024 * 1024),
        cost_estimate=pl.CostEstimate(flops=400_000, bytes_accessed=2_500_000, transcendentals=0),
        name="join",
    )(core, keep, arrived, table)


def cells_kernel(
    normed_merge_ref, triple_ref, grad_attn_ref, unit_ref, scale_ref, qkv_ref, gain_ref, merge_ref,
    merged_keep_ref, field_keep_ref, home_ref, x_ref,
):
    grad_normed = rounded(dot_nt(triple_ref[...], qkv_ref[...]))
    x_ref[...] = grad_attn_ref[...].astype(F32) + norm_grad(
        grad_normed, unit_ref[...], scale_ref[...], gain_ref[...]
    )
    to_cells = onehot(288, 288, of_col=cell_of_token)
    leaving = []
    for level in range(LEVELS):
        ordered = jnp.concatenate(
            [x_ref[WIN * kind + 72 * level : WIN * kind + 72 * level + 72, :] for kind in range(TYPES)], axis=0
        )
        cells = dot(to_cells, ordered.astype(BF))
        leaving.append(cells[:144])
        field_keep_ref[level] = cells[144:].reshape(HALF, LAT, C).astype(BF)
    home_ref[:HALF] = jnp.concatenate(leaving, axis=1).reshape(HALF, LAT, 2 * C).astype(BF)
    merged = sum(dot(normed_merge_ref[n], merge_ref[C * n : C * (n + 1), :]) for n in range(4))
    merged_cells = dot(onehot(144, MTOK, of_col=cell_of_merged), merged.astype(BF))
    for lat in range(12):
        for lon in range(HALF // 2):
            row = 72 + (lat * 3 + lon) * 2
            merged_keep_ref[lat, lon] = merged_cells[row : row + 2].astype(BF)
    home_ref[HALF:] = merged_cells[:72].reshape(3, LAT, 2 * C).astype(BF)


def to_grid(*args):
    shape = jax.ShapeDtypeStruct
    whole = pl.BlockSpec(memory_space=pltpu.VMEM)
    return pl.pallas_call(
        cells_kernel,
        out_shape=[
            shape((12, HALF // 2, LEVELS, 2 * C), BF),
            shape((LEVELS, HALF, LAT, C), BF),
            shape((HALF + 3, LAT, 2 * C), BF),
        ],
        in_specs=[whole] * 8,
        out_specs=[whole] * 3,
        scratch_shapes=[pltpu.VMEM((TOK, C), F32)],
        compiler_params=pltpu.CompilerParams(vmem_limit_bytes=12 * 1024 * 1024),
        cost_estimate=pl.CostEstimate(flops=1_500_000_000, bytes_accessed=3_000_000, transcendentals=0),
        name="to_grid",
    )(*args)


def first_half(part, refs, staged, leaves):
    _, _, up_ref, _, qkv_ref, merge_ref, proj_ref, table_ref = refs
    up, _, qkv, merge, proj, table = staged
    for b in range(6):
        up[:, 128 * b : 128 * b + 128] = part(O_UP + C * b, C)
    leaves(up, up_ref)
    for b in range(4):
        qkv[:, 128 * b : 128 * b + 128] = part(O_QKV + C * b, C)
    tail = part(O_QKV_TAIL, C // 2)
    qkv[: C // 2, 512:] = tail[:, :64]
    qkv[C // 2 :, 512:] = tail[:, 64:]
    leaves(qkv, qkv_ref)
    for side in range(2):
        terms = part(O_TABLE + TROWS * side, TROWS)
        for high in range(HIGH):
            start = high * LOW + side * LANES
            width = min(LANES, BPOS - start)
            for head in range(HEADS):
                row = high * TH + head * TYPES
                table[head, :, start : start + width] = terms[row : row + TYPES, :width]
    leaves(table, table_ref)
    proj[:, :128] = part(O_PROJ, C)
    tail = part(O_PROJ_TAIL, C // 2)
    proj[: C // 2, 128:] = tail[:, :64]
    proj[C // 2 :, 128:] = tail[:, 64:]
    leaves(proj, proj_ref)
    merge[MSPLIT:, 256:] = part(O_MERGE_LAST, MLP - MSPLIT)
    leaves(merge.at[MSPLIT:, 256:], merge_ref.at[MSPLIT:, 256:])


def second_half(part, refs, staged, leaves):
    _, _, _, down_ref, _, merge_ref, _, _ = refs
    _, down, _, merge, _, _ = staged
    for b in range(2):
        merge[:, 128 * b : 128 * b + 128] = part(O_MERGE + MLP * b, MLP)
    leaves(merge.at[:, :256], merge_ref.at[:, :256])
    for b in range(6):
        down[:, 128 * b : 128 * b + 128] = part(O_DOWN + C * b, C)
    leaves(down, down_ref)
    merge[:MSPLIT, 256:] = part(O_MERGE + 2 * MLP, MSPLIT)
    leaves(merge.at[:MSPLIT, 256:], merge_ref.at[:MSPLIT, 256:])


def scaled(factor, half, sums_ref, outs, staged, sems):
    for which, fill, base in ((0, first_half, 0), (1, second_half, O_MERGE)):

        @pl.when(half == which)
        def _():
            begun = []

            def part(start, rows):
                return sums_ref[start - base : start - base + rows, :].astype(F32) * factor

            def leaves(source, target):
                begun.append(pltpu.make_async_copy(source, target, sems.at[len(begun)]))
                begun[-1].start()

            fill(part, outs, staged, leaves)
            for copy in begun:
                copy.wait()


def finish_own_kernel(
    factor, core_ref, held_ref, partner_ref, forwarded_ref, merged_keep_ref, field_keep_ref, *refs
):
    outs, staged, (sems, merged, field) = refs[:8], refs[8:14], refs[14:]
    core = core_ref[0]
    east = jnp.where(core == 0, partner_ref[...].astype(F32), forwarded_ref[...].astype(F32))
    for level in range(LEVELS):
        field[level, HALF:] = east[:HALF, :, C * level : C * (level + 1)].astype(BF)
    field[:, :HALF] = field_keep_ref[...]
    copies = [pltpu.make_async_copy(field, outs[1], sems.at[5])]
    copies[-1].start()
    cells = east[HALF:].reshape(72, 2 * C)
    for lat in range(12):
        for lon in range(HALF // 2):
            row = (lat * 3 + lon) * 2
            merged[lat, HALF // 2 + lon] = cells[row : row + 2].astype(BF)
    merged[:, : HALF // 2] = merged_keep_ref[...]
    copies.append(pltpu.make_async_copy(merged, outs[0], sems.at[6]))
    copies[-1].start()
    scaled(factor, core, held_ref, outs, staged, sems)
    for copy in copies:
        copy.wait()


def finish_other_kernel(factor, core_ref, other_ref, *refs):
    outs, staged, sems = refs[6:12], refs[12:18], refs[18]
    scaled(factor, 1 - core_ref[0], other_ref, (None, None, *outs), staged, sems)


def finish(core, held, other, cells, factor):
    shape = jax.ShapeDtypeStruct
    whole = pl.BlockSpec(memory_space=pltpu.VMEM)
    scalar = pl.BlockSpec(memory_space=pltpu.SMEM)
    place = pl.BlockSpec(memory_space=pl.ANY)
    sums = [
        shape((C, MLP), F32),
        shape((C, MLP), F32),
        shape((C, 3 * C), F32),
        shape((MLP, 2 * C), F32),
        shape((C, C), F32),
        shape((HEADS, TYPES, BPOS), F32),
    ]
    scratch = [pltpu.VMEM(item.shape, F32) for item in sums] + [pltpu.SemaphoreType.DMA((7,))]
    grid = [shape((12, HALF, LEVELS, 2 * C), BF), shape((LEVELS, 2 * HALF, LAT, C), BF)]
    params = pltpu.CompilerParams(vmem_limit_bytes=16 * 1024 * 1024)
    merged, field, *begun = pl.pallas_call(
        lambda *refs: finish_own_kernel(factor, *refs),
        out_shape=[*grid, *sums],
        in_specs=[scalar] + [whole] * 5,
        out_specs=[place] * 8,
        scratch_shapes=scratch + [pltpu.VMEM(item.shape, BF) for item in grid],
        compiler_params=params,
        cost_estimate=pl.CostEstimate(flops=400_000, bytes_accessed=2_500_000, transcendentals=0),
        name="finish_own",
    )(core, held, *cells)
    rest = pl.pallas_call(
        lambda *refs: finish_other_kernel(factor, *refs),
        out_shape=sums,
        in_specs=[scalar, whole] + [place] * 6,
        out_specs=[place] * 6,
        scratch_shapes=scratch,
        input_output_aliases={2 + n: n for n in range(6)},
        compiler_params=params,
        name="finish_other",
    )(core, other, *begun)
    return merged, field, *rest


def passed_along(value, axis, steps):
    count = lax.axis_size(axis)
    return lax.ppermute(value, axis, [(source, (source + steps) % count) for source in range(count)])


def groups_of(count, apart, size):
    return [
        [start * apart * size + offset + member * apart for member in range(size)]
        for start in range(count // (apart * size))
        for offset in range(apart)
    ]


def summed_over(keep, send, axis, joined, partner, forward):
    count = lax.axis_size(axis)
    along = count // (CORES * ACROSS)
    pairs = [(i, i ^ 1) for i in range(count)]
    arrived = lax.ppermute(send, axis, pairs)
    held = joined(keep, arrived)

    def exchanged(value, apart, size):
        return lax.all_to_all(value, axis, 0, 0, axis_index_groups=groups_of(count, apart, size))

    def reduced(value, apart, size):
        got = exchanged(value.reshape(size, -1, *value.shape[1:]), apart, size)
        return jnp.sum(got.astype(F32), axis=0).astype(BF)

    def gathered(value, apart, size):
        return exchanged(jnp.broadcast_to(value[None], (size, *value.shape)), apart, size).reshape(-1, *value.shape[1:])

    held = reduced(held, CORES, ACROSS)
    held, partner = lax.optimization_barrier((held, partner))
    held = reduced(held.reshape(-1, 2, LANES), CORES * ACROSS, along)
    held = gathered(held, CORES * ACROSS, along).reshape(-1, LANES)
    held, forwarded = forward(held, partner)
    held = gathered(held, CORES, ACROSS)
    return held, lax.ppermute(held, axis, pairs), partner, forwarded


def local(
    fields,
    norm_gain,
    qkv_weight,
    proj_weight,
    bias_table,
    bias_index,
    region_ids,
    mlp_gain,
    up_weight,
    down_weight,
    merge_gain,
    merge_weight,
    cotangent,
):
    count = lax.axis_size("lon")
    core = (lax.axis_index("lon") % CORES).astype(jnp.int32).reshape(1)
    by_lon = fields.transpose(0, 2, 1, 3)
    by_lat = cotangent.transpose(1, 2, 0, 3)
    field_last, cotangent_last, table, index, merge_gain = stage(
        by_lon, by_lat, bias_table.transpose(1, 0, 2), bias_index, merge_gain
    )
    west = passed_along(field_last, "lon", 1)
    west_cotangent = passed_along(cotangent_last, "lon", 1)
    table, core = lax.optimization_barrier((table, core))
    bias, bias_tail = bias_rows(table, index, region_ids)
    half_rows = -(-O_END // (count * 2)) * 2 * count // CORES
    grads, tokens, scores, *results = block(
        half_rows,
        by_lon,
        west,
        by_lat,
        west_cotangent,
        norm_gain.reshape(1, C),
        qkv_weight,
        proj_weight,
        mlp_gain.reshape(1, C),
        up_weight,
        down_weight.T,
        merge_gain,
        merge_weight,
        bias,
        bias_tail,
    )
    pairs = [(i, i ^ 1) for i in range(count)]
    partner_scores = lax.ppermute(scores, "lon", pairs)
    keep, send = pack(core, grads, tokens, results[1])
    merged_keep, field_keep, home = to_grid(*results, qkv_weight, norm_gain.reshape(1, C), merge_weight)
    partner = lax.ppermute(home, "lon", pairs)

    def forward(held, leaving):
        held, leaving = lax.optimization_barrier((held, leaving))
        return held, lax.ppermute(leaving, "lon", [(i, (i - CORES) % count) for i in range(1, count, CORES)])

    table = table_sum(core, scores, partner_scores, index)
    held, other, partner, forwarded = summed_over(
        keep, send, "lon", lambda kept, arrived: join(core, kept, arrived, table), partner, forward
    )
    factor = float(LEVELS * LAT * fields.shape[2] * count) ** (-0.5)
    merged, field_grad, up_grad, down_grad, qkv_grad, merge_grad, proj_grad, table_grad = finish(
        core, held, other, (partner, forwarded, merged_keep, field_keep), factor
    )
    return (
        merged.transpose(2, 0, 1, 3),
        field_grad.transpose(0, 2, 1, 3),
        qkv_grad,
        proj_grad,
        up_grad,
        down_grad.T,
        merge_grad,
        table_grad.transpose(1, 0, 2),
    )


def solution(mesh):
    whole = P("groups", None, "lon", None)

    return jax.shard_map(
        local,
        mesh=mesh,
        in_specs=(whole, *[P()] * 11, whole),
        out_specs=(whole, whole, *[P("groups", None)] * 5, P("groups", None, None)),
        check_vma=False,
    )
```

```python
import jax
import jax.numpy as jnp
from jax import lax
from jax.experimental import pallas as pl
from jax.experimental.pallas import tpu as pltpu
from jax.sharding import PartitionSpec as P

C = 192
MLP = 768
HEADS = 6
HEAD = 32
HALF = 6
WIN = 144
BPOS = 3312
LAT = 24
TYPES = 4
TOK = TYPES * WIN
LEVELS = 2
LANES = 128
MAIN = 128
REST = WIN - MAIN
TH = TYPES * HEADS
LOW = 256
HIGH = -(-BPOS // LOW)
MTOK = 160
EPS = 1e-5
MASKED = -1e30
F32 = jnp.float32
BF = jnp.bfloat16
CORES = 2
ACROSS = 4

TROWS = 320
MSPLIT = 512
O_UP = 0
O_QKV = O_UP + 6 * C
O_QKV_TAIL = O_QKV + 4 * C
O_PROJ = O_QKV_TAIL + C // 2
O_PROJ_TAIL = O_PROJ + C
O_TABLE = O_PROJ_TAIL + C // 2
O_MERGE_LAST = O_TABLE + 2 * TROWS
O_MERGE = O_MERGE_LAST + MLP - MSPLIT
O_DOWN = O_MERGE + 2 * MLP + MSPLIT
O_END = O_DOWN + 6 * C

DS_TAIL = TH * WIN
DS_CORNER = DS_TAIL + TH * REST
DS_END = DS_CORNER + TH * REST


def dot(a, b):
    return jnp.dot(a, b, preferred_element_type=F32)


def dot_nt(a, b):
    return lax.dot_general(a, b, (((1,), (1,)), ((), ())), preferred_element_type=F32)


def dot_tn(a, b):
    return lax.dot_general(a, b, (((0,), (0,)), ((), ())), preferred_element_type=F32)


def div(n, d):
    return (n * -(-(1 << 16) // d)) >> 16


def onehot(rows, cols, of_row=None, of_col=None):
    if of_row is not None:
        target = of_row(lax.broadcasted_iota(jnp.int32, (rows, 1), 0))
        place = lax.broadcasted_iota(jnp.int32, (rows, cols), 1)
    else:
        target = of_col(lax.broadcasted_iota(jnp.int32, (1, cols), 1))
        place = lax.broadcasted_iota(jnp.int32, (rows, cols), 0)
    return jnp.where(place == target, 1.0, 0.0).astype(BF)


def cell_of_token(n):
    kind = div(n, 72)
    rest = n - 72 * kind
    lat = div(rest, 12)
    return (rest - 12 * lat) * LAT + kind * 6 + lat


def token_of_group(n):
    quarter = div(n, 40)
    rest = n - 40 * quarter
    level = div(rest, 18)
    part = rest - 18 * level
    lat = div(part, 6)
    token = level * 72 + (2 * lat + (quarter >> 1)) * 12 + 2 * (part - 6 * lat) + (quarter & 1)
    return jnp.where(rest < 36, token, -1)


def group_of_token(n):
    level = div(n, 72)
    rest = n - 72 * level
    lat = div(rest, 12)
    lon = rest - 12 * lat
    return ((lat & 1) * 2 + (lon & 1)) * 40 + level * 18 + (lat >> 1) * 6 + (lon >> 1)


def cell_of_merged(n):
    kind = div(n, 40)
    rest = n - 40 * kind
    level = div(rest, 18)
    part = rest - 18 * level
    lat = div(part, 6)
    lon = part - 6 * lat
    half = jnp.where(lon < 3, 0, 1)
    row = half * 72 + (3 * kind + lat) * 6 + (lon - 3 * half) * 2 + level
    return jnp.where(rest < 36, row, -1)


def normalised(values):
    centred = values - jnp.mean(values, axis=-1, keepdims=True)
    scale = lax.rsqrt(jnp.mean(centred * centred, axis=-1, keepdims=True) + EPS)
    return centred * scale, scale


def norm_grad(grad, unit, scale, gain):
    scaled = grad * gain
    return scale * (
        scaled
        - jnp.mean(scaled, axis=-1, keepdims=True)
        - unit * jnp.mean(scaled * unit, axis=-1, keepdims=True)
    )


def rounded(values):
    return values.astype(BF).astype(F32)


def low_onehot(low):
    place = lax.broadcasted_iota(jnp.int32, (LOW, 1), 0).astype(F32).astype(BF)
    hit = jnp.broadcast_to(place, (LOW, low.shape[1])) == low.astype(F32).astype(BF)
    return jnp.where(hit, jnp.array(1, BF), jnp.array(0, BF))


def bias_kernel(table_ref, index_ref, regions_ref, main_ref, tail_ref, part_ref, last_ref, turned_ref, mask_ref, region_ref, sem):
    copy = pltpu.make_async_copy(regions_ref, region_ref, sem)
    copy.start()
    for high in range(HIGH):
        width = min(LOW, BPOS - high * LOW)
        for head in range(HEADS):
            piece = table_ref[head, :, high * LOW : high * LOW + width]
            if width < LOW:
                piece = jnp.concatenate([piece, jnp.zeros((TYPES, LOW - width), F32)], axis=1)
            row = high * TH + head * TYPES
            part_ref[row : row + TYPES, :] = piece
    turned_ref[...] = jnp.transpose(index_ref[:, MAIN:])
    parts = part_ref[...].astype(BF)

    def looked_up(index):
        low = low_onehot(index & (LOW - 1))
        high_row = index >> 8
        found = dot(parts, low)
        chosen = found[0:TH]
        for high in range(1, HIGH):
            chosen = jnp.where(high_row == high, found[high * TH : (high + 1) * TH], chosen)
        return chosen

    for start in range(0, REST, 4):
        got = looked_up(jnp.concatenate([turned_ref[start + n : start + n + 1, :MAIN] for n in range(4)], axis=1))
        for n in range(4):
            last_ref[pl.ds(start + n, TH, stride=REST), :] = got[:, n * MAIN : (n + 1) * MAIN]
    got = looked_up(jnp.concatenate([turned_ref[n : n + 1, MAIN:] for n in range(REST)], axis=1))
    for n in range(REST):
        half = got[:, LANES * (n // 8) : LANES * (n // 8 + 1)]
        half = half if n % 8 == 0 else pltpu.roll(half, LANES - REST * (n % 8), 1)
        last_ref[pl.ds(TH * REST + n, TH, stride=REST), :] = half
    copy.wait()
    kind_of = lax.broadcasted_iota(jnp.int32, (TH, 1), 0) & (TYPES - 1)
    column = lax.broadcasted_iota(jnp.int32, (1, LANES), 1)
    labels = []
    for group in range(12):
        label = jnp.zeros((TH, 1), jnp.int32)
        for kind in range(TYPES):
            label = jnp.where(kind_of == kind, region_ref[group // 6, 6 * kind + group % 6], label)
        labels.append(label)
    keys = jnp.zeros((TH, LANES), jnp.int32)
    for group in range(11):
        keys = jnp.where((column >= 12 * group) & (column < 12 * group + 12), labels[group], keys)
    for group in range(12):
        mask_ref[TH * group : TH * (group + 1), :] = jnp.where(keys == labels[group], 0.0, MASKED)

    def row_block(block, carry):
        base = pl.multiple_of(block * 8, 8)
        rows = index_ref[pl.ds(base, 8), :MAIN]
        for part in range(2):
            index = jnp.concatenate([rows[4 * part + n : 4 * part + n + 1] for n in range(4)], axis=1)
            got = looked_up(index)
            for n in range(4):
                row = base + 4 * part + n
                mask = mask_ref[pl.ds(pl.multiple_of(div(row, 12) * TH, 8), TH), :]
                main_ref[pl.ds(row, TH, stride=WIN), :] = got[:, n * MAIN : (n + 1) * MAIN] + mask
        return carry

    lax.fori_loop(0, WIN // 8, row_block, 0, unroll=True)
    apart = jnp.where(labels[10] == labels[11], 0.0, MASKED)
    split = 132 - MAIN
    for n in range(REST):
        group = (MAIN + n) // 12
        rows = pl.ds(n, TH, stride=REST)
        last_ref[rows, :] = last_ref[rows, :] + mask_ref[TH * group : TH * (group + 1), :]
        rows = pl.ds(TH * REST + n, TH, stride=REST)
        other = (column < split) if n >= split else (column >= split)
        last_ref[rows, :] = last_ref[rows, :] + jnp.where(other, apart, 0.0)
    for th in range(TH):
        rows = slice(th * WIN, th * WIN + MAIN)
        tail_ref[rows, :REST] = jnp.transpose(last_ref[th * REST : (th + 1) * REST, :])
        rows = slice(th * WIN + MAIN, (th + 1) * WIN)
        tail_ref[rows, :REST] = jnp.transpose(last_ref[(TH + th) * REST : (TH + th + 1) * REST, :])[:REST]


def stage_kernel(fields_ref, cotangent_ref, table_ref, index_ref, gain_ref, field_ref, half_ref, table_out, index_out, gain_out, sems):
    copies = [
        pltpu.make_async_copy(source, target, sems.at[n])
        for n, (source, target) in enumerate(
            [
                (fields_ref.at[:, HALF:], field_ref),
                (cotangent_ref.at[:, HALF // 2 :], half_ref),
                (table_ref, table_out),
                (index_ref, index_out),
                (gain_ref, gain_out.at[0]),
            ]
        )
    ]
    for copy in copies:
        copy.start()
    for copy in copies:
        copy.wait()


def stage(fields, cotangent, table, index, gain):
    shape = jax.ShapeDtypeStruct
    whole = pl.BlockSpec(memory_space=pltpu.VMEM)
    return pl.pallas_call(
        stage_kernel,
        out_shape=[
            shape((LEVELS, HALF, LAT, C), BF),
            shape((12, HALF // 2, LEVELS, 2 * C), BF),
            shape(table.shape, F32),
            shape(index.shape, jnp.int32),
            shape((1, 4 * C), F32),
        ],
        in_specs=[pl.BlockSpec(memory_space=pltpu.HBM)] * 5,
        out_specs=[whole] * 5,
        scratch_shapes=[pltpu.SemaphoreType.DMA((5,))],
        compiler_params=pltpu.CompilerParams(vmem_limit_bytes=4 * 1024 * 1024),
        name="stage",
    )(*(pltpu.with_memory_space_constraint(a, pltpu.HBM) for a in (fields, cotangent, table, index, gain)))


def bias_rows(table, index, regions):
    whole = pl.BlockSpec(memory_space=pltpu.VMEM)
    return pl.pallas_call(
        bias_kernel,
        out_shape=[jax.ShapeDtypeStruct((TH * WIN, LANES), F32)] * 2,
        in_specs=[whole, whole, pl.BlockSpec(memory_space=pltpu.HBM)],
        out_specs=[whole, whole],
        scratch_shapes=[
            pltpu.VMEM((HIGH * TH, LOW), F32),
            pltpu.VMEM((2 * TH * REST, LANES), F32),
            pltpu.VMEM((REST, WIN), jnp.int32),
            pltpu.VMEM((12 * TH, LANES), F32),
            pltpu.SMEM((LEVELS, LAT), jnp.int32),
            pltpu.SemaphoreType.DMA,
        ],
        compiler_params=pltpu.CompilerParams(vmem_limit_bytes=16 * 1024 * 1024),
        cost_estimate=pl.CostEstimate(flops=14_000_000_000, bytes_accessed=4_000_000, transcendentals=0),
        name="bias_rows",
    )(table, index, pltpu.with_memory_space_constraint(regions, pltpu.HBM))


def block_kernel(
    own_ref, west_ref, own_cotangent_ref, west_cotangent_ref,
    norm_gain_ref, qkv_ref, proj_ref, mlp_gain_ref, up_ref, down_ref, merge_gain_ref, merge_ref,
    bias_ref, bias_tail_ref,
    grads_ref, tokens_ref, ds_ref, normed_merge_ref, triple_ref, grad_attn_ref, unit_ref, scale_ref,
    x_ref, q_ref, k_ref, v_ref, p_ref, mixed_ref,
    unit_mlp_ref, scale_mlp_ref, normed_mlp_ref, hidden_ref, slope_ref, after_mlp_ref,
    group_ref, grad_after_ref, grad_up_ref, grad_mixed_ref,
    cells_ref, grad_merged_ref, scaled_ref,
):
    to_tokens = onehot(288, 288, of_row=cell_of_token)
    for level in range(LEVELS):
        cells = jnp.concatenate(
            [
                west_ref[level].astype(F32).reshape(144, C),
                own_ref[level, :HALF].astype(F32).reshape(144, C),
            ],
            axis=0,
        ).astype(BF)
        ordered = dot(to_tokens, cells)
        for kind in range(TYPES):
            x_ref[WIN * kind + 72 * level : WIN * kind + 72 * level + 72, :] = ordered[72 * kind : 72 * kind + 72]
    for lat in range(12):
        for lon in range(HALF // 2):
            row = (lat * 3 + lon) * 2
            cells_ref[row : row + 2, :] = west_cotangent_ref[lat, lon].astype(F32)
            cells_ref[72 + row : 74 + row, :] = own_cotangent_ref[lat, lon].astype(F32)
    grad_merged_ref[...] = dot(onehot(MTOK, 144, of_row=cell_of_merged), cells_ref[...].astype(BF)).astype(BF)
    for n in range(4):
        value = rounded(dot_nt(grad_merged_ref[...], merge_ref[C * n : C * (n + 1), :]))
        scaled_ref[n] = value * merge_gain_ref[:, C * n : C * (n + 1)]
    unit, scale = normalised(x_ref[...])
    unit_ref[...] = unit
    scale_ref[...] = scale
    tokens = (unit * norm_gain_ref[...]).astype(BF)
    tokens_ref[...] = tokens
    q_ref[...] = dot(tokens, qkv_ref[:, 0:C]).astype(BF)
    k_ref[...] = dot(tokens, qkv_ref[:, C : 2 * C]).astype(BF)
    v_ref[...] = dot(tokens, qkv_ref[:, 2 * C :]).astype(BF)
    lane = lax.broadcasted_iota(jnp.int32, (1, C), 1)
    of_head = [
        jnp.where((lane >= HEAD * h) & (lane < HEAD * (h + 1)), 1.0, 0.0).astype(BF) for h in range(HEADS)
    ]
    temper = HEAD ** (-0.5)

    def attend(kind, carry):
        rows = pl.ds(pl.multiple_of(kind * WIN, 16), WIN)
        q, k, v = q_ref[rows, :], k_ref[rows, :], v_ref[rows, :]
        mixed = jnp.zeros((WIN, C), F32)
        products = dot_nt(jnp.concatenate([q * of_head[h] for h in range(HEADS)], axis=0), k)
        for h in range(HEADS):
            th = h * TYPES + kind
            scores_at = pl.ds(pl.multiple_of(th * WIN, 16), WIN)
            bias = jnp.concatenate([bias_ref[scores_at, :], bias_tail_ref[scores_at, :REST]], axis=1)
            scores = products[WIN * h : WIN * (h + 1)] * temper + bias
            weights = jnp.exp(scores - jnp.max(scores, axis=-1, keepdims=True))
            p = weights * (1.0 / jnp.sum(weights, axis=-1, keepdims=True))
            p_ref[th] = p
            mixed = mixed + dot(p.astype(BF), v * of_head[h])
        mixed_ref[rows, :] = mixed.astype(BF)
        return carry

    lax.fori_loop(0, TYPES, attend, 0, unroll=True)
    after_attn = rounded(x_ref[...] + rounded(dot(mixed_ref[...], proj_ref[...])))
    x_ref[...] = after_attn
    unit, scale = normalised(after_attn)
    unit_mlp_ref[...] = unit
    scale_mlp_ref[...] = scale
    normed_mlp = (unit * mlp_gain_ref[...]).astype(BF)
    normed_mlp_ref[...] = normed_mlp
    for part in range(3):
        cols = slice(256 * part, 256 * part + 256)
        u = dot(normed_mlp, up_ref[:, cols])
        below = 0.5 * (1.0 + lax.erf(u * 0.5**0.5))
        hidden_ref[:, cols] = (u * below).astype(BF)
        slope_ref[:, cols] = below + u * (jnp.exp(u * u * (-0.5)) * 0.3989422804014327)
    after_mlp_ref[...] = (x_ref[...] + dot_nt(hidden_ref[...], down_ref[...])).astype(BF)

    to_groups = onehot(160, WIN, of_row=token_of_group)
    for kind in range(TYPES):
        grouped = dot(to_groups, after_mlp_ref[WIN * kind : WIN * kind + WIN, :])
        for quarter in range(4):
            group_ref[quarter, 40 * kind : 40 * kind + 40, :] = grouped[40 * quarter : 40 * quarter + 40]
    quarters = [group_ref[n] for n in range(4)]
    mean = jnp.sum(sum(quarters), axis=-1, keepdims=True) * (1.0 / MLP)
    centred = [v - mean for v in quarters]
    variance = jnp.sum(sum(v * v for v in centred), axis=-1, keepdims=True) * (1.0 / MLP)
    scale_merge = lax.rsqrt(variance + EPS)
    for n in range(4):
        unit = centred[n] * scale_merge
        group_ref[n] = unit
        normed_merge = (unit * merge_gain_ref[:, C * n : C * (n + 1)]).astype(BF)
        normed_merge_ref[n] = normed_merge
    scaled, total, along = [], 0.0, 0.0
    for n in range(4):
        value = scaled_ref[n]
        total = total + value
        along = along + value * group_ref[n]
        scaled.append(value)
    total = jnp.sum(total, axis=-1, keepdims=True) * (1.0 / MLP)
    along = jnp.sum(along, axis=-1, keepdims=True) * (1.0 / MLP)
    for n in range(4):
        group_ref[n] = scale_merge * (scaled[n] - total - group_ref[n] * along)
    from_groups = onehot(WIN, 160, of_row=group_of_token)
    for kind in range(TYPES):
        grouped = jnp.concatenate([group_ref[n, 40 * kind : 40 * kind + 40, :] for n in range(4)], axis=0)
        grad_after_ref[WIN * kind : WIN * kind + WIN, :] = dot(from_groups, grouped.astype(BF)).astype(BF)

    grad_after = grad_after_ref[...]
    for part in range(3):
        cols = slice(256 * part, 256 * part + 256)
        grad_up_ref[:, cols] = (rounded(dot(grad_after, down_ref[:, cols])) * slope_ref[:, cols]).astype(BF)
    grad_normed = rounded(dot_nt(grad_up_ref[...], up_ref[...]))
    grad_attn = (
        grad_after.astype(F32)
        + norm_grad(grad_normed, unit_mlp_ref[...], scale_mlp_ref[...], mlp_gain_ref[...])
    ).astype(BF)
    grad_attn_ref[...] = grad_attn

    grad_mixed_ref[...] = dot_nt(grad_attn, proj_ref[...]).astype(BF)

    def down_terms():
        grad = dot_tn(grad_after_ref[...], hidden_ref[...]).astype(BF)
        for b in range(6):
            grads_ref[O_DOWN + C * b : O_DOWN + C * (b + 1), :] = grad[:, 128 * b : 128 * b + 128]

    def up_terms():
        grad = dot_tn(normed_mlp_ref[...], grad_up_ref[...]).astype(BF)
        for b in range(6):
            grads_ref[O_UP + C * b : O_UP + C * (b + 1), :] = grad[:, 128 * b : 128 * b + 128]

    def merge_terms():
        for n in range(4):
            grad = dot_tn(normed_merge_ref[n], grad_merged_ref[...]).astype(BF)
            for b in range(2):
                start = O_MERGE + MLP * b + C * n
                grads_ref[start : start + C, :] = grad[:, 128 * b : 128 * b + 128]
            kept = max(0, min(C, MSPLIT - C * n))
            if kept:
                start = O_MERGE + 2 * MLP + C * n
                grads_ref[start : start + kept, :] = grad[:kept, 256:]
            if kept < C:
                start = O_MERGE_LAST + C * n + kept - MSPLIT
                grads_ref[start : start + C - kept, :] = grad[kept:, 256:]

    def proj_terms():
        grad_proj = dot_tn(mixed_ref[...], grad_attn_ref[...]).astype(BF)
        grads_ref[O_PROJ : O_PROJ + C, :] = grad_proj[:, :128]
        grads_ref[O_PROJ_TAIL : O_PROJ_TAIL + C // 2, :] = jnp.concatenate(
            [grad_proj[: C // 2, 128:], grad_proj[C // 2 :, 128:]], axis=1
        )

    last_keys = onehot(REST, WIN, of_row=lambda n: n + MAIN)
    ds_ref[DS_CORNER:, :] = jnp.zeros((TH * REST, LANES), BF)
    grads_ref[O_QKV:O_PROJ, :] = jnp.zeros((O_PROJ - O_QKV, LANES), BF)
    grads_ref[O_TABLE:O_MERGE_LAST, :] = jnp.zeros((O_MERGE_LAST - O_TABLE, LANES), BF)

    def attend_back(kind, carry):
        rows = pl.ds(kind * WIN, WIN)
        v, grad = v_ref[rows, :], grad_mixed_ref[rows, :]
        q_turned, k_turned, grad_turned = (jnp.transpose(a) for a in (q_ref[rows, :], k_ref[rows, :], grad))
        products = dot_nt(jnp.concatenate([grad * of_head[h] for h in range(HEADS)], axis=0), v)
        dq, dk, dv = [], [], []
        for h in range(HEADS):
            th = h * TYPES + kind
            lanes = slice(HEAD * h, HEAD * (h + 1))
            p = p_ref[th]
            weighted = p * products[WIN * h : WIN * (h + 1)]
            ds = weighted - p * jnp.sum(weighted, axis=-1, keepdims=True)
            ds = ds.astype(BF)
            ds_ref[pl.ds(th * WIN, WIN), :] = ds[:, :MAIN]
            turned = dot_nt(jnp.concatenate([k_turned[lanes], last_keys], axis=0), ds)
            tail = turned[HEAD:].astype(BF)
            ds_ref[pl.ds(DS_TAIL + th * REST, REST), :] = tail[:, :MAIN]
            ds_ref[pl.ds(DS_CORNER + th * REST, REST), :REST] = tail[:, MAIN:]
            dq.append(turned[:HEAD])
            dk.append(dot(q_turned[lanes], ds))
            dv.append(dot(grad_turned[lanes], p.astype(BF)))
        triple = jnp.concatenate([a * temper for a in dq + dk] + dv, axis=0).astype(BF)
        triple_ref[rows, :] = jnp.transpose(triple)
        return carry

    for kind, terms in enumerate((down_terms, up_terms, merge_terms, proj_terms)):
        attend_back(kind, 0)
        terms()


def block(half_rows, *args):
    shape = jax.ShapeDtypeStruct
    whole = pl.BlockSpec(memory_space=pltpu.VMEM)
    scratch = [
        ((TOK, C), F32), ((TOK, C), BF), ((TOK, C), BF),
        ((TOK, C), BF), ((TH, WIN, WIN), F32), ((TOK, C), BF),
        ((TOK, C), F32), ((TOK, 1), F32), ((TOK, C), BF), ((TOK, MLP), BF), ((TOK, MLP), F32), ((TOK, C), BF),
        ((4, MTOK, C), F32), ((TOK, C), BF), ((TOK, MLP), BF), ((TOK, C), BF),
        ((144, 2 * C), F32), ((MTOK, 2 * C), BF), ((4, MTOK, C), F32),
    ]
    return pl.pallas_call(
        block_kernel,
        out_shape=[
            shape((2 * half_rows, LANES), BF),
            shape((TOK, C), BF),
            shape((DS_END, LANES), BF),
            shape((4, MTOK, C), BF),
            shape((TOK, 3 * C), BF),
            shape((TOK, C), BF),
            shape((TOK, C), F32),
            shape((TOK, 1), F32),
        ],
        in_specs=[whole] * len(args),
        out_specs=[whole] * 8,
        scratch_shapes=[pltpu.VMEM(*item) for item in scratch],
        compiler_params=pltpu.CompilerParams(vmem_limit_bytes=24 * 1024 * 1024),
        cost_estimate=pl.CostEstimate(flops=24_000_000_000, bytes_accessed=12_000_000, transcendentals=2_000_000),
        name="block",
    )(*args)


def pack_kernel(core_ref, grads_ref, tokens_ref, triple_ref, keep_ref, send_ref):
    half = keep_ref.shape[0]
    core = core_ref[0]
    grad_qkv = dot_tn(tokens_ref[...], triple_ref[...]).astype(BF)
    tail = jnp.concatenate([grad_qkv[: C // 2, 512:], grad_qkv[C // 2 :, 512:]], axis=1)
    keep_ref[...] = grads_ref[pl.ds(pl.multiple_of(core * half, 16), half), :]
    send_ref[...] = grads_ref[pl.ds(pl.multiple_of((1 - core) * half, 16), half), :]
    for owner, target_ref in ((0, keep_ref), (1, send_ref)):

        @pl.when(core == owner)
        def _():
            for b in range(4):
                target_ref[O_QKV + C * b : O_QKV + C * (b + 1), :] = grad_qkv[:, 128 * b : 128 * b + 128]
            target_ref[O_QKV_TAIL : O_QKV_TAIL + C // 2, :] = tail


def pack(core, grads, tokens, triple):
    half = jax.ShapeDtypeStruct((grads.shape[0] // 2, LANES), BF)
    whole = pl.BlockSpec(memory_space=pltpu.VMEM)
    return pl.pallas_call(
        pack_kernel,
        out_shape=[half, half],
        in_specs=[pl.BlockSpec(memory_space=pltpu.SMEM)] + [whole] * 3,
        out_specs=[whole] * 2,
        compiler_params=pltpu.CompilerParams(vmem_limit_bytes=12 * 1024 * 1024),
        cost_estimate=pl.CostEstimate(flops=600_000_000, bytes_accessed=4_000_000, transcendentals=0),
        name="pack",
    )(core, grads, tokens, triple)


def table_kernel(core_ref, own_ref, partner_ref, index_ref, table_ref, ds_ref, turned_ref):
    def table_terms(index, slab):
        high_row = index >> 8
        spread = [jnp.where(high_row == n, slab, 0.0) for n in range(HIGH)]
        spread.append(jnp.zeros((TROWS - HIGH * TH, index.shape[1]), F32))
        return dot_nt(jnp.concatenate(spread, axis=0).astype(BF), low_onehot(index & (LOW - 1)))

    def row_block(block, carry):
        base = pl.multiple_of(block * 8, 8)
        rows = index_ref[pl.ds(base, 8), :MAIN]
        index = jnp.concatenate([rows[n : n + 1] for n in range(8)], axis=1)
        slab = jnp.concatenate([ds_ref[pl.ds(base + n, TH, stride=WIN), :] for n in range(8)], axis=1)
        return carry + table_terms(index, slab)

    @pl.when(core_ref[0] == 0)
    def _():
        ds_ref[...] = own_ref[...].astype(F32) + partner_ref[...].astype(F32)
        turned_ref[...] = jnp.transpose(index_ref[:, MAIN:])
        table = lax.fori_loop(0, WIN // 8, row_block, jnp.zeros((TROWS, LOW), F32), unroll=True)
        index = jnp.concatenate([turned_ref[n : n + 1, :MAIN] for n in range(REST)], axis=1)
        slab = jnp.concatenate([ds_ref[pl.ds(DS_TAIL + n, TH, stride=REST), :] for n in range(REST)], axis=1)
        table = table + table_terms(index, slab)
        index = jnp.concatenate([turned_ref[n : n + 1, MAIN:] for n in range(REST)], axis=1)
        slab = jnp.concatenate(
            [ds_ref[pl.ds(DS_CORNER + n, TH, stride=REST), :][:, :REST] for n in range(REST)], axis=1
        )
        table = (table + table_terms(index, slab)).astype(BF)
        table_ref[:TROWS, :] = table[:, :LANES]
        table_ref[TROWS:, :] = table[:, LANES:]

    @pl.when(core_ref[0] == 1)
    def _():
        table_ref[...] = jnp.zeros(table_ref.shape, BF)


def table_sum(core, own, partner, index):
    whole = pl.BlockSpec(memory_space=pltpu.VMEM)
    return pl.pallas_call(
        table_kernel,
        out_shape=jax.ShapeDtypeStruct((2 * TROWS, LANES), BF),
        in_specs=[pl.BlockSpec(memory_space=pltpu.SMEM)] + [whole] * 3,
        out_specs=whole,
        scratch_shapes=[pltpu.VMEM((DS_END, LANES), F32), pltpu.VMEM((REST, WIN), jnp.int32)],
        compiler_params=pltpu.CompilerParams(vmem_limit_bytes=12 * 1024 * 1024),
        cost_estimate=pl.CostEstimate(flops=4_000_000_000, bytes_accessed=3_000_000, transcendentals=0),
        name="table_sum",
    )(core, own, partner, index)


def join_kernel(core_ref, keep_ref, arrived_ref, table_ref, held_ref):
    held_ref[...] = (keep_ref[...].astype(F32) + arrived_ref[...].astype(F32)).astype(BF)

    @pl.when(core_ref[0] == 0)
    def _():
        held_ref[O_TABLE : O_TABLE + 2 * TROWS, :] = table_ref[...]


def join(core, keep, arrived, table):
    whole = pl.BlockSpec(memory_space=pltpu.VMEM)
    return pl.pallas_call(
        join_kernel,
        out_shape=jax.ShapeDtypeStruct(keep.shape, BF),
        in_specs=[pl.BlockSpec(memory_space=pltpu.SMEM)] + [whole] * 3,
        out_specs=whole,
        compiler_params=pltpu.CompilerParams(vmem_limit_bytes=8 * 1024 * 1024),
        cost_estimate=pl.CostEstimate(flops=400_000, bytes_accessed=2_500_000, transcendentals=0),
        name="join",
    )(core, keep, arrived, table)


def cells_kernel(
    normed_merge_ref, triple_ref, grad_attn_ref, unit_ref, scale_ref, qkv_ref, gain_ref, merge_ref,
    merged_keep_ref, field_keep_ref, home_ref, x_ref,
):
    merged = sum(dot(normed_merge_ref[n], merge_ref[C * n : C * (n + 1), :]) for n in range(4))
    grad_normed = rounded(dot_nt(triple_ref[...], qkv_ref[...]))
    merged_cells = dot(onehot(144, MTOK, of_col=cell_of_merged), merged.astype(BF))
    x_ref[...] = grad_attn_ref[...].astype(F32) + norm_grad(
        grad_normed, unit_ref[...], scale_ref[...], gain_ref[...]
    )
    to_cells = onehot(288, 288, of_col=cell_of_token)
    leaving = []
    for level in range(LEVELS):
        ordered = jnp.concatenate(
            [x_ref[WIN * kind + 72 * level : WIN * kind + 72 * level + 72, :] for kind in range(TYPES)], axis=0
        )
        cells = dot(to_cells, ordered.astype(BF))
        leaving.append(cells[:144])
        field_keep_ref[level] = cells[144:].reshape(HALF, LAT, C).astype(BF)
    home_ref[:HALF] = jnp.concatenate(leaving, axis=1).reshape(HALF, LAT, 2 * C).astype(BF)
    for lat in range(12):
        for lon in range(HALF // 2):
            row = 72 + (lat * 3 + lon) * 2
            merged_keep_ref[lat, lon] = merged_cells[row : row + 2].astype(BF)
    home_ref[HALF:] = merged_cells[:72].reshape(3, LAT, 2 * C).astype(BF)


def to_grid(*args):
    shape = jax.ShapeDtypeStruct
    whole = pl.BlockSpec(memory_space=pltpu.VMEM)
    return pl.pallas_call(
        cells_kernel,
        out_shape=[
            shape((12, HALF // 2, LEVELS, 2 * C), BF),
            shape((LEVELS, HALF, LAT, C), BF),
            shape((HALF + 3, LAT, 2 * C), BF),
        ],
        in_specs=[whole] * 8,
        out_specs=[whole] * 3,
        scratch_shapes=[pltpu.VMEM((TOK, C), F32)],
        compiler_params=pltpu.CompilerParams(vmem_limit_bytes=12 * 1024 * 1024),
        cost_estimate=pl.CostEstimate(flops=1_500_000_000, bytes_accessed=3_000_000, transcendentals=0),
        name="to_grid",
    )(*args)


def first_half(part, refs, staged, leaves):
    _, _, up_ref, _, qkv_ref, merge_ref, proj_ref, table_ref = refs
    up, _, qkv, merge, proj, table = staged
    for b in range(6):
        up[:, 128 * b : 128 * b + 128] = part(O_UP + C * b, C)
    leaves(up, up_ref)
    for b in range(4):
        qkv[:, 128 * b : 128 * b + 128] = part(O_QKV + C * b, C)
    tail = part(O_QKV_TAIL, C // 2)
    qkv[: C // 2, 512:] = tail[:, :64]
    qkv[C // 2 :, 512:] = tail[:, 64:]
    leaves(qkv, qkv_ref)
    for side in range(2):
        terms = part(O_TABLE + TROWS * side, TROWS)
        for high in range(HIGH):
            start = high * LOW + side * LANES
            width = min(LANES, BPOS - start)
            for head in range(HEADS):
                row = high * TH + head * TYPES
                table[head, :, start : start + width] = terms[row : row + TYPES, :width]
    leaves(table, table_ref)
    proj[:, :128] = part(O_PROJ, C)
    tail = part(O_PROJ_TAIL, C // 2)
    proj[: C // 2, 128:] = tail[:, :64]
    proj[C // 2 :, 128:] = tail[:, 64:]
    leaves(proj, proj_ref)
    merge[MSPLIT:, 256:] = part(O_MERGE_LAST, MLP - MSPLIT)
    leaves(merge.at[MSPLIT:, 256:], merge_ref.at[MSPLIT:, 256:])


def second_half(part, refs, staged, leaves):
    _, _, _, down_ref, _, merge_ref, _, _ = refs
    _, down, _, merge, _, _ = staged
    for b in range(2):
        merge[:, 128 * b : 128 * b + 128] = part(O_MERGE + MLP * b, MLP)
    leaves(merge.at[:, :256], merge_ref.at[:, :256])
    for b in range(6):
        down[:, 128 * b : 128 * b + 128] = part(O_DOWN + C * b, C)
    leaves(down, down_ref)
    merge[:MSPLIT, 256:] = part(O_MERGE + 2 * MLP, MSPLIT)
    leaves(merge.at[:MSPLIT, 256:], merge_ref.at[:MSPLIT, 256:])


def scaled(factor, half, sums_ref, outs, staged, sems):
    for which, fill, base in ((0, first_half, 0), (1, second_half, O_MERGE)):

        @pl.when(half == which)
        def _():
            begun = []

            def part(start, rows):
                return sums_ref[start - base : start - base + rows, :].astype(F32) * factor

            def leaves(source, target):
                begun.append(pltpu.make_async_copy(source, target, sems.at[len(begun)]))
                begun[-1].start()

            fill(part, outs, staged, leaves)
            for copy in begun:
                copy.wait()


def finish_own_kernel(
    factor, core_ref, held_ref, partner_ref, forwarded_ref, merged_keep_ref, field_keep_ref, *refs
):
    outs, staged, (sems, merged, field) = refs[:8], refs[8:14], refs[14:]
    core = core_ref[0]
    east = jnp.where(core == 0, partner_ref[...].astype(F32), forwarded_ref[...].astype(F32))
    for level in range(LEVELS):
        field[level, HALF:] = east[:HALF, :, C * level : C * (level + 1)].astype(BF)
    field[:, :HALF] = field_keep_ref[...]
    copies = [pltpu.make_async_copy(field, outs[1], sems.at[5])]
    copies[-1].start()
    cells = east[HALF:].reshape(72, 2 * C)
    for lat in range(12):
        for lon in range(HALF // 2):
            row = (lat * 3 + lon) * 2
            merged[lat, HALF // 2 + lon] = cells[row : row + 2].astype(BF)
    merged[:, : HALF // 2] = merged_keep_ref[...]
    copies.append(pltpu.make_async_copy(merged, outs[0], sems.at[6]))
    copies[-1].start()
    scaled(factor, core, held_ref, outs, staged, sems)
    for copy in copies:
        copy.wait()


def finish_other_kernel(factor, core_ref, other_ref, *refs):
    outs, staged, sems = refs[6:12], refs[12:18], refs[18]
    scaled(factor, 1 - core_ref[0], other_ref, (None, None, *outs), staged, sems)


def finish(core, held, other, cells, factor):
    shape = jax.ShapeDtypeStruct
    whole = pl.BlockSpec(memory_space=pltpu.VMEM)
    scalar = pl.BlockSpec(memory_space=pltpu.SMEM)
    place = pl.BlockSpec(memory_space=pl.ANY)
    sums = [
        shape((C, MLP), F32),
        shape((C, MLP), F32),
        shape((C, 3 * C), F32),
        shape((MLP, 2 * C), F32),
        shape((C, C), F32),
        shape((HEADS, TYPES, BPOS), F32),
    ]
    scratch = [pltpu.VMEM(item.shape, F32) for item in sums] + [pltpu.SemaphoreType.DMA((7,))]
    grid = [shape((12, HALF, LEVELS, 2 * C), BF), shape((LEVELS, 2 * HALF, LAT, C), BF)]
    params = pltpu.CompilerParams(vmem_limit_bytes=16 * 1024 * 1024)
    merged, field, *begun = pl.pallas_call(
        lambda *refs: finish_own_kernel(factor, *refs),
        out_shape=[*grid, *sums],
        in_specs=[scalar] + [whole] * 5,
        out_specs=[place] * 8,
        scratch_shapes=scratch + [pltpu.VMEM(item.shape, BF) for item in grid],
        compiler_params=params,
        cost_estimate=pl.CostEstimate(flops=400_000, bytes_accessed=2_500_000, transcendentals=0),
        name="finish_own",
    )(core, held, *cells)
    rest = pl.pallas_call(
        lambda *refs: finish_other_kernel(factor, *refs),
        out_shape=sums,
        in_specs=[scalar, whole] + [place] * 6,
        out_specs=[place] * 6,
        scratch_shapes=scratch,
        input_output_aliases={2 + n: n for n in range(6)},
        compiler_params=params,
        name="finish_other",
    )(core, other, *begun)
    return merged, field, *rest


def passed_along(value, axis, steps):
    count = lax.axis_size(axis)
    return lax.ppermute(value, axis, [(source, (source + steps) % count) for source in range(count)])


def groups_of(count, apart, size):
    return [
        [start * apart * size + offset + member * apart for member in range(size)]
        for start in range(count // (apart * size))
        for offset in range(apart)
    ]


def summed_over(keep, send, axis, joined, partner, forward):
    count = lax.axis_size(axis)
    along = count // (CORES * ACROSS)
    pairs = [(i, i ^ 1) for i in range(count)]
    arrived = lax.ppermute(send, axis, pairs)
    held = joined(keep, arrived)

    def exchanged(value, apart, size):
        return lax.all_to_all(value, axis, 0, 0, axis_index_groups=groups_of(count, apart, size))

    def reduced(value, apart, size):
        got = exchanged(value.reshape(size, -1, *value.shape[1:]), apart, size)
        return jnp.sum(got.astype(F32), axis=0).astype(BF)

    def gathered(value, apart, size):
        return exchanged(jnp.broadcast_to(value[None], (size, *value.shape)), apart, size).reshape(-1, *value.shape[1:])

    held = reduced(held, CORES, ACROSS)
    held, partner = lax.optimization_barrier((held, partner))
    held = reduced(held.reshape(-1, 2, LANES), CORES * ACROSS, along)
    held = gathered(held, CORES * ACROSS, along).reshape(-1, LANES)
    held = gathered(held, CORES, ACROSS)
    held, forwarded = forward(held, partner)
    return held, lax.ppermute(held, axis, pairs), partner, forwarded


def local(
    fields,
    norm_gain,
    qkv_weight,
    proj_weight,
    bias_table,
    bias_index,
    region_ids,
    mlp_gain,
    up_weight,
    down_weight,
    merge_gain,
    merge_weight,
    cotangent,
):
    count = lax.axis_size("lon")
    core = (lax.axis_index("lon") % CORES).astype(jnp.int32).reshape(1)
    by_lon = fields.transpose(0, 2, 1, 3)
    by_lat = cotangent.transpose(1, 2, 0, 3)
    field_last, cotangent_last, table, index, merge_gain = stage(
        by_lon, by_lat, bias_table.transpose(1, 0, 2), bias_index, merge_gain
    )
    west = passed_along(field_last, "lon", 1)
    west_cotangent = passed_along(cotangent_last, "lon", 1)
    table, core = lax.optimization_barrier((table, core))
    bias, bias_tail = bias_rows(table, index, region_ids)
    half_rows = -(-O_END // (count * 2)) * 2 * count // CORES
    grads, tokens, scores, *results = block(
        half_rows,
        by_lon,
        west,
        by_lat,
        west_cotangent,
        norm_gain.reshape(1, C),
        qkv_weight,
        proj_weight,
        mlp_gain.reshape(1, C),
        up_weight,
        down_weight.T,
        merge_gain,
        merge_weight,
        bias,
        bias_tail,
    )
    pairs = [(i, i ^ 1) for i in range(count)]
    partner_scores = lax.ppermute(scores, "lon", pairs)
    keep, send = pack(core, grads, tokens, results[1])
    merged_keep, field_keep, home = to_grid(*results, qkv_weight, norm_gain.reshape(1, C), merge_weight)
    partner = lax.ppermute(home, "lon", pairs)

    def forward(held, leaving):
        held, leaving = lax.optimization_barrier((held, leaving))
        return held, lax.ppermute(leaving, "lon", [(i, (i - CORES) % count) for i in range(1, count, CORES)])

    table = table_sum(core, scores, partner_scores, index)
    held, other, partner, forwarded = summed_over(
        keep, send, "lon", lambda kept, arrived: join(core, kept, arrived, table), partner, forward
    )
    factor = float(LEVELS * LAT * fields.shape[2] * count) ** (-0.5)
    merged, field_grad, up_grad, down_grad, qkv_grad, merge_grad, proj_grad, table_grad = finish(
        core, held, other, (partner, forwarded, merged_keep, field_keep), factor
    )
    return (
        merged.transpose(2, 0, 1, 3),
        field_grad.transpose(0, 2, 1, 3),
        qkv_grad,
        proj_grad,
        up_grad,
        down_grad.T,
        merge_grad,
        table_grad.transpose(1, 0, 2),
    )


def solution(mesh):
    whole = P("groups", None, "lon", None)

    return jax.shard_map(
        local,
        mesh=mesh,
        in_specs=(whole, *[P()] * 11, whole),
        out_specs=(whole, whole, *[P("groups", None)] * 5, P("groups", None, None)),
        check_vma=False,
    )
```

```python
import jax
import jax.numpy as jnp
from jax import lax
from jax.experimental import pallas as pl
from jax.experimental.pallas import tpu as pltpu
from jax.sharding import PartitionSpec as P

C = 192
MLP = 768
HEADS = 6
HEAD = 32
HALF = 6
WIN = 144
BPOS = 3312
LAT = 24
TYPES = 4
TOK = TYPES * WIN
LEVELS = 2
LANES = 128
MAIN = 128
REST = WIN - MAIN
TH = TYPES * HEADS
LOW = 256
HIGH = -(-BPOS // LOW)
MTOK = 160
EPS = 1e-5
MASKED = -1e30
F32 = jnp.float32
BF = jnp.bfloat16
CORES = 2
ACROSS = 4

TROWS = 320
MSPLIT = 512
O_UP = 0
O_QKV = O_UP + 6 * C
O_QKV_TAIL = O_QKV + 4 * C
O_PROJ = O_QKV_TAIL + C // 2
O_PROJ_TAIL = O_PROJ + C
O_TABLE = O_PROJ_TAIL + C // 2
O_MERGE_LAST = O_TABLE + 2 * TROWS
O_MERGE = O_MERGE_LAST + MLP - MSPLIT
O_DOWN = O_MERGE + 2 * MLP + MSPLIT
O_END = O_DOWN + 6 * C

DS_TAIL = TH * WIN
DS_CORNER = DS_TAIL + TH * REST
DS_END = DS_CORNER + TH * REST


def dot(a, b):
    return jnp.dot(a, b, preferred_element_type=F32)


def dot_nt(a, b):
    return lax.dot_general(a, b, (((1,), (1,)), ((), ())), preferred_element_type=F32)


def dot_tn(a, b):
    return lax.dot_general(a, b, (((0,), (0,)), ((), ())), preferred_element_type=F32)


def div(n, d):
    return (n * -(-(1 << 16) // d)) >> 16


def onehot(rows, cols, of_row=None, of_col=None):
    if of_row is not None:
        target = of_row(lax.broadcasted_iota(jnp.int32, (rows, 1), 0))
        place = lax.broadcasted_iota(jnp.int32, (rows, cols), 1)
    else:
        target = of_col(lax.broadcasted_iota(jnp.int32, (1, cols), 1))
        place = lax.broadcasted_iota(jnp.int32, (rows, cols), 0)
    return jnp.where(place == target, 1.0, 0.0).astype(BF)


def cell_of_token(n):
    kind = div(n, 72)
    rest = n - 72 * kind
    lat = div(rest, 12)
    return (rest - 12 * lat) * LAT + kind * 6 + lat


def token_of_group(n):
    quarter = div(n, 40)
    rest = n - 40 * quarter
    level = div(rest, 18)
    part = rest - 18 * level
    lat = div(part, 6)
    token = level * 72 + (2 * lat + (quarter >> 1)) * 12 + 2 * (part - 6 * lat) + (quarter & 1)
    return jnp.where(rest < 36, token, -1)


def group_of_token(n):
    level = div(n, 72)
    rest = n - 72 * level
    lat = div(rest, 12)
    lon = rest - 12 * lat
    return ((lat & 1) * 2 + (lon & 1)) * 40 + level * 18 + (lat >> 1) * 6 + (lon >> 1)


def cell_of_merged(n):
    kind = div(n, 40)
    rest = n - 40 * kind
    level = div(rest, 18)
    part = rest - 18 * level
    lat = div(part, 6)
    lon = part - 6 * lat
    half = jnp.where(lon < 3, 0, 1)
    row = half * 72 + (3 * kind + lat) * 6 + (lon - 3 * half) * 2 + level
    return jnp.where(rest < 36, row, -1)


def normalised(values):
    centred = values - jnp.mean(values, axis=-1, keepdims=True)
    scale = lax.rsqrt(jnp.mean(centred * centred, axis=-1, keepdims=True) + EPS)
    return centred * scale, scale


def norm_grad(grad, unit, scale, gain):
    scaled = grad * gain
    return scale * (
        scaled
        - jnp.mean(scaled, axis=-1, keepdims=True)
        - unit * jnp.mean(scaled * unit, axis=-1, keepdims=True)
    )


def rounded(values):
    return values.astype(BF).astype(F32)


def low_onehot(low):
    place = lax.broadcasted_iota(jnp.int32, (LOW, 1), 0).astype(F32).astype(BF)
    hit = jnp.broadcast_to(place, (LOW, low.shape[1])) == low.astype(F32).astype(BF)
    return jnp.where(hit, jnp.array(1, BF), jnp.array(0, BF))


def bias_kernel(table_ref, index_ref, regions_ref, main_ref, tail_ref, part_ref, last_ref, turned_ref, mask_ref, region_ref, sem):
    copy = pltpu.make_async_copy(regions_ref, region_ref, sem)
    copy.start()
    for high in range(HIGH):
        width = min(LOW, BPOS - high * LOW)
        for head in range(HEADS):
            piece = table_ref[head, :, high * LOW : high * LOW + width]
            if width < LOW:
                piece = jnp.concatenate([piece, jnp.zeros((TYPES, LOW - width), F32)], axis=1)
            row = high * TH + head * TYPES
            part_ref[row : row + TYPES, :] = piece
    turned_ref[...] = jnp.transpose(index_ref[:, MAIN:])
    parts = part_ref[...].astype(BF)

    def looked_up(index):
        low = low_onehot(index & (LOW - 1))
        high_row = index >> 8
        found = dot(parts, low)
        chosen = found[0:TH]
        for high in range(1, HIGH):
            chosen = jnp.where(high_row == high, found[high * TH : (high + 1) * TH], chosen)
        return chosen

    for start in range(0, REST, 4):
        got = looked_up(jnp.concatenate([turned_ref[start + n : start + n + 1, :MAIN] for n in range(4)], axis=1))
        for n in range(4):
            last_ref[pl.ds(start + n, TH, stride=REST), :] = got[:, n * MAIN : (n + 1) * MAIN]
    got = looked_up(jnp.concatenate([turned_ref[n : n + 1, MAIN:] for n in range(REST)], axis=1))
    for n in range(REST):
        half = got[:, LANES * (n // 8) : LANES * (n // 8 + 1)]
        half = half if n % 8 == 0 else pltpu.roll(half, LANES - REST * (n % 8), 1)
        last_ref[pl.ds(TH * REST + n, TH, stride=REST), :] = half
    copy.wait()
    kind_of = lax.broadcasted_iota(jnp.int32, (TH, 1), 0) & (TYPES - 1)
    column = lax.broadcasted_iota(jnp.int32, (1, LANES), 1)
    labels = []
    for group in range(12):
        label = jnp.zeros((TH, 1), jnp.int32)
        for kind in range(TYPES):
            label = jnp.where(kind_of == kind, region_ref[group // 6, 6 * kind + group % 6], label)
        labels.append(label)
    keys = jnp.zeros((TH, LANES), jnp.int32)
    for group in range(11):
        keys = jnp.where((column >= 12 * group) & (column < 12 * group + 12), labels[group], keys)
    for group in range(12):
        mask_ref[TH * group : TH * (group + 1), :] = jnp.where(keys == labels[group], 0.0, MASKED)

    def row_block(block, carry):
        base = pl.multiple_of(block * 8, 8)
        rows = index_ref[pl.ds(base, 8), :MAIN]
        for part in range(4):
            index = jnp.concatenate([rows[2 * part + n : 2 * part + n + 1] for n in range(2)], axis=1)
            got = looked_up(index)
            for n in range(2):
                row = base + 2 * part + n
                mask = mask_ref[pl.ds(pl.multiple_of(div(row, 12) * TH, 8), TH), :]
                main_ref[pl.ds(row, TH, stride=WIN), :] = got[:, n * MAIN : (n + 1) * MAIN] + mask
        return carry

    lax.fori_loop(0, WIN // 8, row_block, 0, unroll=True)
    apart = jnp.where(labels[10] == labels[11], 0.0, MASKED)
    split = 132 - MAIN
    for n in range(REST):
        group = (MAIN + n) // 12
        rows = pl.ds(n, TH, stride=REST)
        last_ref[rows, :] = last_ref[rows, :] + mask_ref[TH * group : TH * (group + 1), :]
        rows = pl.ds(TH * REST + n, TH, stride=REST)
        other = (column < split) if n >= split else (column >= split)
        last_ref[rows, :] = last_ref[rows, :] + jnp.where(other, apart, 0.0)
    for th in range(TH):
        rows = slice(th * WIN, th * WIN + MAIN)
        tail_ref[rows, :REST] = jnp.transpose(last_ref[th * REST : (th + 1) * REST, :])
        rows = slice(th * WIN + MAIN, (th + 1) * WIN)
        tail_ref[rows, :REST] = jnp.transpose(last_ref[(TH + th) * REST : (TH + th + 1) * REST, :])[:REST]


def stage_kernel(fields_ref, cotangent_ref, table_ref, index_ref, gain_ref, field_ref, half_ref, table_out, index_out, gain_out, sems):
    copies = [
        pltpu.make_async_copy(source, target, sems.at[n])
        for n, (source, target) in enumerate(
            [
                (fields_ref.at[:, HALF:], field_ref),
                (cotangent_ref.at[:, HALF // 2 :], half_ref),
                (table_ref, table_out),
                (index_ref, index_out),
                (gain_ref, gain_out.at[0]),
            ]
        )
    ]
    for copy in copies:
        copy.start()
    for copy in copies:
        copy.wait()


def stage(fields, cotangent, table, index, gain):
    shape = jax.ShapeDtypeStruct
    whole = pl.BlockSpec(memory_space=pltpu.VMEM)
    return pl.pallas_call(
        stage_kernel,
        out_shape=[
            shape((LEVELS, HALF, LAT, C), BF),
            shape((12, HALF // 2, LEVELS, 2 * C), BF),
            shape(table.shape, F32),
            shape(index.shape, jnp.int32),
            shape((1, 4 * C), F32),
        ],
        in_specs=[pl.BlockSpec(memory_space=pltpu.HBM)] * 5,
        out_specs=[whole] * 5,
        scratch_shapes=[pltpu.SemaphoreType.DMA((5,))],
        compiler_params=pltpu.CompilerParams(vmem_limit_bytes=4 * 1024 * 1024),
        name="stage",
    )(*(pltpu.with_memory_space_constraint(a, pltpu.HBM) for a in (fields, cotangent, table, index, gain)))


def bias_rows(table, index, regions):
    whole = pl.BlockSpec(memory_space=pltpu.VMEM)
    return pl.pallas_call(
        bias_kernel,
        out_shape=[jax.ShapeDtypeStruct((TH * WIN, LANES), F32)] * 2,
        in_specs=[whole, whole, pl.BlockSpec(memory_space=pltpu.HBM)],
        out_specs=[whole, whole],
        scratch_shapes=[
            pltpu.VMEM((HIGH * TH, LOW), F32),
            pltpu.VMEM((2 * TH * REST, LANES), F32),
            pltpu.VMEM((REST, WIN), jnp.int32),
            pltpu.VMEM((12 * TH, LANES), F32),
            pltpu.SMEM((LEVELS, LAT), jnp.int32),
            pltpu.SemaphoreType.DMA,
        ],
        compiler_params=pltpu.CompilerParams(vmem_limit_bytes=16 * 1024 * 1024),
        cost_estimate=pl.CostEstimate(flops=14_000_000_000, bytes_accessed=4_000_000, transcendentals=0),
        name="bias_rows",
    )(table, index, pltpu.with_memory_space_constraint(regions, pltpu.HBM))


def block_kernel(
    own_ref, west_ref, own_cotangent_ref, west_cotangent_ref,
    norm_gain_ref, qkv_ref, proj_ref, mlp_gain_ref, up_ref, down_ref, merge_gain_ref, merge_ref,
    bias_ref, bias_tail_ref,
    grads_ref, tokens_ref, ds_ref, normed_merge_ref, triple_ref, grad_attn_ref, unit_ref, scale_ref,
    x_ref, q_ref, k_ref, v_ref, p_ref, mixed_ref,
    unit_mlp_ref, scale_mlp_ref, normed_mlp_ref, hidden_ref, slope_ref, after_mlp_ref,
    group_ref, grad_after_ref, grad_up_ref, grad_mixed_ref,
    cells_ref, grad_merged_ref, scaled_ref,
):
    to_tokens = onehot(288, 288, of_row=cell_of_token)
    for level in range(LEVELS):
        cells = jnp.concatenate(
            [
                west_ref[level].astype(F32).reshape(144, C),
                own_ref[level, :HALF].astype(F32).reshape(144, C),
            ],
            axis=0,
        ).astype(BF)
        ordered = dot(to_tokens, cells)
        for kind in range(TYPES):
            x_ref[WIN * kind + 72 * level : WIN * kind + 72 * level + 72, :] = ordered[72 * kind : 72 * kind + 72]
    for lat in range(12):
        for lon in range(HALF // 2):
            row = (lat * 3 + lon) * 2
            cells_ref[row : row + 2, :] = west_cotangent_ref[lat, lon].astype(F32)
            cells_ref[72 + row : 74 + row, :] = own_cotangent_ref[lat, lon].astype(F32)
    grad_merged_ref[...] = dot(onehot(MTOK, 144, of_row=cell_of_merged), cells_ref[...].astype(BF)).astype(BF)
    for n in range(4):
        value = rounded(dot_nt(grad_merged_ref[...], merge_ref[C * n : C * (n + 1), :]))
        scaled_ref[n] = value * merge_gain_ref[:, C * n : C * (n + 1)]
    unit, scale = normalised(x_ref[...])
    unit_ref[...] = unit
    scale_ref[...] = scale
    tokens = (unit * norm_gain_ref[...]).astype(BF)
    tokens_ref[...] = tokens
    q_ref[...] = dot(tokens, qkv_ref[:, 0:C]).astype(BF)
    k_ref[...] = dot(tokens, qkv_ref[:, C : 2 * C]).astype(BF)
    v_ref[...] = dot(tokens, qkv_ref[:, 2 * C :]).astype(BF)
    lane = lax.broadcasted_iota(jnp.int32, (1, C), 1)
    of_head = [
        jnp.where((lane >= HEAD * h) & (lane < HEAD * (h + 1)), 1.0, 0.0).astype(BF) for h in range(HEADS)
    ]
    temper = HEAD ** (-0.5)

    def attend(kind, carry):
        rows = pl.ds(pl.multiple_of(kind * WIN, 16), WIN)
        q, k, v = q_ref[rows, :], k_ref[rows, :], v_ref[rows, :]
        mixed = jnp.zeros((WIN, C), F32)
        products = dot_nt(jnp.concatenate([q * of_head[h] for h in range(HEADS)], axis=0), k)
        for h in range(HEADS):
            th = h * TYPES + kind
            scores_at = pl.ds(pl.multiple_of(th * WIN, 16), WIN)
            bias = jnp.concatenate([bias_ref[scores_at, :], bias_tail_ref[scores_at, :REST]], axis=1)
            scores = products[WIN * h : WIN * (h + 1)] * temper + bias
            weights = jnp.exp(scores - jnp.max(scores, axis=-1, keepdims=True))
            p = weights * (1.0 / jnp.sum(weights, axis=-1, keepdims=True))
            p_ref[th] = p
            mixed = mixed + dot(p.astype(BF), v * of_head[h])
        mixed_ref[rows, :] = mixed.astype(BF)
        return carry

    lax.fori_loop(0, TYPES, attend, 0, unroll=True)
    after_attn = rounded(x_ref[...] + rounded(dot(mixed_ref[...], proj_ref[...])))
    x_ref[...] = after_attn
    unit, scale = normalised(after_attn)
    unit_mlp_ref[...] = unit
    scale_mlp_ref[...] = scale
    normed_mlp = (unit * mlp_gain_ref[...]).astype(BF)
    normed_mlp_ref[...] = normed_mlp
    for part in range(3):
        cols = slice(256 * part, 256 * part + 256)
        u = dot(normed_mlp, up_ref[:, cols])
        below = 0.5 * (1.0 + lax.erf(u * 0.5**0.5))
        hidden_ref[:, cols] = (u * below).astype(BF)
        slope_ref[:, cols] = below + u * (jnp.exp(u * u * (-0.5)) * 0.3989422804014327)
    after_mlp_ref[...] = (x_ref[...] + dot_nt(hidden_ref[...], down_ref[...])).astype(BF)

    to_groups = onehot(160, WIN, of_row=token_of_group)
    for kind in range(TYPES):
        grouped = dot(to_groups, after_mlp_ref[WIN * kind : WIN * kind + WIN, :])
        for quarter in range(4):
            group_ref[quarter, 40 * kind : 40 * kind + 40, :] = grouped[40 * quarter : 40 * quarter + 40]
    quarters = [group_ref[n] for n in range(4)]
    mean = jnp.sum(sum(quarters), axis=-1, keepdims=True) * (1.0 / MLP)
    centred = [v - mean for v in quarters]
    variance = jnp.sum(sum(v * v for v in centred), axis=-1, keepdims=True) * (1.0 / MLP)
    scale_merge = lax.rsqrt(variance + EPS)
    for n in range(4):
        unit = centred[n] * scale_merge
        group_ref[n] = unit
        normed_merge = (unit * merge_gain_ref[:, C * n : C * (n + 1)]).astype(BF)
        normed_merge_ref[n] = normed_merge
    scaled, total, along = [], 0.0, 0.0
    for n in range(4):
        value = scaled_ref[n]
        total = total + value
        along = along + value * group_ref[n]
        scaled.append(value)
    total = jnp.sum(total, axis=-1, keepdims=True) * (1.0 / MLP)
    along = jnp.sum(along, axis=-1, keepdims=True) * (1.0 / MLP)
    for n in range(4):
        group_ref[n] = scale_merge * (scaled[n] - total - group_ref[n] * along)
    from_groups = onehot(WIN, 160, of_row=group_of_token)
    for kind in range(TYPES):
        grouped = jnp.concatenate([group_ref[n, 40 * kind : 40 * kind + 40, :] for n in range(4)], axis=0)
        grad_after_ref[WIN * kind : WIN * kind + WIN, :] = dot(from_groups, grouped.astype(BF)).astype(BF)

    grad_after = grad_after_ref[...]
    for part in range(3):
        cols = slice(256 * part, 256 * part + 256)
        grad_up_ref[:, cols] = (rounded(dot(grad_after, down_ref[:, cols])) * slope_ref[:, cols]).astype(BF)
    grad_normed = rounded(dot_nt(grad_up_ref[...], up_ref[...]))
    grad_attn = (
        grad_after.astype(F32)
        + norm_grad(grad_normed, unit_mlp_ref[...], scale_mlp_ref[...], mlp_gain_ref[...])
    ).astype(BF)
    grad_attn_ref[...] = grad_attn

    grad_mixed_ref[...] = dot_nt(grad_attn, proj_ref[...]).astype(BF)

    def down_terms():
        grad = dot_tn(grad_after_ref[...], hidden_ref[...]).astype(BF)
        for b in range(6):
            grads_ref[O_DOWN + C * b : O_DOWN + C * (b + 1), :] = grad[:, 128 * b : 128 * b + 128]

    def up_terms():
        grad = dot_tn(normed_mlp_ref[...], grad_up_ref[...]).astype(BF)
        for b in range(6):
            grads_ref[O_UP + C * b : O_UP + C * (b + 1), :] = grad[:, 128 * b : 128 * b + 128]

    def merge_terms():
        for n in range(4):
            grad = dot_tn(normed_merge_ref[n], grad_merged_ref[...]).astype(BF)
            for b in range(2):
                start = O_MERGE + MLP * b + C * n
                grads_ref[start : start + C, :] = grad[:, 128 * b : 128 * b + 128]
            kept = max(0, min(C, MSPLIT - C * n))
            if kept:
                start = O_MERGE + 2 * MLP + C * n
                grads_ref[start : start + kept, :] = grad[:kept, 256:]
            if kept < C:
                start = O_MERGE_LAST + C * n + kept - MSPLIT
                grads_ref[start : start + C - kept, :] = grad[kept:, 256:]

    def proj_terms():
        grad_proj = dot_tn(mixed_ref[...], grad_attn_ref[...]).astype(BF)
        grads_ref[O_PROJ : O_PROJ + C, :] = grad_proj[:, :128]
        grads_ref[O_PROJ_TAIL : O_PROJ_TAIL + C // 2, :] = jnp.concatenate(
            [grad_proj[: C // 2, 128:], grad_proj[C // 2 :, 128:]], axis=1
        )

    last_keys = onehot(REST, WIN, of_row=lambda n: n + MAIN)
    ds_ref[DS_CORNER:, :] = jnp.zeros((TH * REST, LANES), BF)
    grads_ref[O_QKV:O_PROJ, :] = jnp.zeros((O_PROJ - O_QKV, LANES), BF)
    grads_ref[O_TABLE:O_MERGE_LAST, :] = jnp.zeros((O_MERGE_LAST - O_TABLE, LANES), BF)

    def attend_back(kind, carry):
        rows = pl.ds(kind * WIN, WIN)
        v, grad = v_ref[rows, :], grad_mixed_ref[rows, :]
        q_turned, k_turned, grad_turned = (jnp.transpose(a) for a in (q_ref[rows, :], k_ref[rows, :], grad))
        products = dot_nt(jnp.concatenate([grad * of_head[h] for h in range(HEADS)], axis=0), v)
        dq, dk, dv = [], [], []
        for h in range(HEADS):
            th = h * TYPES + kind
            lanes = slice(HEAD * h, HEAD * (h + 1))
            p = p_ref[th]
            weighted = p * products[WIN * h : WIN * (h + 1)]
            ds = weighted - p * jnp.sum(weighted, axis=-1, keepdims=True)
            ds = ds.astype(BF)
            ds_ref[pl.ds(th * WIN, WIN), :] = ds[:, :MAIN]
            turned = dot_nt(jnp.concatenate([k_turned[lanes], last_keys], axis=0), ds)
            tail = turned[HEAD:].astype(BF)
            ds_ref[pl.ds(DS_TAIL + th * REST, REST), :] = tail[:, :MAIN]
            ds_ref[pl.ds(DS_CORNER + th * REST, REST), :REST] = tail[:, MAIN:]
            dq.append(turned[:HEAD])
            dk.append(dot(q_turned[lanes], ds))
            dv.append(dot(grad_turned[lanes], p.astype(BF)))
        triple = jnp.concatenate([a * temper for a in dq + dk] + dv, axis=0).astype(BF)
        triple_ref[rows, :] = jnp.transpose(triple)
        return carry

    for kind, terms in enumerate((down_terms, up_terms, merge_terms, proj_terms)):
        attend_back(kind, 0)
        terms()


def block(half_rows, *args):
    shape = jax.ShapeDtypeStruct
    whole = pl.BlockSpec(memory_space=pltpu.VMEM)
    scratch = [
        ((TOK, C), F32), ((TOK, C), BF), ((TOK, C), BF),
        ((TOK, C), BF), ((TH, WIN, WIN), F32), ((TOK, C), BF),
        ((TOK, C), F32), ((TOK, 1), F32), ((TOK, C), BF), ((TOK, MLP), BF), ((TOK, MLP), F32), ((TOK, C), BF),
        ((4, MTOK, C), F32), ((TOK, C), BF), ((TOK, MLP), BF), ((TOK, C), BF),
        ((144, 2 * C), F32), ((MTOK, 2 * C), BF), ((4, MTOK, C), F32),
    ]
    return pl.pallas_call(
        block_kernel,
        out_shape=[
            shape((2 * half_rows, LANES), BF),
            shape((TOK, C), BF),
            shape((DS_END, LANES), BF),
            shape((4, MTOK, C), BF),
            shape((TOK, 3 * C), BF),
            shape((TOK, C), BF),
            shape((TOK, C), F32),
            shape((TOK, 1), F32),
        ],
        in_specs=[whole] * len(args),
        out_specs=[whole] * 8,
        scratch_shapes=[pltpu.VMEM(*item) for item in scratch],
        compiler_params=pltpu.CompilerParams(vmem_limit_bytes=24 * 1024 * 1024),
        cost_estimate=pl.CostEstimate(flops=24_000_000_000, bytes_accessed=12_000_000, transcendentals=2_000_000),
        name="block",
    )(*args)


def pack_kernel(core_ref, grads_ref, tokens_ref, triple_ref, keep_ref, send_ref):
    half = keep_ref.shape[0]
    core = core_ref[0]
    grad_qkv = dot_tn(tokens_ref[...], triple_ref[...]).astype(BF)
    tail = jnp.concatenate([grad_qkv[: C // 2, 512:], grad_qkv[C // 2 :, 512:]], axis=1)
    keep_ref[...] = grads_ref[pl.ds(pl.multiple_of(core * half, 16), half), :]
    send_ref[...] = grads_ref[pl.ds(pl.multiple_of((1 - core) * half, 16), half), :]
    for owner, target_ref in ((0, keep_ref), (1, send_ref)):

        @pl.when(core == owner)
        def _():
            for b in range(4):
                target_ref[O_QKV + C * b : O_QKV + C * (b + 1), :] = grad_qkv[:, 128 * b : 128 * b + 128]
            target_ref[O_QKV_TAIL : O_QKV_TAIL + C // 2, :] = tail


def pack(core, grads, tokens, triple):
    half = jax.ShapeDtypeStruct((grads.shape[0] // 2, LANES), BF)
    whole = pl.BlockSpec(memory_space=pltpu.VMEM)
    return pl.pallas_call(
        pack_kernel,
        out_shape=[half, half],
        in_specs=[pl.BlockSpec(memory_space=pltpu.SMEM)] + [whole] * 3,
        out_specs=[whole] * 2,
        compiler_params=pltpu.CompilerParams(vmem_limit_bytes=12 * 1024 * 1024),
        cost_estimate=pl.CostEstimate(flops=600_000_000, bytes_accessed=4_000_000, transcendentals=0),
        name="pack",
    )(core, grads, tokens, triple)


def table_kernel(core_ref, own_ref, partner_ref, index_ref, table_ref, ds_ref, turned_ref):
    def table_terms(index, slab):
        high_row = index >> 8
        spread = [jnp.where(high_row == n, slab, 0.0) for n in range(HIGH)]
        spread.append(jnp.zeros((TROWS - HIGH * TH, index.shape[1]), F32))
        return dot_nt(jnp.concatenate(spread, axis=0).astype(BF), low_onehot(index & (LOW - 1)))

    def row_block(block, carry):
        base = pl.multiple_of(block * 8, 8)
        rows = index_ref[pl.ds(base, 8), :MAIN]
        index = jnp.concatenate([rows[n : n + 1] for n in range(8)], axis=1)
        slab = jnp.concatenate([ds_ref[pl.ds(base + n, TH, stride=WIN), :] for n in range(8)], axis=1)
        return carry + table_terms(index, slab)

    @pl.when(core_ref[0] == 0)
    def _():
        ds_ref[...] = own_ref[...].astype(F32) + partner_ref[...].astype(F32)
        turned_ref[...] = jnp.transpose(index_ref[:, MAIN:])
        table = lax.fori_loop(0, WIN // 8, row_block, jnp.zeros((TROWS, LOW), F32), unroll=True)
        index = jnp.concatenate([turned_ref[n : n + 1, :MAIN] for n in range(REST)], axis=1)
        slab = jnp.concatenate([ds_ref[pl.ds(DS_TAIL + n, TH, stride=REST), :] for n in range(REST)], axis=1)
        table = table + table_terms(index, slab)
        index = jnp.concatenate([turned_ref[n : n + 1, MAIN:] for n in range(REST)], axis=1)
        slab = jnp.concatenate(
            [ds_ref[pl.ds(DS_CORNER + n, TH, stride=REST), :][:, :REST] for n in range(REST)], axis=1
        )
        table = (table + table_terms(index, slab)).astype(BF)
        table_ref[:TROWS, :] = table[:, :LANES]
        table_ref[TROWS:, :] = table[:, LANES:]

    @pl.when(core_ref[0] == 1)
    def _():
        table_ref[...] = jnp.zeros(table_ref.shape, BF)


def table_sum(core, own, partner, index):
    whole = pl.BlockSpec(memory_space=pltpu.VMEM)
    return pl.pallas_call(
        table_kernel,
        out_shape=jax.ShapeDtypeStruct((2 * TROWS, LANES), BF),
        in_specs=[pl.BlockSpec(memory_space=pltpu.SMEM)] + [whole] * 3,
        out_specs=whole,
        scratch_shapes=[pltpu.VMEM((DS_END, LANES), F32), pltpu.VMEM((REST, WIN), jnp.int32)],
        compiler_params=pltpu.CompilerParams(vmem_limit_bytes=12 * 1024 * 1024),
        cost_estimate=pl.CostEstimate(flops=4_000_000_000, bytes_accessed=3_000_000, transcendentals=0),
        name="table_sum",
    )(core, own, partner, index)


def join_kernel(core_ref, keep_ref, arrived_ref, table_ref, held_ref):
    held_ref[...] = (keep_ref[...].astype(F32) + arrived_ref[...].astype(F32)).astype(BF)

    @pl.when(core_ref[0] == 0)
    def _():
        held_ref[O_TABLE : O_TABLE + 2 * TROWS, :] = table_ref[...]


def join(core, keep, arrived, table):
    whole = pl.BlockSpec(memory_space=pltpu.VMEM)
    return pl.pallas_call(
        join_kernel,
        out_shape=jax.ShapeDtypeStruct(keep.shape, BF),
        in_specs=[pl.BlockSpec(memory_space=pltpu.SMEM)] + [whole] * 3,
        out_specs=whole,
        compiler_params=pltpu.CompilerParams(vmem_limit_bytes=8 * 1024 * 1024),
        cost_estimate=pl.CostEstimate(flops=400_000, bytes_accessed=2_500_000, transcendentals=0),
        name="join",
    )(core, keep, arrived, table)


def cells_kernel(
    normed_merge_ref, triple_ref, grad_attn_ref, unit_ref, scale_ref, qkv_ref, gain_ref, merge_ref,
    merged_keep_ref, field_keep_ref, home_ref, x_ref,
):
    merged = sum(dot(normed_merge_ref[n], merge_ref[C * n : C * (n + 1), :]) for n in range(4))
    grad_normed = rounded(dot_nt(triple_ref[...], qkv_ref[...]))
    merged_cells = dot(onehot(144, MTOK, of_col=cell_of_merged), merged.astype(BF))
    x_ref[...] = grad_attn_ref[...].astype(F32) + norm_grad(
        grad_normed, unit_ref[...], scale_ref[...], gain_ref[...]
    )
    to_cells = onehot(288, 288, of_col=cell_of_token)
    leaving = []
    for level in range(LEVELS):
        ordered = jnp.concatenate(
            [x_ref[WIN * kind + 72 * level : WIN * kind + 72 * level + 72, :] for kind in range(TYPES)], axis=0
        )
        cells = dot(to_cells, ordered.astype(BF))
        leaving.append(cells[:144])
        field_keep_ref[level] = cells[144:].reshape(HALF, LAT, C).astype(BF)
    home_ref[:HALF] = jnp.concatenate(leaving, axis=1).reshape(HALF, LAT, 2 * C).astype(BF)
    for lat in range(12):
        for lon in range(HALF // 2):
            row = 72 + (lat * 3 + lon) * 2
            merged_keep_ref[lat, lon] = merged_cells[row : row + 2].astype(BF)
    home_ref[HALF:] = merged_cells[:72].reshape(3, LAT, 2 * C).astype(BF)


def to_grid(*args):
    shape = jax.ShapeDtypeStruct
    whole = pl.BlockSpec(memory_space=pltpu.VMEM)
    return pl.pallas_call(
        cells_kernel,
        out_shape=[
            shape((12, HALF // 2, LEVELS, 2 * C), BF),
            shape((LEVELS, HALF, LAT, C), BF),
            shape((HALF + 3, LAT, 2 * C), BF),
        ],
        in_specs=[whole] * 8,
        out_specs=[whole] * 3,
        scratch_shapes=[pltpu.VMEM((TOK, C), F32)],
        compiler_params=pltpu.CompilerParams(vmem_limit_bytes=12 * 1024 * 1024),
        cost_estimate=pl.CostEstimate(flops=1_500_000_000, bytes_accessed=3_000_000, transcendentals=0),
        name="to_grid",
    )(*args)


def first_half(part, refs, staged, leaves):
    _, _, up_ref, _, qkv_ref, merge_ref, proj_ref, table_ref = refs
    up, _, qkv, merge, proj, table = staged
    for b in range(6):
        up[:, 128 * b : 128 * b + 128] = part(O_UP + C * b, C)
    leaves(up, up_ref)
    for b in range(4):
        qkv[:, 128 * b : 128 * b + 128] = part(O_QKV + C * b, C)
    tail = part(O_QKV_TAIL, C // 2)
    qkv[: C // 2, 512:] = tail[:, :64]
    qkv[C // 2 :, 512:] = tail[:, 64:]
    leaves(qkv, qkv_ref)
    for side in range(2):
        terms = part(O_TABLE + TROWS * side, TROWS)
        for high in range(HIGH):
            start = high * LOW + side * LANES
            width = min(LANES, BPOS - start)
            for head in range(HEADS):
                row = high * TH + head * TYPES
                table[head, :, start : start + width] = terms[row : row + TYPES, :width]
    leaves(table, table_ref)
    proj[:, :128] = part(O_PROJ, C)
    tail = part(O_PROJ_TAIL, C // 2)
    proj[: C // 2, 128:] = tail[:, :64]
    proj[C // 2 :, 128:] = tail[:, 64:]
    leaves(proj, proj_ref)
    merge[MSPLIT:, 256:] = part(O_MERGE_LAST, MLP - MSPLIT)
    leaves(merge.at[MSPLIT:, 256:], merge_ref.at[MSPLIT:, 256:])


def second_half(part, refs, staged, leaves):
    _, _, _, down_ref, _, merge_ref, _, _ = refs
    _, down, _, merge, _, _ = staged
    for b in range(2):
        merge[:, 128 * b : 128 * b + 128] = part(O_MERGE + MLP * b, MLP)
    leaves(merge.at[:, :256], merge_ref.at[:, :256])
    for b in range(6):
        down[:, 128 * b : 128 * b + 128] = part(O_DOWN + C * b, C)
    leaves(down, down_ref)
    merge[:MSPLIT, 256:] = part(O_MERGE + 2 * MLP, MSPLIT)
    leaves(merge.at[:MSPLIT, 256:], merge_ref.at[:MSPLIT, 256:])


def scaled(factor, half, sums_ref, outs, staged, sems):
    for which, fill, base in ((0, first_half, 0), (1, second_half, O_MERGE)):

        @pl.when(half == which)
        def _():
            begun = []

            def part(start, rows):
                return sums_ref[start - base : start - base + rows, :].astype(F32) * factor

            def leaves(source, target):
                begun.append(pltpu.make_async_copy(source, target, sems.at[len(begun)]))
                begun[-1].start()

            fill(part, outs, staged, leaves)
            for copy in begun:
                copy.wait()


def finish_own_kernel(
    factor, core_ref, held_ref, partner_ref, forwarded_ref, merged_keep_ref, field_keep_ref, *refs
):
    outs, staged, (sems, merged, field) = refs[:8], refs[8:14], refs[14:]
    core = core_ref[0]
    east = jnp.where(core == 0, partner_ref[...].astype(F32), forwarded_ref[...].astype(F32))
    for level in range(LEVELS):
        field[level, HALF:] = east[:HALF, :, C * level : C * (level + 1)].astype(BF)
    field[:, :HALF] = field_keep_ref[...]
    copies = [pltpu.make_async_copy(field, outs[1], sems.at[5])]
    copies[-1].start()
    cells = east[HALF:].reshape(72, 2 * C)
    for lat in range(12):
        for lon in range(HALF // 2):
            row = (lat * 3 + lon) * 2
            merged[lat, HALF // 2 + lon] = cells[row : row + 2].astype(BF)
    merged[:, : HALF // 2] = merged_keep_ref[...]
    copies.append(pltpu.make_async_copy(merged, outs[0], sems.at[6]))
    copies[-1].start()
    scaled(factor, core, held_ref, outs, staged, sems)
    for copy in copies:
        copy.wait()


def finish_other_kernel(factor, core_ref, other_ref, *refs):
    outs, staged, sems = refs[6:12], refs[12:18], refs[18]
    scaled(factor, 1 - core_ref[0], other_ref, (None, None, *outs), staged, sems)


def finish(core, held, other, cells, factor):
    shape = jax.ShapeDtypeStruct
    whole = pl.BlockSpec(memory_space=pltpu.VMEM)
    scalar = pl.BlockSpec(memory_space=pltpu.SMEM)
    place = pl.BlockSpec(memory_space=pl.ANY)
    sums = [
        shape((C, MLP), F32),
        shape((C, MLP), F32),
        shape((C, 3 * C), F32),
        shape((MLP, 2 * C), F32),
        shape((C, C), F32),
        shape((HEADS, TYPES, BPOS), F32),
    ]
    scratch = [pltpu.VMEM(item.shape, F32) for item in sums] + [pltpu.SemaphoreType.DMA((7,))]
    grid = [shape((12, HALF, LEVELS, 2 * C), BF), shape((LEVELS, 2 * HALF, LAT, C), BF)]
    params = pltpu.CompilerParams(vmem_limit_bytes=16 * 1024 * 1024)
    merged, field, *begun = pl.pallas_call(
        lambda *refs: finish_own_kernel(factor, *refs),
        out_shape=[*grid, *sums],
        in_specs=[scalar] + [whole] * 5,
        out_specs=[place] * 8,
        scratch_shapes=scratch + [pltpu.VMEM(item.shape, BF) for item in grid],
        compiler_params=params,
        cost_estimate=pl.CostEstimate(flops=400_000, bytes_accessed=2_500_000, transcendentals=0),
        name="finish_own",
    )(core, held, *cells)
    rest = pl.pallas_call(
        lambda *refs: finish_other_kernel(factor, *refs),
        out_shape=sums,
        in_specs=[scalar, whole] + [place] * 6,
        out_specs=[place] * 6,
        scratch_shapes=scratch,
        input_output_aliases={2 + n: n for n in range(6)},
        compiler_params=params,
        name="finish_other",
    )(core, other, *begun)
    return merged, field, *rest


def passed_along(value, axis, steps):
    count = lax.axis_size(axis)
    return lax.ppermute(value, axis, [(source, (source + steps) % count) for source in range(count)])


def groups_of(count, apart, size):
    return [
        [start * apart * size + offset + member * apart for member in range(size)]
        for start in range(count // (apart * size))
        for offset in range(apart)
    ]


def summed_over(keep, send, axis, joined, partner, forward):
    count = lax.axis_size(axis)
    along = count // (CORES * ACROSS)
    pairs = [(i, i ^ 1) for i in range(count)]
    arrived = lax.ppermute(send, axis, pairs)
    held = joined(keep, arrived)

    def exchanged(value, apart, size):
        return lax.all_to_all(value, axis, 0, 0, axis_index_groups=groups_of(count, apart, size))

    def reduced(value, apart, size):
        got = exchanged(value.reshape(size, -1, *value.shape[1:]), apart, size)
        return jnp.sum(got.astype(F32), axis=0).astype(BF)

    def gathered(value, apart, size):
        return exchanged(jnp.broadcast_to(value[None], (size, *value.shape)), apart, size).reshape(-1, *value.shape[1:])

    held = reduced(held, CORES, ACROSS)
    held, partner = lax.optimization_barrier((held, partner))
    held = reduced(held.reshape(-1, 2, LANES), CORES * ACROSS, along)
    held = gathered(held, CORES * ACROSS, along).reshape(-1, LANES)
    held = gathered(held, CORES, ACROSS)
    held, forwarded = forward(held, partner)
    return held, lax.ppermute(held, axis, pairs), partner, forwarded


def local(
    fields,
    norm_gain,
    qkv_weight,
    proj_weight,
    bias_table,
    bias_index,
    region_ids,
    mlp_gain,
    up_weight,
    down_weight,
    merge_gain,
    merge_weight,
    cotangent,
):
    count = lax.axis_size("lon")
    core = (lax.axis_index("lon") % CORES).astype(jnp.int32).reshape(1)
    by_lon = fields.transpose(0, 2, 1, 3)
    by_lat = cotangent.transpose(1, 2, 0, 3)
    field_last, cotangent_last, table, index, merge_gain = stage(
        by_lon, by_lat, bias_table.transpose(1, 0, 2), bias_index, merge_gain
    )
    west = passed_along(field_last, "lon", 1)
    west_cotangent = passed_along(cotangent_last, "lon", 1)
    table, core = lax.optimization_barrier((table, core))
    bias, bias_tail = bias_rows(table, index, region_ids)
    half_rows = -(-O_END // (count * 2)) * 2 * count // CORES
    grads, tokens, scores, *results = block(
        half_rows,
        by_lon,
        west,
        by_lat,
        west_cotangent,
        norm_gain.reshape(1, C),
        qkv_weight,
        proj_weight,
        mlp_gain.reshape(1, C),
        up_weight,
        down_weight.T,
        merge_gain,
        merge_weight,
        bias,
        bias_tail,
    )
    pairs = [(i, i ^ 1) for i in range(count)]
    partner_scores = lax.ppermute(scores, "lon", pairs)
    keep, send = pack(core, grads, tokens, results[1])
    merged_keep, field_keep, home = to_grid(*results, qkv_weight, norm_gain.reshape(1, C), merge_weight)
    partner = lax.ppermute(home, "lon", pairs)

    def forward(held, leaving):
        held, leaving = lax.optimization_barrier((held, leaving))
        return held, lax.ppermute(leaving, "lon", [(i, (i - CORES) % count) for i in range(1, count, CORES)])

    table = table_sum(core, scores, partner_scores, index)
    held, other, partner, forwarded = summed_over(
        keep, send, "lon", lambda kept, arrived: join(core, kept, arrived, table), partner, forward
    )
    factor = float(LEVELS * LAT * fields.shape[2] * count) ** (-0.5)
    merged, field_grad, up_grad, down_grad, qkv_grad, merge_grad, proj_grad, table_grad = finish(
        core, held, other, (partner, forwarded, merged_keep, field_keep), factor
    )
    return (
        merged.transpose(2, 0, 1, 3),
        field_grad.transpose(0, 2, 1, 3),
        qkv_grad,
        proj_grad,
        up_grad,
        down_grad.T,
        merge_grad,
        table_grad.transpose(1, 0, 2),
    )


def solution(mesh):
    whole = P("groups", None, "lon", None)

    return jax.shard_map(
        local,
        mesh=mesh,
        in_specs=(whole, *[P()] * 11, whole),
        out_specs=(whole, whole, *[P("groups", None)] * 5, P("groups", None, None)),
        check_vma=False,
    )
```

```python
import jax
import jax.numpy as jnp
from jax import lax
from jax.experimental import pallas as pl
from jax.experimental.pallas import tpu as pltpu
from jax.sharding import PartitionSpec as P

C = 192
MLP = 768
HEADS = 6
HEAD = 32
HALF = 6
WIN = 144
BPOS = 3312
LAT = 24
TYPES = 4
TOK = TYPES * WIN
LEVELS = 2
LANES = 128
MAIN = 128
REST = WIN - MAIN
TH = TYPES * HEADS
LOW = 256
HIGH = -(-BPOS // LOW)
MTOK = 160
EPS = 1e-5
MASKED = -1e30
F32 = jnp.float32
BF = jnp.bfloat16
CORES = 2
ACROSS = 4

TROWS = 320
MSPLIT = 512
O_UP = 0
O_QKV = O_UP + 6 * C
O_QKV_TAIL = O_QKV + 4 * C
O_PROJ = O_QKV_TAIL + C // 2
O_PROJ_TAIL = O_PROJ + C
O_TABLE = O_PROJ_TAIL + C // 2
O_MERGE_LAST = O_TABLE + 2 * TROWS
O_MERGE = O_MERGE_LAST + MLP - MSPLIT
O_DOWN = O_MERGE + 2 * MLP + MSPLIT
O_END = O_DOWN + 6 * C

DS_TAIL = TH * WIN
DS_CORNER = DS_TAIL + TH * REST
DS_END = DS_CORNER + TH * REST


def dot(a, b):
    return jnp.dot(a, b, preferred_element_type=F32)


def dot_nt(a, b):
    return lax.dot_general(a, b, (((1,), (1,)), ((), ())), preferred_element_type=F32)


def dot_tn(a, b):
    return lax.dot_general(a, b, (((0,), (0,)), ((), ())), preferred_element_type=F32)


def div(n, d):
    return (n * -(-(1 << 16) // d)) >> 16


def onehot(rows, cols, of_row=None, of_col=None):
    if of_row is not None:
        target = of_row(lax.broadcasted_iota(jnp.int32, (rows, 1), 0))
        place = lax.broadcasted_iota(jnp.int32, (rows, cols), 1)
    else:
        target = of_col(lax.broadcasted_iota(jnp.int32, (1, cols), 1))
        place = lax.broadcasted_iota(jnp.int32, (rows, cols), 0)
    return jnp.where(place == target, 1.0, 0.0).astype(BF)


def cell_of_token(n):
    kind = div(n, 72)
    rest = n - 72 * kind
    lat = div(rest, 12)
    return (rest - 12 * lat) * LAT + kind * 6 + lat


def token_of_group(n):
    quarter = div(n, 40)
    rest = n - 40 * quarter
    level = div(rest, 18)
    part = rest - 18 * level
    lat = div(part, 6)
    token = level * 72 + (2 * lat + (quarter >> 1)) * 12 + 2 * (part - 6 * lat) + (quarter & 1)
    return jnp.where(rest < 36, token, -1)


def group_of_token(n):
    level = div(n, 72)
    rest = n - 72 * level
    lat = div(rest, 12)
    lon = rest - 12 * lat
    return ((lat & 1) * 2 + (lon & 1)) * 40 + level * 18 + (lat >> 1) * 6 + (lon >> 1)


def cell_of_merged(n):
    kind = div(n, 40)
    rest = n - 40 * kind
    level = div(rest, 18)
    part = rest - 18 * level
    lat = div(part, 6)
    lon = part - 6 * lat
    half = jnp.where(lon < 3, 0, 1)
    row = half * 72 + (3 * kind + lat) * 6 + (lon - 3 * half) * 2 + level
    return jnp.where(rest < 36, row, -1)


def normalised(values):
    centred = values - jnp.mean(values, axis=-1, keepdims=True)
    scale = lax.rsqrt(jnp.mean(centred * centred, axis=-1, keepdims=True) + EPS)
    return centred * scale, scale


def norm_grad(grad, unit, scale, gain):
    scaled = grad * gain
    return scale * (
        scaled
        - jnp.mean(scaled, axis=-1, keepdims=True)
        - unit * jnp.mean(scaled * unit, axis=-1, keepdims=True)
    )


def rounded(values):
    return values.astype(BF).astype(F32)


def low_onehot(low):
    place = lax.broadcasted_iota(jnp.int32, (LOW, 1), 0).astype(F32).astype(BF)
    hit = jnp.broadcast_to(place, (LOW, low.shape[1])) == low.astype(F32).astype(BF)
    return jnp.where(hit, jnp.array(1, BF), jnp.array(0, BF))


def bias_kernel(table_ref, index_ref, regions_ref, main_ref, tail_ref, part_ref, last_ref, turned_ref, mask_ref, region_ref, sem):
    copy = pltpu.make_async_copy(regions_ref, region_ref, sem)
    copy.start()
    for high in range(HIGH):
        width = min(LOW, BPOS - high * LOW)
        for head in range(HEADS):
            piece = table_ref[head, :, high * LOW : high * LOW + width]
            if width < LOW:
                piece = jnp.concatenate([piece, jnp.zeros((TYPES, LOW - width), F32)], axis=1)
            row = high * TH + head * TYPES
            part_ref[row : row + TYPES, :] = piece
    turned_ref[...] = jnp.transpose(index_ref[:, MAIN:])
    parts = part_ref[...].astype(BF)

    def looked_up(index):
        low = low_onehot(index & (LOW - 1))
        high_row = index >> 8
        found = dot(parts, low)
        chosen = found[0:TH]
        for high in range(1, HIGH):
            chosen = jnp.where(high_row == high, found[high * TH : (high + 1) * TH], chosen)
        return chosen

    for start in range(0, REST, 4):
        got = looked_up(jnp.concatenate([turned_ref[start + n : start + n + 1, :MAIN] for n in range(4)], axis=1))
        for n in range(4):
            last_ref[pl.ds(start + n, TH, stride=REST), :] = got[:, n * MAIN : (n + 1) * MAIN]
    got = looked_up(jnp.concatenate([turned_ref[n : n + 1, MAIN:] for n in range(REST)], axis=1))
    for n in range(REST):
        half = got[:, LANES * (n // 8) : LANES * (n // 8 + 1)]
        half = half if n % 8 == 0 else pltpu.roll(half, LANES - REST * (n % 8), 1)
        last_ref[pl.ds(TH * REST + n, TH, stride=REST), :] = half
    copy.wait()
    kind_of = lax.broadcasted_iota(jnp.int32, (TH, 1), 0) & (TYPES - 1)
    column = lax.broadcasted_iota(jnp.int32, (1, LANES), 1)
    labels = []
    for group in range(12):
        label = jnp.zeros((TH, 1), jnp.int32)
        for kind in range(TYPES):
            label = jnp.where(kind_of == kind, region_ref[group // 6, 6 * kind + group % 6], label)
        labels.append(label)
    keys = jnp.zeros((TH, LANES), jnp.int32)
    for group in range(11):
        keys = jnp.where((column >= 12 * group) & (column < 12 * group + 12), labels[group], keys)
    for group in range(12):
        mask_ref[TH * group : TH * (group + 1), :] = jnp.where(keys == labels[group], 0.0, MASKED)

    def row_block(block, carry):
        base = pl.multiple_of(block * 8, 8)
        rows = index_ref[pl.ds(base, 8), :MAIN]
        for part in range(4):
            index = jnp.concatenate([rows[2 * part + n : 2 * part + n + 1] for n in range(2)], axis=1)
            got = looked_up(index)
            for n in range(2):
                row = base + 2 * part + n
                mask = mask_ref[pl.ds(pl.multiple_of(div(row, 12) * TH, 8), TH), :]
                main_ref[pl.ds(row, TH, stride=WIN), :] = got[:, n * MAIN : (n + 1) * MAIN] + mask
        return carry

    lax.fori_loop(0, WIN // 8, row_block, 0, unroll=True)
    apart = jnp.where(labels[10] == labels[11], 0.0, MASKED)
    split = 132 - MAIN
    for n in range(REST):
        group = (MAIN + n) // 12
        rows = pl.ds(n, TH, stride=REST)
        last_ref[rows, :] = last_ref[rows, :] + mask_ref[TH * group : TH * (group + 1), :]
        rows = pl.ds(TH * REST + n, TH, stride=REST)
        other = (column < split) if n >= split else (column >= split)
        last_ref[rows, :] = last_ref[rows, :] + jnp.where(other, apart, 0.0)
    for th in range(TH):
        rows = slice(th * WIN, th * WIN + MAIN)
        tail_ref[rows, :REST] = jnp.transpose(last_ref[th * REST : (th + 1) * REST, :])
        rows = slice(th * WIN + MAIN, (th + 1) * WIN)
        tail_ref[rows, :REST] = jnp.transpose(last_ref[(TH + th) * REST : (TH + th + 1) * REST, :])[:REST]


def stage_kernel(fields_ref, cotangent_ref, table_ref, index_ref, gain_ref, leaving_ref, table_out, index_out, gain_out, field_ref, half_ref, cells_ref, sems):
    copies = [
        pltpu.make_async_copy(source, target, sems.at[n])
        for n, (source, target) in enumerate(
            [
                (fields_ref.at[:, HALF:], field_ref),
                (cotangent_ref.at[:, HALF // 2 :], half_ref),
                (table_ref, table_out),
                (index_ref, index_out),
                (gain_ref, gain_out.at[0]),
            ]
        )
    ]
    for copy in copies:
        copy.start()
    for copy in copies[:2]:
        copy.wait()
    leaving_ref[:HALF] = jnp.concatenate([field_ref[level].astype(F32) for level in range(LEVELS)], axis=-1).astype(BF)
    for lat in range(12):
        for lon in range(HALF // 2):
            row = (lat * 3 + lon) * 2
            cells_ref[row : row + 2, :] = half_ref[lat, lon].astype(F32)
    leaving_ref[HALF:] = cells_ref[...].reshape(3, LAT, 2 * C).astype(BF)
    for copy in copies[2:]:
        copy.wait()


def stage(fields, cotangent, table, index, gain):
    shape = jax.ShapeDtypeStruct
    whole = pl.BlockSpec(memory_space=pltpu.VMEM)
    return pl.pallas_call(
        stage_kernel,
        out_shape=[
            shape((HALF + 3, LAT, 2 * C), BF),
            shape(table.shape, F32),
            shape(index.shape, jnp.int32),
            shape((1, 4 * C), F32),
        ],
        in_specs=[pl.BlockSpec(memory_space=pltpu.HBM)] * 5,
        out_specs=[whole] * 4,
        scratch_shapes=[
            pltpu.VMEM((LEVELS, HALF, LAT, C), BF),
            pltpu.VMEM((12, HALF // 2, LEVELS, 2 * C), BF),
            pltpu.VMEM((72, 2 * C), F32),
            pltpu.SemaphoreType.DMA((5,)),
        ],
        compiler_params=pltpu.CompilerParams(vmem_limit_bytes=4 * 1024 * 1024),
        name="stage",
    )(*(pltpu.with_memory_space_constraint(a, pltpu.HBM) for a in (fields, cotangent, table, index, gain)))


def bias_rows(table, index, regions):
    whole = pl.BlockSpec(memory_space=pltpu.VMEM)
    return pl.pallas_call(
        bias_kernel,
        out_shape=[jax.ShapeDtypeStruct((TH * WIN, LANES), F32)] * 2,
        in_specs=[whole, whole, pl.BlockSpec(memory_space=pltpu.HBM)],
        out_specs=[whole, whole],
        scratch_shapes=[
            pltpu.VMEM((HIGH * TH, LOW), F32),
            pltpu.VMEM((2 * TH * REST, LANES), F32),
            pltpu.VMEM((REST, WIN), jnp.int32),
            pltpu.VMEM((12 * TH, LANES), F32),
            pltpu.SMEM((LEVELS, LAT), jnp.int32),
            pltpu.SemaphoreType.DMA,
        ],
        compiler_params=pltpu.CompilerParams(vmem_limit_bytes=16 * 1024 * 1024),
        cost_estimate=pl.CostEstimate(flops=14_000_000_000, bytes_accessed=4_000_000, transcendentals=0),
        name="bias_rows",
    )(table, index, pltpu.with_memory_space_constraint(regions, pltpu.HBM))


def block_kernel(
    own_ref, west_ref, own_cotangent_ref,
    norm_gain_ref, qkv_ref, proj_ref, mlp_gain_ref, up_ref, down_ref, merge_gain_ref, merge_ref,
    bias_ref, bias_tail_ref,
    grads_ref, tokens_ref, ds_ref, normed_merge_ref, triple_ref, grad_attn_ref, unit_ref, scale_ref,
    x_ref, q_ref, k_ref, v_ref, p_ref, mixed_ref,
    unit_mlp_ref, scale_mlp_ref, normed_mlp_ref, hidden_ref, slope_ref, after_mlp_ref,
    group_ref, grad_after_ref, grad_up_ref, grad_mixed_ref,
    cells_ref, grad_merged_ref, scaled_ref,
):
    to_tokens = onehot(288, 288, of_row=cell_of_token)
    west = west_ref[:HALF].astype(F32).reshape(144, 2 * C)
    for level in range(LEVELS):
        cells = jnp.concatenate(
            [
                west[:, C * level : C * (level + 1)],
                own_ref[level, :HALF].astype(F32).reshape(144, C),
            ],
            axis=0,
        ).astype(BF)
        ordered = dot(to_tokens, cells)
        for kind in range(TYPES):
            x_ref[WIN * kind + 72 * level : WIN * kind + 72 * level + 72, :] = ordered[72 * kind : 72 * kind + 72]
    cells_ref[:72, :] = west_ref[HALF:].astype(F32).reshape(72, 2 * C)
    for lat in range(12):
        for lon in range(HALF // 2):
            row = (lat * 3 + lon) * 2
            cells_ref[72 + row : 74 + row, :] = own_cotangent_ref[lat, lon].astype(F32)
    grad_merged_ref[...] = dot(onehot(MTOK, 144, of_row=cell_of_merged), cells_ref[...].astype(BF)).astype(BF)
    for n in range(4):
        value = rounded(dot_nt(grad_merged_ref[...], merge_ref[C * n : C * (n + 1), :]))
        scaled_ref[n] = value * merge_gain_ref[:, C * n : C * (n + 1)]
    unit, scale = normalised(x_ref[...])
    unit_ref[...] = unit
    scale_ref[...] = scale
    tokens = (unit * norm_gain_ref[...]).astype(BF)
    tokens_ref[...] = tokens
    q_ref[...] = dot(tokens, qkv_ref[:, 0:C]).astype(BF)
    k_ref[...] = dot(tokens, qkv_ref[:, C : 2 * C]).astype(BF)
    v_ref[...] = dot(tokens, qkv_ref[:, 2 * C :]).astype(BF)
    lane = lax.broadcasted_iota(jnp.int32, (1, C), 1)
    of_head = [
        jnp.where((lane >= HEAD * h) & (lane < HEAD * (h + 1)), 1.0, 0.0).astype(BF) for h in range(HEADS)
    ]
    temper = HEAD ** (-0.5)

    def attend(kind, carry):
        rows = pl.ds(pl.multiple_of(kind * WIN, 16), WIN)
        q, k, v = q_ref[rows, :], k_ref[rows, :], v_ref[rows, :]
        mixed = jnp.zeros((WIN, C), F32)
        products = dot_nt(jnp.concatenate([q * of_head[h] for h in range(HEADS)], axis=0), k)
        for h in range(HEADS):
            th = h * TYPES + kind
            scores_at = pl.ds(pl.multiple_of(th * WIN, 16), WIN)
            bias = jnp.concatenate([bias_ref[scores_at, :], bias_tail_ref[scores_at, :REST]], axis=1)
            scores = products[WIN * h : WIN * (h + 1)] * temper + bias
            weights = jnp.exp(scores - jnp.max(scores, axis=-1, keepdims=True))
            p = weights * (1.0 / jnp.sum(weights, axis=-1, keepdims=True))
            p_ref[th] = p
            mixed = mixed + dot(p.astype(BF), v * of_head[h])
        mixed_ref[rows, :] = mixed.astype(BF)
        return carry

    lax.fori_loop(0, TYPES, attend, 0, unroll=True)
    after_attn = rounded(x_ref[...] + rounded(dot(mixed_ref[...], proj_ref[...])))
    x_ref[...] = after_attn
    unit, scale = normalised(after_attn)
    unit_mlp_ref[...] = unit
    scale_mlp_ref[...] = scale
    normed_mlp = (unit * mlp_gain_ref[...]).astype(BF)
    normed_mlp_ref[...] = normed_mlp
    for part in range(3):
        cols = slice(256 * part, 256 * part + 256)
        u = dot(normed_mlp, up_ref[:, cols])
        below = 0.5 * (1.0 + lax.erf(u * 0.5**0.5))
        hidden_ref[:, cols] = (u * below).astype(BF)
        slope_ref[:, cols] = below + u * (jnp.exp(u * u * (-0.5)) * 0.3989422804014327)
    after_mlp_ref[...] = (x_ref[...] + dot_nt(hidden_ref[...], down_ref[...])).astype(BF)

    to_groups = onehot(160, WIN, of_row=token_of_group)
    for kind in range(TYPES):
        grouped = dot(to_groups, after_mlp_ref[WIN * kind : WIN * kind + WIN, :])
        for quarter in range(4):
            group_ref[quarter, 40 * kind : 40 * kind + 40, :] = grouped[40 * quarter : 40 * quarter + 40]
    quarters = [group_ref[n] for n in range(4)]
    mean = jnp.sum(sum(quarters), axis=-1, keepdims=True) * (1.0 / MLP)
    centred = [v - mean for v in quarters]
    variance = jnp.sum(sum(v * v for v in centred), axis=-1, keepdims=True) * (1.0 / MLP)
    scale_merge = lax.rsqrt(variance + EPS)
    for n in range(4):
        unit = centred[n] * scale_merge
        group_ref[n] = unit
        normed_merge = (unit * merge_gain_ref[:, C * n : C * (n + 1)]).astype(BF)
        normed_merge_ref[n] = normed_merge
    scaled, total, along = [], 0.0, 0.0
    for n in range(4):
        value = scaled_ref[n]
        total = total + value
        along = along + value * group_ref[n]
        scaled.append(value)
    total = jnp.sum(total, axis=-1, keepdims=True) * (1.0 / MLP)
    along = jnp.sum(along, axis=-1, keepdims=True) * (1.0 / MLP)
    for n in range(4):
        group_ref[n] = scale_merge * (scaled[n] - total - group_ref[n] * along)
    from_groups = onehot(WIN, 160, of_row=group_of_token)
    for kind in range(TYPES):
        grouped = jnp.concatenate([group_ref[n, 40 * kind : 40 * kind + 40, :] for n in range(4)], axis=0)
        grad_after_ref[WIN * kind : WIN * kind + WIN, :] = dot(from_groups, grouped.astype(BF)).astype(BF)

    grad_after = grad_after_ref[...]
    for part in range(3):
        cols = slice(256 * part, 256 * part + 256)
        grad_up_ref[:, cols] = (rounded(dot(grad_after, down_ref[:, cols])) * slope_ref[:, cols]).astype(BF)
    grad_normed = rounded(dot_nt(grad_up_ref[...], up_ref[...]))
    grad_attn = (
        grad_after.astype(F32)
        + norm_grad(grad_normed, unit_mlp_ref[...], scale_mlp_ref[...], mlp_gain_ref[...])
    ).astype(BF)
    grad_attn_ref[...] = grad_attn

    grad_mixed_ref[...] = dot_nt(grad_attn, proj_ref[...]).astype(BF)

    def down_terms():
        grad = dot_tn(grad_after_ref[...], hidden_ref[...]).astype(BF)
        for b in range(6):
            grads_ref[O_DOWN + C * b : O_DOWN + C * (b + 1), :] = grad[:, 128 * b : 128 * b + 128]

    def up_terms():
        grad = dot_tn(normed_mlp_ref[...], grad_up_ref[...]).astype(BF)
        for b in range(6):
            grads_ref[O_UP + C * b : O_UP + C * (b + 1), :] = grad[:, 128 * b : 128 * b + 128]

    def merge_terms():
        for n in range(4):
            grad = dot_tn(normed_merge_ref[n], grad_merged_ref[...]).astype(BF)
            for b in range(2):
                start = O_MERGE + MLP * b + C * n
                grads_ref[start : start + C, :] = grad[:, 128 * b : 128 * b + 128]
            kept = max(0, min(C, MSPLIT - C * n))
            if kept:
                start = O_MERGE + 2 * MLP + C * n
                grads_ref[start : start + kept, :] = grad[:kept, 256:]
            if kept < C:
                start = O_MERGE_LAST + C * n + kept - MSPLIT
                grads_ref[start : start + C - kept, :] = grad[kept:, 256:]

    def proj_terms():
        grad_proj = dot_tn(mixed_ref[...], grad_attn_ref[...]).astype(BF)
        grads_ref[O_PROJ : O_PROJ + C, :] = grad_proj[:, :128]
        grads_ref[O_PROJ_TAIL : O_PROJ_TAIL + C // 2, :] = jnp.concatenate(
            [grad_proj[: C // 2, 128:], grad_proj[C // 2 :, 128:]], axis=1
        )

    last_keys = onehot(REST, WIN, of_row=lambda n: n + MAIN)
    ds_ref[DS_CORNER:, :] = jnp.zeros((TH * REST, LANES), BF)
    grads_ref[O_QKV:O_PROJ, :] = jnp.zeros((O_PROJ - O_QKV, LANES), BF)
    grads_ref[O_TABLE:O_MERGE_LAST, :] = jnp.zeros((O_MERGE_LAST - O_TABLE, LANES), BF)

    def attend_back(kind, carry):
        rows = pl.ds(kind * WIN, WIN)
        v, grad = v_ref[rows, :], grad_mixed_ref[rows, :]
        q_turned, k_turned, grad_turned = (jnp.transpose(a) for a in (q_ref[rows, :], k_ref[rows, :], grad))
        products = dot_nt(jnp.concatenate([grad * of_head[h] for h in range(HEADS)], axis=0), v)
        dq, dk, dv = [], [], []
        for h in range(HEADS):
            th = h * TYPES + kind
            lanes = slice(HEAD * h, HEAD * (h + 1))
            p = p_ref[th]
            weighted = p * products[WIN * h : WIN * (h + 1)]
            ds = weighted - p * jnp.sum(weighted, axis=-1, keepdims=True)
            ds = ds.astype(BF)
            ds_ref[pl.ds(th * WIN, WIN), :] = ds[:, :MAIN]
            turned = dot_nt(jnp.concatenate([k_turned[lanes], last_keys], axis=0), ds)
            tail = turned[HEAD:].astype(BF)
            ds_ref[pl.ds(DS_TAIL + th * REST, REST), :] = tail[:, :MAIN]
            ds_ref[pl.ds(DS_CORNER + th * REST, REST), :REST] = tail[:, MAIN:]
            dq.append(turned[:HEAD])
            dk.append(dot(q_turned[lanes], ds))
            dv.append(dot(grad_turned[lanes], p.astype(BF)))
        triple = jnp.concatenate([a * temper for a in dq + dk] + dv, axis=0).astype(BF)
        triple_ref[rows, :] = jnp.transpose(triple)
        return carry

    for kind, terms in enumerate((down_terms, up_terms, merge_terms, proj_terms)):
        attend_back(kind, 0)
        terms()


def block(half_rows, *args):
    shape = jax.ShapeDtypeStruct
    whole = pl.BlockSpec(memory_space=pltpu.VMEM)
    scratch = [
        ((TOK, C), F32), ((TOK, C), BF), ((TOK, C), BF),
        ((TOK, C), BF), ((TH, WIN, WIN), F32), ((TOK, C), BF),
        ((TOK, C), F32), ((TOK, 1), F32), ((TOK, C), BF), ((TOK, MLP), BF), ((TOK, MLP), F32), ((TOK, C), BF),
        ((4, MTOK, C), F32), ((TOK, C), BF), ((TOK, MLP), BF), ((TOK, C), BF),
        ((144, 2 * C), F32), ((MTOK, 2 * C), BF), ((4, MTOK, C), F32),
    ]
    return pl.pallas_call(
        block_kernel,
        out_shape=[
            shape((2 * half_rows, LANES), BF),
            shape((TOK, C), BF),
            shape((DS_END, LANES), BF),
            shape((4, MTOK, C), BF),
            shape((TOK, 3 * C), BF),
            shape((TOK, C), BF),
            shape((TOK, C), F32),
            shape((TOK, 1), F32),
        ],
        in_specs=[whole] * len(args),
        out_specs=[whole] * 8,
        scratch_shapes=[pltpu.VMEM(*item) for item in scratch],
        compiler_params=pltpu.CompilerParams(vmem_limit_bytes=24 * 1024 * 1024),
        cost_estimate=pl.CostEstimate(flops=24_000_000_000, bytes_accessed=12_000_000, transcendentals=2_000_000),
        name="block",
    )(*args)


def pack_kernel(core_ref, grads_ref, tokens_ref, triple_ref, keep_ref, send_ref):
    half = keep_ref.shape[0]
    core = core_ref[0]
    grad_qkv = dot_tn(tokens_ref[...], triple_ref[...]).astype(BF)
    tail = jnp.concatenate([grad_qkv[: C // 2, 512:], grad_qkv[C // 2 :, 512:]], axis=1)
    keep_ref[...] = grads_ref[pl.ds(pl.multiple_of(core * half, 16), half), :]
    send_ref[...] = grads_ref[pl.ds(pl.multiple_of((1 - core) * half, 16), half), :]
    for owner, target_ref in ((0, keep_ref), (1, send_ref)):

        @pl.when(core == owner)
        def _():
            for b in range(4):
                target_ref[O_QKV + C * b : O_QKV + C * (b + 1), :] = grad_qkv[:, 128 * b : 128 * b + 128]
            target_ref[O_QKV_TAIL : O_QKV_TAIL + C // 2, :] = tail


def pack(core, grads, tokens, triple):
    half = jax.ShapeDtypeStruct((grads.shape[0] // 2, LANES), BF)
    whole = pl.BlockSpec(memory_space=pltpu.VMEM)
    return pl.pallas_call(
        pack_kernel,
        out_shape=[half, half],
        in_specs=[pl.BlockSpec(memory_space=pltpu.SMEM)] + [whole] * 3,
        out_specs=[whole] * 2,
        compiler_params=pltpu.CompilerParams(vmem_limit_bytes=12 * 1024 * 1024),
        cost_estimate=pl.CostEstimate(flops=600_000_000, bytes_accessed=4_000_000, transcendentals=0),
        name="pack",
    )(core, grads, tokens, triple)


def table_kernel(core_ref, own_ref, partner_ref, index_ref, table_ref, ds_ref, turned_ref):
    def table_terms(index, slab):
        high_row = index >> 8
        spread = [jnp.where(high_row == n, slab, 0.0) for n in range(HIGH)]
        spread.append(jnp.zeros((TROWS - HIGH * TH, index.shape[1]), F32))
        return dot_nt(jnp.concatenate(spread, axis=0).astype(BF), low_onehot(index & (LOW - 1)))

    def row_block(block, carry):
        base = pl.multiple_of(block * 8, 8)
        rows = index_ref[pl.ds(base, 8), :MAIN]
        index = jnp.concatenate([rows[n : n + 1] for n in range(8)], axis=1)
        slab = jnp.concatenate([ds_ref[pl.ds(base + n, TH, stride=WIN), :] for n in range(8)], axis=1)
        return carry + table_terms(index, slab)

    @pl.when(core_ref[0] == 0)
    def _():
        ds_ref[...] = own_ref[...].astype(F32) + partner_ref[...].astype(F32)
        turned_ref[...] = jnp.transpose(index_ref[:, MAIN:])
        table = lax.fori_loop(0, WIN // 8, row_block, jnp.zeros((TROWS, LOW), F32), unroll=True)
        index = jnp.concatenate([turned_ref[n : n + 1, :MAIN] for n in range(REST)], axis=1)
        slab = jnp.concatenate([ds_ref[pl.ds(DS_TAIL + n, TH, stride=REST), :] for n in range(REST)], axis=1)
        table = table + table_terms(index, slab)
        index = jnp.concatenate([turned_ref[n : n + 1, MAIN:] for n in range(REST)], axis=1)
        slab = jnp.concatenate(
            [ds_ref[pl.ds(DS_CORNER + n, TH, stride=REST), :][:, :REST] for n in range(REST)], axis=1
        )
        table = (table + table_terms(index, slab)).astype(BF)
        table_ref[:TROWS, :] = table[:, :LANES]
        table_ref[TROWS:, :] = table[:, LANES:]

    @pl.when(core_ref[0] == 1)
    def _():
        table_ref[...] = jnp.zeros(table_ref.shape, BF)


def table_sum(core, own, partner, index):
    whole = pl.BlockSpec(memory_space=pltpu.VMEM)
    return pl.pallas_call(
        table_kernel,
        out_shape=jax.ShapeDtypeStruct((2 * TROWS, LANES), BF),
        in_specs=[pl.BlockSpec(memory_space=pltpu.SMEM)] + [whole] * 3,
        out_specs=whole,
        scratch_shapes=[pltpu.VMEM((DS_END, LANES), F32), pltpu.VMEM((REST, WIN), jnp.int32)],
        compiler_params=pltpu.CompilerParams(vmem_limit_bytes=12 * 1024 * 1024),
        cost_estimate=pl.CostEstimate(flops=4_000_000_000, bytes_accessed=3_000_000, transcendentals=0),
        name="table_sum",
    )(core, own, partner, index)


def join_kernel(core_ref, keep_ref, arrived_ref, table_ref, held_ref):
    held_ref[...] = (keep_ref[...].astype(F32) + arrived_ref[...].astype(F32)).astype(BF)

    @pl.when(core_ref[0] == 0)
    def _():
        held_ref[O_TABLE : O_TABLE + 2 * TROWS, :] = table_ref[...]


def join(core, keep, arrived, table):
    whole = pl.BlockSpec(memory_space=pltpu.VMEM)
    return pl.pallas_call(
        join_kernel,
        out_shape=jax.ShapeDtypeStruct(keep.shape, BF),
        in_specs=[pl.BlockSpec(memory_space=pltpu.SMEM)] + [whole] * 3,
        out_specs=whole,
        compiler_params=pltpu.CompilerParams(vmem_limit_bytes=8 * 1024 * 1024),
        cost_estimate=pl.CostEstimate(flops=400_000, bytes_accessed=2_500_000, transcendentals=0),
        name="join",
    )(core, keep, arrived, table)


def cells_kernel(
    normed_merge_ref, triple_ref, grad_attn_ref, unit_ref, scale_ref, qkv_ref, gain_ref, merge_ref,
    merged_keep_ref, field_keep_ref, home_ref, x_ref,
):
    merged = sum(dot(normed_merge_ref[n], merge_ref[C * n : C * (n + 1), :]) for n in range(4))
    grad_normed = rounded(dot_nt(triple_ref[...], qkv_ref[...]))
    merged_cells = dot(onehot(144, MTOK, of_col=cell_of_merged), merged.astype(BF))
    x_ref[...] = grad_attn_ref[...].astype(F32) + norm_grad(
        grad_normed, unit_ref[...], scale_ref[...], gain_ref[...]
    )
    to_cells = onehot(288, 288, of_col=cell_of_token)
    leaving = []
    for level in range(LEVELS):
        ordered = jnp.concatenate(
            [x_ref[WIN * kind + 72 * level : WIN * kind + 72 * level + 72, :] for kind in range(TYPES)], axis=0
        )
        cells = dot(to_cells, ordered.astype(BF))
        leaving.append(cells[:144])
        field_keep_ref[level] = cells[144:].reshape(HALF, LAT, C).astype(BF)
    home_ref[:HALF] = jnp.concatenate(leaving, axis=1).reshape(HALF, LAT, 2 * C).astype(BF)
    for lat in range(12):
        for lon in range(HALF // 2):
            row = 72 + (lat * 3 + lon) * 2
            merged_keep_ref[lat, lon] = merged_cells[row : row + 2].astype(BF)
    home_ref[HALF:] = merged_cells[:72].reshape(3, LAT, 2 * C).astype(BF)


def to_grid(*args):
    shape = jax.ShapeDtypeStruct
    whole = pl.BlockSpec(memory_space=pltpu.VMEM)
    return pl.pallas_call(
        cells_kernel,
        out_shape=[
            shape((12, HALF // 2, LEVELS, 2 * C), BF),
            shape((LEVELS, HALF, LAT, C), BF),
            shape((HALF + 3, LAT, 2 * C), BF),
        ],
        in_specs=[whole] * 8,
        out_specs=[whole] * 3,
        scratch_shapes=[pltpu.VMEM((TOK, C), F32)],
        compiler_params=pltpu.CompilerParams(vmem_limit_bytes=12 * 1024 * 1024),
        cost_estimate=pl.CostEstimate(flops=1_500_000_000, bytes_accessed=3_000_000, transcendentals=0),
        name="to_grid",
    )(*args)


def first_half(part, refs, staged, leaves):
    _, _, up_ref, _, qkv_ref, merge_ref, proj_ref, table_ref = refs
    up, _, qkv, merge, proj, table = staged
    for b in range(6):
        up[:, 128 * b : 128 * b + 128] = part(O_UP + C * b, C)
    leaves(up, up_ref)
    for b in range(4):
        qkv[:, 128 * b : 128 * b + 128] = part(O_QKV + C * b, C)
    tail = part(O_QKV_TAIL, C // 2)
    qkv[: C // 2, 512:] = tail[:, :64]
    qkv[C // 2 :, 512:] = tail[:, 64:]
    leaves(qkv, qkv_ref)
    for side in range(2):
        terms = part(O_TABLE + TROWS * side, TROWS)
        for high in range(HIGH):
            start = high * LOW + side * LANES
            width = min(LANES, BPOS - start)
            for head in range(HEADS):
                row = high * TH + head * TYPES
                table[head, :, start : start + width] = terms[row : row + TYPES, :width]
    leaves(table, table_ref)
    proj[:, :128] = part(O_PROJ, C)
    tail = part(O_PROJ_TAIL, C // 2)
    proj[: C // 2, 128:] = tail[:, :64]
    proj[C // 2 :, 128:] = tail[:, 64:]
    leaves(proj, proj_ref)
    merge[MSPLIT:, 256:] = part(O_MERGE_LAST, MLP - MSPLIT)
    leaves(merge.at[MSPLIT:, 256:], merge_ref.at[MSPLIT:, 256:])


def second_half(part, refs, staged, leaves):
    _, _, _, down_ref, _, merge_ref, _, _ = refs
    _, down, _, merge, _, _ = staged
    for b in range(2):
        merge[:, 128 * b : 128 * b + 128] = part(O_MERGE + MLP * b, MLP)
    leaves(merge.at[:, :256], merge_ref.at[:, :256])
    for b in range(6):
        down[:, 128 * b : 128 * b + 128] = part(O_DOWN + C * b, C)
    leaves(down, down_ref)
    merge[:MSPLIT, 256:] = part(O_MERGE + 2 * MLP, MSPLIT)
    leaves(merge.at[:MSPLIT, 256:], merge_ref.at[:MSPLIT, 256:])


def scaled(factor, half, sums_ref, outs, staged, sems):
    for which, fill, base in ((0, first_half, 0), (1, second_half, O_MERGE)):

        @pl.when(half == which)
        def _():
            begun = []

            def part(start, rows):
                return sums_ref[start - base : start - base + rows, :].astype(F32) * factor

            def leaves(source, target):
                begun.append(pltpu.make_async_copy(source, target, sems.at[len(begun)]))
                begun[-1].start()

            fill(part, outs, staged, leaves)
            for copy in begun:
                copy.wait()


def finish_own_kernel(
    factor, core_ref, held_ref, partner_ref, forwarded_ref, merged_keep_ref, field_keep_ref, *refs
):
    outs, staged, (sems, merged, field) = refs[:8], refs[8:14], refs[14:]
    core = core_ref[0]
    east = jnp.where(core == 0, partner_ref[...].astype(F32), forwarded_ref[...].astype(F32))
    for level in range(LEVELS):
        field[level, HALF:] = east[:HALF, :, C * level : C * (level + 1)].astype(BF)
    field[:, :HALF] = field_keep_ref[...]
    copies = [pltpu.make_async_copy(field, outs[1], sems.at[5])]
    copies[-1].start()
    cells = east[HALF:].reshape(72, 2 * C)
    for lat in range(12):
        for lon in range(HALF // 2):
            row = (lat * 3 + lon) * 2
            merged[lat, HALF // 2 + lon] = cells[row : row + 2].astype(BF)
    merged[:, : HALF // 2] = merged_keep_ref[...]
    copies.append(pltpu.make_async_copy(merged, outs[0], sems.at[6]))
    copies[-1].start()
    scaled(factor, core, held_ref, outs, staged, sems)
    for copy in copies:
        copy.wait()


def finish_other_kernel(factor, core_ref, other_ref, *refs):
    outs, staged, sems = refs[6:12], refs[12:18], refs[18]
    scaled(factor, 1 - core_ref[0], other_ref, (None, None, *outs), staged, sems)


def finish(core, held, other, cells, factor):
    shape = jax.ShapeDtypeStruct
    whole = pl.BlockSpec(memory_space=pltpu.VMEM)
    scalar = pl.BlockSpec(memory_space=pltpu.SMEM)
    place = pl.BlockSpec(memory_space=pl.ANY)
    sums = [
        shape((C, MLP), F32),
        shape((C, MLP), F32),
        shape((C, 3 * C), F32),
        shape((MLP, 2 * C), F32),
        shape((C, C), F32),
        shape((HEADS, TYPES, BPOS), F32),
    ]
    scratch = [pltpu.VMEM(item.shape, F32) for item in sums] + [pltpu.SemaphoreType.DMA((7,))]
    grid = [shape((12, HALF, LEVELS, 2 * C), BF), shape((LEVELS, 2 * HALF, LAT, C), BF)]
    params = pltpu.CompilerParams(vmem_limit_bytes=16 * 1024 * 1024)
    merged, field, *begun = pl.pallas_call(
        lambda *refs: finish_own_kernel(factor, *refs),
        out_shape=[*grid, *sums],
        in_specs=[scalar] + [whole] * 5,
        out_specs=[place] * 8,
        scratch_shapes=scratch + [pltpu.VMEM(item.shape, BF) for item in grid],
        compiler_params=params,
        cost_estimate=pl.CostEstimate(flops=400_000, bytes_accessed=2_500_000, transcendentals=0),
        name="finish_own",
    )(core, held, *cells)
    rest = pl.pallas_call(
        lambda *refs: finish_other_kernel(factor, *refs),
        out_shape=sums,
        in_specs=[scalar, whole] + [place] * 6,
        out_specs=[place] * 6,
        scratch_shapes=scratch,
        input_output_aliases={2 + n: n for n in range(6)},
        compiler_params=params,
        name="finish_other",
    )(core, other, *begun)
    return merged, field, *rest


def passed_along(value, axis, steps):
    count = lax.axis_size(axis)
    return lax.ppermute(value, axis, [(source, (source + steps) % count) for source in range(count)])


def groups_of(count, apart, size):
    return [
        [start * apart * size + offset + member * apart for member in range(size)]
        for start in range(count // (apart * size))
        for offset in range(apart)
    ]


def summed_over(keep, send, axis, joined, partner, forward):
    count = lax.axis_size(axis)
    along = count // (CORES * ACROSS)
    pairs = [(i, i ^ 1) for i in range(count)]
    arrived = lax.ppermute(send, axis, pairs)
    held = joined(keep, arrived)

    def exchanged(value, apart, size):
        return lax.all_to_all(value, axis, 0, 0, axis_index_groups=groups_of(count, apart, size))

    def reduced(value, apart, size):
        got = exchanged(value.reshape(size, -1, *value.shape[1:]), apart, size)
        return jnp.sum(got.astype(F32), axis=0).astype(BF)

    def gathered(value, apart, size):
        return exchanged(jnp.broadcast_to(value[None], (size, *value.shape)), apart, size).reshape(-1, *value.shape[1:])

    held = reduced(held, CORES, ACROSS)
    held, partner = lax.optimization_barrier((held, partner))
    held = reduced(held.reshape(-1, 2, LANES), CORES * ACROSS, along)
    held = gathered(held, CORES * ACROSS, along).reshape(-1, LANES)
    held = gathered(held, CORES, ACROSS)
    held, forwarded = forward(held, partner)
    return held, lax.ppermute(held, axis, pairs), partner, forwarded


def local(
    fields,
    norm_gain,
    qkv_weight,
    proj_weight,
    bias_table,
    bias_index,
    region_ids,
    mlp_gain,
    up_weight,
    down_weight,
    merge_gain,
    merge_weight,
    cotangent,
):
    count = lax.axis_size("lon")
    core = (lax.axis_index("lon") % CORES).astype(jnp.int32).reshape(1)
    by_lon = fields.transpose(0, 2, 1, 3)
    by_lat = cotangent.transpose(1, 2, 0, 3)
    leaving, table, index, merge_gain = stage(
        by_lon, by_lat, bias_table.transpose(1, 0, 2), bias_index, merge_gain
    )
    west = passed_along(leaving, "lon", 1)
    table, core = lax.optimization_barrier((table, core))
    bias, bias_tail = bias_rows(table, index, region_ids)
    half_rows = -(-O_END // (count * 2)) * 2 * count // CORES
    grads, tokens, scores, *results = block(
        half_rows,
        by_lon,
        west,
        by_lat,
        norm_gain.reshape(1, C),
        qkv_weight,
        proj_weight,
        mlp_gain.reshape(1, C),
        up_weight,
        down_weight.T,
        merge_gain,
        merge_weight,
        bias,
        bias_tail,
    )
    pairs = [(i, i ^ 1) for i in range(count)]
    partner_scores = lax.ppermute(scores, "lon", pairs)
    keep, send = pack(core, grads, tokens, results[1])
    merged_keep, field_keep, home = to_grid(*results, qkv_weight, norm_gain.reshape(1, C), merge_weight)
    partner = lax.ppermute(home, "lon", pairs)

    def forward(held, leaving):
        held, leaving = lax.optimization_barrier((held, leaving))
        return held, lax.ppermute(leaving, "lon", [(i, (i - CORES) % count) for i in range(1, count, CORES)])

    table = table_sum(core, scores, partner_scores, index)
    held, other, partner, forwarded = summed_over(
        keep, send, "lon", lambda kept, arrived: join(core, kept, arrived, table), partner, forward
    )
    factor = float(LEVELS * LAT * fields.shape[2] * count) ** (-0.5)
    merged, field_grad, up_grad, down_grad, qkv_grad, merge_grad, proj_grad, table_grad = finish(
        core, held, other, (partner, forwarded, merged_keep, field_keep), factor
    )
    return (
        merged.transpose(2, 0, 1, 3),
        field_grad.transpose(0, 2, 1, 3),
        qkv_grad,
        proj_grad,
        up_grad,
        down_grad.T,
        merge_grad,
        table_grad.transpose(1, 0, 2),
    )


def solution(mesh):
    whole = P("groups", None, "lon", None)

    return jax.shard_map(
        local,
        mesh=mesh,
        in_specs=(whole, *[P()] * 11, whole),
        out_specs=(whole, whole, *[P("groups", None)] * 5, P("groups", None, None)),
        check_vma=False,
    )
```

```python
import jax
import jax.numpy as jnp
from jax import lax
from jax.experimental import pallas as pl
from jax.experimental.pallas import tpu as pltpu
from jax.sharding import PartitionSpec as P

C = 192
MLP = 768
HEADS = 6
HEAD = 32
HALF = 6
WIN = 144
BPOS = 3312
LAT = 24
TYPES = 4
TOK = TYPES * WIN
LEVELS = 2
LANES = 128
MAIN = 128
REST = WIN - MAIN
TH = TYPES * HEADS
LOW = 256
HIGH = -(-BPOS // LOW)
MTOK = 160
EPS = 1e-5
MASKED = -1e30
F32 = jnp.float32
BF = jnp.bfloat16
CORES = 2
ACROSS = 4

TROWS = 320
MSPLIT = 512
O_UP = 0
O_QKV = O_UP + 6 * C
O_QKV_TAIL = O_QKV + 4 * C
O_PROJ = O_QKV_TAIL + C // 2
O_PROJ_TAIL = O_PROJ + C
O_TABLE = O_PROJ_TAIL + C // 2
O_MERGE_LAST = O_TABLE + 2 * TROWS
O_MERGE = O_MERGE_LAST + MLP - MSPLIT
O_DOWN = O_MERGE + 2 * MLP + MSPLIT
O_END = O_DOWN + 6 * C

DS_TAIL = TH * WIN
DS_CORNER = DS_TAIL + TH * REST
DS_END = DS_CORNER + TH * REST


def dot(a, b):
    return jnp.dot(a, b, preferred_element_type=F32)


def dot_nt(a, b):
    return lax.dot_general(a, b, (((1,), (1,)), ((), ())), preferred_element_type=F32)


def dot_tn(a, b):
    return lax.dot_general(a, b, (((0,), (0,)), ((), ())), preferred_element_type=F32)


def div(n, d):
    return (n * -(-(1 << 16) // d)) >> 16


def onehot(rows, cols, of_row=None, of_col=None):
    if of_row is not None:
        target = of_row(lax.broadcasted_iota(jnp.int32, (rows, 1), 0))
        place = lax.broadcasted_iota(jnp.int32, (rows, cols), 1)
    else:
        target = of_col(lax.broadcasted_iota(jnp.int32, (1, cols), 1))
        place = lax.broadcasted_iota(jnp.int32, (rows, cols), 0)
    return jnp.where(place == target, 1.0, 0.0).astype(BF)


def cell_of_token(n):
    kind = div(n, 72)
    rest = n - 72 * kind
    lat = div(rest, 12)
    return (rest - 12 * lat) * LAT + kind * 6 + lat


def token_of_group(n):
    quarter = div(n, 40)
    rest = n - 40 * quarter
    level = div(rest, 18)
    part = rest - 18 * level
    lat = div(part, 6)
    token = level * 72 + (2 * lat + (quarter >> 1)) * 12 + 2 * (part - 6 * lat) + (quarter & 1)
    return jnp.where(rest < 36, token, -1)


def group_of_token(n):
    level = div(n, 72)
    rest = n - 72 * level
    lat = div(rest, 12)
    lon = rest - 12 * lat
    return ((lat & 1) * 2 + (lon & 1)) * 40 + level * 18 + (lat >> 1) * 6 + (lon >> 1)


def cell_of_merged(n):
    kind = div(n, 40)
    rest = n - 40 * kind
    level = div(rest, 18)
    part = rest - 18 * level
    lat = div(part, 6)
    lon = part - 6 * lat
    half = jnp.where(lon < 3, 0, 1)
    row = half * 72 + (3 * kind + lat) * 6 + (lon - 3 * half) * 2 + level
    return jnp.where(rest < 36, row, -1)


def normalised(values):
    centred = values - jnp.mean(values, axis=-1, keepdims=True)
    scale = lax.rsqrt(jnp.mean(centred * centred, axis=-1, keepdims=True) + EPS)
    return centred * scale, scale


def norm_grad(grad, unit, scale, gain):
    scaled = grad * gain
    return scale * (
        scaled
        - jnp.mean(scaled, axis=-1, keepdims=True)
        - unit * jnp.mean(scaled * unit, axis=-1, keepdims=True)
    )


def rounded(values):
    return values.astype(BF).astype(F32)


def low_onehot(low):
    place = lax.broadcasted_iota(jnp.int32, (LOW, 1), 0).astype(F32).astype(BF)
    hit = jnp.broadcast_to(place, (LOW, low.shape[1])) == low.astype(F32).astype(BF)
    return jnp.where(hit, jnp.array(1, BF), jnp.array(0, BF))


def bias_kernel(table_ref, index_ref, regions_ref, main_ref, tail_ref, part_ref, last_ref, turned_ref, mask_ref, region_ref, sem):
    copy = pltpu.make_async_copy(regions_ref, region_ref, sem)
    copy.start()
    for high in range(HIGH):
        width = min(LOW, BPOS - high * LOW)
        for head in range(HEADS):
            piece = table_ref[head, :, high * LOW : high * LOW + width]
            if width < LOW:
                piece = jnp.concatenate([piece, jnp.zeros((TYPES, LOW - width), F32)], axis=1)
            row = high * TH + head * TYPES
            part_ref[row : row + TYPES, :] = piece
    turned_ref[...] = jnp.transpose(index_ref[:, MAIN:])
    parts = part_ref[...].astype(BF)

    def looked_up(index):
        low = low_onehot(index & (LOW - 1))
        high_row = index >> 8
        found = dot(parts, low)
        chosen = found[0:TH]
        for high in range(1, HIGH):
            chosen = jnp.where(high_row == high, found[high * TH : (high + 1) * TH], chosen)
        return chosen

    for start in range(0, REST, 4):
        got = looked_up(jnp.concatenate([turned_ref[start + n : start + n + 1, :MAIN] for n in range(4)], axis=1))
        for n in range(4):
            last_ref[pl.ds(start + n, TH, stride=REST), :] = got[:, n * MAIN : (n + 1) * MAIN]
    got = looked_up(jnp.concatenate([turned_ref[n : n + 1, MAIN:] for n in range(REST)], axis=1))
    for n in range(REST):
        half = got[:, LANES * (n // 8) : LANES * (n // 8 + 1)]
        half = half if n % 8 == 0 else pltpu.roll(half, LANES - REST * (n % 8), 1)
        last_ref[pl.ds(TH * REST + n, TH, stride=REST), :] = half
    copy.wait()
    kind_of = lax.broadcasted_iota(jnp.int32, (TH, 1), 0) & (TYPES - 1)
    column = lax.broadcasted_iota(jnp.int32, (1, LANES), 1)
    labels = []
    for group in range(12):
        label = jnp.zeros((TH, 1), jnp.int32)
        for kind in range(TYPES):
            label = jnp.where(kind_of == kind, region_ref[group // 6, 6 * kind + group % 6], label)
        labels.append(label)
    keys = jnp.zeros((TH, LANES), jnp.int32)
    for group in range(11):
        keys = jnp.where((column >= 12 * group) & (column < 12 * group + 12), labels[group], keys)
    for group in range(12):
        mask_ref[TH * group : TH * (group + 1), :] = jnp.where(keys == labels[group], 0.0, MASKED)

    def row_block(block, carry):
        base = pl.multiple_of(block * 8, 8)
        rows = index_ref[pl.ds(base, 8), :MAIN]
        for part in range(4):
            index = jnp.concatenate([rows[2 * part + n : 2 * part + n + 1] for n in range(2)], axis=1)
            got = looked_up(index)
            for n in range(2):
                row = base + 2 * part + n
                mask = mask_ref[pl.ds(pl.multiple_of(div(row, 12) * TH, 8), TH), :]
                main_ref[pl.ds(row, TH, stride=WIN), :] = got[:, n * MAIN : (n + 1) * MAIN] + mask
        return carry

    lax.fori_loop(0, WIN // 8, row_block, 0, unroll=True)
    apart = jnp.where(labels[10] == labels[11], 0.0, MASKED)
    split = 132 - MAIN
    for n in range(REST):
        group = (MAIN + n) // 12
        rows = pl.ds(n, TH, stride=REST)
        last_ref[rows, :] = last_ref[rows, :] + mask_ref[TH * group : TH * (group + 1), :]
        rows = pl.ds(TH * REST + n, TH, stride=REST)
        other = (column < split) if n >= split else (column >= split)
        last_ref[rows, :] = last_ref[rows, :] + jnp.where(other, apart, 0.0)
    for th in range(TH):
        rows = slice(th * WIN, th * WIN + MAIN)
        tail_ref[rows, :REST] = jnp.transpose(last_ref[th * REST : (th + 1) * REST, :])
        rows = slice(th * WIN + MAIN, (th + 1) * WIN)
        tail_ref[rows, :REST] = jnp.transpose(last_ref[(TH + th) * REST : (TH + th + 1) * REST, :])[:REST]


def stage_kernel(fields_ref, cotangent_ref, table_ref, index_ref, gain_ref, leaving_ref, table_out, index_out, gain_out, field_ref, half_ref, cells_ref, sems):
    copies = [
        pltpu.make_async_copy(source, target, sems.at[n])
        for n, (source, target) in enumerate(
            [
                (fields_ref.at[:, HALF:], field_ref),
                (cotangent_ref.at[:, HALF // 2 :], half_ref),
                (table_ref, table_out),
                (index_ref, index_out),
                (gain_ref, gain_out.at[0]),
            ]
        )
    ]
    for copy in copies:
        copy.start()
    for copy in copies[:2]:
        copy.wait()
    leaving_ref[:HALF] = jnp.concatenate([field_ref[level].astype(F32) for level in range(LEVELS)], axis=-1).astype(BF)
    for lat in range(12):
        for lon in range(HALF // 2):
            row = (lat * 3 + lon) * 2
            cells_ref[row : row + 2, :] = half_ref[lat, lon].astype(F32)
    leaving_ref[HALF:] = cells_ref[...].reshape(3, LAT, 2 * C).astype(BF)
    for copy in copies[2:]:
        copy.wait()


def stage(fields, cotangent, table, index, gain):
    shape = jax.ShapeDtypeStruct
    whole = pl.BlockSpec(memory_space=pltpu.VMEM)
    return pl.pallas_call(
        stage_kernel,
        out_shape=[
            shape((HALF + 3, LAT, 2 * C), BF),
            shape(table.shape, F32),
            shape(index.shape, jnp.int32),
            shape((1, 4 * C), F32),
        ],
        in_specs=[pl.BlockSpec(memory_space=pltpu.HBM)] * 5,
        out_specs=[whole] * 4,
        scratch_shapes=[
            pltpu.VMEM((LEVELS, HALF, LAT, C), BF),
            pltpu.VMEM((12, HALF // 2, LEVELS, 2 * C), BF),
            pltpu.VMEM((72, 2 * C), F32),
            pltpu.SemaphoreType.DMA((5,)),
        ],
        compiler_params=pltpu.CompilerParams(vmem_limit_bytes=4 * 1024 * 1024),
        name="stage",
    )(*(pltpu.with_memory_space_constraint(a, pltpu.HBM) for a in (fields, cotangent, table, index, gain)))


def bias_rows(table, index, regions):
    whole = pl.BlockSpec(memory_space=pltpu.VMEM)
    return pl.pallas_call(
        bias_kernel,
        out_shape=[jax.ShapeDtypeStruct((TH * WIN, LANES), F32)] * 2,
        in_specs=[whole, whole, pl.BlockSpec(memory_space=pltpu.HBM)],
        out_specs=[whole, whole],
        scratch_shapes=[
            pltpu.VMEM((HIGH * TH, LOW), F32),
            pltpu.VMEM((2 * TH * REST, LANES), F32),
            pltpu.VMEM((REST, WIN), jnp.int32),
            pltpu.VMEM((12 * TH, LANES), F32),
            pltpu.SMEM((LEVELS, LAT), jnp.int32),
            pltpu.SemaphoreType.DMA,
        ],
        compiler_params=pltpu.CompilerParams(vmem_limit_bytes=16 * 1024 * 1024),
        cost_estimate=pl.CostEstimate(flops=14_000_000_000, bytes_accessed=4_000_000, transcendentals=0),
        name="bias_rows",
    )(table, index, pltpu.with_memory_space_constraint(regions, pltpu.HBM))


def block_kernel(
    own_ref, west_ref, own_cotangent_ref,
    norm_gain_ref, qkv_ref, proj_ref, mlp_gain_ref, up_ref, down_ref, merge_gain_ref, merge_ref,
    bias_ref, bias_tail_ref,
    grads_ref, tokens_ref, ds_ref, normed_merge_ref, triple_ref, grad_attn_ref, unit_ref, scale_ref,
    x_ref, q_ref, k_ref, v_ref, p_ref, mixed_ref,
    unit_mlp_ref, scale_mlp_ref, normed_mlp_ref, hidden_ref, slope_ref, after_mlp_ref,
    group_ref, grad_after_ref, grad_up_ref, grad_mixed_ref,
    cells_ref, grad_merged_ref, scaled_ref,
):
    to_tokens = onehot(288, 288, of_row=cell_of_token)
    west = west_ref[:HALF].astype(F32).reshape(144, 2 * C)
    for level in range(LEVELS):
        cells = jnp.concatenate(
            [
                west[:, C * level : C * (level + 1)],
                own_ref[level, :HALF].astype(F32).reshape(144, C),
            ],
            axis=0,
        ).astype(BF)
        ordered = dot(to_tokens, cells)
        for kind in range(TYPES):
            x_ref[WIN * kind + 72 * level : WIN * kind + 72 * level + 72, :] = ordered[72 * kind : 72 * kind + 72]
    cells_ref[:72, :] = west_ref[HALF:].astype(F32).reshape(72, 2 * C)
    for lat in range(12):
        for lon in range(HALF // 2):
            row = (lat * 3 + lon) * 2
            cells_ref[72 + row : 74 + row, :] = own_cotangent_ref[lat, lon].astype(F32)
    grad_merged_ref[...] = dot(onehot(MTOK, 144, of_row=cell_of_merged), cells_ref[...].astype(BF)).astype(BF)
    for n in range(4):
        value = rounded(dot_nt(grad_merged_ref[...], merge_ref[C * n : C * (n + 1), :]))
        scaled_ref[n] = value * merge_gain_ref[:, C * n : C * (n + 1)]
    unit, scale = normalised(x_ref[...])
    unit_ref[...] = unit
    scale_ref[...] = scale
    tokens = (unit * norm_gain_ref[...]).astype(BF)
    tokens_ref[...] = tokens
    q_ref[...] = dot(tokens, qkv_ref[:, 0:C]).astype(BF)
    k_ref[...] = dot(tokens, qkv_ref[:, C : 2 * C]).astype(BF)
    v_ref[...] = dot(tokens, qkv_ref[:, 2 * C :]).astype(BF)
    lane = lax.broadcasted_iota(jnp.int32, (1, C), 1)
    of_head = [
        jnp.where((lane >= HEAD * h) & (lane < HEAD * (h + 1)), 1.0, 0.0).astype(BF) for h in range(HEADS)
    ]
    temper = HEAD ** (-0.5)

    def attend(kind, carry):
        rows = pl.ds(pl.multiple_of(kind * WIN, 16), WIN)
        q, k, v = q_ref[rows, :], k_ref[rows, :], v_ref[rows, :]
        mixed = jnp.zeros((WIN, C), F32)
        products = dot_nt(jnp.concatenate([q * of_head[h] for h in range(HEADS)], axis=0), k)
        for h in range(HEADS):
            th = h * TYPES + kind
            scores_at = pl.ds(pl.multiple_of(th * WIN, 16), WIN)
            bias = jnp.concatenate([bias_ref[scores_at, :], bias_tail_ref[scores_at, :REST]], axis=1)
            scores = products[WIN * h : WIN * (h + 1)] * temper + bias
            weights = jnp.exp(scores - jnp.max(scores, axis=-1, keepdims=True))
            p = weights * (1.0 / jnp.sum(weights, axis=-1, keepdims=True))
            p_ref[th] = p
            mixed = mixed + dot(p.astype(BF), v * of_head[h])
        mixed_ref[rows, :] = mixed.astype(BF)
        return carry

    lax.fori_loop(0, TYPES, attend, 0, unroll=True)
    after_attn = rounded(x_ref[...] + rounded(dot(mixed_ref[...], proj_ref[...])))
    x_ref[...] = after_attn
    unit, scale = normalised(after_attn)
    unit_mlp_ref[...] = unit
    scale_mlp_ref[...] = scale
    normed_mlp = (unit * mlp_gain_ref[...]).astype(BF)
    normed_mlp_ref[...] = normed_mlp
    for part in range(3):
        cols = slice(256 * part, 256 * part + 256)
        u = dot(normed_mlp, up_ref[:, cols])
        below = 0.5 * (1.0 + lax.erf(u * 0.5**0.5))
        hidden_ref[:, cols] = (u * below).astype(BF)
        slope_ref[:, cols] = below + u * (jnp.exp(u * u * (-0.5)) * 0.3989422804014327)
    after_mlp_ref[...] = (x_ref[...] + dot_nt(hidden_ref[...], down_ref[...])).astype(BF)

    to_groups = onehot(160, WIN, of_row=token_of_group)
    for kind in range(TYPES):
        grouped = dot(to_groups, after_mlp_ref[WIN * kind : WIN * kind + WIN, :])
        for quarter in range(4):
            group_ref[quarter, 40 * kind : 40 * kind + 40, :] = grouped[40 * quarter : 40 * quarter + 40]
    quarters = [group_ref[n] for n in range(4)]
    mean = jnp.sum(sum(quarters), axis=-1, keepdims=True) * (1.0 / MLP)
    centred = [v - mean for v in quarters]
    variance = jnp.sum(sum(v * v for v in centred), axis=-1, keepdims=True) * (1.0 / MLP)
    scale_merge = lax.rsqrt(variance + EPS)
    for n in range(4):
        unit = centred[n] * scale_merge
        group_ref[n] = unit
        normed_merge = (unit * merge_gain_ref[:, C * n : C * (n + 1)]).astype(BF)
        normed_merge_ref[n] = normed_merge
    scaled, total, along = [], 0.0, 0.0
    for n in range(4):
        value = scaled_ref[n]
        total = total + value
        along = along + value * group_ref[n]
        scaled.append(value)
    total = jnp.sum(total, axis=-1, keepdims=True) * (1.0 / MLP)
    along = jnp.sum(along, axis=-1, keepdims=True) * (1.0 / MLP)
    for n in range(4):
        group_ref[n] = scale_merge * (scaled[n] - total - group_ref[n] * along)
    from_groups = onehot(WIN, 160, of_row=group_of_token)
    for kind in range(TYPES):
        grouped = jnp.concatenate([group_ref[n, 40 * kind : 40 * kind + 40, :] for n in range(4)], axis=0)
        grad_after_ref[WIN * kind : WIN * kind + WIN, :] = dot(from_groups, grouped.astype(BF)).astype(BF)

    grad_after = grad_after_ref[...]
    for part in range(3):
        cols = slice(256 * part, 256 * part + 256)
        grad_up_ref[:, cols] = (rounded(dot(grad_after, down_ref[:, cols])) * slope_ref[:, cols]).astype(BF)
    grad_normed = rounded(dot_nt(grad_up_ref[...], up_ref[...]))
    grad_attn = (
        grad_after.astype(F32)
        + norm_grad(grad_normed, unit_mlp_ref[...], scale_mlp_ref[...], mlp_gain_ref[...])
    ).astype(BF)
    grad_attn_ref[...] = grad_attn

    grad_mixed_ref[...] = dot_nt(grad_attn, proj_ref[...]).astype(BF)

    def down_terms():
        grad = dot_tn(grad_after_ref[...], hidden_ref[...]).astype(BF)
        for b in range(6):
            grads_ref[O_DOWN + C * b : O_DOWN + C * (b + 1), :] = grad[:, 128 * b : 128 * b + 128]

    def up_terms():
        grad = dot_tn(normed_mlp_ref[...], grad_up_ref[...]).astype(BF)
        for b in range(6):
            grads_ref[O_UP + C * b : O_UP + C * (b + 1), :] = grad[:, 128 * b : 128 * b + 128]

    def merge_terms():
        for n in range(4):
            grad = dot_tn(normed_merge_ref[n], grad_merged_ref[...]).astype(BF)
            for b in range(2):
                start = O_MERGE + MLP * b + C * n
                grads_ref[start : start + C, :] = grad[:, 128 * b : 128 * b + 128]
            kept = max(0, min(C, MSPLIT - C * n))
            if kept:
                start = O_MERGE + 2 * MLP + C * n
                grads_ref[start : start + kept, :] = grad[:kept, 256:]
            if kept < C:
                start = O_MERGE_LAST + C * n + kept - MSPLIT
                grads_ref[start : start + C - kept, :] = grad[kept:, 256:]

    def proj_terms():
        grad_proj = dot_tn(mixed_ref[...], grad_attn_ref[...]).astype(BF)
        grads_ref[O_PROJ : O_PROJ + C, :] = grad_proj[:, :128]
        grads_ref[O_PROJ_TAIL : O_PROJ_TAIL + C // 2, :] = jnp.concatenate(
            [grad_proj[: C // 2, 128:], grad_proj[C // 2 :, 128:]], axis=1
        )

    last_keys = onehot(REST, WIN, of_row=lambda n: n + MAIN)
    ds_ref[DS_CORNER:, :] = jnp.zeros((TH * REST, LANES), BF)
    grads_ref[O_QKV:O_PROJ, :] = jnp.zeros((O_PROJ - O_QKV, LANES), BF)
    grads_ref[O_TABLE:O_MERGE_LAST, :] = jnp.zeros((O_MERGE_LAST - O_TABLE, LANES), BF)

    def attend_back(kind, carry):
        rows = pl.ds(kind * WIN, WIN)
        v, grad = v_ref[rows, :], grad_mixed_ref[rows, :]
        q_turned, k_turned, grad_turned = (jnp.transpose(a) for a in (q_ref[rows, :], k_ref[rows, :], grad))
        products = dot_nt(jnp.concatenate([grad * of_head[h] for h in range(HEADS)], axis=0), v)
        dq, dk, dv = [], [], []
        for h in range(HEADS):
            th = h * TYPES + kind
            lanes = slice(HEAD * h, HEAD * (h + 1))
            p = p_ref[th]
            weighted = p * products[WIN * h : WIN * (h + 1)]
            ds = weighted - p * jnp.sum(weighted, axis=-1, keepdims=True)
            ds = ds.astype(BF)
            ds_ref[pl.ds(th * WIN, WIN), :] = ds[:, :MAIN]
            turned = dot_nt(jnp.concatenate([k_turned[lanes], last_keys], axis=0), ds)
            tail = turned[HEAD:].astype(BF)
            ds_ref[pl.ds(DS_TAIL + th * REST, REST), :] = tail[:, :MAIN]
            ds_ref[pl.ds(DS_CORNER + th * REST, REST), :REST] = tail[:, MAIN:]
            dq.append(turned[:HEAD])
            dk.append(dot(q_turned[lanes], ds))
            dv.append(dot(grad_turned[lanes], p.astype(BF)))
        triple = jnp.concatenate([a * temper for a in dq + dk] + dv, axis=0).astype(BF)
        triple_ref[rows, :] = jnp.transpose(triple)
        return carry

    for kind, terms in enumerate((down_terms, up_terms, merge_terms, proj_terms)):
        attend_back(kind, 0)
        terms()


def block(half_rows, *args):
    shape = jax.ShapeDtypeStruct
    whole = pl.BlockSpec(memory_space=pltpu.VMEM)
    scratch = [
        ((TOK, C), F32), ((TOK, C), BF), ((TOK, C), BF),
        ((TOK, C), BF), ((TH, WIN, WIN), F32), ((TOK, C), BF),
        ((TOK, C), F32), ((TOK, 1), F32), ((TOK, C), BF), ((TOK, MLP), BF), ((TOK, MLP), F32), ((TOK, C), BF),
        ((4, MTOK, C), F32), ((TOK, C), BF), ((TOK, MLP), BF), ((TOK, C), BF),
        ((144, 2 * C), F32), ((MTOK, 2 * C), BF), ((4, MTOK, C), F32),
    ]
    return pl.pallas_call(
        block_kernel,
        out_shape=[
            shape((2 * half_rows, LANES), BF),
            shape((TOK, C), BF),
            shape((DS_END, LANES), BF),
            shape((4, MTOK, C), BF),
            shape((TOK, 3 * C), BF),
            shape((TOK, C), BF),
            shape((TOK, C), F32),
            shape((TOK, 1), F32),
        ],
        in_specs=[whole] * len(args),
        out_specs=[whole] * 8,
        scratch_shapes=[pltpu.VMEM(*item) for item in scratch],
        compiler_params=pltpu.CompilerParams(vmem_limit_bytes=24 * 1024 * 1024),
        cost_estimate=pl.CostEstimate(flops=24_000_000_000, bytes_accessed=12_000_000, transcendentals=2_000_000),
        name="block",
    )(*args)


def pack_kernel(core_ref, grads_ref, tokens_ref, triple_ref, keep_ref, send_ref):
    half = keep_ref.shape[0]
    core = core_ref[0]
    grad_qkv = dot_tn(tokens_ref[...], triple_ref[...]).astype(BF)
    tail = jnp.concatenate([grad_qkv[: C // 2, 512:], grad_qkv[C // 2 :, 512:]], axis=1)
    keep_ref[...] = grads_ref[pl.ds(pl.multiple_of(core * half, 16), half), :]
    send_ref[...] = grads_ref[pl.ds(pl.multiple_of((1 - core) * half, 16), half), :]
    for owner, target_ref in ((0, keep_ref), (1, send_ref)):

        @pl.when(core == owner)
        def _():
            for b in range(4):
                target_ref[O_QKV + C * b : O_QKV + C * (b + 1), :] = grad_qkv[:, 128 * b : 128 * b + 128]
            target_ref[O_QKV_TAIL : O_QKV_TAIL + C // 2, :] = tail


def pack(core, grads, tokens, triple):
    half = jax.ShapeDtypeStruct((grads.shape[0] // 2, LANES), BF)
    whole = pl.BlockSpec(memory_space=pltpu.VMEM)
    return pl.pallas_call(
        pack_kernel,
        out_shape=[half, half],
        in_specs=[pl.BlockSpec(memory_space=pltpu.SMEM)] + [whole] * 3,
        out_specs=[whole] * 2,
        compiler_params=pltpu.CompilerParams(vmem_limit_bytes=12 * 1024 * 1024),
        cost_estimate=pl.CostEstimate(flops=600_000_000, bytes_accessed=4_000_000, transcendentals=0),
        name="pack",
    )(core, grads, tokens, triple)


def table_kernel(core_ref, own_ref, partner_ref, index_ref, table_ref, ds_ref, turned_ref):
    def table_terms(index, slab):
        high_row = index >> 8
        spread = [jnp.where(high_row == n, slab, 0.0) for n in range(HIGH)]
        spread.append(jnp.zeros((TROWS - HIGH * TH, index.shape[1]), F32))
        return dot_nt(jnp.concatenate(spread, axis=0).astype(BF), low_onehot(index & (LOW - 1)))

    def row_block(block, carry):
        base = pl.multiple_of(block * 8, 8)
        rows = index_ref[pl.ds(base, 8), :MAIN]
        index = jnp.concatenate([rows[n : n + 1] for n in range(8)], axis=1)
        slab = jnp.concatenate([ds_ref[pl.ds(base + n, TH, stride=WIN), :] for n in range(8)], axis=1)
        return carry + table_terms(index, slab)

    @pl.when(core_ref[0] == 0)
    def _():
        ds_ref[...] = own_ref[...].astype(F32) + partner_ref[...].astype(F32)
        turned_ref[...] = jnp.transpose(index_ref[:, MAIN:])
        table = lax.fori_loop(0, WIN // 8, row_block, jnp.zeros((TROWS, LOW), F32), unroll=True)
        index = jnp.concatenate([turned_ref[n : n + 1, :MAIN] for n in range(REST)], axis=1)
        slab = jnp.concatenate([ds_ref[pl.ds(DS_TAIL + n, TH, stride=REST), :] for n in range(REST)], axis=1)
        table = table + table_terms(index, slab)
        index = jnp.concatenate([turned_ref[n : n + 1, MAIN:] for n in range(REST)], axis=1)
        slab = jnp.concatenate(
            [ds_ref[pl.ds(DS_CORNER + n, TH, stride=REST), :][:, :REST] for n in range(REST)], axis=1
        )
        table = (table + table_terms(index, slab)).astype(BF)
        table_ref[:TROWS, :] = table[:, :LANES]
        table_ref[TROWS:, :] = table[:, LANES:]

    @pl.when(core_ref[0] == 1)
    def _():
        table_ref[...] = jnp.zeros(table_ref.shape, BF)


def table_sum(core, own, partner, index):
    whole = pl.BlockSpec(memory_space=pltpu.VMEM)
    return pl.pallas_call(
        table_kernel,
        out_shape=jax.ShapeDtypeStruct((2 * TROWS, LANES), BF),
        in_specs=[pl.BlockSpec(memory_space=pltpu.SMEM)] + [whole] * 3,
        out_specs=whole,
        scratch_shapes=[pltpu.VMEM((DS_END, LANES), F32), pltpu.VMEM((REST, WIN), jnp.int32)],
        compiler_params=pltpu.CompilerParams(vmem_limit_bytes=12 * 1024 * 1024),
        cost_estimate=pl.CostEstimate(flops=4_000_000_000, bytes_accessed=3_000_000, transcendentals=0),
        name="table_sum",
    )(core, own, partner, index)


def join_kernel(core_ref, keep_ref, arrived_ref, table_ref, held_ref):
    held_ref[...] = (keep_ref[...].astype(F32) + arrived_ref[...].astype(F32)).astype(BF)

    @pl.when(core_ref[0] == 0)
    def _():
        held_ref[O_TABLE : O_TABLE + 2 * TROWS, :] = table_ref[...]


def join(core, keep, arrived, table):
    whole = pl.BlockSpec(memory_space=pltpu.VMEM)
    return pl.pallas_call(
        join_kernel,
        out_shape=jax.ShapeDtypeStruct(keep.shape, BF),
        in_specs=[pl.BlockSpec(memory_space=pltpu.SMEM)] + [whole] * 3,
        out_specs=whole,
        compiler_params=pltpu.CompilerParams(vmem_limit_bytes=8 * 1024 * 1024),
        cost_estimate=pl.CostEstimate(flops=400_000, bytes_accessed=2_500_000, transcendentals=0),
        name="join",
    )(core, keep, arrived, table)


def spread_kernel(got_ref, out_ref):
    total = got_ref[0].astype(F32)
    for n in range(1, got_ref.shape[0]):
        total = total + got_ref[n].astype(F32)
    total = total.astype(BF)
    for n in range(got_ref.shape[0]):
        out_ref[n] = total


def added_and_spread(got):
    whole = pl.BlockSpec(memory_space=pltpu.VMEM)
    return pl.pallas_call(
        spread_kernel,
        out_shape=jax.ShapeDtypeStruct(got.shape, BF),
        in_specs=[whole],
        out_specs=whole,
        compiler_params=pltpu.CompilerParams(vmem_limit_bytes=8 * 1024 * 1024),
        cost_estimate=pl.CostEstimate(flops=200_000, bytes_accessed=400_000, transcendentals=0),
        name="added_and_spread",
    )(got)


def cells_kernel(
    normed_merge_ref, triple_ref, grad_attn_ref, unit_ref, scale_ref, qkv_ref, gain_ref, merge_ref,
    merged_keep_ref, field_keep_ref, home_ref, x_ref,
):
    merged = sum(dot(normed_merge_ref[n], merge_ref[C * n : C * (n + 1), :]) for n in range(4))
    grad_normed = rounded(dot_nt(triple_ref[...], qkv_ref[...]))
    merged_cells = dot(onehot(144, MTOK, of_col=cell_of_merged), merged.astype(BF))
    x_ref[...] = grad_attn_ref[...].astype(F32) + norm_grad(
        grad_normed, unit_ref[...], scale_ref[...], gain_ref[...]
    )
    to_cells = onehot(288, 288, of_col=cell_of_token)
    leaving = []
    for level in range(LEVELS):
        ordered = jnp.concatenate(
            [x_ref[WIN * kind + 72 * level : WIN * kind + 72 * level + 72, :] for kind in range(TYPES)], axis=0
        )
        cells = dot(to_cells, ordered.astype(BF))
        leaving.append(cells[:144])
        field_keep_ref[level] = cells[144:].reshape(HALF, LAT, C).astype(BF)
    home_ref[:HALF] = jnp.concatenate(leaving, axis=1).reshape(HALF, LAT, 2 * C).astype(BF)
    for lat in range(12):
        for lon in range(HALF // 2):
            row = 72 + (lat * 3 + lon) * 2
            merged_keep_ref[lat, lon] = merged_cells[row : row + 2].astype(BF)
    home_ref[HALF:] = merged_cells[:72].reshape(3, LAT, 2 * C).astype(BF)


def to_grid(*args):
    shape = jax.ShapeDtypeStruct
    whole = pl.BlockSpec(memory_space=pltpu.VMEM)
    return pl.pallas_call(
        cells_kernel,
        out_shape=[
            shape((12, HALF // 2, LEVELS, 2 * C), BF),
            shape((LEVELS, HALF, LAT, C), BF),
            shape((HALF + 3, LAT, 2 * C), BF),
        ],
        in_specs=[whole] * 8,
        out_specs=[whole] * 3,
        scratch_shapes=[pltpu.VMEM((TOK, C), F32)],
        compiler_params=pltpu.CompilerParams(vmem_limit_bytes=12 * 1024 * 1024),
        cost_estimate=pl.CostEstimate(flops=1_500_000_000, bytes_accessed=3_000_000, transcendentals=0),
        name="to_grid",
    )(*args)


def first_half(part, refs, staged, leaves):
    _, _, up_ref, _, qkv_ref, merge_ref, proj_ref, table_ref = refs
    up, _, qkv, merge, proj, table = staged
    for b in range(6):
        up[:, 128 * b : 128 * b + 128] = part(O_UP + C * b, C)
    leaves(up, up_ref)
    for b in range(4):
        qkv[:, 128 * b : 128 * b + 128] = part(O_QKV + C * b, C)
    tail = part(O_QKV_TAIL, C // 2)
    qkv[: C // 2, 512:] = tail[:, :64]
    qkv[C // 2 :, 512:] = tail[:, 64:]
    leaves(qkv, qkv_ref)
    for side in range(2):
        terms = part(O_TABLE + TROWS * side, TROWS)
        for high in range(HIGH):
            start = high * LOW + side * LANES
            width = min(LANES, BPOS - start)
            for head in range(HEADS):
                row = high * TH + head * TYPES
                table[head, :, start : start + width] = terms[row : row + TYPES, :width]
    leaves(table, table_ref)
    proj[:, :128] = part(O_PROJ, C)
    tail = part(O_PROJ_TAIL, C // 2)
    proj[: C // 2, 128:] = tail[:, :64]
    proj[C // 2 :, 128:] = tail[:, 64:]
    leaves(proj, proj_ref)
    merge[MSPLIT:, 256:] = part(O_MERGE_LAST, MLP - MSPLIT)
    leaves(merge.at[MSPLIT:, 256:], merge_ref.at[MSPLIT:, 256:])


def second_half(part, refs, staged, leaves):
    _, _, _, down_ref, _, merge_ref, _, _ = refs
    _, down, _, merge, _, _ = staged
    for b in range(2):
        merge[:, 128 * b : 128 * b + 128] = part(O_MERGE + MLP * b, MLP)
    leaves(merge.at[:, :256], merge_ref.at[:, :256])
    for b in range(6):
        down[:, 128 * b : 128 * b + 128] = part(O_DOWN + C * b, C)
    leaves(down, down_ref)
    merge[:MSPLIT, 256:] = part(O_MERGE + 2 * MLP, MSPLIT)
    leaves(merge.at[:MSPLIT, 256:], merge_ref.at[:MSPLIT, 256:])


def scaled(factor, half, sums_ref, outs, staged, sems):
    for which, fill, base in ((0, first_half, 0), (1, second_half, O_MERGE)):

        @pl.when(half == which)
        def _():
            begun = []

            def part(start, rows):
                return sums_ref[start - base : start - base + rows, :].astype(F32) * factor

            def leaves(source, target):
                begun.append(pltpu.make_async_copy(source, target, sems.at[len(begun)]))
                begun[-1].start()

            fill(part, outs, staged, leaves)
            for copy in begun:
                copy.wait()


def finish_own_kernel(
    factor, core_ref, held_ref, partner_ref, forwarded_ref, merged_keep_ref, field_keep_ref, *refs
):
    outs, staged, (sems, merged, field) = refs[:8], refs[8:14], refs[14:]
    core = core_ref[0]
    east = jnp.where(core == 0, partner_ref[...].astype(F32), forwarded_ref[...].astype(F32))
    for level in range(LEVELS):
        field[level, HALF:] = east[:HALF, :, C * level : C * (level + 1)].astype(BF)
    field[:, :HALF] = field_keep_ref[...]
    copies = [pltpu.make_async_copy(field, outs[1], sems.at[5])]
    copies[-1].start()
    cells = east[HALF:].reshape(72, 2 * C)
    for lat in range(12):
        for lon in range(HALF // 2):
            row = (lat * 3 + lon) * 2
            merged[lat, HALF // 2 + lon] = cells[row : row + 2].astype(BF)
    merged[:, : HALF // 2] = merged_keep_ref[...]
    copies.append(pltpu.make_async_copy(merged, outs[0], sems.at[6]))
    copies[-1].start()
    scaled(factor, core, held_ref, outs, staged, sems)
    for copy in copies:
        copy.wait()


def finish_other_kernel(factor, core_ref, other_ref, *refs):
    outs, staged, sems = refs[6:12], refs[12:18], refs[18]
    scaled(factor, 1 - core_ref[0], other_ref, (None, None, *outs), staged, sems)


def finish(core, held, other, cells, factor):
    shape = jax.ShapeDtypeStruct
    whole = pl.BlockSpec(memory_space=pltpu.VMEM)
    scalar = pl.BlockSpec(memory_space=pltpu.SMEM)
    place = pl.BlockSpec(memory_space=pl.ANY)
    sums = [
        shape((C, MLP), F32),
        shape((C, MLP), F32),
        shape((C, 3 * C), F32),
        shape((MLP, 2 * C), F32),
        shape((C, C), F32),
        shape((HEADS, TYPES, BPOS), F32),
    ]
    scratch = [pltpu.VMEM(item.shape, F32) for item in sums] + [pltpu.SemaphoreType.DMA((7,))]
    grid = [shape((12, HALF, LEVELS, 2 * C), BF), shape((LEVELS, 2 * HALF, LAT, C), BF)]
    params = pltpu.CompilerParams(vmem_limit_bytes=16 * 1024 * 1024)
    merged, field, *begun = pl.pallas_call(
        lambda *refs: finish_own_kernel(factor, *refs),
        out_shape=[*grid, *sums],
        in_specs=[scalar] + [whole] * 5,
        out_specs=[place] * 8,
        scratch_shapes=scratch + [pltpu.VMEM(item.shape, BF) for item in grid],
        compiler_params=params,
        cost_estimate=pl.CostEstimate(flops=400_000, bytes_accessed=2_500_000, transcendentals=0),
        name="finish_own",
    )(core, held, *cells)
    rest = pl.pallas_call(
        lambda *refs: finish_other_kernel(factor, *refs),
        out_shape=sums,
        in_specs=[scalar, whole] + [place] * 6,
        out_specs=[place] * 6,
        scratch_shapes=scratch,
        input_output_aliases={2 + n: n for n in range(6)},
        compiler_params=params,
        name="finish_other",
    )(core, other, *begun)
    return merged, field, *rest


def passed_along(value, axis, steps):
    count = lax.axis_size(axis)
    return lax.ppermute(value, axis, [(source, (source + steps) % count) for source in range(count)])


def groups_of(count, apart, size):
    return [
        [start * apart * size + offset + member * apart for member in range(size)]
        for start in range(count // (apart * size))
        for offset in range(apart)
    ]


def summed_over(keep, send, axis, joined, partner, forward):
    count = lax.axis_size(axis)
    along = count // (CORES * ACROSS)
    pairs = [(i, i ^ 1) for i in range(count)]
    arrived = lax.ppermute(send, axis, pairs)
    held = joined(keep, arrived)

    def exchanged(value, apart, size):
        return lax.all_to_all(value, axis, 0, 0, axis_index_groups=groups_of(count, apart, size))

    def reduced(value, apart, size):
        got = exchanged(value.reshape(size, -1, *value.shape[1:]), apart, size)
        return jnp.sum(got.astype(F32), axis=0).astype(BF)

    def gathered(value, apart, size):
        return exchanged(jnp.broadcast_to(value[None], (size, *value.shape)), apart, size).reshape(-1, *value.shape[1:])

    held = reduced(held, CORES, ACROSS)
    held, partner = lax.optimization_barrier((held, partner))
    held = exchanged(held.reshape(along, -1, 2, LANES), CORES * ACROSS, along)
    held = exchanged(added_and_spread(held), CORES * ACROSS, along).reshape(-1, LANES)
    held = gathered(held, CORES, ACROSS)
    held, forwarded = forward(held, partner)
    return held, lax.ppermute(held, axis, pairs), partner, forwarded


def local(
    fields,
    norm_gain,
    qkv_weight,
    proj_weight,
    bias_table,
    bias_index,
    region_ids,
    mlp_gain,
    up_weight,
    down_weight,
    merge_gain,
    merge_weight,
    cotangent,
):
    count = lax.axis_size("lon")
    core = (lax.axis_index("lon") % CORES).astype(jnp.int32).reshape(1)
    by_lon = fields.transpose(0, 2, 1, 3)
    by_lat = cotangent.transpose(1, 2, 0, 3)
    leaving, table, index, merge_gain = stage(
        by_lon, by_lat, bias_table.transpose(1, 0, 2), bias_index, merge_gain
    )
    west = passed_along(leaving, "lon", 1)
    table, core = lax.optimization_barrier((table, core))
    bias, bias_tail = bias_rows(table, index, region_ids)
    half_rows = -(-O_END // (count * 2)) * 2 * count // CORES
    grads, tokens, scores, *results = block(
        half_rows,
        by_lon,
        west,
        by_lat,
        norm_gain.reshape(1, C),
        qkv_weight,
        proj_weight,
        mlp_gain.reshape(1, C),
        up_weight,
        down_weight.T,
        merge_gain,
        merge_weight,
        bias,
        bias_tail,
    )
    pairs = [(i, i ^ 1) for i in range(count)]
    partner_scores = lax.ppermute(scores, "lon", pairs)
    keep, send = pack(core, grads, tokens, results[1])
    merged_keep, field_keep, home = to_grid(*results, qkv_weight, norm_gain.reshape(1, C), merge_weight)
    partner = lax.ppermute(home, "lon", pairs)

    def forward(held, leaving):
        held, leaving = lax.optimization_barrier((held, leaving))
        return held, lax.ppermute(leaving, "lon", [(i, (i - CORES) % count) for i in range(1, count, CORES)])

    table = table_sum(core, scores, partner_scores, index)
    held, other, partner, forwarded = summed_over(
        keep, send, "lon", lambda kept, arrived: join(core, kept, arrived, table), partner, forward
    )
    factor = float(LEVELS * LAT * fields.shape[2] * count) ** (-0.5)
    merged, field_grad, up_grad, down_grad, qkv_grad, merge_grad, proj_grad, table_grad = finish(
        core, held, other, (partner, forwarded, merged_keep, field_keep), factor
    )
    return (
        merged.transpose(2, 0, 1, 3),
        field_grad.transpose(0, 2, 1, 3),
        qkv_grad,
        proj_grad,
        up_grad,
        down_grad.T,
        merge_grad,
        table_grad.transpose(1, 0, 2),
    )


def solution(mesh):
    whole = P("groups", None, "lon", None)

    return jax.shard_map(
        local,
        mesh=mesh,
        in_specs=(whole, *[P()] * 11, whole),
        out_specs=(whole, whole, *[P("groups", None)] * 5, P("groups", None, None)),
        check_vma=False,
    )
```
